512 devices in a mesh: section: 8 (over x, core), dp: 32 (over z, y_lo), mp: 2 (over y_hi).
Axes of the slice: x: 4, y: 4 (y_hi: 2, y_lo: 2; y = y_hi * 2 + y_lo), z: 16, core: 2. Of those that a mesh axis runs over, the one named last changes fastest.
Arguments:
- layer_inputs: bfloat16 [8, 128, 4096], P('section', None, 'mp'), may hold values from -6 to 6
- pre_act: bfloat16 [8, 128, 8192], P('section', None, 'dp'), may hold values from -6 to 6
- out_grad: bfloat16 [128, 4096], P(None, 'mp'), may hold values from -4 to 4
- w_in: bfloat16 [32, 8, 32, 4096], P('dp', 'section', None, 'mp'), may hold values from -0.09375 to 0.09375
- w_out: bfloat16 [32, 8, 32, 4096], P('dp', 'section', None, 'mp'), may hold values from -0.0625 to 0.0625
Outputs:
- in_grads: bfloat16 [8, 128, 4096], P('section', None, 'mp')
- grad_in: float32 [32, 8, 32, 4096], P('dp', 'section', None, 'mp')
- grad_out: float32 [32, 8, 32, 4096], P('dp', 'section', None, 'mp')
The draws below stay inside these ranges and needn't reach their ends.
All inputs are finite; a program needn't handle non-finite values.
Results may differ from the reference program's by a relative error of at most 0.035.
Values may be sent and summed in bfloat16 or wider, within the bound.
A program may use at most 64 MiB of HBM per device.

```python
import jax
import jax.numpy as jnp
from jax import lax

D = 4096
FF = 8192
TOKS = 128
SECTIONS = 8
FB = 32
N_SECTION = 8
N_DP = 32
N_MP = 2


def block_levels(rng, shape, shards, low, largest):
    gain, own = 1.0, jax.random.fold_in(rng, 6)
    for dim, blocks in shards:
        draws = jnp.exp(jax.random.uniform(jax.random.fold_in(own, dim), (blocks,), jnp.float32, low / len(shards), largest / len(shards)))
        gain = gain * jnp.repeat(draws, shape[dim] // blocks).reshape([-1 if axis == dim else 1 for axis in range(len(shape))])
    return gain


def centred(stream_key, extent, scale, bound, split=(), held_as=jnp.bfloat16):
    level = block_levels(stream_key, extent, split, -0.22, 0.18) if split else 1.0
    entries = jax.random.normal(stream_key, extent, jnp.float32) * scale * level
    return jnp.minimum(jnp.maximum(entries, -bound), bound).astype(held_as)


def setup_inputs(seed: int = 0) -> dict:
    streams_of = jax.random.split(jax.random.key(seed), 6)
    layer_inputs = centred(streams_of[0], (SECTIONS, TOKS, D), 1.0, 6.0, ((0, 8), (2, 2)))
    pre_act = centred(streams_of[1], (SECTIONS, TOKS, FF), 1.0, 6.0, ((0, 8), (2, 32)))
    out_grad = centred(streams_of[2], (TOKS, D), 0.3, 4.0, ((1, 2),))
    w_in = centred(streams_of[3], (N_DP, N_SECTION, FB, D), D ** -0.5, 0.09375, ((0, 32), (1, 8), (3, 2)))
    w_out = centred(streams_of[4], (N_DP, N_SECTION, FB, D), FF ** -0.5, 0.0625, ((0, 32), (1, 8), (3, 2)))
    return dict(layer_inputs=layer_inputs, pre_act=pre_act, out_grad=out_grad, w_in=w_in, w_out=w_out)


def gelu_slope(value):
    cdf = 0.5 * (1.0 + lax.erf(value * 0.7071067811865476))
    dens = jnp.exp(-0.5 * value * value) * 0.3989422804014327
    return cdf + value * dens


def rounded(value):
    return lax.optimization_barrier(value.astype(jnp.bfloat16)).astype(jnp.float32)


def reference(layer_inputs, pre_act, out_grad, w_in, w_out):
    in_rows = w_in.reshape(FF, D)
    out_rows = w_out.reshape(FF, D)
    feat = D // N_MP
    units = FF // N_DP
    upper = out_grad
    grad_in = jnp.zeros((FF, D), jnp.float32)
    grad_out = jnp.zeros((FF, D), jnp.float32)
    results = []
    for spot in reversed(range(SECTIONS)):
        back = jnp.zeros((TOKS, FF), jnp.float32)
        for block in range(N_MP):
            piece = jnp.dot(upper[:, block * feat:(block + 1) * feat], out_rows[:, block * feat:(block + 1) * feat].T, preferred_element_type=jnp.float32)
            back = back + rounded(piece)
        saved = pre_act[spot].astype(jnp.float32)
        gee = (back * gelu_slope(saved)).astype(jnp.bfloat16)
        total = upper.astype(jnp.float32)
        for block in range(N_DP):
            piece = jnp.dot(gee[:, block * units:(block + 1) * units], in_rows[block * units:(block + 1) * units, :], preferred_element_type=jnp.float32)
            total = total + rounded(piece)
        result = total.astype(jnp.bfloat16)
        hidden = jax.nn.gelu(saved, approximate=False).astype(jnp.bfloat16)
        grad_in = grad_in + rounded(jnp.dot(gee.T, layer_inputs[spot], preferred_element_type=jnp.float32))
        grad_out = grad_out + rounded(jnp.dot(hidden.T, upper, preferred_element_type=jnp.float32))
        results.append(result)
        upper = result
    in_grads = jnp.stack(results[::-1], axis=0)
    return (in_grads, grad_in.reshape(N_DP, N_SECTION, FB, D), grad_out.reshape(N_DP, N_SECTION, FB, D))
```

```python
import contextlib

import jax
import jax.numpy as jnp
from jax import lax
from jax.experimental import pallas as pl
from jax.experimental.pallas import tpu as pltpu
from jax.sharding import Mesh
from jax.sharding import PartitionSpec as P

AXES = ("x", "core", "z", "ylo", "yhi")
MESH_ID = pl.DeviceIdType.MESH
BF16, F32 = jnp.bfloat16, jnp.float32
LANES = 128
PROFILE = False


def scope(name):
    return jax.named_scope(name) if PROFILE else contextlib.nullcontext()


def gelu_parts(v):
    cdf = 0.5 * (1.0 + lax.erf(v * 0.7071067811865476))
    dens = jnp.exp(-0.5 * v * v) * 0.3989422804014327
    return cdf, dens


def kernel(
    li_hbm, pa_hbm, og_hbm, wi_hbm, wo_hbm,
    ig_out, gi_out, go_out,
    wbuf, pa, pa_all, pb, pc, slope, h_t, hall, li, og,
    xs, a_buf, b_buf, gbuf, gz, gt, up, gsum,
    lsem, wx_s, wx_r, wz_s, wz_r, st_s, st_r, ph_s, ph_r, li_s, li_r,
    g_s, g_r, uz_s, uz_r, ux_s, ux_r, ud_s, ud_r, o_s,
):
    nx, nz = lax.axis_size("x"), lax.axis_size("z")
    nsec = 2 * nx
    fb, width = wi_hbm.shape
    fe = width // 2
    tok = nz * 8
    tiles = nz * fb // LANES
    per_tile = LANES // fb
    x, core, z = lax.axis_index("x"), lax.axis_index("core"), lax.axis_index("z")
    ylo, yhi = lax.axis_index("ylo"), lax.axis_index("yhi")
    sec = x * 2 + core
    y = yhi * 2 + ylo
    other = 1 - ylo
    partner = yhi * 2 + other

    def dev(sec_=None, z_=None, y_=None):
        sec_ = sec if sec_ is None else sec_
        y_ = y if y_ is None else y_
        return (sec_ // 2, lax.rem(sec_, 2), z if z_ is None else z_, lax.rem(y_, 2), y_ // 2)

    def copy(src, dst, ssem, rsem, to):
        return pltpu.make_async_remote_copy(
            src_ref=src, dst_ref=dst, send_sem=ssem, recv_sem=rsem, device_id=to, device_id_type=MESH_ID
        )

    def send(*args):
        cp = copy(*args)
        cp.start()
        return cp

    def await_bytes(ref, sem):
        pltpu.make_async_copy(ref, ref, sem).wait()

    def zat(d):
        return lax.rem(z + d + nz, nz)

    def sat(d):
        return lax.rem(sec + d, nsec)

    def xat(d):
        return lax.rem(x + d + nx, nx) * 2 + core

    def yat(d):
        return lax.rem(y + d, 4)

    y_order = (2, 1, 3)
    sec_order = sorted(((dx, dc) for dx in range(nx) for dc in range(2) if dx or dc), key=lambda p: -min(p[0], nx - p[0]))
    x_order = [dx for dx, dc in sec_order if dc == 0]

    def peer(dx, dc):
        return lax.rem(x + dx, nx) * 2 + (1 - core if dc else core)

    mine = pl.ds(pl.multiple_of(ylo * fe, LANES), fe)
    theirs = pl.ds(pl.multiple_of(other * fe, LANES), fe)

    w_hbm = (wi_hbm, wo_hbm)
    local = [pltpu.make_async_copy(pa_hbm, pa, lsem.at[0])]
    for m in range(2):
        local.append(pltpu.make_async_copy(w_hbm[m].at[:, mine], wbuf.at[m, ylo, z], lsem.at[1 + m]))
    local.append(pltpu.make_async_copy(og_hbm, og, lsem.at[3]))
    local.append(pltpu.make_async_copy(li_hbm, li.at[core, x], lsem.at[4]))
    for cp in local:
        cp.start()

    barrier = pltpu.get_barrier_semaphore()
    greeted = 0
    for to in (
        [dev(z_=zat(d)) for d in range(1, nz)] + [dev(sec_=sat(d)) for d in range(1, nsec)] + [dev(y_=yat(d)) for d in range(1, 4)]
    ):
        pl.semaphore_signal(barrier, inc=1, device_id=to, device_id_type=MESH_ID)
        greeted += 1
    local[0].wait()
    v = pa[...].astype(F32).reshape(tok, nsec * fb)
    h_t[...] = jnp.swapaxes(v * gelu_parts(v)[0], 0, 1).astype(BF16).reshape(nsec, fb, tok)
    with scope("barrier"):
        pl.semaphore_wait(barrier, greeted)

    for d in range(1, nz):
        send(pa.at[zat(d)], pa_all.at[z], st_s.at[0], st_r.at[0], dev(z_=zat(d)))
    swaps = [
        send(w_hbm[m].at[:, theirs], wbuf.at[m, ylo, z], wx_s.at[m], wx_r.at[m], dev(y_=partner))
        for m in range(2)
    ]
    for d in range(1, nsec):
        send(h_t.at[sat(d)], hall.at[sec], st_s.at[3], st_r.at[3], dev(sec_=sat(d)))
    hall[sec] = h_t[sec]
    pa_all[z] = pa[z]

    half = nz // 2

    def hop(k):
        last = k == half
        for which in range(2):
            l = ylo if which == 0 else other
            for m in range(2):
                if k == 1:
                    if which == 0:
                        local[1 + m].wait()
                    else:
                        swaps[m].wait_recv()
                for way, step in ((0, 1), (1, -1)):
                    if k > 1:
                        await_bytes(wbuf.at[m, l, 0], wz_r.at[way, k - 2, m, l])
                    if last and way != m:
                        continue
                    src = wbuf.at[m, l, zat(-step * (k - 1))]
                    send(src, src, wz_s.at[way], wz_r.at[way, k - 1, m, l], dev(z_=zat(step)))

    def stage_b():
        await_bytes(pa_all.at[pl.ds(0, nz - 1)], st_r.at[0])
        group = lax.broadcasted_iota(jnp.int32, (8, LANES), 1) // fb
        for ct in range(nsec // per_tile):
            for t in range(tiles):
                out = [jnp.zeros((8, LANES), F32)] * per_tile
                for j in range(per_tile):
                    v = pa_all[t * per_tile + j, :, ct * LANES:(ct + 1) * LANES].astype(F32)
                    for k in range(per_tile):
                        shift = (j - k) * fb % LANES
                        r = pltpu.roll(v, shift, 1) if shift else v
                        out[k] = jnp.where(group == j, r, out[k])
                for k in range(per_tile):
                    pb[ct * per_tile + k, t] = out[k].astype(BF16)
        for d in range(1, nsec):
            send(pb.at[sat(d)], pc.at[ylo, sec], st_s.at[1], st_r.at[1], dev(sec_=sat(d)))
        pc[ylo, sec] = pb[sec]

    def stage_c():
        await_bytes(pc.at[0, pl.ds(0, nsec - 1)], st_r.at[1])
        send(pc.at[ylo], pc.at[ylo], st_s.at[2], st_r.at[2], dev(y_=partner))

    def stage_d():
        await_bytes(pc.at[0], st_r.at[2])

        def one(s, carry):
            for l in range(2):
                v = pc[l, s].astype(F32)
                cdf, dens = gelu_parts(v)
                slope[s, l * tiles:(l + 1) * tiles] = cdf + v * dens
            return carry

        lax.fori_loop(0, nsec, one, 0)

    cut = tok // 2
    lo, hi = pl.ds(0, cut), pl.ds(cut, cut)
    ring = nx > 2

    def li_first():
        local[4].wait()
        src = li.at[core, x]
        send(src, src, li_s.at[0], li_r.at[0], dev(sec_=xat(1)))
        if ring:
            send(src, src, li_s.at[1], li_r.at[1], dev(sec_=xat(-1)))

    def li_second():
        await_bytes(li.at[0, 0], li_r.at[0])
        if ring:
            src = li.at[core, lax.rem(x + nx - 1, nx), lo]
            send(src, src, li_s.at[2], li_r.at[2], dev(sec_=xat(1)))
            await_bytes(li.at[0, 0], li_r.at[1])
            src = li.at[core, lax.rem(x + 1, nx), hi]
            send(src, src, li_s.at[3], li_r.at[3], dev(sec_=xat(-1)))

    def li_third():
        if ring:
            await_bytes(li.at[0, 0, lo], li_r.at[2])
            await_bytes(li.at[0, 0, hi], li_r.at[3])
        send(li.at[core], li.at[core], li_s.at[4], li_r.at[4], dev(sec_=peer(0, 1)))

    def first_term():
        local[3].wait()
        await_bytes(hall.at[pl.ds(0, nsec - 1)], st_r.at[3])
        gsum[0] = jnp.dot(hall[nsec - 1], og[...].reshape(tok, width), preferred_element_type=F32)
        gsum[1] = jnp.zeros((fb, width), F32)
        for j in range(nsec):
            xs[nsec - 1, j] = og[z, :, pl.ds(pl.multiple_of(ylo * fe + j * LANES, LANES), LANES)]

    plan = [(2, first_term), (3, stage_b), (3, li_first), (5, stage_c), (6, stage_d), (6, li_second)]
    for k in range(1, half + 1):
        with scope(f"hop{k}"):
            hop(k)
        with scope(f"stage{k}"):
            for at, f in plan:
                if min(at, half) == k:
                    f()
    with scope("gather_end"):
        for l in range(2):
            for way in range(2):
                await_bytes(wbuf.at[way, l, 0], wz_r.at[way, half - 1, way, l])
    li_third()

    def slot(t, core_, x_, ylo_=0, z_=0):
        return (((t * 2 + core_) * nx + x_) * 2 + ylo_) * nz + z_

    def spread_z(t):
        src = xs.at[t - 1 if isinstance(t, int) and t > 0 else lax.rem(t + nsec, nsec + 1), sec]
        dst = up.at[slot(t, core, x, ylo, z)]

        def to(d, c):
            send(src, dst, uz_s.at[0], uz_r.at[t], dev(z_=zat(d)))
            return c

        def to_partner(d, c):
            send(src, dst, uz_s.at[0], uz_r.at[t], dev(z_=zat(d), y_=partner))
            return c

        lax.fori_loop(1, nz, to, 0)
        lax.fori_loop(0, nz, to_partner, 0)
        dst[...] = src[...]

    def await_z(t):
        await_bytes(up.at[pl.ds(0, 2 * nz - 1)], uz_r.at[t])

    block = 2 * nz

    def spread_x(t):
        await_z(t)
        src = up.at[pl.ds(slot(t, core, x), block)]
        for dx in x_order:
            send(src, src, ux_s.at[0], ux_r.at[t], dev(sec_=peer(dx, 0)))

    def spread_core(t):
        await_bytes(up.at[pl.ds(0, (nx - 1) * block)], ux_r.at[t])
        src = up.at[pl.ds(slot(t, core, 0), nx * block)]
        send(src, src, ud_s.at[0], ud_r.at[t], dev(sec_=peer(0, 1)))

    def write_out(t):
        for l in range(2):
            for k in range(nsec):
                pltpu.make_async_copy(
                    up.at[pl.ds(slot(t, k % 2, k // 2, l), nz)],
                    ig_out.at[:, :, pl.ds(l * fe + k * LANES, LANES)],
                    o_s.at[0],
                ).start()

    def out_term(t):
        await_bytes(up.at[pl.ds(0, nx * block)], ud_r.at[t])
        rows = hall[t - 1]
        for l in range(2):
            rhs = jnp.concatenate(
                [up[pl.ds(slot(t, k % 2, k // 2, l), nz)].reshape(tok, LANES) for k in range(nsec)], axis=1
            )
            gsum[0, :, l * fe:(l + 1) * fe] += jnp.dot(rows, rhs, preferred_element_type=F32)

        @pl.when(sec == t)
        def _():
            write_out(t)

    def spread_g(t):
        def to(d, c):
            send(gbuf.at[t, ylo * tiles + zat(d) // per_tile], gz.at[t * nz + z], g_s.at[0], g_r.at[t], dev(z_=zat(d)))
            return c

        lax.fori_loop(1, nz, to, 0)
        gz[t * nz + z] = gbuf[t, ylo * tiles + z // per_tile]

    def in_term(t):
        await_bytes(gz.at[pl.ds(0, nz - 1)], g_r.at[t])
        gt[...] = jnp.swapaxes(gz[pl.ds(t * nz, nz)].astype(F32).reshape(tok, LANES), 0, 1)
        rows = gt[pl.ds(pl.multiple_of(lax.rem(z, per_tile) * fb, fb), fb), :].astype(BF16)
        gsum[1] += jnp.dot(rows, li[lax.rem(t, 2), t // 2], preferred_element_type=F32)

    def application(i, carry):
        s = nsec - 1 - i
        with scope("a_mm"):
            upper = xs[s]
            lhs = jnp.concatenate([upper[j] for j in range(nsec)], axis=1)
            w_out = wbuf[1].reshape(2 * nz * fb, fe)
            part = lax.dot_general(lhs, w_out, (((1,), (1,)), ((), ())), preferred_element_type=F32).astype(BF16)
            a_buf[s, y] = part
        for d in y_order:
            send(a_buf.at[s, y], a_buf.at[s, y], ph_s.at[0, s], ph_r.at[0, s], dev(y_=yat(d)))

        with scope("bg_a"):
            @pl.when(s <= nsec - 2)
            def _():
                spread_z(s + 1)

            @pl.when(s <= nsec - 3)
            def _():
                spread_x(s + 2)

            @pl.when(s <= nsec - 3)
            def _():
                @pl.when(s == nsec - 3)
                def _():
                    await_bytes(li.at[0], li_r.at[4])

                in_term(s + 2)

            @pl.when(s <= nsec - 4)
            def _():
                out_term(s + 3)

        with scope("wait_a"):
            await_bytes(a_buf.at[s, pl.ds(0, 3)], ph_r.at[0, s])
        with scope("b_mm"):
            back = a_buf[s, 0].astype(F32)
            for k in range(1, 4):
                back = back + a_buf[s, k].astype(F32)
            g = []
            for t in range(2 * tiles):
                g_tile = (back[:, t * LANES:(t + 1) * LANES] * slope[s, t]).astype(BF16)
                gbuf[s, t] = g_tile
                g.append(g_tile)
            g = jnp.concatenate(g, axis=1)
            w_in = wbuf[0].reshape(2 * nz * fb, fe)
            b_buf[s * nsec + sec] = jnp.dot(g, w_in, preferred_element_type=F32).astype(BF16)
        for dx, dc in sec_order:
            send(b_buf.at[s * nsec + sec], b_buf.at[s * nsec + sec], ph_s.at[1, s], ph_r.at[1, s], dev(sec_=peer(dx, dc)))

        with scope("bg_b"):
            spread_g(s)

            @pl.when(s <= nsec - 3)
            def _():
                spread_core(s + 2)

        with scope("wait_b"):
            await_bytes(b_buf.at[pl.ds(0, nsec - 1)], ph_r.at[1, s])
        with scope("sum_b"):
            for j in range(nsec):
                total = upper[j].astype(F32)
                for k in range(nsec):
                    total = total + b_buf[s * nsec + k, :, j * LANES:(j + 1) * LANES].astype(F32)
                xs[lax.rem(s + nsec, nsec + 1), j] = total.astype(BF16)
        return carry

    lax.fori_loop(0, nsec, application, 0)

    with scope("t_z0"):
        spread_z(0)
    with scope("t_x1"):
        spread_x(1)
    with scope("t_terms"):
        in_term(1)
        out_term(2)
    with scope("t_in0"):
        in_term(0)
        outs = [pltpu.make_async_copy(gsum.at[1], gi_out, o_s.at[1])]
        outs[0].start()
    with scope("t_core1"):
        spread_core(1)
    with scope("t_z0w"):
        await_z(0)

    @pl.when(sec != 0)
    def _():
        src = up.at[pl.ds(slot(0, core, x), block)]
        send(src, src, ux_s.at[1], ux_r.at[0], dev(sec_=0))

    with scope("t_out1"):
        out_term(1)
        outs.append(pltpu.make_async_copy(gsum.at[0], go_out, o_s.at[2]))
        outs[1].start()
    with scope("t_x0w"):
        @pl.when(sec == 0)
        def _():
            await_bytes(up.at[pl.ds(0, (nsec - 1) * block)], ux_r.at[0])
            write_out(0)

    with scope("drain"):
        await_bytes(pa_all.at[pl.ds(0, nz - 1)], st_s.at[0])
        await_bytes(pc.at[0, pl.ds(0, nsec - 1)], st_s.at[1])
        await_bytes(pc.at[0], st_s.at[2])
        await_bytes(hall.at[pl.ds(0, nsec - 1)], st_s.at[3])
        for cp in swaps:
            cp.wait_send()
        for way in range(2):
            await_bytes(wbuf.at[0, :, pl.ds(0, nz - 1)], wz_s.at[way])
        await_bytes(li.at[0, 0], li_s.at[0])
        if ring:
            await_bytes(li.at[0, 0], li_s.at[1])
            await_bytes(li.at[0, 0, lo], li_s.at[2])
            await_bytes(li.at[0, 0, hi], li_s.at[3])
        await_bytes(li.at[0], li_s.at[4])

        def sent(s, c):
            await_bytes(a_buf.at[0, pl.ds(0, 3)], ph_s.at[0, s])
            await_bytes(b_buf.at[pl.ds(0, nsec - 1)], ph_s.at[1, s])
            return c

        lax.fori_loop(0, nsec, sent, 0)
        await_bytes(gz.at[pl.ds(0, nsec * (nz - 1))], g_s.at[0])
        await_bytes(up.at[pl.ds(0, nsec * (2 * nz - 1))], uz_s.at[0])
        await_bytes(up.at[pl.ds(0, (nsec - 1) * (nx - 1) * block)], ux_s.at[0])
        await_bytes(up.at[pl.ds(0, (nsec - 1) * nx * block)], ud_s.at[0])

        @pl.when(sec != 0)
        def _():
            await_bytes(up.at[pl.ds(0, block)], ux_s.at[1])

        for cp in outs:
            cp.wait()
        await_bytes(up.at[pl.ds(0, nsec * block)], o_s.at[0])


def body(layer_inputs, pre_act, out_grad, w_in, w_out):
    nz, nx = lax.axis_size("z"), lax.axis_size("x")
    nsec = 2 * nx
    tok, width = out_grad.shape
    fb = w_in.shape[2]
    hid = pre_act.shape[2]
    fe = width // 2
    tiles = nz * fb // LANES
    half = nz // 2
    dma = pltpu.SemaphoreType.DMA
    vmem = pltpu.VMEM
    scratch = [
        vmem((2, 2, nz, fb, fe), BF16),
        vmem((nz, 8, hid), BF16),
        vmem((nz, 8, hid), BF16),
        vmem((nsec, tiles, 8, LANES), BF16),
        vmem((2, nsec, tiles, 8, LANES), BF16),
        vmem((nsec, 2 * tiles, 8, LANES), F32),
        vmem((nsec, fb, tok), BF16),
        vmem((nsec, fb, tok), BF16),
        vmem((2, nx, tok, width), BF16),
        vmem((nz, 8, width), BF16),
        vmem((nsec + 1, nsec, 8, LANES), BF16),
        vmem((nsec, 4, 8, 2 * nz * fb), BF16),
        vmem((nsec * nsec, 8, fe), BF16),
        vmem((nsec, 2 * tiles, 8, LANES), BF16),
        vmem((nsec * nz, 8, LANES), BF16),
        vmem((LANES, tok), F32),
        vmem((nsec * nsec * 2 * nz, 8, LANES), BF16),
        vmem((2, fb, width), F32),
        dma((5,)),
        dma((2,)), dma((2,)),
        dma((2,)), dma((2, half, 2, 2)),
        dma((4,)), dma((4,)),
        dma((2, nsec)), dma((2, nsec)),
        dma((5,)), dma((5,)),
        dma((1,)), dma((nsec,)),
        dma((1,)), dma((nsec,)),
        dma((2,)), dma((nsec,)),
        dma((1,)), dma((nsec,)),
        dma((3,)),
    ]
    any_ = pl.BlockSpec(memory_space=pltpu.HBM)
    ig, gi, go = pl.pallas_call(
        kernel,
        out_shape=(
            jax.ShapeDtypeStruct((nz, 8, width), BF16),
            jax.ShapeDtypeStruct((fb, width), F32),
            jax.ShapeDtypeStruct((fb, width), F32),
        ),
        in_specs=[any_] * 5,
        out_specs=(any_,) * 3,
        scratch_shapes=scratch,
        name="chain",
        compiler_params=pltpu.CompilerParams(
            collective_id=0, has_side_effects=True, vmem_limit_bytes=67043328
        ),
    )(
        layer_inputs.reshape(tok, width),
        pre_act.reshape(nz, 8, hid),
        out_grad.reshape(nz, 8, width),
        w_in.reshape(fb, width),
        w_out.reshape(fb, width),
    )
    return (
        ig.reshape(1, tok, width),
        gi.reshape(1, 1, fb, width),
        go.reshape(1, 1, fb, width),
    )


def solution(mesh):
    shape = mesh.shape
    split = Mesh(
        mesh.devices.reshape(shape["section"] // 2, 2, shape["dp"] // 2, 2, shape["mp"]), AXES
    )
    sec, dp = ("x", "core"), ("z", "ylo")
    placed = (
        P(sec, None, "yhi"),
        P(sec, None, dp),
        P(None, "yhi"),
        P(dp, sec, None, "yhi"),
        P(dp, sec, None, "yhi"),
    )
    return jax.shard_map(
        body,
        mesh=split,
        in_specs=placed,
        out_specs=(P(sec, None, "yhi"), P(dp, sec, None, "yhi"), P(dp, sec, None, "yhi")),
        check_vma=False,
    )
```

```python
import contextlib

import jax
import jax.numpy as jnp
from jax import lax
from jax.experimental import pallas as pl
from jax.experimental.pallas import tpu as pltpu
from jax.sharding import Mesh
from jax.sharding import PartitionSpec as P

AXES = ("x", "core", "z", "ylo", "yhi")
MESH_ID = pl.DeviceIdType.MESH
BF16, F32 = jnp.bfloat16, jnp.float32
LANES = 128
PROFILE = False


def scope(name):
    return jax.named_scope(name) if PROFILE else contextlib.nullcontext()


def gelu_parts(v):
    cdf = 0.5 * (1.0 + lax.erf(v * 0.7071067811865476))
    dens = jnp.exp(-0.5 * v * v) * 0.3989422804014327
    return cdf, dens


def kernel(
    li_hbm, pa_hbm, og_hbm, wi_hbm, wo_hbm,
    ig_out, gi_out, go_out,
    wbuf, pa, pa_all, pb, pc, slope, h_t, hall, li, og,
    xs, a_buf, b_buf, gbuf, gz, gt, up,
    lsem, wx_s, wx_r, wz_s, wz_r, st_s, st_r, ph_s, ph_r, li_s, li_r,
    g_s, g_r, uz_s, uz_r, ux_s, ux_r, ud_s, ud_r,
):
    nx, nz = lax.axis_size("x"), lax.axis_size("z")
    nsec = 2 * nx
    fb, width = wi_hbm.shape
    fe = width // 2
    tok = nz * 8
    tiles = nz * fb // LANES
    per_tile = LANES // fb
    x, core, z = lax.axis_index("x"), lax.axis_index("core"), lax.axis_index("z")
    ylo, yhi = lax.axis_index("ylo"), lax.axis_index("yhi")
    sec = x * 2 + core
    y = yhi * 2 + ylo
    other = 1 - ylo
    partner = yhi * 2 + other

    def dev(sec_=None, z_=None, y_=None):
        sec_ = sec if sec_ is None else sec_
        y_ = y if y_ is None else y_
        return (sec_ // 2, lax.rem(sec_, 2), z if z_ is None else z_, lax.rem(y_, 2), y_ // 2)

    def copy(src, dst, ssem, rsem, to):
        return pltpu.make_async_remote_copy(
            src_ref=src, dst_ref=dst, send_sem=ssem, recv_sem=rsem, device_id=to, device_id_type=MESH_ID
        )

    def send(*args):
        cp = copy(*args)
        cp.start()
        return cp

    def await_bytes(ref, sem):
        pltpu.make_async_copy(ref, ref, sem).wait()

    def zat(d):
        return lax.rem(z + d + nz, nz)

    def sat(d):
        return lax.rem(sec + d, nsec)

    def xat(d):
        return lax.rem(x + d + nx, nx) * 2 + core

    def yat(d):
        return lax.rem(y + d, 4)

    y_order = (2, 1, 3)
    sec_order = sorted(((dx, dc) for dx in range(nx) for dc in range(2) if dx or dc), key=lambda p: -min(p[0], nx - p[0]))
    x_order = [dx for dx, dc in sec_order if dc == 0]

    def peer(dx, dc):
        return lax.rem(x + dx, nx) * 2 + (1 - core if dc else core)

    mine = pl.ds(pl.multiple_of(ylo * fe, LANES), fe)
    theirs = pl.ds(pl.multiple_of(other * fe, LANES), fe)

    w_hbm = (wi_hbm, wo_hbm)
    local = [pltpu.make_async_copy(pa_hbm, pa, lsem.at[0])]
    for m in range(2):
        local.append(pltpu.make_async_copy(w_hbm[m].at[:, mine], wbuf.at[m, ylo, z], lsem.at[1 + m]))
    local.append(pltpu.make_async_copy(og_hbm, og, lsem.at[3]))
    local.append(pltpu.make_async_copy(li_hbm, li.at[core, x], lsem.at[4]))
    for cp in local:
        cp.start()

    barrier = pltpu.get_barrier_semaphore()
    greeted = 0
    for to in (
        [dev(z_=zat(d)) for d in range(1, nz)] + [dev(sec_=sat(d)) for d in range(1, nsec)] + [dev(y_=yat(d)) for d in range(1, 4)]
    ):
        pl.semaphore_signal(barrier, inc=1, device_id=to, device_id_type=MESH_ID)
        greeted += 1
    local[0].wait()
    v = pa[...].astype(F32).reshape(tok, nsec * fb)
    h_t[...] = jnp.swapaxes(v * gelu_parts(v)[0], 0, 1).astype(BF16).reshape(nsec, fb, tok)
    with scope("barrier"):
        pl.semaphore_wait(barrier, greeted)

    for d in range(1, nz):
        send(pa.at[zat(d)], pa_all.at[z], st_s.at[0], st_r.at[0], dev(z_=zat(d)))
    swaps = [
        send(w_hbm[m].at[:, theirs], wbuf.at[m, ylo, z], wx_s.at[m], wx_r.at[m], dev(y_=partner))
        for m in range(2)
    ]
    for d in range(1, nsec):
        send(h_t.at[sat(d)], hall.at[sec], st_s.at[3], st_r.at[3], dev(sec_=sat(d)))
    hall[sec] = h_t[sec]
    pa_all[z] = pa[z]

    half = nz // 2

    def hop(k):
        last = k == half
        for which in range(2):
            l = ylo if which == 0 else other
            for m in range(2):
                if k == 1:
                    if which == 0:
                        local[1 + m].wait()
                    else:
                        swaps[m].wait_recv()
                for way, step in ((0, 1), (1, -1)):
                    if k > 1:
                        await_bytes(wbuf.at[m, l, 0], wz_r.at[way, k - 2, m, l])
                    if last and way != m:
                        continue
                    src = wbuf.at[m, l, zat(-step * (k - 1))]
                    send(src, src, wz_s.at[way], wz_r.at[way, k - 1, m, l], dev(z_=zat(step)))

    def stage_b():
        await_bytes(pa_all.at[pl.ds(0, nz - 1)], st_r.at[0])
        group = lax.broadcasted_iota(jnp.int32, (8, LANES), 1) // fb
        for ct in range(nsec // per_tile):
            for t in range(tiles):
                out = [jnp.zeros((8, LANES), F32)] * per_tile
                for j in range(per_tile):
                    v = pa_all[t * per_tile + j, :, ct * LANES:(ct + 1) * LANES].astype(F32)
                    for k in range(per_tile):
                        shift = (j - k) * fb % LANES
                        r = pltpu.roll(v, shift, 1) if shift else v
                        out[k] = jnp.where(group == j, r, out[k])
                for k in range(per_tile):
                    pb[ct * per_tile + k, t] = out[k].astype(BF16)
        for d in range(1, nsec):
            send(pb.at[sat(d)], pc.at[ylo, sec], st_s.at[1], st_r.at[1], dev(sec_=sat(d)))
        pc[ylo, sec] = pb[sec]

    def stage_c():
        await_bytes(pc.at[0, pl.ds(0, nsec - 1)], st_r.at[1])
        send(pc.at[ylo], pc.at[ylo], st_s.at[2], st_r.at[2], dev(y_=partner))

    def stage_d():
        await_bytes(pc.at[0], st_r.at[2])

        def one(s, carry):
            for l in range(2):
                v = pc[l, s].astype(F32)
                cdf, dens = gelu_parts(v)
                slope[s, l * tiles:(l + 1) * tiles] = cdf + v * dens
            return carry

        lax.fori_loop(0, nsec, one, 0)

    cut = tok // 2
    lo, hi = pl.ds(0, cut), pl.ds(cut, cut)
    ring = nx > 2

    def li_first():
        local[4].wait()
        src = li.at[core, x]
        send(src, src, li_s.at[0], li_r.at[0], dev(sec_=xat(1)))
        if ring:
            send(src, src, li_s.at[1], li_r.at[1], dev(sec_=xat(-1)))

    def li_second():
        await_bytes(li.at[0, 0], li_r.at[0])
        if ring:
            src = li.at[core, lax.rem(x + nx - 1, nx), lo]
            send(src, src, li_s.at[2], li_r.at[2], dev(sec_=xat(1)))
            await_bytes(li.at[0, 0], li_r.at[1])
            src = li.at[core, lax.rem(x + 1, nx), hi]
            send(src, src, li_s.at[3], li_r.at[3], dev(sec_=xat(-1)))

    def li_third():
        if ring:
            await_bytes(li.at[0, 0, lo], li_r.at[2])
            await_bytes(li.at[0, 0, hi], li_r.at[3])
        send(li.at[core], li.at[core], li_s.at[4], li_r.at[4], dev(sec_=peer(0, 1)))

    def first_term():
        local[3].wait()
        await_bytes(hall.at[pl.ds(0, nsec - 1)], st_r.at[3])
        go_out[...] = jnp.dot(hall[nsec - 1], og[...].reshape(tok, width), preferred_element_type=F32)
        gi_out[...] = jnp.zeros((fb, width), F32)
        for j in range(nsec):
            xs[nsec - 1, j] = og[z, :, pl.ds(pl.multiple_of(ylo * fe + j * LANES, LANES), LANES)]

    plan = [(2, first_term), (3, stage_b), (3, li_first), (5, stage_c), (6, stage_d), (6, li_second)]
    for k in range(1, half + 1):
        with scope(f"hop{k}"):
            hop(k)
        with scope(f"stage{k}"):
            for at, f in plan:
                if min(at, half) == k:
                    f()
    with scope("gather_end"):
        for l in range(2):
            for way in range(2):
                await_bytes(wbuf.at[way, l, 0], wz_r.at[way, half - 1, way, l])
    li_third()

    def slot(t, core_, x_, ylo_=0, z_=0):
        return (((t * 2 + core_) * nx + x_) * 2 + ylo_) * nz + z_

    def spread_z(t):
        src = xs.at[nsec if isinstance(t, int) and t == 0 else t - 1, sec]
        dst = up.at[slot(t, core, x, ylo, z)]

        def both(d):
            send(src, dst, uz_s.at[0], uz_r.at[t], dev(z_=zat(d), y_=partner))
            send(src, dst, uz_s.at[0], uz_r.at[t], dev(z_=zat(d)))

        both(nz // 2)

        def pair(i, c):
            both(nz // 2 - i)
            both(nz // 2 + i)
            return c

        lax.fori_loop(1, nz // 2, pair, 0)
        send(src, dst, uz_s.at[0], uz_r.at[t], dev(y_=partner))
        dst[...] = src[...]

    def await_z(t):
        await_bytes(up.at[pl.ds(0, 2 * nz - 1)], uz_r.at[t])

    block = 2 * nz

    def spread_x(t):
        await_z(t)
        src = up.at[pl.ds(slot(t, core, x), block)]
        for dx in x_order:
            send(src, src, ux_s.at[0], ux_r.at[t], dev(sec_=peer(dx, 0)))

    def spread_core(t):
        await_bytes(up.at[pl.ds(0, (nx - 1) * block)], ux_r.at[t])
        src = up.at[pl.ds(slot(t, core, 0), nx * block)]
        send(src, src, ud_s.at[0], ud_r.at[t], dev(sec_=peer(0, 1)))

    def write_out(t):
        for l in range(2):
            for k in range(nsec):
                ig_out[:, :, l * fe + k * LANES:l * fe + (k + 1) * LANES] = up[pl.ds(slot(t, k % 2, k // 2, l), nz)]

    def out_term(t):
        await_bytes(up.at[pl.ds(0, nx * block)], ud_r.at[t])
        rows = hall[t - 1]
        for l in range(2):
            rhs = jnp.concatenate(
                [up[pl.ds(slot(t, k % 2, k // 2, l), nz)].reshape(tok, LANES) for k in range(nsec)], axis=1
            )
            go_out[:, l * fe:(l + 1) * fe] += jnp.dot(rows, rhs, preferred_element_type=F32)

        @pl.when(sec == t)
        def _():
            write_out(t)

    def spread_g(t):
        def to(d, c):
            send(gbuf.at[t, ylo * tiles + zat(d) // per_tile], gz.at[t * nz + z], g_s.at[0], g_r.at[t], dev(z_=zat(d)))
            return c

        lax.fori_loop(1, nz, to, 0)
        gz[t * nz + z] = gbuf[t, ylo * tiles + z // per_tile]

    def in_term(t):
        await_bytes(gz.at[pl.ds(0, nz - 1)], g_r.at[t])
        gt[...] = jnp.swapaxes(gz[pl.ds(t * nz, nz)].astype(F32).reshape(tok, LANES), 0, 1)
        rows = gt[pl.ds(pl.multiple_of(lax.rem(z, per_tile) * fb, fb), fb), :].astype(BF16)
        gi_out[...] += jnp.dot(rows, li[lax.rem(t, 2), t // 2], preferred_element_type=F32)

    def application(s, final):
        with scope("a_mm"):
            upper = xs[s]
            lhs = jnp.concatenate([upper[j] for j in range(nsec)], axis=1)
            w_out = wbuf[1].reshape(2 * nz * fb, fe)
            part = lax.dot_general(lhs, w_out, (((1,), (1,)), ((), ())), preferred_element_type=F32).astype(BF16)
            a_buf[s, y] = part
        for d in y_order:
            send(a_buf.at[s, y], a_buf.at[s, y], ph_s.at[0, s], ph_r.at[0, s], dev(y_=yat(d)))

        with scope("bg_a"):
            @pl.when(s <= nsec - 2)
            def _():
                spread_z(s + 1)

            @pl.when(s <= nsec - 3)
            def _():
                spread_x(s + 2)

                @pl.when(s == nsec - 3)
                def _():
                    await_bytes(li.at[0], li_r.at[4])

                in_term(s + 2)

            @pl.when(s <= nsec - 4)
            def _():
                out_term(s + 3)

        with scope("wait_a"):
            await_bytes(a_buf.at[s, pl.ds(0, 3)], ph_r.at[0, s])
        with scope("b_mm"):
            back = a_buf[s, 0].astype(F32)
            for k in range(1, 4):
                back = back + a_buf[s, k].astype(F32)
            g = []
            for t in range(2 * tiles):
                g_tile = (back[:, t * LANES:(t + 1) * LANES] * slope[s, t]).astype(BF16)
                gbuf[s, t] = g_tile
                g.append(g_tile)
            g = jnp.concatenate(g, axis=1)
            w_in = wbuf[0].reshape(2 * nz * fb, fe)
            part = jnp.dot(g, w_in, preferred_element_type=F32).astype(BF16)
            for j in range(nsec):
                b_buf[s, sec, j] = part[:, j * LANES:(j + 1) * LANES]
        if final:
            for dx, dc in sec_order:
                to = peer(dx, dc)
                send(b_buf.at[s, sec, to], b_buf.at[s, sec, to], ph_s.at[1, s], ph_r.at[1, s], dev(sec_=to))
        else:
            for dx, dc in sec_order:
                send(b_buf.at[s, sec], b_buf.at[s, sec], ph_s.at[1, s], ph_r.at[1, s], dev(sec_=peer(dx, dc)))

        with scope("bg_b"):
            spread_g(s)

            @pl.when(s <= nsec - 3)
            def _():
                spread_core(s + 2)

        with scope("wait_b"):
            if final:
                await_bytes(b_buf.at[0, 0, pl.ds(0, nsec - 1)], ph_r.at[1, s])
            else:
                await_bytes(b_buf.at[0, pl.ds(0, nsec - 1)], ph_r.at[1, s])
        with scope("sum_b"):
            for j in [sec] if final else range(nsec):
                total = xs[s, j].astype(F32)
                for k in range(nsec):
                    total = total + b_buf[s, k, j].astype(F32)
                xs[nsec if final else s - 1, j] = total.astype(BF16)

    def step(i, carry):
        application(nsec - 1 - i, False)
        return carry

    lax.fori_loop(0, nsec - 1, step, 0)
    application(0, True)

    with scope("t_z0"):
        spread_z(0)
    with scope("t_x1"):
        spread_x(1)
    with scope("t_terms"):
        in_term(1)
        out_term(2)
    with scope("t_in0"):
        in_term(0)
    with scope("t_core1"):
        spread_core(1)
    with scope("t_z0w"):
        await_z(0)

    def columns(l):
        return pl.ds(pl.multiple_of(l * fe + sec * LANES, LANES), LANES)

    @pl.when(sec != 0)
    def _():
        for l in range(2):
            send(
                up.at[pl.ds(slot(0, core, x, l), nz)],
                ig_out.at[:, :, columns(l)],
                ux_s.at[1],
                ux_r.at[0],
                dev(sec_=0),
            )

    @pl.when(sec == 0)
    def _():
        for l in range(2):
            ig_out[:, :, l * fe:l * fe + LANES] = up[pl.ds(slot(0, 0, 0, l), nz)]

    with scope("t_out1"):
        out_term(1)
    with scope("t_x0w"):
        @pl.when(sec == 0)
        def _():
            await_bytes(up.at[pl.ds(0, (nsec - 1) * block)], ux_r.at[0])

    with scope("drain"):
        await_bytes(pa_all.at[pl.ds(0, nz - 1)], st_s.at[0])
        await_bytes(pc.at[0, pl.ds(0, nsec - 1)], st_s.at[1])
        await_bytes(pc.at[0], st_s.at[2])
        await_bytes(hall.at[pl.ds(0, nsec - 1)], st_s.at[3])
        for cp in swaps:
            cp.wait_send()
        for way in range(2):
            await_bytes(wbuf.at[0, :, pl.ds(0, nz - 1)], wz_s.at[way])
        await_bytes(li.at[0, 0], li_s.at[0])
        if ring:
            await_bytes(li.at[0, 0], li_s.at[1])
            await_bytes(li.at[0, 0, lo], li_s.at[2])
            await_bytes(li.at[0, 0, hi], li_s.at[3])
        await_bytes(li.at[0], li_s.at[4])

        def sent(s, c):
            await_bytes(a_buf.at[0, pl.ds(0, 3)], ph_s.at[0, s])
            await_bytes(b_buf.at[0, pl.ds(0, nsec - 1)], ph_s.at[1, s])
            return c

        lax.fori_loop(1, nsec, sent, 0)
        await_bytes(a_buf.at[0, pl.ds(0, 3)], ph_s.at[0, 0])
        await_bytes(b_buf.at[0, 0, pl.ds(0, nsec - 1)], ph_s.at[1, 0])
        await_bytes(gz.at[pl.ds(0, nsec * (nz - 1))], g_s.at[0])
        await_bytes(up.at[pl.ds(0, nsec * (2 * nz - 1))], uz_s.at[0])
        await_bytes(up.at[pl.ds(0, (nsec - 1) * (nx - 1) * block)], ux_s.at[0])
        await_bytes(up.at[pl.ds(0, (nsec - 1) * nx * block)], ud_s.at[0])

        @pl.when(sec != 0)
        def _():
            await_bytes(up.at[pl.ds(0, block)], ux_s.at[1])


def finish(ig, gi, go, ig_out, gi_out, go_out, sems):
    copies = [pltpu.make_async_copy(src, dst, sems.at[k]) for k, (src, dst) in enumerate(((ig, ig_out), (gi, gi_out), (go, go_out)))]
    for cp in copies:
        cp.start()
    for cp in copies:
        cp.wait()


def body(layer_inputs, pre_act, out_grad, w_in, w_out):
    nz, nx = lax.axis_size("z"), lax.axis_size("x")
    nsec = 2 * nx
    tok, width = out_grad.shape
    fb = w_in.shape[2]
    hid = pre_act.shape[2]
    fe = width // 2
    tiles = nz * fb // LANES
    half = nz // 2
    dma = pltpu.SemaphoreType.DMA
    vmem = pltpu.VMEM
    scratch = [
        vmem((2, 2, nz, fb, fe), BF16),
        vmem((nz, 8, hid), BF16),
        vmem((nz, 8, hid), BF16),
        vmem((nsec, tiles, 8, LANES), BF16),
        vmem((2, nsec, tiles, 8, LANES), BF16),
        vmem((nsec, 2 * tiles, 8, LANES), F32),
        vmem((nsec, fb, tok), BF16),
        vmem((nsec, fb, tok), BF16),
        vmem((2, nx, tok, width), BF16),
        vmem((nz, 8, width), BF16),
        vmem((nsec + 1, nsec, 8, LANES), BF16),
        vmem((nsec, 4, 8, 2 * nz * fb), BF16),
        vmem((nsec, nsec, nsec, 8, LANES), BF16),
        vmem((nsec, 2 * tiles, 8, LANES), BF16),
        vmem((nsec * nz, 8, LANES), BF16),
        vmem((LANES, tok), F32),
        vmem((nsec * nsec * 2 * nz, 8, LANES), BF16),
        dma((5,)),
        dma((2,)), dma((2,)),
        dma((2,)), dma((2, half, 2, 2)),
        dma((4,)), dma((4,)),
        dma((2, nsec)), dma((2, nsec)),
        dma((5,)), dma((5,)),
        dma((1,)), dma((nsec,)),
        dma((1,)), dma((nsec,)),
        dma((2,)), dma((nsec,)),
        dma((1,)), dma((nsec,)),
    ]
    hbm, on_chip = pl.BlockSpec(memory_space=pltpu.HBM), pl.BlockSpec(memory_space=pltpu.VMEM)
    shapes = (
        jax.ShapeDtypeStruct((nz, 8, width), BF16),
        jax.ShapeDtypeStruct((fb, width), F32),
        jax.ShapeDtypeStruct((fb, width), F32),
    )
    operands = (
        layer_inputs.reshape(tok, width),
        pre_act.reshape(nz, 8, hid),
        out_grad.reshape(nz, 8, width),
        w_in.reshape(fb, width),
        w_out.reshape(fb, width),
    )
    results = pl.pallas_call(
        kernel,
        out_shape=shapes,
        in_specs=[hbm] * 5,
        out_specs=(on_chip,) * 3,
        scratch_shapes=scratch,
        name="chain",
        compiler_params=pltpu.CompilerParams(
            collective_id=0, has_side_effects=True, vmem_limit_bytes=32 * 1024 * 1024
        ),
    )(*(pltpu.with_memory_space_constraint(v, pltpu.HBM) for v in operands))
    ig, gi, go = pl.pallas_call(
        finish,
        out_shape=shapes,
        in_specs=[on_chip] * 3,
        out_specs=(hbm,) * 3,
        scratch_shapes=[dma((3,))],
        name="finish",
    )(*(pltpu.with_memory_space_constraint(v, pltpu.VMEM) for v in results))
    return (
        ig.reshape(1, tok, width),
        gi.reshape(1, 1, fb, width),
        go.reshape(1, 1, fb, width),
    )


def solution(mesh):
    shape = mesh.shape
    split = Mesh(
        mesh.devices.reshape(shape["section"] // 2, 2, shape["dp"] // 2, 2, shape["mp"]), AXES
    )
    sec, dp = ("x", "core"), ("z", "ylo")
    placed = (
        P(sec, None, "yhi"),
        P(sec, None, dp),
        P(None, "yhi"),
        P(dp, sec, None, "yhi"),
        P(dp, sec, None, "yhi"),
    )
    return jax.shard_map(
        body,
        mesh=split,
        in_specs=placed,
        out_specs=(P(sec, None, "yhi"), P(dp, sec, None, "yhi"), P(dp, sec, None, "yhi")),
        check_vma=False,
    )
```

```python
import contextlib

import jax
import jax.numpy as jnp
from jax import lax
from jax.experimental import pallas as pl
from jax.experimental.pallas import tpu as pltpu
from jax.sharding import Mesh
from jax.sharding import PartitionSpec as P

AXES = ("x", "core", "z", "ylo", "yhi")
MESH_ID = pl.DeviceIdType.MESH
BF16, F32 = jnp.bfloat16, jnp.float32
LANES = 128
PROFILE = False


def scope(name):
    return jax.named_scope(name) if PROFILE else contextlib.nullcontext()


def gelu_parts(v):
    cdf = 0.5 * (1.0 + lax.erf(v * 0.7071067811865476))
    dens = jnp.exp(-0.5 * v * v) * 0.3989422804014327
    return cdf, dens


def kernel(
    li_hbm, pa_hbm, og_hbm, wi_hbm, wo_hbm,
    ig_out, gi_out, go_out,
    wbuf, pa, pa_all, pb, pc, slope, pa_t, pre_t, hall, li, og,
    a_top, b_top, r_top, q_top, z_top, g_top,
    xs, a_buf, b_buf, gbuf, gz, gt, up,
    lsem, wx_s, wx_r, wz_s, wz_r, st_s, st_r, top_s, top_r, ph_s, ph_r, li_s, li_r,
    g_s, g_r, uz_s, uz_r, ux_s, ux_r, ud_s, ud_r,
):
    nx, nz = lax.axis_size("x"), lax.axis_size("z")
    nsec = 2 * nx
    fb, width = wi_hbm.shape
    fe = width // 2
    tok = nz * 8
    tiles = nz * fb // LANES
    per_tile = LANES // fb
    x, core, z = lax.axis_index("x"), lax.axis_index("core"), lax.axis_index("z")
    ylo, yhi = lax.axis_index("ylo"), lax.axis_index("yhi")
    sec = x * 2 + core
    y = yhi * 2 + ylo
    other = 1 - ylo
    partner = yhi * 2 + other

    def dev(sec_=None, z_=None, y_=None):
        sec_ = sec if sec_ is None else sec_
        y_ = y if y_ is None else y_
        return (sec_ // 2, lax.rem(sec_, 2), z if z_ is None else z_, lax.rem(y_, 2), y_ // 2)

    def copy(src, dst, ssem, rsem, to):
        return pltpu.make_async_remote_copy(
            src_ref=src, dst_ref=dst, send_sem=ssem, recv_sem=rsem, device_id=to, device_id_type=MESH_ID
        )

    def send(*args):
        cp = copy(*args)
        cp.start()
        return cp

    def await_bytes(ref, sem):
        pltpu.make_async_copy(ref, ref, sem).wait()

    def zat(d):
        return lax.rem(z + d + nz, nz)

    def sat(d):
        return lax.rem(sec + d, nsec)

    def xat(d):
        return lax.rem(x + d + nx, nx) * 2 + core

    def yat(d):
        return lax.rem(y + d, 4)

    y_order = (2, 1, 3)
    sec_order = sorted(((dx, dc) for dx in range(nx) for dc in range(2) if dx or dc), key=lambda p: -min(p[0], nx - p[0]))
    x_order = [dx for dx, dc in sec_order if dc == 0]

    def peer(dx, dc):
        return lax.rem(x + dx, nx) * 2 + (1 - core if dc else core)

    mine = pl.ds(pl.multiple_of(ylo * fe, LANES), fe)
    theirs = pl.ds(pl.multiple_of(other * fe, LANES), fe)

    w_hbm = (wi_hbm, wo_hbm)
    local = [pltpu.make_async_copy(pa_hbm, pa, lsem.at[0])]
    for m in range(2):
        local.append(pltpu.make_async_copy(w_hbm[m].at[:, mine], wbuf.at[m, ylo, z], lsem.at[1 + m]))
    local.append(pltpu.make_async_copy(og_hbm, og, lsem.at[3]))
    local.append(pltpu.make_async_copy(li_hbm, li.at[core, x], lsem.at[4]))
    for cp in local:
        cp.start()

    barrier = pltpu.get_barrier_semaphore()
    greeted = 0
    for to in (
        [dev(z_=zat(d)) for d in range(1, nz)] + [dev(sec_=sat(d)) for d in range(1, nsec)] + [dev(y_=yat(d)) for d in range(1, 4)]
    ):
        pl.semaphore_signal(barrier, inc=1, device_id=to, device_id_type=MESH_ID)
        greeted += 1
    local[0].wait()
    v = pa[...].astype(F32).reshape(tok, nsec * fb)
    pa_t[...] = jnp.swapaxes(v, 0, 1).astype(BF16).reshape(nsec, fb, tok)
    with scope("barrier"):
        pl.semaphore_wait(barrier, greeted)

    for d in range(1, nz):
        send(pa.at[zat(d)], pa_all.at[z], st_s.at[0], st_r.at[0], dev(z_=zat(d)))
    swaps = [
        send(w_hbm[m].at[:, theirs], wbuf.at[m, ylo, z], wx_s.at[m], wx_r.at[m], dev(y_=partner))
        for m in range(2)
    ]
    top = nsec - 1
    for d in range(1, nsec):
        send(pa_t.at[sat(d)], pre_t.at[sec], st_s.at[3], st_r.at[3], dev(sec_=sat(d)))
    pre_t[sec] = pa_t[sec]
    pa_all[z] = pa[z]

    half = nz // 2

    def hop(k):
        last = k == half
        for which in range(2):
            l = ylo if which == 0 else other
            for m in range(2):
                if k == 1:
                    if which == 0:
                        local[1 + m].wait()
                    else:
                        swaps[m].wait_recv()
                for way, step in ((0, 1), (1, -1)):
                    if k > 1:
                        await_bytes(wbuf.at[m, l, 0], wz_r.at[way, k - 2, m, l])
                    if last and way != m:
                        continue
                    src = wbuf.at[m, l, zat(-step * (k - 1))]
                    send(src, src, wz_s.at[way], wz_r.at[way, k - 1, m, l], dev(z_=zat(step)))

    def stage_b():
        await_bytes(pa_all.at[pl.ds(0, nz - 1)], st_r.at[0])
        group = lax.broadcasted_iota(jnp.int32, (8, LANES), 1) // fb
        for ct in range(nsec // per_tile):
            for t in range(tiles):
                out = [jnp.zeros((8, LANES), F32)] * per_tile
                for j in range(per_tile):
                    v = pa_all[t * per_tile + j, :, ct * LANES:(ct + 1) * LANES].astype(F32)
                    for k in range(per_tile):
                        shift = (j - k) * fb % LANES
                        r = pltpu.roll(v, shift, 1) if shift else v
                        out[k] = jnp.where(group == j, r, out[k])
                for k in range(per_tile):
                    pb[ct * per_tile + k, t] = out[k].astype(BF16)
        for d in range(1, nsec):
            send(pb.at[sat(d)], pc.at[ylo, sec], st_s.at[1], st_r.at[1], dev(sec_=sat(d)))
        pc[ylo, sec] = pb[sec]

    def stage_c():
        await_bytes(pc.at[0, pl.ds(0, nsec - 1)], st_r.at[1])
        send(pc.at[ylo], pc.at[ylo], st_s.at[2], st_r.at[2], dev(y_=partner))

    def stage_d():
        await_bytes(pc.at[0], st_r.at[2])

        def one(s, carry):
            for l in range(2):
                v = pc[l, s].astype(F32)
                cdf, dens = gelu_parts(v)
                slope[s, l * tiles:(l + 1) * tiles] = cdf + v * dens
            return carry

        lax.fori_loop(0, nsec, one, 0)

    cut = tok // 2
    lo, hi = pl.ds(0, cut), pl.ds(cut, cut)
    ring = nx > 2

    def li_first():
        local[4].wait()
        src = li.at[core, x]
        send(src, src, li_s.at[0], li_r.at[0], dev(sec_=xat(1)))
        if ring:
            send(src, src, li_s.at[1], li_r.at[1], dev(sec_=xat(-1)))

    def li_second():
        await_bytes(li.at[0, 0], li_r.at[0])
        if ring:
            src = li.at[core, lax.rem(x + nx - 1, nx), lo]
            send(src, src, li_s.at[2], li_r.at[2], dev(sec_=xat(1)))
            await_bytes(li.at[0, 0], li_r.at[1])
            src = li.at[core, lax.rem(x + 1, nx), hi]
            send(src, src, li_s.at[3], li_r.at[3], dev(sec_=xat(-1)))

    def li_third():
        if ring:
            await_bytes(li.at[0, 0, lo], li_r.at[2])
            await_bytes(li.at[0, 0, hi], li_r.at[3])
        send(li.at[core], li.at[core], li_s.at[4], li_r.at[4], dev(sec_=peer(0, 1)))

    def slot(t, core_, x_, ylo_=0, z_=0):
        return (((t * 2 + core_) * nx + x_) * 2 + ylo_) * nz + z_

    def spread_z(t):
        src = xs.at[nsec if isinstance(t, int) and t == 0 else t - 1, sec]
        dst = up.at[slot(t, core, x, ylo, z)]

        def both(d):
            send(src, dst, uz_s.at[0], uz_r.at[t], dev(z_=zat(d), y_=partner))
            send(src, dst, uz_s.at[0], uz_r.at[t], dev(z_=zat(d)))

        both(nz // 2)

        def pair(i, c):
            both(nz // 2 - i)
            both(nz // 2 + i)
            return c

        lax.fori_loop(1, nz // 2, pair, 0)
        send(src, dst, uz_s.at[0], uz_r.at[t], dev(y_=partner))
        dst[...] = src[...]

    def top_first():
        local[3].wait()
        rows = wbuf[1, :, z].reshape(2 * fb, fe)
        a_top[y] = lax.dot_general(
            rows, og[:, :, mine].reshape(tok, fe), (((1,), (1,)), ((), ())), preferred_element_type=F32
        ).astype(BF16)
        for d in y_order:
            send(a_top.at[y], a_top.at[y], top_s.at[0], top_r.at[0], dev(y_=yat(d)))
        await_bytes(pre_t.at[pl.ds(0, nsec - 1)], st_r.at[3])
        send(pre_t.at[top], pre_t.at[nsec], st_s.at[4], st_r.at[4], dev(y_=partner))

    def top_second():
        await_bytes(pre_t.at[0], st_r.at[4])
        own, theirs_ = pre_t[top].astype(F32), pre_t[nsec].astype(F32)
        v = jnp.concatenate([jnp.where(ylo == 0, own, theirs_), jnp.where(ylo == 0, theirs_, own)], axis=0)
        cdf, dens = gelu_parts(v)
        await_bytes(a_top.at[pl.ds(0, 3)], top_r.at[0])
        back = a_top[0].astype(F32)
        for k in range(1, 4):
            back = back + a_top[k].astype(F32)
        g = (back * (cdf + v * dens)).astype(BF16)
        g_top[...] = jnp.where(ylo == 0, g[:fb], g[fb:])
        rows = jnp.swapaxes(g.astype(F32), 0, 1).astype(BF16)
        part = jnp.dot(rows, wbuf[0, :, z].reshape(2 * fb, fe), preferred_element_type=F32).astype(BF16)
        for j in range(nsec):
            b_top[j] = part[:, j * LANES:(j + 1) * LANES].reshape(nz, 8, LANES)
        for dx, dc in sec_order:
            to = peer(dx, dc)
            send(b_top.at[to], r_top.at[sec], top_s.at[1], top_r.at[1], dev(sec_=to))
        r_top[sec] = b_top[sec]

    def top_third():
        await_bytes(r_top.at[pl.ds(0, nsec - 1)], top_r.at[1])
        total = r_top[0].astype(F32)
        for k in range(1, nsec):
            total = total + r_top[k].astype(F32)
        q_top[...] = total.astype(BF16)
        for d in sorted(range(1, nz), key=lambda d: -min(d, nz - d)):
            send(q_top.at[zat(d)], z_top.at[z], top_s.at[2], top_r.at[2], dev(z_=zat(d)))
        z_top[z] = q_top[z]

    def top_fourth():
        await_bytes(z_top.at[pl.ds(0, nz - 1)], top_r.at[2])
        total = og[z, :, pl.ds(pl.multiple_of(ylo * fe + sec * LANES, LANES), LANES)].astype(F32)
        for k in range(nz):
            total = total + z_top[k].astype(F32)
        src = xs.at[top - 1, sec]
        src[...] = total.astype(BF16)
        for dx, dc in sec_order:
            send(src, src, top_s.at[3], top_r.at[3], dev(sec_=peer(dx, dc)))

    def first_term():
        for s in range(nsec):
            v = pre_t[s].astype(F32)
            hall[s] = (v * gelu_parts(v)[0]).astype(BF16)
        go_out[...] = jnp.dot(hall[top], og[...].reshape(tok, width), preferred_element_type=F32)

    plan = [
        (1, top_first), (2, top_second), (3, stage_b), (3, li_first), (4, top_third), (5, stage_c), (5, first_term),
        (6, stage_d), (6, li_second), (7, top_fourth),
    ]
    for k in range(1, half + 1):
        with scope(f"hop{k}"):
            hop(k)
        with scope(f"stage{k}"):
            for at, f in plan:
                if min(at, half) == k:
                    f()
    with scope("gather_end"):
        for l in range(2):
            for way in range(2):
                await_bytes(wbuf.at[way, l, 0], wz_r.at[way, half - 1, way, l])
    with scope("top_end"):
        await_bytes(xs.at[0, pl.ds(0, nsec - 1)], top_r.at[3])
    li_third()

    def await_z(t):
        await_bytes(up.at[pl.ds(0, 2 * nz - 1)], uz_r.at[t])

    block = 2 * nz

    def spread_x(t):
        await_z(t)
        src = up.at[pl.ds(slot(t, core, x), block)]
        for dx in x_order:
            send(src, src, ux_s.at[0], ux_r.at[t], dev(sec_=peer(dx, 0)))

    def spread_core(t):
        await_bytes(up.at[pl.ds(0, (nx - 1) * block)], ux_r.at[t])
        src = up.at[pl.ds(slot(t, core, 0), nx * block)]
        send(src, src, ud_s.at[0], ud_r.at[t], dev(sec_=peer(0, 1)))

    def write_out(t):
        for l in range(2):
            for k in range(nsec):
                ig_out[:, :, l * fe + k * LANES:l * fe + (k + 1) * LANES] = up[pl.ds(slot(t, k % 2, k // 2, l), nz)]

    def out_term(t):
        await_bytes(up.at[pl.ds(0, nx * block)], ud_r.at[t])
        rows = hall[t - 1]
        for l in range(2):
            rhs = jnp.concatenate(
                [up[pl.ds(slot(t, k % 2, k // 2, l), nz)].reshape(tok, LANES) for k in range(nsec)], axis=1
            )
            go_out[:, l * fe:(l + 1) * fe] += jnp.dot(rows, rhs, preferred_element_type=F32)

        @pl.when(sec == t)
        def _():
            write_out(t)

    def spread_g(t):
        def to(d, c):
            send(gbuf.at[t, ylo * tiles + zat(d) // per_tile], gz.at[t * nz + z], g_s.at[0], g_r.at[t], dev(z_=zat(d)))
            return c

        lax.fori_loop(1, nz, to, 0)
        gz[t * nz + z] = gbuf[t, ylo * tiles + z // per_tile]

    def in_term(t):
        await_bytes(gz.at[pl.ds(0, nz - 1)], g_r.at[t])
        gt[...] = jnp.swapaxes(gz[pl.ds(t * nz, nz)].astype(F32).reshape(tok, LANES), 0, 1)
        rows = gt[pl.ds(pl.multiple_of(lax.rem(z, per_tile) * fb, fb), fb), :].astype(BF16)
        gi_out[...] += jnp.dot(rows, li[lax.rem(t, 2), t // 2], preferred_element_type=F32)

    def application(s, final):
        with scope("a_mm"):
            upper = xs[s]
            lhs = jnp.concatenate([upper[j] for j in range(nsec)], axis=1)
            w_out = wbuf[1].reshape(2 * nz * fb, fe)
            part = lax.dot_general(lhs, w_out, (((1,), (1,)), ((), ())), preferred_element_type=F32).astype(BF16)
            a_buf[s, y] = part
        for d in y_order:
            send(a_buf.at[s, y], a_buf.at[s, y], ph_s.at[0, s], ph_r.at[0, s], dev(y_=yat(d)))

        with scope("bg_a"):
            spread_z(s + 1)

            @pl.when(s <= top - 2)
            def _():
                spread_x(s + 2)

            @pl.when(s == top - 2)
            def _():
                await_bytes(li.at[0], li_r.at[4])
                gi_out[...] = jnp.dot(g_top[...], li[top % 2, top // 2], preferred_element_type=F32)

            @pl.when(s <= top - 3)
            def _():
                in_term(s + 2)
                out_term(s + 3)

        with scope("wait_a"):
            await_bytes(a_buf.at[s, pl.ds(0, 3)], ph_r.at[0, s])
        with scope("b_mm"):
            back = a_buf[s, 0].astype(F32)
            for k in range(1, 4):
                back = back + a_buf[s, k].astype(F32)
            g = []
            for t in range(2 * tiles):
                g_tile = (back[:, t * LANES:(t + 1) * LANES] * slope[s, t]).astype(BF16)
                gbuf[s, t] = g_tile
                g.append(g_tile)
            g = jnp.concatenate(g, axis=1)
            w_in = wbuf[0].reshape(2 * nz * fb, fe)
            part = jnp.dot(g, w_in, preferred_element_type=F32).astype(BF16)
            for j in range(nsec):
                b_buf[s, sec, j] = part[:, j * LANES:(j + 1) * LANES]
        if final:
            for dx, dc in sec_order:
                to = peer(dx, dc)
                send(b_buf.at[s, sec, to], b_buf.at[s, sec, to], ph_s.at[1, s], ph_r.at[1, s], dev(sec_=to))
        else:
            for dx, dc in sec_order:
                send(b_buf.at[s, sec], b_buf.at[s, sec], ph_s.at[1, s], ph_r.at[1, s], dev(sec_=peer(dx, dc)))

        with scope("bg_b"):
            spread_g(s)

            @pl.when(s <= top - 2)
            def _():
                spread_core(s + 2)

        with scope("wait_b"):
            if final:
                await_bytes(b_buf.at[0, 0, pl.ds(0, nsec - 1)], ph_r.at[1, s])
            else:
                await_bytes(b_buf.at[0, pl.ds(0, nsec - 1)], ph_r.at[1, s])
        with scope("sum_b"):
            for j in [sec] if final else range(nsec):
                total = xs[s, j].astype(F32)
                for k in range(nsec):
                    total = total + b_buf[s, k, j].astype(F32)
                xs[nsec if final else s - 1, j] = total.astype(BF16)

    def step(i, carry):
        application(top - 1 - i, False)
        return carry

    lax.fori_loop(0, top - 1, step, 0)
    application(0, True)

    with scope("t_z0"):
        spread_z(0)
    with scope("t_x1"):
        spread_x(1)
    with scope("t_terms"):
        in_term(1)
        out_term(2)
    with scope("t_in0"):
        in_term(0)
    with scope("t_core1"):
        spread_core(1)
    with scope("t_z0w"):
        await_z(0)

    def columns(l):
        return pl.ds(pl.multiple_of(l * fe + sec * LANES, LANES), LANES)

    @pl.when(sec != 0)
    def _():
        for l in range(2):
            send(
                up.at[pl.ds(slot(0, core, x, l), nz)],
                ig_out.at[:, :, columns(l)],
                ux_s.at[1],
                ux_r.at[0],
                dev(sec_=0),
            )

    @pl.when(sec == 0)
    def _():
        for l in range(2):
            ig_out[:, :, l * fe:l * fe + LANES] = up[pl.ds(slot(0, 0, 0, l), nz)]

    with scope("t_out1"):
        out_term(1)
    with scope("t_x0w"):
        @pl.when(sec == 0)
        def _():
            await_bytes(up.at[pl.ds(0, (nsec - 1) * block)], ux_r.at[0])

    with scope("drain"):
        await_bytes(pa_all.at[pl.ds(0, nz - 1)], st_s.at[0])
        await_bytes(pc.at[0, pl.ds(0, nsec - 1)], st_s.at[1])
        await_bytes(pc.at[0], st_s.at[2])
        await_bytes(pre_t.at[pl.ds(0, nsec - 1)], st_s.at[3])
        await_bytes(pre_t.at[0], st_s.at[4])
        await_bytes(a_top.at[pl.ds(0, 3)], top_s.at[0])
        await_bytes(r_top.at[pl.ds(0, nsec - 1)], top_s.at[1])
        await_bytes(z_top.at[pl.ds(0, nz - 1)], top_s.at[2])
        await_bytes(xs.at[0, pl.ds(0, nsec - 1)], top_s.at[3])
        for cp in swaps:
            cp.wait_send()
        for way in range(2):
            await_bytes(wbuf.at[0, :, pl.ds(0, nz - 1)], wz_s.at[way])
        await_bytes(li.at[0, 0], li_s.at[0])
        if ring:
            await_bytes(li.at[0, 0], li_s.at[1])
            await_bytes(li.at[0, 0, lo], li_s.at[2])
            await_bytes(li.at[0, 0, hi], li_s.at[3])
        await_bytes(li.at[0], li_s.at[4])

        def sent(s, c):
            await_bytes(a_buf.at[0, pl.ds(0, 3)], ph_s.at[0, s])
            await_bytes(b_buf.at[0, pl.ds(0, nsec - 1)], ph_s.at[1, s])
            return c

        lax.fori_loop(1, top, sent, 0)
        await_bytes(a_buf.at[0, pl.ds(0, 3)], ph_s.at[0, 0])
        await_bytes(b_buf.at[0, 0, pl.ds(0, nsec - 1)], ph_s.at[1, 0])
        await_bytes(gz.at[pl.ds(0, top * (nz - 1))], g_s.at[0])
        await_bytes(up.at[pl.ds(0, nsec * (2 * nz - 1))], uz_s.at[0])
        await_bytes(up.at[pl.ds(0, (nsec - 1) * (nx - 1) * block)], ux_s.at[0])
        await_bytes(up.at[pl.ds(0, (nsec - 1) * nx * block)], ud_s.at[0])

        @pl.when(sec != 0)
        def _():
            await_bytes(up.at[pl.ds(0, block)], ux_s.at[1])


def finish(ig, gi, go, ig_out, gi_out, go_out, sems):
    copies = [pltpu.make_async_copy(src, dst, sems.at[k]) for k, (src, dst) in enumerate(((ig, ig_out), (gi, gi_out), (go, go_out)))]
    for cp in copies:
        cp.start()
    for cp in copies:
        cp.wait()


def body(layer_inputs, pre_act, out_grad, w_in, w_out):
    nz, nx = lax.axis_size("z"), lax.axis_size("x")
    nsec = 2 * nx
    tok, width = out_grad.shape
    fb = w_in.shape[2]
    hid = pre_act.shape[2]
    fe = width // 2
    tiles = nz * fb // LANES
    half = nz // 2
    dma = pltpu.SemaphoreType.DMA
    vmem = pltpu.VMEM
    scratch = [
        vmem((2, 2, nz, fb, fe), BF16),
        vmem((nz, 8, hid), BF16),
        vmem((nz, 8, hid), BF16),
        vmem((nsec, tiles, 8, LANES), BF16),
        vmem((2, nsec, tiles, 8, LANES), BF16),
        vmem((nsec, 2 * tiles, 8, LANES), F32),
        vmem((nsec, fb, tok), BF16),
        vmem((nsec + 1, fb, tok), BF16),
        vmem((nsec, fb, tok), BF16),
        vmem((2, nx, tok, width), BF16),
        vmem((nz, 8, width), BF16),
        vmem((4, 2 * fb, tok), BF16),
        vmem((nsec, nz, 8, LANES), BF16),
        vmem((nsec, nz, 8, LANES), BF16),
        vmem((nz, 8, LANES), BF16),
        vmem((nz, 8, LANES), BF16),
        vmem((fb, tok), BF16),
        vmem((nsec + 1, nsec, 8, LANES), BF16),
        vmem((nsec, 4, 8, 2 * nz * fb), BF16),
        vmem((nsec, nsec, nsec, 8, LANES), BF16),
        vmem((nsec, 2 * tiles, 8, LANES), BF16),
        vmem((nsec * nz, 8, LANES), BF16),
        vmem((LANES, tok), F32),
        vmem((nsec * nsec * 2 * nz, 8, LANES), BF16),
        dma((5,)),
        dma((2,)), dma((2,)),
        dma((2,)), dma((2, half, 2, 2)),
        dma((5,)), dma((5,)),
        dma((4,)), dma((4,)),
        dma((2, nsec)), dma((2, nsec)),
        dma((5,)), dma((5,)),
        dma((1,)), dma((nsec,)),
        dma((1,)), dma((nsec,)),
        dma((2,)), dma((nsec,)),
        dma((1,)), dma((nsec,)),
    ]
    hbm, on_chip = pl.BlockSpec(memory_space=pltpu.HBM), pl.BlockSpec(memory_space=pltpu.VMEM)
    shapes = (
        jax.ShapeDtypeStruct((nz, 8, width), BF16),
        jax.ShapeDtypeStruct((fb, width), F32),
        jax.ShapeDtypeStruct((fb, width), F32),
    )
    operands = (
        layer_inputs.reshape(tok, width),
        pre_act.reshape(nz, 8, hid),
        out_grad.reshape(nz, 8, width),
        w_in.reshape(fb, width),
        w_out.reshape(fb, width),
    )
    results = pl.pallas_call(
        kernel,
        out_shape=shapes,
        in_specs=[hbm] * 5,
        out_specs=(on_chip,) * 3,
        scratch_shapes=scratch,
        name="chain",
        compiler_params=pltpu.CompilerParams(
            collective_id=0, has_side_effects=True, vmem_limit_bytes=32 * 1024 * 1024
        ),
    )(*(pltpu.with_memory_space_constraint(v, pltpu.HBM) for v in operands))
    ig, gi, go = pl.pallas_call(
        finish,
        out_shape=shapes,
        in_specs=[on_chip] * 3,
        out_specs=(hbm,) * 3,
        scratch_shapes=[dma((3,))],
        name="finish",
    )(*(pltpu.with_memory_space_constraint(v, pltpu.VMEM) for v in results))
    return (
        ig.reshape(1, tok, width),
        gi.reshape(1, 1, fb, width),
        go.reshape(1, 1, fb, width),
    )


def solution(mesh):
    shape = mesh.shape
    split = Mesh(
        mesh.devices.reshape(shape["section"] // 2, 2, shape["dp"] // 2, 2, shape["mp"]), AXES
    )
    sec, dp = ("x", "core"), ("z", "ylo")
    placed = (
        P(sec, None, "yhi"),
        P(sec, None, dp),
        P(None, "yhi"),
        P(dp, sec, None, "yhi"),
        P(dp, sec, None, "yhi"),
    )
    return jax.shard_map(
        body,
        mesh=split,
        in_specs=placed,
        out_specs=(P(sec, None, "yhi"), P(dp, sec, None, "yhi"), P(dp, sec, None, "yhi")),
        check_vma=False,
    )
```

```python
import contextlib

import jax
import jax.numpy as jnp
from jax import lax
from jax.experimental import pallas as pl
from jax.experimental.pallas import tpu as pltpu
from jax.sharding import Mesh
from jax.sharding import PartitionSpec as P

AXES = ("x", "core", "z", "ylo", "yhi")
MESH_ID = pl.DeviceIdType.MESH
BF16, F32 = jnp.bfloat16, jnp.float32
LANES = 128
PROFILE = False


def scope(name):
    return jax.named_scope(name) if PROFILE else contextlib.nullcontext()


def gelu_parts(v):
    cdf = 0.5 * (1.0 + lax.erf(v * 0.7071067811865476))
    dens = jnp.exp(-0.5 * v * v) * 0.3989422804014327
    return cdf, dens


def kernel(
    li_hbm, pa_hbm, og_hbm, wi_hbm, wo_hbm,
    ig_out, gi_out, go_out,
    wbuf, pa, pa_all, pb, pc, slope, pa_t, pre_t, pre_top, hall, li, og,
    a_top, b_top, r_top, q_top, z_top, g_top, g_pass,
    w_t, xs, a_buf, b_buf, a_acc, b_acc, gbuf, gz, gt, up, x_end,
    lsem, wx_s, wx_r, wd_s, wd_r, wz_s, wz_r, st_s, st_r, pt_s, pt_r, top_s, top_r, ph_s, ph_r, li_s, li_r,
    g_s, g_r, uz_s, uz_r, ux_s, ux_r, ud_s, ud_r, go,
):
    nx, nz = lax.axis_size("x"), lax.axis_size("z")
    nsec = 2 * nx
    top = nsec - 1
    fb, width = wi_hbm.shape
    fe = width // 2
    tok = nz * 8
    tiles = nz * fb // LANES
    per_tile = LANES // fb
    x, core, z = lax.axis_index("x"), lax.axis_index("core"), lax.axis_index("z")
    ylo, yhi = lax.axis_index("ylo"), lax.axis_index("yhi")
    sec = x * 2 + core
    y = yhi * 2 + ylo
    other = 1 - ylo
    partner = yhi * 2 + other

    def dev(x_=None, core_=None, z_=None, y_=None):
        y_ = y if y_ is None else y_
        return (
            x if x_ is None else x_,
            core if core_ is None else core_,
            z if z_ is None else z_,
            lax.rem(y_, 2),
            y_ // 2,
        )

    def send(src, dst, ssem, rsem, to):
        cp = pltpu.make_async_remote_copy(
            src_ref=src, dst_ref=dst, send_sem=ssem, recv_sem=rsem, device_id=to, device_id_type=MESH_ID
        )
        cp.start()
        return cp

    def await_bytes(ref, sem):
        pltpu.make_async_copy(ref, ref, sem).wait()

    def zat(d):
        return lax.rem(z + d + nz, nz)

    def xat(d):
        return lax.rem(x + d + nx, nx)

    def yat(d):
        return lax.rem(y + d, 4)

    y_order = (2, 1, 3)
    x_order = sorted(range(1, nx), key=lambda d: -min(d, nx - d))
    z_order = sorted(range(1, nz), key=lambda d: -min(d, nz - d))
    sections = [(d, False) for d in x_order] + [(d, True) for d in x_order] + [(0, True)]

    def peer(d, cross):
        return xat(d), (1 - core if cross else core)

    mine = pl.ds(pl.multiple_of(ylo * fe, LANES), fe)
    theirs = pl.ds(pl.multiple_of(other * fe, LANES), fe)

    w_hbm = (wi_hbm, wo_hbm)
    pa_in = pltpu.make_async_copy(pa_hbm, pa, lsem.at[0])
    w_in_ = [pltpu.make_async_copy(w_hbm[m].at[:, mine], wbuf.at[m, ylo, 1, z], lsem.at[1 + m]) for m in range(2)]
    og_in = pltpu.make_async_copy(og_hbm, og, lsem.at[3])
    li_in = pltpu.make_async_copy(li_hbm, li.at[core, x], lsem.at[4])
    pa_in.start()

    @pl.when(core == 1)
    def _():
        for cp in w_in_:
            cp.start()

    og_in.start()
    li_in.start()

    barrier = pltpu.get_barrier_semaphore()
    greeted = [dev(z_=zat(d)) for d in range(1, nz)] + [dev(*peer(*p)) for p in sections]
    greeted += [dev(y_=yat(d)) for d in range(1, 4)] + [dev(core_=1 - core, y_=partner)]
    for to in greeted:
        pl.semaphore_signal(barrier, inc=1, device_id=to, device_id_type=MESH_ID)
    pa_in.wait()
    v = pa[...].astype(F32).reshape(tok, nsec * fb)
    pa_t[...] = jnp.swapaxes(v, 0, 1).astype(BF16).reshape(nsec, fb, tok)
    with scope("barrier"):
        pl.semaphore_wait(barrier, len(greeted))

    for d in z_order:
        send(pa.at[zat(d)], pa_all.at[z], st_s.at[0], st_r.at[0], dev(z_=zat(d)))
    pa_all[z] = pa[z]

    swaps = [
        send(w_hbm[m].at[:, theirs], wbuf.at[m, ylo, core, z], wx_s.at[m], wx_r.at[core, m], dev(core_=1, y_=partner))
        for m in range(2)
    ]

    @pl.when(core == 0)
    def _():
        for m in range(2):
            send(w_hbm[m].at[:, mine], wbuf.at[m, ylo, 0, z], wd_s.at[m], wd_r.at[m], dev(core_=1))

    for p in sections:
        to = peer(*p)
        send(pa_t.at[to[0] * 2 + to[1]], pre_t.at[sec], st_s.at[3], st_r.at[3], dev(*to))
    pre_t[sec] = pa_t[sec]

    def spread_pre():
        await_bytes(pre_t.at[pl.ds(0, nsec - 1)], st_r.at[3])
        dst = pre_top.at[ylo, core]
        send(pre_t.at[top], dst, pt_s.at[0], pt_r.at[0], dev(core_=1, y_=partner))

        @pl.when(core == 0)
        def _():
            send(pre_t.at[top], dst, pt_s.at[1], pt_r.at[0], dev(core_=1))

        @pl.when(core == 1)
        def _():
            dst[...] = pre_t[top]

    def stage_b():
        await_bytes(pa_all.at[pl.ds(0, nz - 1)], st_r.at[0])
        group = lax.broadcasted_iota(jnp.int32, (8, LANES), 1) // fb
        for ct in range(nsec // per_tile):
            for t in range(tiles):
                out = [jnp.zeros((8, LANES), F32)] * per_tile
                for j in range(per_tile):
                    v = pa_all[t * per_tile + j, :, ct * LANES:(ct + 1) * LANES].astype(F32)
                    for k in range(per_tile):
                        shift = (j - k) * fb % LANES
                        r = pltpu.roll(v, shift, 1) if shift else v
                        out[k] = jnp.where(group == j, r, out[k])
                for k in range(per_tile):
                    c = ct * per_tile + k
                    pb[c // 2, c % 2, t] = out[k].astype(BF16)
        dst = pc.at[ylo, sec]
        for d in x_order:
            send(pb.at[xat(d)], dst, st_s.at[1], st_r.at[1], dev(x_=xat(d), core_=1))

        @pl.when(core == 0)
        def _():
            send(pb.at[x], dst, st_s.at[5], st_r.at[1], dev(core_=1))

        @pl.when(core == 1)
        def _():
            dst[...] = pb[x]

    cut = tok // 2
    lo, hi = pl.ds(0, cut), pl.ds(cut, cut)
    ring = nx > 2

    def li_first():
        li_in.wait()
        src = li.at[core, x]
        send(src, src, li_s.at[0], li_r.at[0], dev(x_=xat(1)))
        if ring:
            send(src, src, li_s.at[1], li_r.at[1], dev(x_=xat(-1)))

    def li_second():
        await_bytes(li.at[0, 0], li_r.at[0])
        if ring:
            src = li.at[core, xat(-1), lo]
            send(src, src, li_s.at[2], li_r.at[2], dev(x_=xat(1)))
            await_bytes(li.at[0, 0], li_r.at[1])
            src = li.at[core, xat(1), hi]
            send(src, src, li_s.at[3], li_r.at[3], dev(x_=xat(-1)))

    def li_third():
        if ring:
            await_bytes(li.at[0, 0, lo], li_r.at[2])
            await_bytes(li.at[0, 0, hi], li_r.at[3])
        send(li.at[core], li.at[core], li_s.at[4], li_r.at[4], dev(core_=1 - core))

    def first_out_term():
        for s in range(nsec):
            v = pre_t[s].astype(F32)
            hall[s] = (v * gelu_parts(v)[0]).astype(BF16)
        go_out[...] = jnp.dot(hall[top], og[...].reshape(tok, width), preferred_element_type=F32)

    def first_in_term():
        await_bytes(li.at[0], li_r.at[4])
        gi_out[...] = jnp.dot(g_top[...], li[top % 2, top // 2], preferred_element_type=F32)

    block = 4 * nz

    def slot(t, x_, ylo_=0, z_=0):
        return ((((t * nx + x_) * 2 + ylo_) * nz) + z_) * 2

    def columns(t, x_, l):
        return up[pl.ds(slot(t, x_, l), 2 * nz)].reshape(nz, 2, 8, LANES)

    def out_term(t):
        rows = hall[t - 1]
        for l in range(2):
            parts = []
            for k in range(nx):
                v = columns(t, k, l)
                parts += [v[:, c].reshape(tok, LANES) for c in range(2)]
            go_out[:, l * fe:(l + 1) * fe] += jnp.dot(rows, jnp.concatenate(parts, axis=1), preferred_element_type=F32)

        @pl.when(sec == t)
        def _():
            for l in range(2):
                for k in range(nx):
                    v = columns(t, k, l)
                    for c in range(2):
                        at = l * fe + (2 * k + c) * LANES
                        ig_out[:, :, at:at + LANES] = v[:, c]

    def in_term(t):
        @pl.when(core == 1)
        def _():
            await_bytes(gz.at[pl.ds(0, nz - 1)], g_r.at[t])

        @pl.when(core == 0)
        def _():
            await_bytes(gz.at[pl.ds(0, nz)], g_r.at[t])

        gt[...] = jnp.swapaxes(gz[pl.ds(t * nz, nz)].astype(F32).reshape(tok, LANES), 0, 1)
        rows = gt[pl.ds(pl.multiple_of(lax.rem(z, per_tile) * fb, fb), fb), :].astype(BF16)
        gi_out[...] += jnp.dot(rows, li[lax.rem(t, 2), t // 2], preferred_element_type=F32)

    half = nz // 2
    hu, hn, hj = 2 * nz * fb, fe // 2, nsec // 2

    def hop(k):
        last = k == half
        for which in range(2):
            l = ylo if which == 0 else other
            for m in range(2):
                if k == 1:
                    if which == 0:
                        w_in_[m].wait()
                        await_bytes(wbuf.at[m, 0, 0, 0], wd_r.at[m])
                    else:
                        for c in range(2):
                            await_bytes(wbuf.at[m, 0, 0, 0], wx_r.at[c, m])
                for way, step in ((0, 1), (1, -1)):
                    if k > 1:
                        await_bytes(wbuf.at[m, 0, :, 0], wz_r.at[way, k - 2, m, l])
                    if last and way != m:
                        continue
                    src = wbuf.at[m, l, :, zat(-step * (k - 1))]
                    send(src, src, wz_s.at[way], wz_r.at[way, k - 1, m, l], dev(z_=zat(step)))

    def stage_c():
        await_bytes(pc.at[0, pl.ds(0, nsec - 1)], st_r.at[1])
        send(pc.at[ylo], pc.at[ylo], st_s.at[2], st_r.at[2], dev(y_=partner))

    def stage_d():
        await_bytes(pc.at[0], st_r.at[2])

        def one(s, carry):
            for l in range(2):
                v = pc[l, s].astype(F32)
                cdf, dens = gelu_parts(v)
                slope[s, l] = (cdf + v * dens).reshape(2 * tiles, 8, LANES)
            return carry

        lax.fori_loop(0, top, one, 0)

    def top_first():
        og_in.wait()
        rows = wbuf[1, :, :, z].reshape(4 * fb, fe)
        a_top[y] = lax.dot_general(
            rows, og[:, :, mine].reshape(tok, fe), (((1,), (1,)), ((), ())), preferred_element_type=F32
        ).astype(BF16)
        for d in y_order:
            send(a_top.at[y], a_top.at[y], top_s.at[0], top_r.at[0], dev(y_=yat(d)))
        spread_pre()

    def top_second():
        await_bytes(pre_t.at[pl.ds(0, 3)], pt_r.at[0])
        v = pre_top[...].astype(F32).reshape(4 * fb, tok)
        cdf, dens = gelu_parts(v)
        await_bytes(a_top.at[pl.ds(0, 3)], top_r.at[0])
        back = a_top[0].astype(F32)
        for k in range(1, 4):
            back = back + a_top[k].astype(F32)
        g = (back * (cdf + v * dens)).astype(BF16)
        g_pass[...] = jnp.where(ylo == 0, g[:fb], g[2 * fb:3 * fb])
        send(g_pass, g_top, top_s.at[4], top_r.at[4], dev(core_=0))
        g_top[...] = jnp.where(ylo == 0, g[fb:2 * fb], g[3 * fb:])
        rows = jnp.swapaxes(g.astype(F32), 0, 1).astype(BF16)
        part = jnp.dot(rows, wbuf[0, :, :, z].reshape(4 * fb, fe), preferred_element_type=F32).astype(BF16)
        for j in range(nsec):
            b_top[j // 2, :, j % 2] = part[:, j * LANES:(j + 1) * LANES].reshape(nz, 8, LANES)
        for d in x_order:
            send(b_top.at[xat(d)], r_top.at[x], top_s.at[1], top_r.at[1], dev(x_=xat(d)))
        r_top[x] = b_top[x]

    def top_third():
        await_bytes(r_top.at[pl.ds(0, nx - 1)], top_r.at[1])
        total = r_top[0].astype(F32)
        for k in range(1, nx):
            total = total + r_top[k].astype(F32)
        q_top[...] = total.astype(BF16)
        for d in z_order:
            send(q_top.at[zat(d)], z_top.at[z], top_s.at[2], top_r.at[2], dev(z_=zat(d)))
        z_top[z] = q_top[z]

    own = pl.ds(2 * x, 2)

    def top_fourth():
        await_bytes(z_top.at[pl.ds(0, nz - 1)], top_r.at[2])
        for c in range(2):
            at = pl.multiple_of(ylo * fe + (2 * x + c) * LANES, LANES)
            total = og[z, :, pl.ds(at, LANES)].astype(F32)
            for k in range(nz):
                total = total + z_top[k, c].astype(F32)
            xs[top - 1, 2 * x + c] = total.astype(BF16)
        src = xs.at[top - 1, own]
        for d in x_order:
            send(src, src, top_s.at[3], top_r.at[3], dev(x_=xat(d)))

    def spread_z(t):
        src = xs.at[nsec if isinstance(t, int) and t == 0 else t - 1, own]
        dst = up.at[pl.ds(slot(t, x, ylo, z), 2)]

        def both(d):
            for to in (partner, y):
                send(src, dst, uz_s.at[0], uz_r.at[t], dev(core_=0, z_=zat(d), y_=to))

        both(half)

        def pair(i, c):
            both(half - i)
            both(half + i)
            return c

        lax.fori_loop(1, half, pair, 0)
        both(0)

    def spread_g(t):
        def to(d, c):
            tile = zat(d) // per_tile
            for c_ in range(2):
                send(gbuf.at[t, ylo, c_ * tiles + tile], gz.at[t * nz + z], g_s.at[0], g_r.at[t], dev(core_=c_, z_=zat(d)))
            return c

        lax.fori_loop(1, nz, to, 0)
        tile = z // per_tile
        send(gbuf.at[t, ylo, tile], gz.at[t * nz + z], g_s.at[0], g_r.at[t], dev(core_=0))
        gz[t * nz + z] = gbuf[t, ylo, tiles + tile]

    def turn(away):
        t = lax.rem(z // per_tile + away + tiles, tiles)

        def one(i, c):
            l, c_ = i // 2, lax.rem(i, 2)
            v = wbuf[1, l, c_, pl.ds(t * per_tile, per_tile)].reshape(LANES, fe)
            w_t[l, c_ * tiles + t] = jnp.swapaxes(v, 0, 1)
            return c

        lax.fori_loop(0, 4, one, 0)

    def a_half(s, l, part):
        a_buf[s, l, y] = part.astype(BF16)
        for d in y_order:
            send(a_buf.at[s, l, y], a_buf.at[s, l, y], ph_s.at[0, l, s], ph_r.at[0, l, s], dev(y_=yat(d)))

    def a_part(s, l, n):
        lhs = jnp.concatenate([xs[s, n * hj + j] for j in range(hj)], axis=1)
        w_out = jnp.concatenate([w_t[l, t, n * hn:(n + 1) * hn] for t in range(2 * tiles)], axis=1)
        return jnp.dot(lhs, w_out, preferred_element_type=F32)

    def a_first(s, l):
        lhs = jnp.concatenate([xs[s, j] for j in range(nsec)], axis=1)
        return lax.dot_general(lhs, wbuf[1, l].reshape(hu, fe), (((1,), (1,)), ((), ())), preferred_element_type=F32)

    def release(t):
        pl.semaphore_signal(go.at[t], inc=1, device_id=dev(core_=0), device_id_type=MESH_ID)

    def await_up(t):
        await_bytes(up.at[pl.ds(0, nx * block)], ud_r.at[t])

    def application(s, final):
        with scope("bg_a"):
            @pl.when(s <= top - 2)
            def _():
                release(s + 2)

            spread_z(s + 1)

            @pl.when(s == top - 2)
            def _():
                first_in_term()

            @pl.when(s == top - 1)
            def _():
                turn(tiles // 2)

            @pl.when(s <= top - 3)
            def _():
                in_term(s + 2)
                await_up(s + 3)
                out_term(s + 3)

        for l in range(2):
            with scope(f"wait_a{l}"):
                await_bytes(a_buf.at[s, l, pl.ds(0, 3)], ph_r.at[0, l, s])
            with scope(f"b_mm{l}"):
                back = a_buf[s, l, 0].astype(F32)
                for k in range(1, 4):
                    back = back + a_buf[s, l, k].astype(F32)
                g = []
                for t in range(2 * tiles):
                    g_tile = (back[:, t * LANES:(t + 1) * LANES] * slope[s, l, t]).astype(BF16)
                    gbuf[s, l, t] = g_tile
                    g.append(g_tile)
                g = jnp.concatenate(g, axis=1)
                if l == 0:
                    for n in range(2):
                        w_in = wbuf[0, l, :, :, :, n * hn:(n + 1) * hn].reshape(hu, hn)
                        b_acc[n] = jnp.dot(g, w_in, preferred_element_type=F32)
        for n in range(2):
            w_in = wbuf[0, 1, :, :, :, n * hn:(n + 1) * hn].reshape(hu, hn)
            part = (b_acc[n] + jnp.dot(g, w_in, preferred_element_type=F32)).astype(BF16)
            for j in range(hj):
                b_buf[s, n, x, j] = part[:, j * LANES:(j + 1) * LANES]
            if not final:
                src = b_buf.at[s, n, x]
                for d in x_order:
                    send(src, src, ph_s.at[1, n, s], ph_r.at[1, n, s], dev(x_=xat(d)))
        hx = nx // 2
        if final:
            for d in x_order:
                to = xat(d)
                src = b_buf.at[s, to // hx, x, pl.ds(2 * lax.rem(to, hx), 2)]
                send(src, src, ph_s.at[1, 0, s], ph_r.at[1, 0, s], dev(x_=to))

        with scope("bg_b"):
            spread_g(s)

        if final:
            with scope("wait_b"):
                await_bytes(gz.at[pl.ds(0, 2 * (nx - 1))], ph_r.at[1, 0, s])
            for c in range(2):
                total = xs[s, 2 * x + c].astype(F32)
                for k in range(nx):
                    total = total + b_buf[s, x // hx, k, 2 * lax.rem(x, hx) + c].astype(F32)
                xs[nsec, 2 * x + c] = total.astype(BF16)
            return
        for n in range(2):
            with scope(f"wait_b{n}"):
                await_bytes(b_buf.at[s, n, pl.ds(0, nx - 1)], ph_r.at[1, n, s])
            with scope(f"a_mm{n}"):
                for j in range(hj):
                    total = xs[s, n * hj + j].astype(F32)
                    for k in range(nx):
                        total = total + b_buf[s, n, k, j].astype(F32)
                    xs[s - 1, n * hj + j] = total.astype(BF16)
                if n == 0:
                    for l in range(2):
                        a_acc[l] = a_part(s - 1, l, 0)
        for l in range(2):
            with scope(f"a_last{l}"):
                a_half(s - 1, l, a_acc[l] + a_part(s - 1, l, 1))

    @pl.when(core == 1)
    def _():
        plan = [
            (1, top_first), (2, top_second), (3, stage_b), (3, li_first), (4, top_third), (5, stage_c), (5, first_out_term),
            (6, stage_d), (6, li_second), (7, top_fourth),
        ]
        plan += [(half if d else 5, lambda d=d: turn(d)) for d in (0, -1, 1) if d % tiles != tiles // 2]
        for k in range(1, half + 1):
            with scope(f"hop{k}"):
                hop(k)
            with scope(f"stage{k}"):
                for at, f in plan:
                    if min(at, half) == k:
                        f()
        with scope("gather_end"):
            for l in range(2):
                for way in range(2):
                    await_bytes(wbuf.at[way, 0, :, 0], wz_r.at[way, half - 1, way, l])
        with scope("top_end"):
            await_bytes(xs.at[0, pl.ds(0, 2 * (nx - 1))], top_r.at[3])
        for l in range(2):
            a_half(top - 1, l, a_first(top - 1, l))
        li_third()

        def step(i, carry):
            application(top - 1 - i, False)
            return carry

        lax.fori_loop(0, top - 1, step, 0)
        application(0, True)

        with scope("t_z0"):
            spread_z(0)
            release(1)
        with scope("t_terms"):
            in_term(1)
            await_up(2)
            out_term(2)
        with scope("t_in0"):
            in_term(0)
        with scope("t_up1"):
            await_up(1)
        with scope("t_out1"):
            out_term(1)

        with scope("drain"):
            await_bytes(pc.at[0, pl.ds(0, nx - 1)], st_s.at[1])
            await_bytes(pc.at[0], st_s.at[2])
            await_bytes(a_top.at[pl.ds(0, 3)], top_s.at[0])
            await_bytes(r_top.at[pl.ds(0, nx - 1)], top_s.at[1])
            await_bytes(z_top.at[pl.ds(0, nz - 1)], top_s.at[2])
            await_bytes(xs.at[0, pl.ds(0, 2 * (nx - 1))], top_s.at[3])
            await_bytes(g_top, top_s.at[4])
            for way in range(2):
                await_bytes(wbuf.at[0, :, :, pl.ds(0, nz - 1)], wz_s.at[way])

            def sent(s, c):
                for h in range(2):
                    await_bytes(a_buf.at[0, h, pl.ds(0, 3)], ph_s.at[0, h, s])
                    await_bytes(b_buf.at[0, h, pl.ds(0, nx - 1)], ph_s.at[1, h, s])
                return c

            lax.fori_loop(1, top, sent, 0)
            for h in range(2):
                await_bytes(a_buf.at[0, h, pl.ds(0, 3)], ph_s.at[0, h, 0])
            await_bytes(gz.at[pl.ds(0, 2 * (nx - 1))], ph_s.at[1, 0, 0])
            await_bytes(up.at[pl.ds(0, top * (2 * nz - 1))], g_s.at[0])
            await_bytes(up.at[pl.ds(0, nsec * block)], uz_s.at[0])

    def await_z(t):
        await_bytes(up.at[pl.ds(0, block)], uz_r.at[t])

    def spread_x(t):
        await_z(t)
        pl.semaphore_wait(go.at[t], 1)
        src = up.at[pl.ds(slot(t, x), block)]
        for d in x_order:
            send(src, src, ux_s.at[0], ux_r.at[t], dev(x_=xat(d)))

    def spread_core(t):
        await_bytes(up.at[pl.ds(0, (nx - 1) * block)], ux_r.at[t])
        src = up.at[pl.ds(slot(t, 0), nx * block)]
        send(src, src, ud_s.at[0], ud_r.at[t], dev(core_=1))

    @pl.when(core == 0)
    def _():
        spread_pre()
        stage_b()
        li_first()
        og_in.wait()
        first_out_term()
        li_second()
        li_third()
        await_bytes(g_top, top_r.at[4])
        first_in_term()

        def move(i, carry):
            t = top - i
            with scope("s_x"):
                spread_x(t)
            with scope("s_in"):
                @pl.when(t < top)
                def _():
                    in_term(t)

            with scope("s_core"):
                spread_core(t)
            with scope("s_out"):
                out_term(t)
            return carry

        lax.fori_loop(0, top - 1, move, 0)
        with scope("s_x1"):
            spread_x(1)
        with scope("s_in01"):
            in_term(1)
            in_term(0)
        with scope("s_core1"):
            spread_core(1)
        with scope("s_z0"):
            await_z(0)
        for l in range(2):
            v = columns(0, x, l)
            for c in range(2):
                at = pl.multiple_of(l * fe + (2 * x + c) * LANES, LANES)

                @pl.when(x == 0)
                def _():
                    ig_out[:, :, pl.ds(at, LANES)] = v[:, c]

                @pl.when(x != 0)
                def _():
                    x_end[l, c] = v[:, c]
                    send(x_end.at[l, c], ig_out.at[:, :, pl.ds(at, LANES)], ux_s.at[1], ux_r.at[0], dev(x_=0))

        with scope("s_out1"):
            out_term(1)
        with scope("s_x0w"):
            @pl.when(x == 0)
            def _():
                await_bytes(up.at[pl.ds(0, (nx - 1) * block)], ux_r.at[0])

        with scope("s_drain"):
            await_bytes(pc.at[0, pl.ds(0, nx - 1)], st_s.at[1])
            await_bytes(pc.at[0, 0], st_s.at[5])
            for m in range(2):
                await_bytes(wbuf.at[m, 0, 0, 0], wd_s.at[m])
            await_bytes(pre_t.at[0], pt_s.at[1])
            await_bytes(up.at[pl.ds(0, top * (nx - 1) * block)], ux_s.at[0])
            await_bytes(up.at[pl.ds(0, top * nx * block)], ud_s.at[0])

            @pl.when(x != 0)
            def _():
                await_bytes(up.at[pl.ds(0, block)], ux_s.at[1])

    await_bytes(pa_all.at[pl.ds(0, nz - 1)], st_s.at[0])
    await_bytes(pre_t.at[pl.ds(0, nsec - 1)], st_s.at[3])
    await_bytes(pre_t.at[0], pt_s.at[0])
    for cp in swaps:
        cp.wait_send()
    await_bytes(li.at[0, 0], li_s.at[0])
    if ring:
        await_bytes(li.at[0, 0], li_s.at[1])
        await_bytes(li.at[0, 0, lo], li_s.at[2])
        await_bytes(li.at[0, 0, hi], li_s.at[3])
    await_bytes(li.at[0], li_s.at[4])


def finish(ig, gi, go, ig_out, gi_out, go_out, sems):
    copies = [pltpu.make_async_copy(src, dst, sems.at[k]) for k, (src, dst) in enumerate(((ig, ig_out), (gi, gi_out), (go, go_out)))]
    for cp in copies:
        cp.start()
    for cp in copies:
        cp.wait()


def body(layer_inputs, pre_act, out_grad, w_in, w_out):
    nz, nx = lax.axis_size("z"), lax.axis_size("x")
    nsec = 2 * nx
    tok, width = out_grad.shape
    fb = w_in.shape[2]
    hid = pre_act.shape[2]
    fe = width // 2
    tiles = nz * fb // LANES
    half = nz // 2
    dma = pltpu.SemaphoreType.DMA
    vmem = pltpu.VMEM
    scratch = [
        vmem((2, 2, 2, nz, fb, fe), BF16),
        vmem((nz, 8, hid), BF16),
        vmem((nz, 8, hid), BF16),
        vmem((nx, 2, tiles, 8, LANES), BF16),
        vmem((2, nsec, 2, tiles, 8, LANES), BF16),
        vmem((nsec, 2, 2 * tiles, 8, LANES), F32),
        vmem((nsec, fb, tok), BF16),
        vmem((nsec, fb, tok), BF16),
        vmem((2, 2, fb, tok), BF16),
        vmem((nsec, fb, tok), BF16),
        vmem((2, nx, tok, width), BF16),
        vmem((nz, 8, width), BF16),
        vmem((4, 4 * fb, tok), BF16),
        vmem((nx, nz, 2, 8, LANES), BF16),
        vmem((nx, nz, 2, 8, LANES), BF16),
        vmem((nz, 2, 8, LANES), BF16),
        vmem((nz, 2, 8, LANES), BF16),
        vmem((fb, tok), BF16),
        vmem((fb, tok), BF16),
        vmem((2, 2 * tiles, fe, LANES), BF16),
        vmem((nsec + 1, nsec, 8, LANES), BF16),
        vmem((nsec, 2, 4, 8, 2 * nz * fb), BF16),
        vmem((nsec, 2, nx, nx, 8, LANES), BF16),
        vmem((2, 8, 2 * nz * fb), F32),
        vmem((2, 8, fe // 2), F32),
        vmem((nsec, 2, 2 * tiles, 8, LANES), BF16),
        vmem((nsec * nz, 8, LANES), BF16),
        vmem((LANES, tok), F32),
        vmem((nsec * nx * 4 * nz, 8, LANES), BF16),
        vmem((2, 2, nz, 8, LANES), BF16),
        dma((5,)),
        dma((2,)), dma((2, 2)),
        dma((2,)), dma((2,)),
        dma((2,)), dma((2, half, 2, 2)),
        dma((6,)), dma((4,)),
        dma((2,)), dma((1,)),
        dma((5,)), dma((5,)),
        dma((2, 2, nsec)), dma((2, 2, nsec)),
        dma((5,)), dma((5,)),
        dma((1,)), dma((nsec,)),
        dma((1,)), dma((nsec,)),
        dma((2,)), dma((nsec,)),
        dma((1,)), dma((nsec,)),
        pltpu.SemaphoreType.REGULAR((nsec,)),
    ]
    hbm, on_chip = pl.BlockSpec(memory_space=pltpu.HBM), pl.BlockSpec(memory_space=pltpu.VMEM)
    shapes = (
        jax.ShapeDtypeStruct((nz, 8, width), BF16),
        jax.ShapeDtypeStruct((fb, width), F32),
        jax.ShapeDtypeStruct((fb, width), F32),
    )
    operands = (
        layer_inputs.reshape(tok, width),
        pre_act.reshape(nz, 8, hid),
        out_grad.reshape(nz, 8, width),
        w_in.reshape(fb, width),
        w_out.reshape(fb, width),
    )
    results = pl.pallas_call(
        kernel,
        out_shape=shapes,
        in_specs=[hbm] * 5,
        out_specs=(on_chip,) * 3,
        scratch_shapes=scratch,
        name="chain",
        compiler_params=pltpu.CompilerParams(
            collective_id=0, has_side_effects=True, vmem_limit_bytes=40 * 1024 * 1024
        ),
    )(*(pltpu.with_memory_space_constraint(v, pltpu.HBM) for v in operands))
    ig, gi, go = pl.pallas_call(
        finish,
        out_shape=shapes,
        in_specs=[on_chip] * 3,
        out_specs=(hbm,) * 3,
        scratch_shapes=[dma((3,))],
        name="finish",
    )(*(pltpu.with_memory_space_constraint(v, pltpu.VMEM) for v in results))
    return (
        ig.reshape(1, tok, width),
        gi.reshape(1, 1, fb, width),
        go.reshape(1, 1, fb, width),
    )


def solution(mesh):
    shape = mesh.shape
    split = Mesh(
        mesh.devices.reshape(shape["section"] // 2, 2, shape["dp"] // 2, 2, shape["mp"]), AXES
    )
    sec, dp = ("x", "core"), ("z", "ylo")
    placed = (
        P(sec, None, "yhi"),
        P(sec, None, dp),
        P(None, "yhi"),
        P(dp, sec, None, "yhi"),
        P(dp, sec, None, "yhi"),
    )
    return jax.shard_map(
        body,
        mesh=split,
        in_specs=placed,
        out_specs=(P(sec, None, "yhi"), P(dp, sec, None, "yhi"), P(dp, sec, None, "yhi")),
        check_vma=False,
    )
```

```python
import contextlib

import jax
import jax.numpy as jnp
from jax import lax
from jax.experimental import pallas as pl
from jax.experimental.pallas import tpu as pltpu
from jax.sharding import Mesh
from jax.sharding import PartitionSpec as P

AXES = ("x", "core", "z", "ylo", "yhi")
MESH_ID = pl.DeviceIdType.MESH
BF16, F32 = jnp.bfloat16, jnp.float32
LANES = 128
PROFILE = False


def scope(name):
    return jax.named_scope(name) if PROFILE else contextlib.nullcontext()


def gelu_parts(v):
    cdf = 0.5 * (1.0 + lax.erf(v * 0.7071067811865476))
    dens = jnp.exp(-0.5 * v * v) * 0.3989422804014327
    return cdf, dens


def kernel(
    li_hbm, pa_hbm, og_hbm, wi_hbm, wo_hbm,
    ig_out, gi_out, go_out,
    wbuf, pa, pa_all, pb, pc, slope, pa_t, pre_t, pre_top, hall, li, og,
    a_top, b_top, r_top, q_top, z_top, g_top, g_pass,
    w_t, xs, a_buf, b_buf, a_acc, b_acc, gbuf, gz, gt, up, x_end,
    lsem, wx_s, wx_r, wd_s, wd_r, wz_s, wz_r, st_s, st_r, pt_s, pt_r, top_s, top_r, ph_s, ph_r, li_s, li_r,
    g_s, g_r, uz_s, uz_r, ux_s, ux_r, ud_s, ud_r, go, near,
):
    nx, nz = lax.axis_size("x"), lax.axis_size("z")
    nsec = 2 * nx
    top = nsec - 1
    fb, width = wi_hbm.shape
    fe = width // 2
    tok = nz * 8
    tiles = nz * fb // LANES
    per_tile = LANES // fb
    x, core, z = lax.axis_index("x"), lax.axis_index("core"), lax.axis_index("z")
    ylo, yhi = lax.axis_index("ylo"), lax.axis_index("yhi")
    sec = x * 2 + core
    y = yhi * 2 + ylo
    other = 1 - ylo
    partner = yhi * 2 + other

    def dev(x_=None, core_=None, z_=None, y_=None):
        y_ = y if y_ is None else y_
        return (
            x if x_ is None else x_,
            core if core_ is None else core_,
            z if z_ is None else z_,
            lax.rem(y_, 2),
            y_ // 2,
        )

    def send(src, dst, ssem, rsem, to):
        cp = pltpu.make_async_remote_copy(
            src_ref=src, dst_ref=dst, send_sem=ssem, recv_sem=rsem, device_id=to, device_id_type=MESH_ID
        )
        cp.start()
        return cp

    def await_bytes(ref, sem):
        pltpu.make_async_copy(ref, ref, sem).wait()

    def zat(d):
        return lax.rem(z + d + nz, nz)

    def xat(d):
        return lax.rem(x + d + nx, nx)

    def yat(d):
        return lax.rem(y + d, 4)

    y_order = (2, 1, 3)
    x_order = sorted(range(1, nx), key=lambda d: -min(d, nx - d))
    z_order = sorted(range(1, nz), key=lambda d: -min(d, nz - d))
    sections = [(d, False) for d in x_order] + [(d, True) for d in x_order] + [(0, True)]

    def peer(d, cross):
        return xat(d), (1 - core if cross else core)

    mine = pl.ds(pl.multiple_of(ylo * fe, LANES), fe)
    theirs = pl.ds(pl.multiple_of(other * fe, LANES), fe)

    w_hbm = (wi_hbm, wo_hbm)
    pa_in = pltpu.make_async_copy(pa_hbm, pa.at[core], lsem.at[0])
    w_in_ = [pltpu.make_async_copy(w_hbm[m].at[:, mine], wbuf.at[m, ylo, 1, z], lsem.at[1 + m]) for m in range(2)]
    og_in = pltpu.make_async_copy(og_hbm, og, lsem.at[3])
    li_in = pltpu.make_async_copy(li_hbm, li.at[core, x], lsem.at[4])
    pa_in.start()

    @pl.when(core == 1)
    def _():
        for cp in w_in_:
            cp.start()

    og_in.start()
    li_in.start()

    barrier = pltpu.get_barrier_semaphore()
    greeted = [dev(z_=zat(d)) for d in (1, -1)] + [dev(*peer(*p)) for p in sections]
    greeted += [dev(y_=yat(d)) for d in range(1, 4)] + [dev(core_=1 - core, y_=partner)]
    for to in greeted:
        pl.semaphore_signal(barrier, inc=1, device_id=to, device_id_type=MESH_ID)
    pa_in.wait()
    v = pa[core].astype(F32).reshape(tok, nsec * fb)
    pa_t[...] = jnp.swapaxes(v, 0, 1).astype(BF16).reshape(nsec, fb, tok)
    with scope("barrier"):
        pl.semaphore_wait(barrier, len(greeted))

    half = nz // 2

    def meet(r):
        for d in (1, -1):
            pl.semaphore_signal(near.at[r], inc=1, device_id=dev(z_=zat(d)), device_id_type=MESH_ID)
        pl.semaphore_wait(near.at[r], 2)

    def pa_first():
        await_bytes(pa.at[1], st_r.at[5])
        for h in range(2):
            @pl.when(yhi == h)
            def _():
                for d in z_order:
                    if d % 2 == h:
                        for c in range(2):
                            dst = pa_all.at[c, lax.rem(z, 2), z // 2]
                            send(pa.at[c, zat(d)], dst, st_s.at[0], st_r.at[0], dev(z_=zat(d)))
                if h == 0:
                    for c in range(2):
                        pa_all[c, lax.rem(z, 2), z // 2] = pa[c, z]

    def await_pa(sem):
        for h in range(2):
            @pl.when(yhi == h)
            def _():
                await_bytes(pa.at[0, pl.ds(0, 2 * (half - 1 + h))], sem)

    def pa_second():
        await_pa(st_r.at[0])
        mine_ = pa_all.at[:, lax.rem(z + yhi, 2)]
        send(mine_, mine_, st_s.at[6], st_r.at[4], dev(y_=yat(2)))

    swaps = [
        send(w_hbm[m].at[:, theirs], wbuf.at[m, ylo, core, z], wx_s.at[m], wx_r.at[core, m], dev(core_=1, y_=partner))
        for m in range(2)
    ]

    @pl.when(core == 0)
    def _():
        for m in range(2):
            send(w_hbm[m].at[:, mine], wbuf.at[m, ylo, 0, z], wd_s.at[m], wd_r.at[m], dev(core_=1))

    @pl.when(core == 1)
    def _():
        send(pa.at[1], pa.at[1], st_s.at[5], st_r.at[5], dev(core_=0))

    for p in sections:
        to = peer(*p)
        send(pa_t.at[to[0] * 2 + to[1]], pre_t.at[sec], st_s.at[3], st_r.at[3], dev(*to))
    pre_t[sec] = pa_t[sec]

    def spread_pre():
        await_bytes(pre_t.at[pl.ds(0, nsec - 1)], st_r.at[3])
        dst = pre_top.at[ylo, core]
        send(pre_t.at[top], dst, pt_s.at[0], pt_r.at[0], dev(core_=1, y_=partner))

        @pl.when(core == 0)
        def _():
            send(pre_t.at[top], dst, pt_s.at[1], pt_r.at[0], dev(core_=1))

        @pl.when(core == 1)
        def _():
            dst[...] = pre_t[top]

    def stage_b():
        await_bytes(pa_all.at[:, 0], st_r.at[4])
        group = lax.broadcasted_iota(jnp.int32, (8, LANES), 1) // fb
        for c in range(2):
            for ct in range(nsec // per_tile):
                for t in range(tiles):
                    out = [jnp.zeros((8, LANES), F32)] * per_tile
                    for j in range(per_tile):
                        at = t * per_tile + j
                        v = pa_all[c, at % 2, at // 2, :, ct * LANES:(ct + 1) * LANES].astype(F32)
                        for k in range(per_tile):
                            shift = (j - k) * fb % LANES
                            r = pltpu.roll(v, shift, 1) if shift else v
                            out[k] = jnp.where(group == j, r, out[k])
                    for k in range(per_tile):
                        to = ct * per_tile + k
                        pb[to // 2, c, to % 2, t] = out[k].astype(BF16)
        for d in x_order + [0]:
            send(pb.at[xat(d)], pc.at[ylo, pl.ds(2 * x, 2)], st_s.at[1], st_r.at[1], dev(x_=xat(d), core_=1))

    cut = tok // 2
    lo, hi = pl.ds(0, cut), pl.ds(cut, cut)
    ring = nx > 2

    def li_first():
        li_in.wait()
        src = li.at[core, x]
        send(src, src, li_s.at[0], li_r.at[0], dev(x_=xat(1)))
        if ring:
            send(src, src, li_s.at[1], li_r.at[1], dev(x_=xat(-1)))

    def li_second():
        await_bytes(li.at[0, 0], li_r.at[0])
        if ring:
            src = li.at[core, xat(-1), lo]
            send(src, src, li_s.at[2], li_r.at[2], dev(x_=xat(1)))
            await_bytes(li.at[0, 0], li_r.at[1])
            src = li.at[core, xat(1), hi]
            send(src, src, li_s.at[3], li_r.at[3], dev(x_=xat(-1)))

    def li_third():
        if ring:
            await_bytes(li.at[0, 0, lo], li_r.at[2])
            await_bytes(li.at[0, 0, hi], li_r.at[3])
        send(li.at[core], li.at[core], li_s.at[4], li_r.at[4], dev(core_=1 - core))

    def first_out_term():
        for s in range(nsec):
            v = pre_t[s].astype(F32)
            hall[s] = (v * gelu_parts(v)[0]).astype(BF16)
        go_out[...] = jnp.dot(hall[top], og[...].reshape(tok, width), preferred_element_type=F32)

    def first_in_term():
        await_bytes(li.at[0], li_r.at[4])
        gi_out[...] = jnp.dot(g_top[...], li[top % 2, top // 2], preferred_element_type=F32)

    block = 4 * nz

    def slot(t, x_, ylo_=0, z_=0):
        return ((((t * nx + x_) * 2 + ylo_) * nz) + z_) * 2

    def columns(t, x_, l):
        return up[pl.ds(slot(t, x_, l), 2 * nz)].reshape(nz, 2, 8, LANES)

    def out_term(t):
        rows = hall[t - 1]
        for l in range(2):
            parts = []
            for k in range(nx):
                v = columns(t, k, l)
                parts += [v[:, c].reshape(tok, LANES) for c in range(2)]
            go_out[:, l * fe:(l + 1) * fe] += jnp.dot(rows, jnp.concatenate(parts, axis=1), preferred_element_type=F32)

        @pl.when(sec == t)
        def _():
            for l in range(2):
                for k in range(nx):
                    v = columns(t, k, l)
                    for c in range(2):
                        at = l * fe + (2 * k + c) * LANES
                        ig_out[:, :, at:at + LANES] = v[:, c]

    def in_term(t):
        @pl.when(core == 1)
        def _():
            await_bytes(gz.at[pl.ds(0, nz - 1)], g_r.at[t])

        @pl.when(core == 0)
        def _():
            await_bytes(gz.at[pl.ds(0, nz)], g_r.at[t])

        gt[...] = jnp.swapaxes(gz[pl.ds(t * nz, nz)].astype(F32).reshape(tok, LANES), 0, 1)
        rows = gt[pl.ds(pl.multiple_of(lax.rem(z, per_tile) * fb, fb), fb), :].astype(BF16)
        gi_out[...] += jnp.dot(rows, li[lax.rem(t, 2), t // 2], preferred_element_type=F32)

    hu, hn, hj = 2 * nz * fb, fe // 2, nsec // 2
    def hop(m, k, parts=(0, 1)):
        for which in parts:
            l = which if k == half else ylo if which == 0 else other
            if k == 1:
                if which == 0:
                    w_in_[m].wait()
                    await_bytes(wbuf.at[m, 0, 0, 0], wd_r.at[m])
                else:
                    for c in range(2):
                        await_bytes(wbuf.at[m, 0, 0, 0], wx_r.at[c, m])
            for way, step in ((0, 1), (1, -1)):
                if k > 1:
                    await_bytes(wbuf.at[m, 0, :, 0], wz_r.at[way, k - 2, m, l])
                if k == half and way != which:
                    continue
                src = wbuf.at[m, l, :, zat(-step * (k - 1))]
                send(src, src, wz_s.at[way], wz_r.at[way, k - 1, m, l], dev(z_=zat(step)))

    def all_met():
        pl.semaphore_wait(near.at[half - 1], 1)

    def await_last(m):
        for way in range(2):
            await_bytes(wbuf.at[m, 0, :, 0], wz_r.at[way, half - 1, m, way])

    def stage_c():
        await_bytes(pc.at[0], st_r.at[1])
        send(pc.at[ylo], pc.at[ylo], st_s.at[2], st_r.at[2], dev(y_=partner))

    def stage_d():
        await_bytes(pc.at[0], st_r.at[2])

        def one(s, carry):
            for l in range(2):
                v = pc[l, s].astype(F32)
                cdf, dens = gelu_parts(v)
                slope[s, l] = (cdf + v * dens).reshape(2 * tiles, 8, LANES)
            return carry

        lax.fori_loop(0, top, one, 0)

    def top_first():
        og_in.wait()
        rows = wbuf[1, :, :, z].reshape(4 * fb, fe)
        a_top[y] = lax.dot_general(
            rows, og[:, :, mine].reshape(tok, fe), (((1,), (1,)), ((), ())), preferred_element_type=F32
        ).astype(BF16)
        for d in y_order:
            send(a_top.at[y], a_top.at[y], top_s.at[0], top_r.at[0], dev(y_=yat(d)))
        spread_pre()

    def top_second():
        await_bytes(pre_t.at[pl.ds(0, 3)], pt_r.at[0])
        v = pre_top[...].astype(F32).reshape(4 * fb, tok)
        cdf, dens = gelu_parts(v)
        await_bytes(a_top.at[pl.ds(0, 3)], top_r.at[0])
        back = a_top[0].astype(F32)
        for k in range(1, 4):
            back = back + a_top[k].astype(F32)
        g = (back * (cdf + v * dens)).astype(BF16)
        g_pass[...] = jnp.where(ylo == 0, g[:fb], g[2 * fb:3 * fb])
        send(g_pass, g_top, top_s.at[4], top_r.at[4], dev(core_=0))
        g_top[...] = jnp.where(ylo == 0, g[fb:2 * fb], g[3 * fb:])
        rows = jnp.swapaxes(g.astype(F32), 0, 1).astype(BF16)
        part = jnp.dot(rows, wbuf[0, :, :, z].reshape(4 * fb, fe), preferred_element_type=F32).astype(BF16)
        for j in range(nsec):
            b_top[j // 2, :, j % 2] = part[:, j * LANES:(j + 1) * LANES].reshape(nz, 8, LANES)
        for d in x_order:
            send(b_top.at[xat(d)], r_top.at[x], top_s.at[1], top_r.at[1], dev(x_=xat(d)))
        r_top[x] = b_top[x]

    def top_third():
        await_bytes(r_top.at[pl.ds(0, nx - 1)], top_r.at[1])
        total = r_top[0].astype(F32)
        for k in range(1, nx):
            total = total + r_top[k].astype(F32)
        q_top[...] = total.astype(BF16)
        for d in z_order:
            send(q_top.at[zat(d)], z_top.at[z], top_s.at[2], top_r.at[2], dev(z_=zat(d)))
        z_top[z] = q_top[z]

    own = pl.ds(2 * x, 2)

    def top_fourth():
        await_bytes(z_top.at[pl.ds(0, nz - 1)], top_r.at[2])
        for c in range(2):
            at = pl.multiple_of(ylo * fe + (2 * x + c) * LANES, LANES)
            total = og[z, :, pl.ds(at, LANES)].astype(F32)
            for k in range(nz):
                total = total + z_top[k, c].astype(F32)
            xs[top - 1, 2 * x + c] = total.astype(BF16)
        src = xs.at[top - 1, own]
        for d in x_order:
            send(src, src, top_s.at[3], top_r.at[3], dev(x_=xat(d)))

    def spread_z(t):
        src = xs.at[nsec if isinstance(t, int) and t == 0 else t - 1, own]
        dst = up.at[pl.ds(slot(t, x, ylo, z), 2)]

        def both(d):
            for to in (partner, y):
                send(src, dst, uz_s.at[0], uz_r.at[t], dev(core_=0, z_=zat(d), y_=to))

        both(half)

        def pair(i, c):
            both(half - i)
            both(half + i)
            return c

        lax.fori_loop(1, half, pair, 0)
        both(0)

    def spread_g(t):
        def to(d, c):
            tile = zat(d) // per_tile
            for c_ in range(2):
                send(gbuf.at[t, ylo, c_ * tiles + tile], gz.at[t * nz + z], g_s.at[0], g_r.at[t], dev(core_=c_, z_=zat(d)))
            return c

        lax.fori_loop(1, nz, to, 0)
        tile = z // per_tile
        send(gbuf.at[t, ylo, tile], gz.at[t * nz + z], g_s.at[0], g_r.at[t], dev(core_=0))
        gz[t * nz + z] = gbuf[t, ylo, tiles + tile]

    def turn(away):
        t = lax.rem(z // per_tile + away + tiles, tiles)

        def one(i, c):
            l, c_ = i // 2, lax.rem(i, 2)
            v = wbuf[1, l, c_, pl.ds(t * per_tile, per_tile)].reshape(LANES, fe)
            w_t[l, c_ * tiles + t] = jnp.swapaxes(v, 0, 1)
            return c

        lax.fori_loop(0, 4, one, 0)

    def a_half(s, l, part):
        a_buf[s, l, y] = part.astype(BF16)
        for d in y_order:
            send(a_buf.at[s, l, y], a_buf.at[s, l, y], ph_s.at[0, l, s], ph_r.at[0, l, s], dev(y_=yat(d)))

    def a_part(s, l, n):
        lhs = jnp.concatenate([xs[s, n * hj + j] for j in range(hj)], axis=1)
        w_out = jnp.concatenate([w_t[l, t, n * hn:(n + 1) * hn] for t in range(2 * tiles)], axis=1)
        return jnp.dot(lhs, w_out, preferred_element_type=F32)

    def a_first(s, l):
        lhs = jnp.concatenate([xs[s, j] for j in range(nsec)], axis=1)
        return lax.dot_general(lhs, wbuf[1, l].reshape(hu, fe), (((1,), (1,)), ((), ())), preferred_element_type=F32)

    def release(t):
        pl.semaphore_signal(go.at[t], inc=1, device_id=dev(core_=0), device_id_type=MESH_ID)

    def await_up(t):
        await_bytes(up.at[pl.ds(0, nx * block)], ud_r.at[t])

    def application(s, final):
        with scope("bg_a"):
            @pl.when(s <= top - 3)
            def _():
                release(s + 3)

            @pl.when(s <= top - 2)
            def _():
                spread_z(s + 1)

            @pl.when(s == top - 2)
            def _():
                first_in_term()

            @pl.when(s <= top - 3)
            def _():
                in_term(s + 2)

            @pl.when(s <= top - 5)
            def _():
                await_up(s + 5)
                out_term(s + 5)

        for l in range(2):
            with scope(f"wait_a{l}"):
                await_bytes(a_buf.at[s, l, pl.ds(0, 3)], ph_r.at[0, l, s])
            with scope(f"b_mm{l}"):
                back = a_buf[s, l, 0].astype(F32)
                for k in range(1, 4):
                    back = back + a_buf[s, l, k].astype(F32)
                g = []
                for t in range(2 * tiles):
                    g_tile = (back[:, t * LANES:(t + 1) * LANES] * slope[s, l, t]).astype(BF16)
                    gbuf[s, l, t] = g_tile
                    g.append(g_tile)
                g = jnp.concatenate(g, axis=1)
                if l == 0:
                    for n in range(2):
                        w_in = wbuf[0, l, :, :, :, n * hn:(n + 1) * hn].reshape(hu, hn)
                        b_acc[n] = jnp.dot(g, w_in, preferred_element_type=F32)
        for n in range(2):
            w_in = wbuf[0, 1, :, :, :, n * hn:(n + 1) * hn].reshape(hu, hn)
            part = (b_acc[n] + jnp.dot(g, w_in, preferred_element_type=F32)).astype(BF16)
            for j in range(hj):
                b_buf[s, n, x, j] = part[:, j * LANES:(j + 1) * LANES]
            if not final:
                src = b_buf.at[s, n, x]
                for d in x_order:
                    send(src, src, ph_s.at[1, n, s], ph_r.at[1, n, s], dev(x_=xat(d)))
        hx = nx // 2
        if final:
            for d in x_order:
                to = xat(d)
                src = b_buf.at[s, to // hx, x, pl.ds(2 * lax.rem(to, hx), 2)]
                send(src, src, ph_s.at[1, 0, s], ph_r.at[1, 0, s], dev(x_=to))

        with scope("bg_b"):
            spread_g(s)

            @pl.when(s == top - 1)
            def _():
                spread_z(top)

        if final:
            with scope("wait_b"):
                await_bytes(gz.at[pl.ds(0, 2 * (nx - 1))], ph_r.at[1, 0, s])
            for c in range(2):
                total = xs[s, 2 * x + c].astype(F32)
                for k in range(nx):
                    total = total + b_buf[s, x // hx, k, 2 * lax.rem(x, hx) + c].astype(F32)
                xs[nsec, 2 * x + c] = total.astype(BF16)
            return
        for n in range(2):
            with scope(f"wait_b{n}"):
                await_bytes(b_buf.at[s, n, pl.ds(0, nx - 1)], ph_r.at[1, n, s])
            with scope(f"a_mm{n}"):
                for j in range(hj):
                    total = xs[s, n * hj + j].astype(F32)
                    for k in range(nx):
                        total = total + b_buf[s, n, k, j].astype(F32)
                    xs[s - 1, n * hj + j] = total.astype(BF16)
                if n == 0:
                    for l in range(2):
                        a_acc[l] = a_part(s - 1, l, 0)
        for l in range(2):
            with scope(f"a_last{l}"):
                a_half(s - 1, l, a_acc[l] + a_part(s - 1, l, 1))

    @pl.when(core == 1)
    def _():
        plan = [
            (1, top_first), (2, top_second), (2, li_first), (4, all_met), (4, top_third), (5, first_out_term), (6, li_second),
            (6, stage_c), (7, stage_d), (7, top_fourth),
        ]
        plan += [(half if d else 5, lambda d=d: turn(d)) for d in (0, -1, 1) if d % tiles != tiles // 2]
        for k in range(1, half + 1):
            with scope(f"hop{k}"):
                if k == 1:
                    hop(1, 1, (0,))
                    hop(0, 1, (0,))
                    hop(1, 1, (1,))
                else:
                    hop(1, k)
                    hop(0, k - 1, (1,) if k == 2 else (0, 1))
            with scope(f"stage{k}"):
                for at, f in plan:
                    if min(at, half) == k:
                        f()
        with scope("gather_out"):
            await_last(1)
        with scope("top_end"):
            await_bytes(xs.at[0, pl.ds(0, 2 * (nx - 1))], top_r.at[3])
        for l in range(2):
            a_half(top - 1, l, a_first(top - 1, l))
        with scope("hop_end"):
            hop(0, half)
            turn(tiles // 2)
        with scope("gather_in"):
            await_last(0)
        li_third()

        def step(i, carry):
            application(top - 1 - i, False)
            return carry

        lax.fori_loop(0, top - 1, step, 0)
        application(0, True)

        with scope("t_z0"):
            spread_z(0)
            release(2)
            release(1)
        with scope("t_terms"):
            in_term(1)
            for t in range(min(top, 4), 2, -1):
                await_up(t)
                out_term(t)
        with scope("t_in0"):
            in_term(0)
        with scope("t_up2"):
            await_up(2)
            out_term(2)
        with scope("t_up1"):
            await_up(1)
        with scope("t_out1"):
            out_term(1)

        with scope("drain"):
            await_bytes(pa.at[1], st_s.at[5])
            await_bytes(pc.at[0], st_s.at[2])
            await_bytes(a_top.at[pl.ds(0, 3)], top_s.at[0])
            await_bytes(r_top.at[pl.ds(0, nx - 1)], top_s.at[1])
            await_bytes(z_top.at[pl.ds(0, nz - 1)], top_s.at[2])
            await_bytes(xs.at[0, pl.ds(0, 2 * (nx - 1))], top_s.at[3])
            await_bytes(g_top, top_s.at[4])
            for way in range(2):
                await_bytes(wbuf.at[0, :, :, pl.ds(0, nz - 1)], wz_s.at[way])

            def sent(s, c):
                for h in range(2):
                    await_bytes(a_buf.at[0, h, pl.ds(0, 3)], ph_s.at[0, h, s])
                    await_bytes(b_buf.at[0, h, pl.ds(0, nx - 1)], ph_s.at[1, h, s])
                return c

            lax.fori_loop(1, top, sent, 0)
            for h in range(2):
                await_bytes(a_buf.at[0, h, pl.ds(0, 3)], ph_s.at[0, h, 0])
            await_bytes(gz.at[pl.ds(0, 2 * (nx - 1))], ph_s.at[1, 0, 0])
            await_bytes(up.at[pl.ds(0, top * (2 * nz - 1))], g_s.at[0])
            await_bytes(up.at[pl.ds(0, nsec * block)], uz_s.at[0])

    def await_z(t):
        await_bytes(up.at[pl.ds(0, block)], uz_r.at[t])

    def spread_x(t):
        await_z(t)
        pl.semaphore_wait(go.at[t], 1)
        src = up.at[pl.ds(slot(t, x), block)]
        for d in x_order:
            send(src, src, ux_s.at[0], ux_r.at[t], dev(x_=xat(d)))

    def spread_core(t):
        await_bytes(up.at[pl.ds(0, (nx - 1) * block)], ux_r.at[t])
        src = up.at[pl.ds(slot(t, 0), nx * block)]
        send(src, src, ud_s.at[0], ud_r.at[t], dev(core_=1))

    @pl.when(core == 0)
    def _():
        spread_pre()
        for r in range(half - 1):
            meet(r)
        pl.semaphore_signal(near.at[half - 1], inc=1, device_id=dev(core_=1), device_id_type=MESH_ID)
        pa_first()
        li_first()
        pa_second()
        stage_b()
        og_in.wait()
        first_out_term()
        li_second()
        li_third()
        await_bytes(g_top, top_r.at[4])
        first_in_term()

        def move(i, carry):
            t = top - i
            with scope("s_x"):
                spread_x(t)
            with scope("s_in"):
                @pl.when(t < top)
                def _():
                    in_term(t)

            with scope("s_core"):
                spread_core(t)
            with scope("s_out"):
                out_term(t)
            return carry

        lax.fori_loop(0, top - 2, move, 0)
        with scope("s_x21"):
            spread_x(2)
            spread_x(1)
        with scope("s_in"):
            for t in (2, 1, 0):
                in_term(t)
        with scope("s_core2"):
            spread_core(2)
            out_term(2)
        with scope("s_core1"):
            spread_core(1)
        with scope("s_z0"):
            await_z(0)
        for l in range(2):
            v = columns(0, x, l)
            for c in range(2):
                at = pl.multiple_of(l * fe + (2 * x + c) * LANES, LANES)

                @pl.when(x == 0)
                def _():
                    ig_out[:, :, pl.ds(at, LANES)] = v[:, c]

                @pl.when(x != 0)
                def _():
                    x_end[l, c] = v[:, c]
                    send(x_end.at[l, c], ig_out.at[:, :, pl.ds(at, LANES)], ux_s.at[1], ux_r.at[0], dev(x_=0))

        with scope("s_out1"):
            out_term(1)
        with scope("s_x0w"):
            @pl.when(x == 0)
            def _():
                await_bytes(up.at[pl.ds(0, (nx - 1) * block)], ux_r.at[0])

        with scope("s_drain"):
            await_pa(st_s.at[0])
            await_bytes(pa_all.at[:, 0], st_s.at[6])
            await_bytes(pc.at[0], st_s.at[1])
            for m in range(2):
                await_bytes(wbuf.at[m, 0, 0, 0], wd_s.at[m])
            await_bytes(pre_t.at[0], pt_s.at[1])
            await_bytes(up.at[pl.ds(0, top * (nx - 1) * block)], ux_s.at[0])
            await_bytes(up.at[pl.ds(0, top * nx * block)], ud_s.at[0])

            @pl.when(x != 0)
            def _():
                await_bytes(up.at[pl.ds(0, block)], ux_s.at[1])

    await_bytes(pre_t.at[pl.ds(0, nsec - 1)], st_s.at[3])
    await_bytes(pre_t.at[0], pt_s.at[0])
    for cp in swaps:
        cp.wait_send()
    await_bytes(li.at[0, 0], li_s.at[0])
    if ring:
        await_bytes(li.at[0, 0], li_s.at[1])
        await_bytes(li.at[0, 0, lo], li_s.at[2])
        await_bytes(li.at[0, 0, hi], li_s.at[3])
    await_bytes(li.at[0], li_s.at[4])


def finish(ig, gi, go, ig_out, gi_out, go_out, sems):
    copies = [pltpu.make_async_copy(src, dst, sems.at[k]) for k, (src, dst) in enumerate(((ig, ig_out), (gi, gi_out), (go, go_out)))]
    for cp in copies:
        cp.start()
    for cp in copies:
        cp.wait()


def body(layer_inputs, pre_act, out_grad, w_in, w_out):
    nz, nx = lax.axis_size("z"), lax.axis_size("x")
    nsec = 2 * nx
    tok, width = out_grad.shape
    fb = w_in.shape[2]
    hid = pre_act.shape[2]
    fe = width // 2
    tiles = nz * fb // LANES
    half = nz // 2
    dma = pltpu.SemaphoreType.DMA
    vmem = pltpu.VMEM
    scratch = [
        vmem((2, 2, 2, nz, fb, fe), BF16),
        vmem((2, nz, 8, hid), BF16),
        vmem((2, 2, half, 8, hid), BF16),
        vmem((nx, 2, 2, tiles, 8, LANES), BF16),
        vmem((2, nsec, 2, tiles, 8, LANES), BF16),
        vmem((nsec, 2, 2 * tiles, 8, LANES), F32),
        vmem((nsec, fb, tok), BF16),
        vmem((nsec, fb, tok), BF16),
        vmem((2, 2, fb, tok), BF16),
        vmem((nsec, fb, tok), BF16),
        vmem((2, nx, tok, width), BF16),
        vmem((nz, 8, width), BF16),
        vmem((4, 4 * fb, tok), BF16),
        vmem((nx, nz, 2, 8, LANES), BF16),
        vmem((nx, nz, 2, 8, LANES), BF16),
        vmem((nz, 2, 8, LANES), BF16),
        vmem((nz, 2, 8, LANES), BF16),
        vmem((fb, tok), BF16),
        vmem((fb, tok), BF16),
        vmem((2, 2 * tiles, fe, LANES), BF16),
        vmem((nsec + 1, nsec, 8, LANES), BF16),
        vmem((nsec, 2, 4, 8, 2 * nz * fb), BF16),
        vmem((nsec, 2, nx, nx, 8, LANES), BF16),
        vmem((2, 8, 2 * nz * fb), F32),
        vmem((2, 8, fe // 2), F32),
        vmem((nsec, 2, 2 * tiles, 8, LANES), BF16),
        vmem((nsec * nz, 8, LANES), BF16),
        vmem((LANES, tok), F32),
        vmem((nsec * nx * 4 * nz, 8, LANES), BF16),
        vmem((2, 2, nz, 8, LANES), BF16),
        dma((5,)),
        dma((2,)), dma((2, 2)),
        dma((2,)), dma((2,)),
        dma((2,)), dma((2, half, 2, 2)),
        dma((7,)), dma((6,)),
        dma((2,)), dma((1,)),
        dma((5,)), dma((5,)),
        dma((2, 2, nsec)), dma((2, 2, nsec)),
        dma((5,)), dma((5,)),
        dma((1,)), dma((nsec,)),
        dma((1,)), dma((nsec,)),
        dma((2,)), dma((nsec,)),
        dma((1,)), dma((nsec,)),
        pltpu.SemaphoreType.REGULAR((nsec,)),
        pltpu.SemaphoreType.REGULAR((half,)),
    ]
    hbm, on_chip = pl.BlockSpec(memory_space=pltpu.HBM), pl.BlockSpec(memory_space=pltpu.VMEM)
    shapes = (
        jax.ShapeDtypeStruct((nz, 8, width), BF16),
        jax.ShapeDtypeStruct((fb, width), F32),
        jax.ShapeDtypeStruct((fb, width), F32),
    )
    operands = (
        layer_inputs.reshape(tok, width),
        pre_act.reshape(nz, 8, hid),
        out_grad.reshape(nz, 8, width),
        w_in.reshape(fb, width),
        w_out.reshape(fb, width),
    )
    results = pl.pallas_call(
        kernel,
        out_shape=shapes,
        in_specs=[hbm] * 5,
        out_specs=(on_chip,) * 3,
        scratch_shapes=scratch,
        name="chain",
        compiler_params=pltpu.CompilerParams(
            collective_id=0, has_side_effects=True, vmem_limit_bytes=40 * 1024 * 1024
        ),
    )(*(pltpu.with_memory_space_constraint(v, pltpu.HBM) for v in operands))
    ig, gi, go = pl.pallas_call(
        finish,
        out_shape=shapes,
        in_specs=[on_chip] * 3,
        out_specs=(hbm,) * 3,
        scratch_shapes=[dma((3,))],
        name="finish",
    )(*(pltpu.with_memory_space_constraint(v, pltpu.VMEM) for v in results))
    return (
        ig.reshape(1, tok, width),
        gi.reshape(1, 1, fb, width),
        go.reshape(1, 1, fb, width),
    )


def solution(mesh):
    shape = mesh.shape
    split = Mesh(
        mesh.devices.reshape(shape["section"] // 2, 2, shape["dp"] // 2, 2, shape["mp"]), AXES
    )
    sec, dp = ("x", "core"), ("z", "ylo")
    placed = (
        P(sec, None, "yhi"),
        P(sec, None, dp),
        P(None, "yhi"),
        P(dp, sec, None, "yhi"),
        P(dp, sec, None, "yhi"),
    )
    return jax.shard_map(
        body,
        mesh=split,
        in_specs=placed,
        out_specs=(P(sec, None, "yhi"), P(dp, sec, None, "yhi"), P(dp, sec, None, "yhi")),
        check_vma=False,
    )
```

```python
import contextlib
import math

import jax
import jax.numpy as jnp
from jax import lax
from jax.experimental import pallas as pl
from jax.experimental.pallas import tpu as pltpu
from jax.sharding import Mesh
from jax.sharding import PartitionSpec as P

AXES = ("x", "core", "z", "ylo", "yhi")
MESH_ID = pl.DeviceIdType.MESH
BF16, F32 = jnp.bfloat16, jnp.float32
LANES = 128
PROFILE = False


def scope(name):
    return jax.named_scope(name) if PROFILE else contextlib.nullcontext()


def gelu_parts(v):
    cdf = 0.5 * (1.0 + lax.erf(v * 0.7071067811865476))
    dens = jnp.exp(-0.5 * v * v) * 0.3989422804014327
    return cdf, dens


def kernel(
    li_hbm, pa_hbm, og_hbm, wi_hbm, wo_hbm,
    ig_out, gi_out, go_out,
    w_own, wbuf, pa, pa_all, pb, pc, slope, pa_t, pre_t, pre_top, hall, li, og,
    a_top, b_top, r_top, q_top, z_top, g_top, g_pass,
    w_t, xs, a_buf, b_buf, a_acc, b_acc, gbuf, gz, gt, up,
    spare, lsem, out_s, wz_s, wx_r, wd_r, wz_r, st_r, pt_r, top_r, ph_r, li_r, g_r, uz_r, ux_r, ud_r, go, near,
):
    nx, nz = lax.axis_size("x"), lax.axis_size("z")
    nsec = 2 * nx
    top = nsec - 1
    fb, width = wi_hbm.shape
    fe = width // 2
    tok = nz * 8
    tiles = nz * fb // LANES
    per_tile = LANES // fb
    x, core, z = lax.axis_index("x"), lax.axis_index("core"), lax.axis_index("z")
    ylo, yhi = lax.axis_index("ylo"), lax.axis_index("yhi")
    sec = x * 2 + core
    y = yhi * 2 + ylo
    other = 1 - ylo
    partner = yhi * 2 + other

    def dev(x_=None, core_=None, z_=None, y_=None):
        y_ = y if y_ is None else y_
        return (
            x if x_ is None else x_,
            core if core_ is None else core_,
            z if z_ is None else z_,
            lax.rem(y_, 2),
            y_ // 2,
        )

    def send(src, dst, ssem, rsem, to):
        cp = pltpu.make_async_remote_copy(
            src_ref=src, dst_ref=dst, send_sem=ssem, recv_sem=rsem, device_id=to, device_id_type=MESH_ID
        )
        cp.start()
        return cp

    def await_bytes(ref, sem):
        pltpu.make_async_copy(ref, ref, sem).wait()

    def zat(d):
        return lax.rem(z + d + nz, nz)

    def xat(d):
        return lax.rem(x + d + nx, nx)

    def yat(d):
        return lax.rem(y + d, 4)

    y_order = (2, 1, 3)
    x_order = sorted(range(1, nx), key=lambda d: -min(d, nx - d))
    z_order = sorted(range(1, nz), key=lambda d: -min(d, nz - d))
    sections = [(d, False) for d in x_order] + [(d, True) for d in x_order] + [(0, True)]

    def peer(d, cross):
        return xat(d), (1 - core if cross else core)

    mine = pl.ds(pl.multiple_of(ylo * fe, LANES), fe)
    theirs = pl.ds(pl.multiple_of(other * fe, LANES), fe)

    w_hbm = (wi_hbm, wo_hbm)
    pa_in = pltpu.make_async_copy(pa_hbm, pa.at[core], lsem.at[0])
    w_in_ = [pltpu.make_async_copy(w_hbm[m].at[:, mine], wbuf.at[m, ylo, 1, z], lsem.at[1 + m]) for m in range(2)]
    og_in = pltpu.make_async_copy(og_hbm, og, lsem.at[3])
    li_in = pltpu.make_async_copy(li_hbm, li.at[core, x], lsem.at[4])
    barrier = pltpu.get_barrier_semaphore()
    greeted = [dev(z_=zat(d)) for d in (1, -1)] + [dev(*peer(*p)) for p in sections]
    greeted += [dev(y_=yat(d)) for d in range(1, 4)] + [dev(core_=1 - core, y_=partner)]
    for to in greeted:
        pl.semaphore_signal(barrier, inc=1, device_id=to, device_id_type=MESH_ID)

    first = (1, 0)
    own_in = [pltpu.make_async_copy(w_hbm[m], w_own.at[m], lsem.at[5 + m]) for m in range(2)]
    for m in first:
        own_in[m].start()

        @pl.when(core == 1)
        def _():
            w_in_[m].start()

    pa_in.start()

    og_in.start()
    li_in.start()

    with scope("barrier"):
        pl.semaphore_wait(barrier, len(greeted))

    half = nz // 2

    def meet(r):
        for d in (1, -1):
            pl.semaphore_signal(near.at[r], inc=1, device_id=dev(z_=zat(d)), device_id_type=MESH_ID)
        pl.semaphore_wait(near.at[r], 2)

    def pa_first():
        await_bytes(pa.at[1], st_r.at[5])
        for h in range(2):
            @pl.when(yhi == h)
            def _():
                for d in z_order:
                    if d % 2 == h:
                        for c in range(2):
                            dst = pa_all.at[c, lax.rem(z, 2), z // 2]
                            send(pa.at[c, zat(d)], dst, out_s.at[0], st_r.at[0], dev(z_=zat(d)))
                if h == 0:
                    for c in range(2):
                        pa_all[c, lax.rem(z, 2), z // 2] = pa[c, z]

    def await_pa(sem):
        for h in range(2):
            @pl.when(yhi == h)
            def _():
                await_bytes(pa.at[0, pl.ds(0, 2 * (half - 1 + h))], sem)

    def pa_second():
        await_pa(st_r.at[0])
        mine_ = pa_all.at[:, lax.rem(z + yhi, 2)]
        send(mine_, mine_, out_s.at[0], st_r.at[4], dev(y_=yat(2)))

    def ring_send(src, m, l, k, way):
        send(src, src, wz_s.at[way], wz_r.at[k - 1, m, l], dev(z_=zat(1 if way == 0 else -1)))

    swaps = []
    for m in first:
        own_in[m].wait()

        @pl.when(core == 0)
        def _():
            send(w_own.at[m, :, mine], wbuf.at[m, ylo, 0, z], out_s.at[0], wd_r.at[m], dev(core_=1))

        @pl.when(core == 1)
        def _():
            w_in_[m].wait()
            for way in range(2):
                ring_send(wbuf.at[m, ylo, 1, z], m, ylo, 1, way)

        dst = wbuf.at[m, ylo, core, z]
        swaps.append(send(w_own.at[m, :, theirs], dst, out_s.at[0], wx_r.at[core, m], dev(core_=1, y_=partner)))

    pa_in.wait()

    @pl.when(core == 1)
    def _():
        send(pa.at[1], pa.at[1], out_s.at[0], st_r.at[5], dev(core_=0))

    v = pa[core].astype(F32).reshape(tok, nsec * fb)
    pa_t[...] = jnp.swapaxes(v, 0, 1).astype(BF16).reshape(nsec, fb, tok)
    for p in sections:
        to = peer(*p)
        send(pa_t.at[to[0] * 2 + to[1]], pre_t.at[sec], out_s.at[0], st_r.at[3], dev(*to))
    pre_t[sec] = pa_t[sec]

    def spread_pre():
        await_bytes(pre_t.at[pl.ds(0, nsec - 1)], st_r.at[3])
        dst = pre_top.at[ylo, core]
        send(pre_t.at[top], dst, out_s.at[0], pt_r.at[0], dev(core_=1, y_=partner))

        @pl.when(core == 0)
        def _():
            send(pre_t.at[top], dst, out_s.at[0], pt_r.at[0], dev(core_=1))

        @pl.when(core == 1)
        def _():
            dst[...] = pre_t[top]

    def stage_b():
        await_bytes(pa_all.at[:, 0], st_r.at[4])
        group = lax.broadcasted_iota(jnp.int32, (8, LANES), 1) // fb
        for c in range(2):
            for ct in range(nsec // per_tile):
                for t in range(tiles):
                    out = [jnp.zeros((8, LANES), F32)] * per_tile
                    for j in range(per_tile):
                        at = t * per_tile + j
                        v = pa_all[c, at % 2, at // 2, :, ct * LANES:(ct + 1) * LANES].astype(F32)
                        for k in range(per_tile):
                            shift = (j - k) * fb % LANES
                            r = pltpu.roll(v, shift, 1) if shift else v
                            out[k] = jnp.where(group == j, r, out[k])
                    for k in range(per_tile):
                        to = ct * per_tile + k
                        pb[to // 2, c, to % 2, t] = out[k].astype(BF16)
        for d in x_order + [0]:
            send(pb.at[xat(d)], pc.at[ylo, pl.ds(2 * x, 2)], out_s.at[0], st_r.at[1], dev(x_=xat(d), core_=1))

    cut = tok // 2
    lo, hi = pl.ds(0, cut), pl.ds(cut, cut)
    ring = nx > 2

    def li_first():
        li_in.wait()
        src = li.at[core, x]
        send(src, src, out_s.at[1], li_r.at[0], dev(x_=xat(1)))
        if ring:
            send(src, src, out_s.at[1], li_r.at[1], dev(x_=xat(-1)))

    def li_second():
        await_bytes(li.at[0, 0], li_r.at[0])
        if ring:
            src = li.at[core, xat(-1), lo]
            send(src, src, out_s.at[1], li_r.at[2], dev(x_=xat(1)))
            await_bytes(li.at[0, 0], li_r.at[1])
            src = li.at[core, xat(1), hi]
            send(src, src, out_s.at[1], li_r.at[3], dev(x_=xat(-1)))

    def li_third():
        if ring:
            await_bytes(li.at[0, 0, lo], li_r.at[2])
            await_bytes(li.at[0, 0, hi], li_r.at[3])
        send(li.at[core], li.at[core], out_s.at[1], li_r.at[4], dev(core_=1 - core))

    def first_out_term():
        for s in range(nsec):
            v = pre_t[s].astype(F32)
            hall[s] = (v * gelu_parts(v)[0]).astype(BF16)
        go_out[...] = jnp.dot(hall[top], og[...].reshape(tok, width), preferred_element_type=F32)

    def first_in_term():
        await_bytes(li.at[0], li_r.at[4])
        gi_out[...] = jnp.dot(g_top[...], li[top % 2, top // 2], preferred_element_type=F32)

    block = 4 * nz

    def slot(t, x_, ylo_=0, z_=0):
        return ((((t * nx + x_) * 2 + ylo_) * nz) + z_) * 2

    def columns(t, x_, l):
        return up[pl.ds(slot(t, x_, l), 2 * nz)].reshape(nz, 2, 8, LANES)

    def out_term(t):
        rows = hall[t - 1]
        for l in range(2):
            parts = []
            for k in range(nx):
                v = columns(t, k, l)
                parts += [v[:, c].reshape(tok, LANES) for c in range(2)]
            go_out[:, l * fe:(l + 1) * fe] += jnp.dot(rows, jnp.concatenate(parts, axis=1), preferred_element_type=F32)

        @pl.when(sec == t)
        def _():
            for l in range(2):
                for k in range(nx):
                    v = columns(t, k, l)
                    for c in range(2):
                        at = l * fe + (2 * k + c) * LANES
                        ig_out[:, :, at:at + LANES] = v[:, c]

    def in_term(t):
        @pl.when(core == 1)
        def _():
            await_bytes(gz.at[pl.ds(0, nz - 1)], g_r.at[t])

        @pl.when(core == 0)
        def _():
            await_bytes(gz.at[pl.ds(0, nz)], g_r.at[t])

        gt[...] = jnp.swapaxes(gz[pl.ds(t * nz, nz)].astype(F32).reshape(tok, LANES), 0, 1)
        rows = gt[pl.ds(pl.multiple_of(lax.rem(z, per_tile) * fb, fb), fb), :].astype(BF16)
        gi_out[...] += jnp.dot(rows, li[lax.rem(t, 2), t // 2], preferred_element_type=F32)

    hu, hn, hj = 2 * nz * fb, fe // 2, nsec // 2
    def hop(m, k, which):
        l = ylo if which == 0 else other
        if k == 1:
            if which == 0:
                await_bytes(wbuf.at[m, 0, 0, 0], wd_r.at[m])
            else:
                for c in range(2):
                    await_bytes(wbuf.at[m, 0, 0, 0], wx_r.at[c, m])
        if k > 1:
            await_bytes(wbuf.at[m, 0, :, pl.ds(0, 2)], wz_r.at[k - 2, m, l])
        for way, step in ((0, 1), (1, -1)):
            if k == 1 and which == 0:
                ring_send(wbuf.at[m, l, 0, z], m, l, 1, way)
            elif k == half:
                ring_send(wbuf.at[m, l, way, zat(-step * (k - 1))], m, l, k, way)
            else:
                ring_send(wbuf.at[m, l, :, zat(-step * (k - 1))], m, l, k, way)

    def await_last(m):
        for l in range(2):
            await_bytes(wbuf.at[m, 0, :, 0], wz_r.at[half - 1, m, l])

    def all_met():
        pl.semaphore_wait(near.at[half - 1], 1)

    def stage_c():
        await_bytes(pc.at[0], st_r.at[1])
        send(pc.at[ylo], pc.at[ylo], out_s.at[0], st_r.at[2], dev(y_=partner))

    def stage_d():
        await_bytes(pc.at[0], st_r.at[2])

        def one(s, carry):
            for l in range(2):
                v = pc[l, s].astype(F32)
                cdf, dens = gelu_parts(v)
                slope[s, l] = (cdf + v * dens).reshape(2 * tiles, 8, LANES)
            return carry

        lax.fori_loop(0, top, one, 0)

    def top_first():
        og_in.wait()
        rows = wbuf[1, :, :, z].reshape(4 * fb, fe)
        a_top[y] = lax.dot_general(
            rows, og[:, :, mine].reshape(tok, fe), (((1,), (1,)), ((), ())), preferred_element_type=F32
        ).astype(BF16)
        for d in y_order:
            send(a_top.at[y], a_top.at[y], out_s.at[0], top_r.at[0], dev(y_=yat(d)))
        spread_pre()

    def top_second():
        await_bytes(pre_t.at[pl.ds(0, 3)], pt_r.at[0])
        v = pre_top[...].astype(F32).reshape(4 * fb, tok)
        cdf, dens = gelu_parts(v)
        await_bytes(a_top.at[pl.ds(0, 3)], top_r.at[0])
        back = a_top[0].astype(F32)
        for k in range(1, 4):
            back = back + a_top[k].astype(F32)
        g = (back * (cdf + v * dens)).astype(BF16)
        g_pass[...] = jnp.where(ylo == 0, g[:fb], g[2 * fb:3 * fb])
        send(g_pass, g_top, out_s.at[0], top_r.at[4], dev(core_=0))
        g_top[...] = jnp.where(ylo == 0, g[fb:2 * fb], g[3 * fb:])
        rows = jnp.swapaxes(g.astype(F32), 0, 1).astype(BF16)
        part = jnp.dot(rows, wbuf[0, :, :, z].reshape(4 * fb, fe), preferred_element_type=F32).astype(BF16)
        for j in range(nsec):
            b_top[j // 2, :, j % 2] = part[:, j * LANES:(j + 1) * LANES].reshape(nz, 8, LANES)
        for d in x_order:
            send(b_top.at[xat(d)], r_top.at[x], out_s.at[0], top_r.at[1], dev(x_=xat(d)))
        r_top[x] = b_top[x]

    def top_third():
        await_bytes(r_top.at[pl.ds(0, nx - 1)], top_r.at[1])
        total = r_top[0].astype(F32)
        for k in range(1, nx):
            total = total + r_top[k].astype(F32)
        q_top[...] = total.astype(BF16)
        for d in z_order:
            send(q_top.at[zat(d)], z_top.at[z], out_s.at[0], top_r.at[2], dev(z_=zat(d)))
        z_top[z] = q_top[z]

    own = pl.ds(2 * x, 2)

    def top_fourth():
        await_bytes(z_top.at[pl.ds(0, nz - 1)], top_r.at[2])
        for c in range(2):
            at = pl.multiple_of(ylo * fe + (2 * x + c) * LANES, LANES)
            total = og[z, :, pl.ds(at, LANES)].astype(F32)
            for k in range(nz):
                total = total + z_top[k, c].astype(F32)
            xs[top - 1, 2 * x + c] = total.astype(BF16)
        src = xs.at[top - 1, own]
        for d in x_order:
            send(src, src, out_s.at[0], top_r.at[3], dev(x_=xat(d)))

    def spread_z(t):
        src = xs.at[t - 1, own]
        dst = up.at[pl.ds(slot(t, x, ylo, z), 2)]

        def both(d):
            for to in (partner, y):
                send(src, dst, out_s.at[0], uz_r.at[t], dev(core_=0, z_=zat(d), y_=to))

        both(half)

        def pair(i, c):
            both(half - i)
            both(half + i)
            return c

        lax.fori_loop(1, half, pair, 0)
        both(0)

    reach = half // 2
    far = [r for r in range(nz) if min(r, nz - r) > reach]
    low, high = (0, far[0]), (far[-1] + 1, nz)

    def last_z():
        src = xs.at[nsec, own]
        for d in [half] + [d for i in range(1, half) for d in (half - i, half + i)] + [0]:
            r = (nz - d) % nz
            dst = up.at[pl.ds(slot(0, x, ylo, r), 2)]
            for to in (partner, y):
                if d or to is partner:
                    send(src, dst, out_s.at[0], uz_r.at[nsec if r in far else 0], dev(z_=zat(d), y_=to))
        up[pl.ds(slot(0, x, ylo, 0), 2)] = src[...]

    def last_x(kind):
        for l in range(2):
            for a, b in ((far[0], far[-1] + 1),) if kind else (low, high):
                src = up.at[pl.ds(slot(0, x, l, a), 2 * (b - a))]
                send(src, src, out_s.at[0], ux_r.at[nsec if kind else 0], dev(x_=0, core_=0))

    near_tiles, far_tiles = 4 * (nz - len(far)), 4 * len(far)

    def last_out(kind):
        for r in range(nz):
            if (r in far) == bool(kind):
                row = zat(r)
                for l in range(2):
                    for k in range(nx):
                        for c in range(2):
                            at = l * fe + (2 * k + c) * LANES
                            ig_out[row, :, at:at + LANES] = up[slot(0, k, l, r) + c]

    def spread_g(t):
        def to(d, c):
            tile = zat(d) // per_tile
            for c_ in range(2):
                send(gbuf.at[t, ylo, c_ * tiles + tile], gz.at[t * nz + z], out_s.at[0], g_r.at[t], dev(core_=c_, z_=zat(d)))
            return c

        lax.fori_loop(1, nz, to, 0)
        tile = z // per_tile
        send(gbuf.at[t, ylo, tile], gz.at[t * nz + z], out_s.at[0], g_r.at[t], dev(core_=0))
        gz[t * nz + z] = gbuf[t, ylo, tiles + tile]

    def turn(away):
        t = lax.rem(z // per_tile + away + tiles, tiles)

        def one(i, c):
            l, c_ = i // 2, lax.rem(i, 2)
            v = wbuf[1, l, c_, pl.ds(t * per_tile, per_tile)].reshape(LANES, fe)
            w_t[l, c_ * tiles + t] = jnp.swapaxes(v, 0, 1)
            return c

        lax.fori_loop(0, 4, one, 0)

    def a_half(s, l, part=None):
        if part is not None:
            a_buf[s, l, y] = part.astype(BF16)
        for d in y_order:
            send(a_buf.at[s, l, y], a_buf.at[s, l, y], out_s.at[0], ph_r.at[0, l, s % 2 if isinstance(s, int) else lax.rem(s, 2)], dev(y_=yat(d)))

    def a_part(s, l, n):
        lhs = jnp.concatenate([xs[s, n * hj + j] for j in range(hj)], axis=1)
        w_out = jnp.concatenate([w_t[l, t, n * hn:(n + 1) * hn] for t in range(2 * tiles)], axis=1)
        return jnp.dot(lhs, w_out, preferred_element_type=F32)

    def a_tile(l, away, turned):
        lhs = jnp.concatenate([xs[top - 1, j] for j in range(nsec)], axis=1)
        t = lax.rem(z // per_tile + away + tiles, tiles)
        if turned:
            w_out = jnp.concatenate([w_t[l, c * tiles + t] for c in range(2)], axis=1)
            part = jnp.dot(lhs, w_out, preferred_element_type=F32)
        else:
            w_out = wbuf[1, l, :, pl.ds(t * per_tile, per_tile)].reshape(2 * LANES, fe)
            part = lax.dot_general(lhs, w_out, (((1,), (1,)), ((), ())), preferred_element_type=F32)
        for c in range(2):
            at = pl.multiple_of((c * tiles + t) * LANES, LANES)
            a_buf[top - 1, l, y, :, pl.ds(at, LANES)] = part[:, c * LANES:(c + 1) * LANES].astype(BF16)

    def release(t):
        pl.semaphore_signal(go.at[t], inc=1, device_id=dev(core_=0), device_id_type=MESH_ID)

    def await_up(t):
        await_bytes(up.at[pl.ds(0, nx * block)], ud_r.at[t])

    def application(s, final):
        with scope("bg_a"):
            @pl.when(s <= top - 3)
            def _():
                release(s + 3)

            @pl.when(s <= top - 2)
            def _():
                spread_z(s + 1)

            @pl.when(s == top - 2)
            def _():
                first_in_term()

            @pl.when(s <= top - 3)
            def _():
                in_term(s + 2)

            @pl.when(s <= top - 5)
            def _():
                await_up(s + 5)
                out_term(s + 5)

        for l in range(2):
            with scope(f"wait_a{l}"):
                await_bytes(a_buf.at[s, l, pl.ds(0, 3)], ph_r.at[0, l, s % 2 if isinstance(s, int) else lax.rem(s, 2)])
            with scope(f"b_mm{l}"):
                back = a_buf[s, l, 0].astype(F32)
                for k in range(1, 4):
                    back = back + a_buf[s, l, k].astype(F32)
                g = []
                for t in range(2 * tiles):
                    g_tile = (back[:, t * LANES:(t + 1) * LANES] * slope[s, l, t]).astype(BF16)
                    gbuf[s, l, t] = g_tile
                    g.append(g_tile)
                g = jnp.concatenate(g, axis=1)
                if l == 0:
                    for n in range(2):
                        w_in = wbuf[0, l, :, :, :, n * hn:(n + 1) * hn].reshape(hu, hn)
                        b_acc[n] = jnp.dot(g, w_in, preferred_element_type=F32)
        for n in range(2):
            w_in = wbuf[0, 1, :, :, :, n * hn:(n + 1) * hn].reshape(hu, hn)
            part = (b_acc[n] + jnp.dot(g, w_in, preferred_element_type=F32)).astype(BF16)
            for j in range(hj):
                b_buf[s, n, x, j] = part[:, j * LANES:(j + 1) * LANES]
            if not final:
                src = b_buf.at[s, n, x]
                for d in x_order:
                    send(src, src, out_s.at[0], ph_r.at[1, n, s % 2 if isinstance(s, int) else lax.rem(s, 2)], dev(x_=xat(d)))
        hx = nx // 2
        if final:
            for d in x_order:
                to = xat(d)
                src = b_buf.at[s, to // hx, x, pl.ds(2 * lax.rem(to, hx), 2)]
                send(src, src, out_s.at[0], ph_r.at[1, 0, s % 2], dev(x_=to))

        with scope("bg_b"):
            spread_g(s)
            if final:
                release(2)

            @pl.when(s == top - 1)
            def _():
                spread_z(top)

        if final:
            with scope("wait_b"):
                await_bytes(gz.at[pl.ds(0, 2 * (nx - 1))], ph_r.at[1, 0, s % 2])
            for c in range(2):
                total = xs[s, 2 * x + c].astype(F32)
                for k in range(nx):
                    total = total + b_buf[s, x // hx, k, 2 * lax.rem(x, hx) + c].astype(F32)
                xs[nsec, 2 * x + c] = total.astype(BF16)
            return
        for n in range(2):
            with scope(f"wait_b{n}"):
                await_bytes(b_buf.at[s, n, pl.ds(0, nx - 1)], ph_r.at[1, n, s % 2 if isinstance(s, int) else lax.rem(s, 2)])
            with scope(f"a_mm{n}"):
                for j in range(hj):
                    total = xs[s, n * hj + j].astype(F32)
                    for k in range(nx):
                        total = total + b_buf[s, n, k, j].astype(F32)
                    xs[s - 1, n * hj + j] = total.astype(BF16)
                if n == 0:
                    for l in range(2):
                        a_acc[l] = a_part(s - 1, l, 0)
        for l in range(2):
            with scope(f"a_last{l}"):
                a_half(s - 1, l, a_acc[l] + a_part(s - 1, l, 1))

    @pl.when(core == 1)
    def _():
        plan = [
            (1, top_first), (2, top_second), (2, li_first), (4, all_met), (4, top_third), (5, first_out_term), (6, li_second),
            (6, stage_c), (7, stage_d), (7, top_fourth),
        ]
        plan += [(half if d else 5, lambda d=d: turn(d)) for d in (0, -1, 1) if d % tiles != tiles // 2]
        for k in range(1, half + 1):
            with scope(f"hop{k}"):
                if k == 1:
                    blocks = ((1, 1, 0), (0, 1, 0), (1, 1, 1))
                elif k == 2:
                    blocks = ((1, 2, 0), (0, 1, 1), (1, 2, 1))
                else:
                    blocks = ((1, k, 0), (0, k - 1, 0), (1, k, 1), (0, k - 1, 1))
                for b in blocks:
                    hop(*b)
            with scope(f"stage{k}"):
                for at, f in plan:
                    if min(at, half) == k:
                        f()
        early = [d for d in (0, -1, 1) if d % tiles != tiles // 2]
        with scope("top_end"):
            await_bytes(xs.at[0, pl.ds(0, 2 * (nx - 1))], top_r.at[3])
            for l in range(2):
                for d in early:
                    a_tile(l, d, True)
        with scope("gather_out"):
            hop(0, half, 0)
            await_last(1)
        with scope("a_first"):
            for l in range(2):
                a_tile(l, tiles // 2, False)
                a_half(top - 1, l)
        with scope("hop_end"):
            hop(0, half, 1)
            turn(tiles // 2)
        with scope("gather_in"):
            await_last(0)
        li_third()

        def step(i, carry):
            application(top - 1 - i, False)
            return carry

        lax.fori_loop(0, top - 1, step, 0)
        application(0, True)

        with scope("t_z0"):
            last_z()
            release(1)
        with scope("t_terms"):
            in_term(1)
            for t in range(min(top, 4), 2, -1):
                await_up(t)
                out_term(t)
        with scope("t_in0"):
            in_term(0)
        with scope("t_near"):
            await_bytes(up.at[pl.ds(0, near_tiles - 2)], uz_r.at[0])
            last_x(0)
        with scope("t_up2"):
            await_up(2)
            out_term(2)
        with scope("t_far"):
            await_bytes(up.at[pl.ds(0, far_tiles)], uz_r.at[nsec])
            last_x(1)
        with scope("t_up1"):
            await_up(1)
            out_term(1)

    def await_z(t):
        await_bytes(up.at[pl.ds(0, block)], uz_r.at[t])

    def spread_x(t):
        await_z(t)
        pl.semaphore_wait(go.at[t], 1)
        src = up.at[pl.ds(slot(t, x), block)]
        for d in x_order:
            send(src, src, out_s.at[0], ux_r.at[t], dev(x_=xat(d)))

    def spread_core(t):
        await_bytes(up.at[pl.ds(0, (nx - 1) * block)], ux_r.at[t])
        src = up.at[pl.ds(slot(t, 0), nx * block)]
        send(src, src, out_s.at[2], ud_r.at[t], dev(core_=1))

    @pl.when(core == 0)
    def _():
        spread_pre()
        for r in range(half - 1):
            meet(r)
        pl.semaphore_signal(near.at[half - 1], inc=1, device_id=dev(core_=1), device_id_type=MESH_ID)
        pa_first()
        li_first()
        pa_second()
        stage_b()
        og_in.wait()
        first_out_term()
        li_second()
        li_third()
        await_bytes(g_top, top_r.at[4])
        first_in_term()

        def move(i, carry):
            t = top - i
            with scope("s_x"):
                spread_x(t)
            with scope("s_in"):
                @pl.when(t < top)
                def _():
                    in_term(t)

            with scope("s_core"):
                spread_core(t)
            with scope("s_out"):
                out_term(t)
            return carry

        lax.fori_loop(0, top - 2, move, 0)
        with scope("s_x21"):
            spread_x(2)
            spread_x(1)
        with scope("s_in"):
            for t in (2, 1, 0):
                in_term(t)
        with scope("s_core2"):
            spread_core(2)
            out_term(2)
        with scope("s_core1"):
            spread_core(1)
        with scope("s_out1"):
            out_term(1)

        @pl.when(x == 0)
        def _():
            with scope("s_near"):
                await_bytes(up.at[pl.ds(0, nx * near_tiles)], ux_r.at[0])
                last_out(0)
            with scope("s_far"):
                await_bytes(up.at[pl.ds(0, nx * far_tiles)], ux_r.at[nsec])
                last_out(1)

    def size(*shape):
        return math.prod(shape) // (8 * LANES)

    li_block, row = size(tok, width), size(fb, tok)
    both_cores = size(2, fb, fe) + nsec * row
    by_core = (
        size(2, fb, fe) + row + size(2, half, 8, nsec * fb) + nx * size(2, 2, tiles, 8, LANES) + top * (nx - 1) * block,
        size(nz, 8, nsec * fb)
        + size(nsec, 2, tiles, 8, LANES)
        + 3 * size(4 * fb, tok)
        + (nx - 1) * 2 * nz
        + (nz - 1) * 2
        + (nx - 1) * 2
        + row
        + top * 2 * 3 * size(8, hu)
        + (top - 1) * 2 * (nx - 1) * hj
        + (nx - 1) * 2
        + top * (2 * nz - 1)
        + nsec * block - 2
        + block,
    )
    with scope("drain"):
        await_bytes(spare.at[pl.ds(0, (nx + (3 if ring else 1)) * li_block)], out_s.at[1])

        @pl.when(core == 1)
        def _():
            for way in range(2):
                await_bytes(wbuf.at[0, :, :, pl.ds(0, nz - 1)], wz_s.at[way])
            await_bytes(spare.at[pl.ds(0, both_cores + by_core[1])], out_s.at[0])

        @pl.when(core == 0)
        def _():
            await_bytes(spare.at[pl.ds(0, top * nx * block)], out_s.at[2])

        for h in range(2):
            @pl.when((core == 0) & (yhi == h))
            def _():
                pa_tiles = 2 * (half - 1 + h) * size(8, nsec * fb)
                await_bytes(spare.at[pl.ds(0, both_cores + by_core[0] + pa_tiles)], out_s.at[0])


def finish(ig, gi, go, ig_out, gi_out, go_out, sems):
    copies = [pltpu.make_async_copy(src, dst, sems.at[k]) for k, (src, dst) in enumerate(((ig, ig_out), (gi, gi_out), (go, go_out)))]
    for cp in copies:
        cp.start()
    for cp in copies:
        cp.wait()


def body(layer_inputs, pre_act, out_grad, w_in, w_out):
    nz, nx = lax.axis_size("z"), lax.axis_size("x")
    nsec = 2 * nx
    tok, width = out_grad.shape
    fb = w_in.shape[2]
    hid = pre_act.shape[2]
    fe = width // 2
    tiles = nz * fb // LANES
    half = nz // 2
    dma = pltpu.SemaphoreType.DMA
    vmem = pltpu.VMEM
    spare = 2048
    scratch = [
        vmem((2, fb, width), BF16),
        vmem((2, 2, 2, nz, fb, fe), BF16),
        vmem((2, nz, 8, hid), BF16),
        vmem((2, 2, half, 8, hid), BF16),
        vmem((nx, 2, 2, tiles, 8, LANES), BF16),
        vmem((2, nsec, 2, tiles, 8, LANES), BF16),
        vmem((nsec, 2, 2 * tiles, 8, LANES), F32),
        vmem((nsec, fb, tok), BF16),
        vmem((nsec, fb, tok), BF16),
        vmem((2, 2, fb, tok), BF16),
        vmem((nsec, fb, tok), BF16),
        vmem((2, nx, tok, width), BF16),
        vmem((nz, 8, width), BF16),
        vmem((4, 4 * fb, tok), BF16),
        vmem((nx, nz, 2, 8, LANES), BF16),
        vmem((nx, nz, 2, 8, LANES), BF16),
        vmem((nz, 2, 8, LANES), BF16),
        vmem((nz, 2, 8, LANES), BF16),
        vmem((fb, tok), BF16),
        vmem((fb, tok), BF16),
        vmem((2, 2 * tiles, fe, LANES), BF16),
        vmem((nsec + 1, nsec, 8, LANES), BF16),
        vmem((nsec, 2, 4, 8, 2 * nz * fb), BF16),
        vmem((nsec, 2, nx, nx, 8, LANES), BF16),
        vmem((2, 8, 2 * nz * fb), F32),
        vmem((2, 8, fe // 2), F32),
        vmem((nsec, 2, 2 * tiles, 8, LANES), BF16),
        vmem((nsec * nz, 8, LANES), BF16),
        vmem((LANES, tok), F32),
        vmem((nsec * nx * 4 * nz, 8, LANES), BF16),
        vmem((spare, 8, LANES), BF16),
        dma((7,)),
        dma((3,)), dma((2,)),
        dma((2, 2)),
        dma((2,)),
        dma((half, 2, 2)),
        dma((6,)),
        dma((1,)),
        dma((5,)),
        dma((2, 2, 2)),
        dma((5,)),
        dma((nsec,)),
        dma((nsec + 1,)),
        dma((nsec + 1,)),
        dma((nsec,)),
        pltpu.SemaphoreType.REGULAR((nsec,)),
        pltpu.SemaphoreType.REGULAR((half,)),
    ]
    hbm, on_chip = pl.BlockSpec(memory_space=pltpu.HBM), pl.BlockSpec(memory_space=pltpu.VMEM)
    shapes = (
        jax.ShapeDtypeStruct((nz, 8, width), BF16),
        jax.ShapeDtypeStruct((fb, width), F32),
        jax.ShapeDtypeStruct((fb, width), F32),
    )
    operands = (
        layer_inputs.reshape(tok, width),
        pre_act.reshape(nz, 8, hid),
        out_grad.reshape(nz, 8, width),
        w_in.reshape(fb, width),
        w_out.reshape(fb, width),
    )
    results = pl.pallas_call(
        kernel,
        out_shape=shapes,
        in_specs=[hbm] * 5,
        out_specs=(on_chip,) * 3,
        scratch_shapes=scratch,
        name="chain",
        compiler_params=pltpu.CompilerParams(
            collective_id=0, has_side_effects=True, vmem_limit_bytes=40 * 1024 * 1024
        ),
    )(*(pltpu.with_memory_space_constraint(v, pltpu.HBM) for v in operands))
    ig, gi, go = pl.pallas_call(
        finish,
        out_shape=shapes,
        in_specs=[on_chip] * 3,
        out_specs=(hbm,) * 3,
        scratch_shapes=[dma((3,))],
        name="finish",
    )(*(pltpu.with_memory_space_constraint(v, pltpu.VMEM) for v in results))
    return (
        ig.reshape(1, tok, width),
        gi.reshape(1, 1, fb, width),
        go.reshape(1, 1, fb, width),
    )


def solution(mesh):
    shape = mesh.shape
    split = Mesh(
        mesh.devices.reshape(shape["section"] // 2, 2, shape["dp"] // 2, 2, shape["mp"]), AXES
    )
    sec, dp = ("x", "core"), ("z", "ylo")
    placed = (
        P(sec, None, "yhi"),
        P(sec, None, dp),
        P(None, "yhi"),
        P(dp, sec, None, "yhi"),
        P(dp, sec, None, "yhi"),
    )
    return jax.shard_map(
        body,
        mesh=split,
        in_specs=placed,
        out_specs=(P(sec, None, "yhi"), P(dp, sec, None, "yhi"), P(dp, sec, None, "yhi")),
        check_vma=False,
    )
```

```python
import contextlib
import math

import jax
import jax.numpy as jnp
from jax import lax
from jax.experimental import pallas as pl
from jax.experimental.pallas import tpu as pltpu
from jax.sharding import Mesh
from jax.sharding import PartitionSpec as P

AXES = ("x", "core", "z", "ylo", "yhi")
MESH_ID = pl.DeviceIdType.MESH
BF16, F32 = jnp.bfloat16, jnp.float32
LANES = 128
PROFILE = False


def scope(name):
    return jax.named_scope(name) if PROFILE else contextlib.nullcontext()


def gelu_parts(v):
    cdf = 0.5 * (1.0 + lax.erf(v * 0.7071067811865476))
    dens = jnp.exp(-0.5 * v * v) * 0.3989422804014327
    return cdf, dens


def kernel(
    li_hbm, pa_hbm, og_hbm, wi_hbm, wo_hbm,
    ig_out, gi_out, go_out,
    w_own, wbuf, pa, pa_all, pb, pc, slope, pa_t, pre_t, pre_top, hall, li, og,
    a_top, b_top, r_top, q_top, z_top, g_top, g_pass,
    w_t, xs, a_buf, b_buf, a_acc, b_acc, gbuf, gz, gt, up,
    spare, lsem, out_s, wz_s, wx_r, wd_r, wz_r, st_r, pt_r, top_r, ph_r, li_r, g_r, uz_r, ux_r, ud_r, last_r, go, near,
):
    nx, nz = lax.axis_size("x"), lax.axis_size("z")
    nsec = 2 * nx
    top = nsec - 1
    fb, width = wi_hbm.shape
    fe = width // 2
    tok = nz * 8
    tiles = nz * fb // LANES
    per_tile = LANES // fb
    x, core, z = lax.axis_index("x"), lax.axis_index("core"), lax.axis_index("z")
    ylo, yhi = lax.axis_index("ylo"), lax.axis_index("yhi")
    sec = x * 2 + core
    y = yhi * 2 + ylo
    other = 1 - ylo
    partner = yhi * 2 + other

    def dev(x_=None, core_=None, z_=None, y_=None):
        y_ = y if y_ is None else y_
        return (
            x if x_ is None else x_,
            core if core_ is None else core_,
            z if z_ is None else z_,
            lax.rem(y_, 2),
            y_ // 2,
        )

    def send(src, dst, ssem, rsem, to):
        cp = pltpu.make_async_remote_copy(
            src_ref=src, dst_ref=dst, send_sem=ssem, recv_sem=rsem, device_id=to, device_id_type=MESH_ID
        )
        cp.start()
        return cp

    def await_bytes(ref, sem):
        pltpu.make_async_copy(ref, ref, sem).wait()

    def zat(d):
        return lax.rem(z + d + nz, nz)

    def xat(d):
        return lax.rem(x + d + nx, nx)

    def yat(d):
        return lax.rem(y + d, 4)

    y_order = (2, 1, 3)
    x_order = sorted(range(1, nx), key=lambda d: -min(d, nx - d))
    z_order = sorted(range(1, nz), key=lambda d: -min(d, nz - d))
    sections = [(d, False) for d in x_order] + [(d, True) for d in x_order] + [(0, True)]

    def peer(d, cross):
        return xat(d), (1 - core if cross else core)

    mine = pl.ds(pl.multiple_of(ylo * fe, LANES), fe)
    theirs = pl.ds(pl.multiple_of(other * fe, LANES), fe)

    w_hbm = (wi_hbm, wo_hbm)
    pa_in = pltpu.make_async_copy(pa_hbm, pa.at[core], lsem.at[0])
    w_in_ = [pltpu.make_async_copy(w_hbm[m].at[:, mine], wbuf.at[m, ylo, 1, z], lsem.at[1 + m]) for m in range(2)]
    og_in = pltpu.make_async_copy(og_hbm, og, lsem.at[3])
    li_in = pltpu.make_async_copy(li_hbm, li.at[core, x], lsem.at[4])
    barrier = pltpu.get_barrier_semaphore()
    greeted = [dev(z_=zat(d)) for d in (1, -1)] + [dev(*peer(*p)) for p in sections]
    greeted += [dev(y_=yat(d)) for d in range(1, 4)] + [dev(core_=1 - core, y_=partner)]
    for to in greeted:
        pl.semaphore_signal(barrier, inc=1, device_id=to, device_id_type=MESH_ID)

    first = (1, 0)
    own_in = [pltpu.make_async_copy(w_hbm[m], w_own.at[m], lsem.at[5 + m]) for m in range(2)]
    for m in first:
        own_in[m].start()

        @pl.when(core == 1)
        def _():
            w_in_[m].start()

    pa_in.start()

    og_in.start()
    li_in.start()

    with scope("barrier"):
        pl.semaphore_wait(barrier, len(greeted))

    half = nz // 2

    def meet(r):
        for d in (1, -1):
            pl.semaphore_signal(near.at[r], inc=1, device_id=dev(z_=zat(d)), device_id_type=MESH_ID)
        pl.semaphore_wait(near.at[r], 2)

    def pa_first():
        await_bytes(pa.at[1], st_r.at[5])
        for h in range(2):
            @pl.when(yhi == h)
            def _():
                for d in z_order:
                    if d % 2 == h:
                        for c in range(2):
                            dst = pa_all.at[c, lax.rem(z, 2), z // 2]
                            send(pa.at[c, zat(d)], dst, out_s.at[0], st_r.at[0], dev(z_=zat(d)))
                if h == 0:
                    for c in range(2):
                        pa_all[c, lax.rem(z, 2), z // 2] = pa[c, z]

    def await_pa(sem):
        for h in range(2):
            @pl.when(yhi == h)
            def _():
                await_bytes(pa.at[0, pl.ds(0, 2 * (half - 1 + h))], sem)

    def pa_second():
        await_pa(st_r.at[0])
        mine_ = pa_all.at[:, lax.rem(z + yhi, 2)]
        send(mine_, mine_, out_s.at[0], st_r.at[4], dev(y_=yat(2)))

    def ring_send(src, m, l, k, way):
        send(src, src, wz_s.at[way], wz_r.at[k - 1, m, l], dev(z_=zat(1 if way == 0 else -1)))

    swaps = []
    for m in first:
        own_in[m].wait()

        @pl.when(core == 0)
        def _():
            send(w_own.at[m, :, mine], wbuf.at[m, ylo, 0, z], out_s.at[0], wd_r.at[m], dev(core_=1))

        @pl.when(core == 1)
        def _():
            w_in_[m].wait()
            for way in range(2):
                ring_send(wbuf.at[m, ylo, 1, z], m, ylo, 1, way)

        dst = wbuf.at[m, ylo, core, z]
        swaps.append(send(w_own.at[m, :, theirs], dst, out_s.at[0], wx_r.at[core, m], dev(core_=1, y_=partner)))

    pa_in.wait()

    @pl.when(core == 1)
    def _():
        send(pa.at[1], pa.at[1], out_s.at[0], st_r.at[5], dev(core_=0))

    v = pa[core].astype(F32).reshape(tok, nsec * fb)
    pa_t[...] = jnp.swapaxes(v, 0, 1).astype(BF16).reshape(nsec, fb, tok)
    for p in sections:
        to = peer(*p)
        send(pa_t.at[to[0] * 2 + to[1]], pre_t.at[sec], out_s.at[0], st_r.at[3], dev(*to))
    pre_t[sec] = pa_t[sec]

    def spread_pre():
        await_bytes(pre_t.at[pl.ds(0, nsec - 1)], st_r.at[3])
        dst = pre_top.at[ylo, core]
        send(pre_t.at[top], dst, out_s.at[0], pt_r.at[0], dev(core_=1, y_=partner))

        @pl.when(core == 0)
        def _():
            send(pre_t.at[top], dst, out_s.at[0], pt_r.at[0], dev(core_=1))

        @pl.when(core == 1)
        def _():
            dst[...] = pre_t[top]

    def stage_b():
        await_bytes(pa_all.at[:, 0], st_r.at[4])
        group = lax.broadcasted_iota(jnp.int32, (8, LANES), 1) // fb
        for c in range(2):
            for ct in range(nsec // per_tile):
                for t in range(tiles):
                    out = [jnp.zeros((8, LANES), F32)] * per_tile
                    for j in range(per_tile):
                        at = t * per_tile + j
                        v = pa_all[c, at % 2, at // 2, :, ct * LANES:(ct + 1) * LANES].astype(F32)
                        for k in range(per_tile):
                            shift = (j - k) * fb % LANES
                            r = pltpu.roll(v, shift, 1) if shift else v
                            out[k] = jnp.where(group == j, r, out[k])
                    for k in range(per_tile):
                        to = ct * per_tile + k
                        pb[to // 2, c, to % 2, t] = out[k].astype(BF16)
        for d in x_order + [0]:
            send(pb.at[xat(d)], pc.at[ylo, pl.ds(2 * x, 2)], out_s.at[0], st_r.at[1], dev(x_=xat(d), core_=1))

    cut = tok // 2
    lo, hi = pl.ds(0, cut), pl.ds(cut, cut)
    ring = nx > 2

    def li_first():
        li_in.wait()
        src = li.at[core, x]
        send(src, src, out_s.at[1], li_r.at[0], dev(x_=xat(1)))
        if ring:
            send(src, src, out_s.at[1], li_r.at[1], dev(x_=xat(-1)))

    def li_second():
        await_bytes(li.at[0, 0], li_r.at[0])
        if ring:
            src = li.at[core, xat(-1), lo]
            send(src, src, out_s.at[1], li_r.at[2], dev(x_=xat(1)))
            await_bytes(li.at[0, 0], li_r.at[1])
            src = li.at[core, xat(1), hi]
            send(src, src, out_s.at[1], li_r.at[3], dev(x_=xat(-1)))

    def li_third():
        if ring:
            await_bytes(li.at[0, 0, lo], li_r.at[2])
            await_bytes(li.at[0, 0, hi], li_r.at[3])
        send(li.at[core], li.at[core], out_s.at[1], li_r.at[4], dev(core_=1 - core))

    def first_out_term():
        for s in range(nsec):
            v = pre_t[s].astype(F32)
            hall[s] = (v * gelu_parts(v)[0]).astype(BF16)
        go_out[...] = jnp.dot(hall[top], og[...].reshape(tok, width), preferred_element_type=F32)

    def first_in_term():
        await_bytes(li.at[0], li_r.at[4])
        gi_out[...] = jnp.dot(g_top[...], li[top % 2, top // 2], preferred_element_type=F32)

    block = 4 * nz

    def slot(t, x_, ylo_=0, z_=0):
        return ((((t * nx + x_) * 2 + ylo_) * nz) + z_) * 2

    def columns(t, x_, l):
        return up[pl.ds(slot(t, x_, l), 2 * nz)].reshape(nz, 2, 8, LANES)

    def out_term(t):
        rows = hall[t - 1]
        for l in range(2):
            parts = []
            for k in range(nx):
                v = columns(t, k, l)
                parts += [v[:, c].reshape(tok, LANES) for c in range(2)]
            go_out[:, l * fe:(l + 1) * fe] += jnp.dot(rows, jnp.concatenate(parts, axis=1), preferred_element_type=F32)

        @pl.when(sec == t)
        def _():
            for l in range(2):
                for k in range(nx):
                    v = columns(t, k, l)
                    for c in range(2):
                        at = l * fe + (2 * k + c) * LANES
                        ig_out[:, :, at:at + LANES] = v[:, c]

    def in_term(t):
        @pl.when(core == 1)
        def _():
            await_bytes(gz.at[pl.ds(0, nz - 1)], g_r.at[t])

        @pl.when(core == 0)
        def _():
            await_bytes(gz.at[pl.ds(0, nz)], g_r.at[t])

        gt[...] = jnp.swapaxes(gz[pl.ds(t * nz, nz)].astype(F32).reshape(tok, LANES), 0, 1)
        rows = gt[pl.ds(pl.multiple_of(lax.rem(z, per_tile) * fb, fb), fb), :].astype(BF16)
        gi_out[...] += jnp.dot(rows, li[lax.rem(t, 2), t // 2], preferred_element_type=F32)

    hu, hn, hj = 2 * nz * fb, fe // 2, nsec // 2
    def hop(m, k, which):
        l = ylo if which == 0 else other
        if k == 1:
            if which == 0:
                await_bytes(wbuf.at[m, 0, 0, 0], wd_r.at[m])
            else:
                for c in range(2):
                    await_bytes(wbuf.at[m, 0, 0, 0], wx_r.at[c, m])
        if k > 1:
            await_bytes(wbuf.at[m, 0, :, pl.ds(0, 2)], wz_r.at[k - 2, m, l])
        for way, step in ((0, 1), (1, -1)):
            if k == 1 and which == 0:
                ring_send(wbuf.at[m, l, 0, z], m, l, 1, way)
            elif k == half:
                ring_send(wbuf.at[m, l, way, zat(-step * (k - 1))], m, l, k, way)
            else:
                ring_send(wbuf.at[m, l, :, zat(-step * (k - 1))], m, l, k, way)

    def await_last(m):
        for l in range(2):
            await_bytes(wbuf.at[m, 0, :, 0], wz_r.at[half - 1, m, l])

    def all_met():
        pl.semaphore_wait(near.at[half - 1], 1)

    def stage_c():
        await_bytes(pc.at[0], st_r.at[1])
        send(pc.at[ylo], pc.at[ylo], out_s.at[0], st_r.at[2], dev(y_=partner))

    def stage_d():
        await_bytes(pc.at[0], st_r.at[2])

        def one(s, carry):
            for l in range(2):
                v = pc[l, s].astype(F32)
                cdf, dens = gelu_parts(v)
                slope[s, l] = (cdf + v * dens).reshape(2 * tiles, 8, LANES)
            return carry

        lax.fori_loop(0, top, one, 0)

    def top_first():
        og_in.wait()
        rows = wbuf[1, :, :, z].reshape(4 * fb, fe)
        a_top[y] = lax.dot_general(
            rows, og[:, :, mine].reshape(tok, fe), (((1,), (1,)), ((), ())), preferred_element_type=F32
        ).astype(BF16)
        for d in y_order:
            send(a_top.at[y], a_top.at[y], out_s.at[0], top_r.at[0], dev(y_=yat(d)))
        spread_pre()

    def top_second():
        await_bytes(pre_t.at[pl.ds(0, 3)], pt_r.at[0])
        v = pre_top[...].astype(F32).reshape(4 * fb, tok)
        cdf, dens = gelu_parts(v)
        await_bytes(a_top.at[pl.ds(0, 3)], top_r.at[0])
        back = a_top[0].astype(F32)
        for k in range(1, 4):
            back = back + a_top[k].astype(F32)
        g = (back * (cdf + v * dens)).astype(BF16)
        g_pass[...] = jnp.where(ylo == 0, g[:fb], g[2 * fb:3 * fb])
        send(g_pass, g_top, out_s.at[0], top_r.at[4], dev(core_=0))
        g_top[...] = jnp.where(ylo == 0, g[fb:2 * fb], g[3 * fb:])
        rows = jnp.swapaxes(g.astype(F32), 0, 1).astype(BF16)
        part = jnp.dot(rows, wbuf[0, :, :, z].reshape(4 * fb, fe), preferred_element_type=F32).astype(BF16)
        for j in range(nsec):
            b_top[j // 2, :, j % 2] = part[:, j * LANES:(j + 1) * LANES].reshape(nz, 8, LANES)
        for d in x_order:
            send(b_top.at[xat(d)], r_top.at[x], out_s.at[0], top_r.at[1], dev(x_=xat(d)))
        r_top[x] = b_top[x]

    def top_third():
        await_bytes(r_top.at[pl.ds(0, nx - 1)], top_r.at[1])
        total = r_top[0].astype(F32)
        for k in range(1, nx):
            total = total + r_top[k].astype(F32)
        q_top[...] = total.astype(BF16)
        for d in z_order:
            send(q_top.at[zat(d)], z_top.at[z], out_s.at[0], top_r.at[2], dev(z_=zat(d)))
        z_top[z] = q_top[z]

    own = pl.ds(2 * x, 2)

    def top_fourth():
        await_bytes(z_top.at[pl.ds(0, nz - 1)], top_r.at[2])
        for c in range(2):
            at = pl.multiple_of(ylo * fe + (2 * x + c) * LANES, LANES)
            total = og[z, :, pl.ds(at, LANES)].astype(F32)
            for k in range(nz):
                total = total + z_top[k, c].astype(F32)
            xs[top - 1, 2 * x + c] = total.astype(BF16)
        src = xs.at[top - 1, own]
        for d in x_order:
            send(src, src, out_s.at[0], top_r.at[3], dev(x_=xat(d)))

    def spread_z(t):
        src = xs.at[t - 1, own]
        dst = up.at[pl.ds(slot(t, x, ylo, z), 2)]

        def both(d):
            for to in (partner, y):
                send(src, dst, out_s.at[0], uz_r.at[t], dev(core_=0, z_=zat(d), y_=to))

        both(half)

        def pair(i, c):
            both(half - i)
            both(half + i)
            return c

        lax.fori_loop(1, half, pair, 0)
        both(0)

    bounds = sorted({half // 2, 3 * half // 4, half})
    groups = [
        [r for r in range(nz) if (bounds[i - 1] if i else -1) < min(r, nz - r) <= b] for i, b in enumerate(bounds)
    ]
    group_of = {r: i for i, g in enumerate(groups) for r in g}

    def runs(g):
        out = []
        for r in g:
            if out and out[-1][1] == r:
                out[-1][1] = r + 1
            else:
                out.append([r, r + 1])
        return out

    def last_z():
        src = xs.at[nsec, own]
        for d in [half] + [d for i in range(1, half) for d in (half - i, half + i)] + [0]:
            r = (nz - d) % nz
            dst = up.at[pl.ds(slot(0, x, ylo, r), 2)]
            for to in (partner, y):
                if d or to is partner:
                    send(src, dst, out_s.at[0], last_r.at[0, group_of[r]], dev(z_=zat(d), y_=to))
        up[pl.ds(slot(0, x, ylo, 0), 2)] = src[...]

    def last_x(i):
        await_bytes(up.at[pl.ds(0, 4 * len(groups[i]) - (2 if i == 0 else 0))], last_r.at[0, i])
        for l in range(2):
            for a, b in runs(groups[i]):
                src = up.at[pl.ds(slot(0, x, l, a), 2 * (b - a))]
                send(src, src, out_s.at[0], last_r.at[1, i], dev(x_=0, core_=0))

    def last_out(i):
        await_bytes(up.at[pl.ds(0, nx * 4 * len(groups[i]))], last_r.at[1, i])
        for r in groups[i]:
            row = zat(r)
            for l in range(2):
                for k in range(nx):
                    for c in range(2):
                        at = l * fe + (2 * k + c) * LANES
                        ig_out[row, :, at:at + LANES] = up[slot(0, k, l, r) + c]

    def spread_g(t):
        def to(d, c):
            tile = zat(d) // per_tile
            for c_ in range(2):
                send(gbuf.at[t, ylo, c_ * tiles + tile], gz.at[t * nz + z], out_s.at[0], g_r.at[t], dev(core_=c_, z_=zat(d)))
            return c

        lax.fori_loop(1, nz, to, 0)
        tile = z // per_tile
        send(gbuf.at[t, ylo, tile], gz.at[t * nz + z], out_s.at[0], g_r.at[t], dev(core_=0))
        gz[t * nz + z] = gbuf[t, ylo, tiles + tile]

    def turn(away):
        t = lax.rem(z // per_tile + away + tiles, tiles)

        def one(i, c):
            l, c_ = i // 2, lax.rem(i, 2)
            v = wbuf[1, l, c_, pl.ds(t * per_tile, per_tile)].reshape(LANES, fe)
            w_t[l, c_ * tiles + t] = jnp.swapaxes(v, 0, 1)
            return c

        lax.fori_loop(0, 4, one, 0)

    def a_half(s, l, part=None):
        if part is not None:
            a_buf[s, l, y] = part.astype(BF16)
        for d in y_order:
            send(a_buf.at[s, l, y], a_buf.at[s, l, y], out_s.at[0], ph_r.at[0, l, s % 2 if isinstance(s, int) else lax.rem(s, 2)], dev(y_=yat(d)))

    def a_part(s, l, n):
        lhs = jnp.concatenate([xs[s, n * hj + j] for j in range(hj)], axis=1)
        w_out = jnp.concatenate([w_t[l, t, n * hn:(n + 1) * hn] for t in range(2 * tiles)], axis=1)
        return jnp.dot(lhs, w_out, preferred_element_type=F32)

    def a_tile(l, away, turned):
        lhs = jnp.concatenate([xs[top - 1, j] for j in range(nsec)], axis=1)
        t = lax.rem(z // per_tile + away + tiles, tiles)
        if turned:
            w_out = jnp.concatenate([w_t[l, c * tiles + t] for c in range(2)], axis=1)
            part = jnp.dot(lhs, w_out, preferred_element_type=F32)
        else:
            w_out = wbuf[1, l, :, pl.ds(t * per_tile, per_tile)].reshape(2 * LANES, fe)
            part = lax.dot_general(lhs, w_out, (((1,), (1,)), ((), ())), preferred_element_type=F32)
        for c in range(2):
            at = pl.multiple_of((c * tiles + t) * LANES, LANES)
            a_buf[top - 1, l, y, :, pl.ds(at, LANES)] = part[:, c * LANES:(c + 1) * LANES].astype(BF16)

    def release(t):
        pl.semaphore_signal(go.at[t], inc=1, device_id=dev(core_=0), device_id_type=MESH_ID)

    def await_up(t):
        await_bytes(up.at[pl.ds(0, nx * block)], ud_r.at[t])

    def background_a(s):
        with scope("bg_a"):
            @pl.when(s <= top - 3)
            def _():
                release(s + 2)

            @pl.when(s <= top - 2)
            def _():
                spread_z(s + 1)

            @pl.when(s == top - 2)
            def _():
                first_in_term()

            @pl.when(s <= top - 3)
            def _():
                in_term(s + 2)

            @pl.when(s <= top - 4)
            def _():
                await_up(s + 4)
                out_term(s + 4)

    def g_half(s, l):
        with scope(f"wait_a{l}"):
            await_bytes(a_buf.at[s, l, pl.ds(0, 3)], ph_r.at[0, l, s % 2 if isinstance(s, int) else lax.rem(s, 2)])
        back = a_buf[s, l, 0].astype(F32)
        for k in range(1, 4):
            back = back + a_buf[s, l, k].astype(F32)
        g = []
        for t in range(2 * tiles):
            g_tile = (back[:, t * LANES:(t + 1) * LANES] * slope[s, l, t]).astype(BF16)
            gbuf[s, l, t] = g_tile
            g.append(g_tile)
        return jnp.concatenate(g, axis=1)

    def b_tile(n, away):
        t = lax.rem(z // per_tile + away + tiles, tiles)
        pairs = [(l, c) for l in range(2) for c in range(2)]
        lhs = jnp.concatenate([gbuf[top - 1, l, c * tiles + t] for l, c in pairs], axis=1)
        rows = pl.ds(t * per_tile, per_tile)
        w_in = jnp.concatenate([wbuf[0, l, c, rows, :, n * hn:(n + 1) * hn].reshape(LANES, hn) for l, c in pairs], axis=0)
        return jnp.dot(lhs, w_in, preferred_element_type=F32)

    def application(s, final=False, begin=False):
        if not begin:
            background_a(s)
            g_first = g_half(s, 0)
            for n in range(2):
                w_in = wbuf[0, 0, :, :, :, n * hn:(n + 1) * hn].reshape(hu, hn)
                b_acc[n] = jnp.dot(g_first, w_in, preferred_element_type=F32)
            g = g_half(s, 1)
        for n in range(2):
            if begin:
                part = b_tile(n, tiles // 2)
            else:
                w_in = wbuf[0, 1, :, :, :, n * hn:(n + 1) * hn].reshape(hu, hn)
                part = jnp.dot(g, w_in, preferred_element_type=F32)
            part = (b_acc[n] + part).astype(BF16)
            for j in range(hj):
                b_buf[s, n, x, j] = part[:, j * LANES:(j + 1) * LANES]
            if not final:
                src = b_buf.at[s, n, x]
                for d in x_order:
                    send(src, src, out_s.at[0], ph_r.at[1, n, s % 2 if isinstance(s, int) else lax.rem(s, 2)], dev(x_=xat(d)))
        hx = nx // 2
        if final:
            for d in x_order:
                to = xat(d)
                src = b_buf.at[s, to // hx, x, pl.ds(2 * lax.rem(to, hx), 2)]
                send(src, src, out_s.at[0], ph_r.at[1, 0, s % 2], dev(x_=to))

        with scope("bg_b"):
            spread_g(s)
            if begin:
                spread_z(top)

        if final:
            with scope("wait_b"):
                await_bytes(gz.at[pl.ds(0, 2 * (nx - 1))], ph_r.at[1, 0, s % 2])
            for c in range(2):
                total = xs[s, 2 * x + c].astype(F32)
                for k in range(nx):
                    total = total + b_buf[s, x // hx, k, 2 * lax.rem(x, hx) + c].astype(F32)
                xs[nsec, 2 * x + c] = total.astype(BF16)
            return
        for n in range(2):
            with scope(f"wait_b{n}"):
                await_bytes(b_buf.at[s, n, pl.ds(0, nx - 1)], ph_r.at[1, n, s % 2 if isinstance(s, int) else lax.rem(s, 2)])
            with scope(f"a_mm{n}"):
                for j in range(hj):
                    total = xs[s, n * hj + j].astype(F32)
                    for k in range(nx):
                        total = total + b_buf[s, n, k, j].astype(F32)
                    xs[s - 1, n * hj + j] = total.astype(BF16)
                if n == 0:
                    for l in range(2):
                        a_acc[l] = a_part(s - 1, l, 0)
        for l in range(2):
            with scope(f"a_last{l}"):
                a_half(s - 1, l, a_acc[l] + a_part(s - 1, l, 1))

    @pl.when(core == 1)
    def _():
        plan = [
            (1, top_first), (2, top_second), (2, li_first), (4, all_met), (4, top_third), (5, first_out_term), (6, li_second),
            (6, stage_c), (7, stage_d), (7, top_fourth),
        ]
        plan += [(half if d else 5, lambda d=d: turn(d)) for d in (0, -1, 1) if d % tiles != tiles // 2]
        for k in range(1, half + 1):
            with scope(f"hop{k}"):
                if k == 1:
                    blocks = ((1, 1, 0), (0, 1, 0), (1, 1, 1))
                elif k == 2:
                    blocks = ((1, 2, 0), (0, 1, 1), (1, 2, 1))
                else:
                    blocks = ((1, k, 0), (0, k - 1, 0), (1, k, 1), (0, k - 1, 1))
                for b in blocks:
                    hop(*b)
            with scope(f"stage{k}"):
                for at, f in plan:
                    if min(at, half) == k:
                        f()
        early = [d for d in (0, -1, 1) if d % tiles != tiles // 2]
        with scope("top_end"):
            await_bytes(xs.at[0, pl.ds(0, 2 * (nx - 1))], top_r.at[3])
            for l in range(2):
                for d in early:
                    a_tile(l, d, True)
        with scope("gather_out"):
            hop(0, half, 0)
            await_last(1)
        with scope("a_first"):
            for l in range(2):
                a_tile(l, tiles // 2, False)
                a_half(top - 1, l)
        with scope("hop_end"):
            hop(0, half, 1)
            turn(tiles // 2)
        with scope("b_early"):
            for l in range(2):
                g_half(top - 1, l)
            for n in range(2):
                b_acc[n] = sum((b_tile(n, d) for d in early), jnp.zeros((8, hn), F32))
        with scope("gather_in"):
            await_last(0)
        li_third()

        application(top - 1, begin=True)

        def step(i, carry):
            application(top - 2 - i)
            return carry

        lax.fori_loop(0, top - 2, step, 0)
        application(0, final=True)

        with scope("t_z0"):
            last_z()
            release(1)
        with scope("t_terms"):
            in_term(1)
            for t in range(min(top, 3), 2, -1):
                await_up(t)
                out_term(t)
        with scope("t_in0"):
            in_term(0)
        for i in range(len(groups)):
            with scope(f"t_last{i}"):
                last_x(i)
        with scope("t_up2"):
            await_up(2)
            out_term(2)
        with scope("t_up1"):
            await_up(1)
            out_term(1)

    def await_z(t):
        await_bytes(up.at[pl.ds(0, block)], uz_r.at[t])

    def spread_x(t):
        await_z(t)
        if not isinstance(t, int) or t < top:
            pl.semaphore_wait(go.at[t], 1)
        src = up.at[pl.ds(slot(t, x), block)]
        for d in x_order:
            send(src, src, out_s.at[0], ux_r.at[t], dev(x_=xat(d)))

    def spread_core(t):
        await_bytes(up.at[pl.ds(0, (nx - 1) * block)], ux_r.at[t])
        src = up.at[pl.ds(slot(t, 0), nx * block)]
        send(src, src, out_s.at[2], ud_r.at[t], dev(core_=1))

    @pl.when(core == 0)
    def _():
        spread_pre()
        for r in range(half - 1):
            meet(r)
        pl.semaphore_signal(near.at[half - 1], inc=1, device_id=dev(core_=1), device_id_type=MESH_ID)
        pa_first()
        li_first()
        pa_second()
        stage_b()
        og_in.wait()
        first_out_term()
        li_second()
        li_third()
        await_bytes(g_top, top_r.at[4])
        first_in_term()

        def finish_one(t):
            with scope("s_core"):
                spread_core(t)
            with scope("s_out"):
                out_term(t)

        def move(i, carry):
            t = top - 1 - i
            with scope("s_x"):
                spread_x(t)
            with scope("s_in"):
                in_term(t)
            finish_one(t + 1)
            return carry

        with scope("s_x7"):
            spread_x(top)
        lax.fori_loop(0, top - 2, move, 0)
        with scope("s_x1"):
            spread_x(1)
        finish_one(2)
        with scope("s_in"):
            for t in (1, 0):
                in_term(t)
        with scope("s_core1"):
            spread_core(1)
        with scope("s_out1"):
            out_term(1)

        @pl.when(x == 0)
        def _():
            for i in range(len(groups)):
                with scope(f"s_last{i}"):
                    last_out(i)

    def size(*shape):
        return math.prod(shape) // (8 * LANES)

    li_block, row = size(tok, width), size(fb, tok)
    both_cores = size(2, fb, fe) + nsec * row
    by_core = (
        size(2, fb, fe) + row + size(2, half, 8, nsec * fb) + nx * size(2, 2, tiles, 8, LANES) + top * (nx - 1) * block,
        size(nz, 8, nsec * fb)
        + size(nsec, 2, tiles, 8, LANES)
        + 3 * size(4 * fb, tok)
        + (nx - 1) * 2 * nz
        + (nz - 1) * 2
        + (nx - 1) * 2
        + row
        + top * 2 * 3 * size(8, hu)
        + (top - 1) * 2 * (nx - 1) * hj
        + (nx - 1) * 2
        + top * (2 * nz - 1)
        + nsec * block - 2
        + block,
    )
    with scope("drain"):
        await_bytes(spare.at[pl.ds(0, (nx + (3 if ring else 1)) * li_block)], out_s.at[1])

        @pl.when(core == 1)
        def _():
            for way in range(2):
                await_bytes(wbuf.at[0, :, :, pl.ds(0, nz - 1)], wz_s.at[way])
            await_bytes(spare.at[pl.ds(0, both_cores + by_core[1])], out_s.at[0])

        @pl.when(core == 0)
        def _():
            await_bytes(spare.at[pl.ds(0, top * nx * block)], out_s.at[2])

        for h in range(2):
            @pl.when((core == 0) & (yhi == h))
            def _():
                pa_tiles = 2 * (half - 1 + h) * size(8, nsec * fb)
                await_bytes(spare.at[pl.ds(0, both_cores + by_core[0] + pa_tiles)], out_s.at[0])


def finish(ig, gi, go, ig_out, gi_out, go_out, sems):
    copies = [pltpu.make_async_copy(src, dst, sems.at[k]) for k, (src, dst) in enumerate(((ig, ig_out), (gi, gi_out), (go, go_out)))]
    for cp in copies:
        cp.start()
    for cp in copies:
        cp.wait()


def body(layer_inputs, pre_act, out_grad, w_in, w_out):
    nz, nx = lax.axis_size("z"), lax.axis_size("x")
    nsec = 2 * nx
    tok, width = out_grad.shape
    fb = w_in.shape[2]
    hid = pre_act.shape[2]
    fe = width // 2
    tiles = nz * fb // LANES
    half = nz // 2
    dma = pltpu.SemaphoreType.DMA
    vmem = pltpu.VMEM
    spare = 2048
    scratch = [
        vmem((2, fb, width), BF16),
        vmem((2, 2, 2, nz, fb, fe), BF16),
        vmem((2, nz, 8, hid), BF16),
        vmem((2, 2, half, 8, hid), BF16),
        vmem((nx, 2, 2, tiles, 8, LANES), BF16),
        vmem((2, nsec, 2, tiles, 8, LANES), BF16),
        vmem((nsec, 2, 2 * tiles, 8, LANES), F32),
        vmem((nsec, fb, tok), BF16),
        vmem((nsec, fb, tok), BF16),
        vmem((2, 2, fb, tok), BF16),
        vmem((nsec, fb, tok), BF16),
        vmem((2, nx, tok, width), BF16),
        vmem((nz, 8, width), BF16),
        vmem((4, 4 * fb, tok), BF16),
        vmem((nx, nz, 2, 8, LANES), BF16),
        vmem((nx, nz, 2, 8, LANES), BF16),
        vmem((nz, 2, 8, LANES), BF16),
        vmem((nz, 2, 8, LANES), BF16),
        vmem((fb, tok), BF16),
        vmem((fb, tok), BF16),
        vmem((2, 2 * tiles, fe, LANES), BF16),
        vmem((nsec + 1, nsec, 8, LANES), BF16),
        vmem((nsec, 2, 4, 8, 2 * nz * fb), BF16),
        vmem((nsec, 2, nx, nx, 8, LANES), BF16),
        vmem((2, 8, 2 * nz * fb), F32),
        vmem((2, 8, fe // 2), F32),
        vmem((nsec, 2, 2 * tiles, 8, LANES), BF16),
        vmem((nsec * nz, 8, LANES), BF16),
        vmem((LANES, tok), F32),
        vmem((nsec * nx * 4 * nz, 8, LANES), BF16),
        vmem((spare, 8, LANES), BF16),
        dma((7,)),
        dma((3,)), dma((2,)),
        dma((2, 2)),
        dma((2,)),
        dma((half, 2, 2)),
        dma((6,)),
        dma((1,)),
        dma((5,)),
        dma((2, 2, 2)),
        dma((5,)),
        dma((nsec,)),
        dma((nsec,)),
        dma((nsec,)),
        dma((nsec,)),
        dma((2, 3)),
        pltpu.SemaphoreType.REGULAR((nsec,)),
        pltpu.SemaphoreType.REGULAR((half,)),
    ]
    hbm, on_chip = pl.BlockSpec(memory_space=pltpu.HBM), pl.BlockSpec(memory_space=pltpu.VMEM)
    shapes = (
        jax.ShapeDtypeStruct((nz, 8, width), BF16),
        jax.ShapeDtypeStruct((fb, width), F32),
        jax.ShapeDtypeStruct((fb, width), F32),
    )
    operands = (
        layer_inputs.reshape(tok, width),
        pre_act.reshape(nz, 8, hid),
        out_grad.reshape(nz, 8, width),
        w_in.reshape(fb, width),
        w_out.reshape(fb, width),
    )
    results = pl.pallas_call(
        kernel,
        out_shape=shapes,
        in_specs=[hbm] * 5,
        out_specs=(on_chip,) * 3,
        scratch_shapes=scratch,
        name="chain",
        compiler_params=pltpu.CompilerParams(
            collective_id=0, has_side_effects=True, vmem_limit_bytes=40 * 1024 * 1024
        ),
    )(*(pltpu.with_memory_space_constraint(v, pltpu.HBM) for v in operands))
    ig, gi, go = pl.pallas_call(
        finish,
        out_shape=shapes,
        in_specs=[on_chip] * 3,
        out_specs=(hbm,) * 3,
        scratch_shapes=[dma((3,))],
        name="finish",
    )(*(pltpu.with_memory_space_constraint(v, pltpu.VMEM) for v in results))
    return (
        ig.reshape(1, tok, width),
        gi.reshape(1, 1, fb, width),
        go.reshape(1, 1, fb, width),
    )


def solution(mesh):
    shape = mesh.shape
    split = Mesh(
        mesh.devices.reshape(shape["section"] // 2, 2, shape["dp"] // 2, 2, shape["mp"]), AXES
    )
    sec, dp = ("x", "core"), ("z", "ylo")
    placed = (
        P(sec, None, "yhi"),
        P(sec, None, dp),
        P(None, "yhi"),
        P(dp, sec, None, "yhi"),
        P(dp, sec, None, "yhi"),
    )
    return jax.shard_map(
        body,
        mesh=split,
        in_specs=placed,
        out_specs=(P(sec, None, "yhi"), P(dp, sec, None, "yhi"), P(dp, sec, None, "yhi")),
        check_vma=False,
    )
```

```python
import contextlib
import math

import jax
import jax.numpy as jnp
from jax import lax
from jax.experimental import pallas as pl
from jax.experimental.pallas import tpu as pltpu
from jax.sharding import Mesh
from jax.sharding import PartitionSpec as P

AXES = ("x", "core", "z", "ylo", "yhi")
MESH_ID = pl.DeviceIdType.MESH
BF16, F32 = jnp.bfloat16, jnp.float32
LANES = 128
PROFILE = False


def scope(name):
    return jax.named_scope(name) if PROFILE else contextlib.nullcontext()


def gelu_parts(v):
    cdf = 0.5 * (1.0 + lax.erf(v * 0.7071067811865476))
    dens = jnp.exp(-0.5 * v * v) * 0.3989422804014327
    return cdf, dens


def kernel(
    li_hbm, pa_hbm, og_hbm, wi_hbm, wo_hbm,
    ig_out, gi_out, go_out,
    w_own, wbuf, pa, pa_all, pb, pc, slope, pa_t, pre_t, pre_top, hall, li, og,
    a_top, b_top, r_top, q_top, z_top, g_top, g_pass,
    w_t, xs, a_buf, b_buf, a_acc, b_acc, gbuf, gz, gt, up,
    spare, lsem, out_s, wz_s, wx_r, wd_r, wz_r, st_r, pt_r, top_r, ph_r, li_r, g_r, ud_r, flag,
):
    nx, nz = lax.axis_size("x"), lax.axis_size("z")
    nsec = 2 * nx
    top = nsec - 1
    fb, width = wi_hbm.shape
    fe = width // 2
    tok = nz * 8
    tiles = nz * fb // LANES
    per_tile = LANES // fb
    x, core, z = lax.axis_index("x"), lax.axis_index("core"), lax.axis_index("z")
    ylo, yhi = lax.axis_index("ylo"), lax.axis_index("yhi")
    sec = x * 2 + core
    y = yhi * 2 + ylo
    other = 1 - ylo
    partner = yhi * 2 + other

    def dev(x_=None, core_=None, z_=None, y_=None):
        y_ = y if y_ is None else y_
        return (
            x if x_ is None else x_,
            core if core_ is None else core_,
            z if z_ is None else z_,
            lax.rem(y_, 2),
            y_ // 2,
        )

    def send(src, dst, ssem, rsem, to):
        cp = pltpu.make_async_remote_copy(
            src_ref=src, dst_ref=dst, send_sem=ssem, recv_sem=rsem, device_id=to, device_id_type=MESH_ID
        )
        cp.start()
        return cp

    def await_bytes(ref, sem):
        pltpu.make_async_copy(ref, ref, sem).wait()

    def zat(d):
        return lax.rem(z + d + nz, nz)

    def xat(d):
        return lax.rem(x + d + nx, nx)

    def yat(d):
        return lax.rem(y + d, 4)

    y_order = (2, 1, 3)
    x_order = sorted(range(1, nx), key=lambda d: -min(d, nx - d))
    z_order = sorted(range(1, nz), key=lambda d: -min(d, nz - d))
    sections = [(d, False) for d in x_order] + [(d, True) for d in x_order] + [(0, True)]

    def peer(d, cross):
        return xat(d), (1 - core if cross else core)

    mine = pl.ds(pl.multiple_of(ylo * fe, LANES), fe)
    theirs = pl.ds(pl.multiple_of(other * fe, LANES), fe)

    w_hbm = (wi_hbm, wo_hbm)
    pa_in = pltpu.make_async_copy(pa_hbm, pa.at[core], lsem.at[0])
    w_in_ = [pltpu.make_async_copy(w_hbm[m].at[:, mine], wbuf.at[m, ylo, 1, z], lsem.at[1 + m]) for m in range(2)]
    og_in = pltpu.make_async_copy(og_hbm, og, lsem.at[3])
    li_in = pltpu.make_async_copy(li_hbm, li.at[core, x], lsem.at[4])
    barrier = pltpu.get_barrier_semaphore()
    greeted = [dev(z_=zat(d)) for d in (1, -1)] + [dev(*peer(*p)) for p in sections]
    greeted += [dev(y_=yat(d)) for d in range(1, 4)] + [dev(core_=1 - core, y_=partner)]
    for to in greeted:
        pl.semaphore_signal(barrier, inc=1, device_id=to, device_id_type=MESH_ID)

    first = (1, 0)
    own_in = [pltpu.make_async_copy(w_hbm[m], w_own.at[m], lsem.at[5 + m]) for m in range(2)]
    for m in first:
        own_in[m].start()

        @pl.when(core == 1)
        def _():
            w_in_[m].start()

    pa_in.start()

    og_in.start()
    li_in.start()

    with scope("barrier"):
        pl.semaphore_wait(barrier, len(greeted))

    half = nz // 2

    def meet(r):
        for d in (1, -1):
            pl.semaphore_signal(flag.at[r], inc=1, device_id=dev(z_=zat(d)), device_id_type=MESH_ID)
        pl.semaphore_wait(flag.at[r], 2)

    def pa_first():
        await_bytes(pa.at[1], st_r.at[5])
        for h in range(2):
            @pl.when(yhi == h)
            def _():
                for d in z_order:
                    if d % 2 == h:
                        for c in range(2):
                            dst = pa_all.at[c, lax.rem(z, 2), z // 2]
                            send(pa.at[c, zat(d)], dst, out_s.at[0], st_r.at[0], dev(z_=zat(d)))
                if h == 0:
                    for c in range(2):
                        pa_all[c, lax.rem(z, 2), z // 2] = pa[c, z]

    def await_pa(sem):
        for h in range(2):
            @pl.when(yhi == h)
            def _():
                await_bytes(pa.at[0, pl.ds(0, 2 * (half - 1 + h))], sem)

    def pa_second():
        await_pa(st_r.at[0])
        mine_ = pa_all.at[:, lax.rem(z + yhi, 2)]
        send(mine_, mine_, out_s.at[0], st_r.at[4], dev(y_=yat(2)))

    def ring_send(src, m, l, k, way):
        send(src, src, wz_s.at[way], wz_r.at[((k - 1) * 2 + m) * 2 + l], dev(z_=zat(1 if way == 0 else -1)))

    swaps = []
    for m in first:
        own_in[m].wait()

        @pl.when(core == 0)
        def _():
            send(w_own.at[m, :, mine], wbuf.at[m, ylo, 0, z], out_s.at[0], wd_r.at[m], dev(core_=1))

        @pl.when(core == 1)
        def _():
            w_in_[m].wait()
            for way in range(2):
                ring_send(wbuf.at[m, ylo, 1, z], m, ylo, 1, way)

        dst = wbuf.at[m, ylo, core, z]
        swaps.append(send(w_own.at[m, :, theirs], dst, out_s.at[0], wx_r.at[core * 2 + m], dev(core_=1, y_=partner)))

    pa_in.wait()

    @pl.when(core == 1)
    def _():
        send(pa.at[1], pa.at[1], out_s.at[0], st_r.at[5], dev(core_=0))

    v = pa[core].astype(F32).reshape(tok, nsec * fb)
    pa_t[...] = jnp.swapaxes(v, 0, 1).astype(BF16).reshape(nsec, fb, tok)
    for p in sections:
        to = peer(*p)
        send(pa_t.at[to[0] * 2 + to[1]], pre_t.at[sec], out_s.at[0], st_r.at[3], dev(*to))
    pre_t[sec] = pa_t[sec]

    def spread_pre():
        await_bytes(pre_t.at[pl.ds(0, nsec - 1)], st_r.at[3])
        dst = pre_top.at[ylo, core]
        send(pre_t.at[top], dst, out_s.at[0], pt_r.at[0], dev(core_=1, y_=partner))

        @pl.when(core == 0)
        def _():
            send(pre_t.at[top], dst, out_s.at[0], pt_r.at[0], dev(core_=1))

        @pl.when(core == 1)
        def _():
            dst[...] = pre_t[top]

    def stage_b():
        await_bytes(pa_all.at[:, 0], st_r.at[4])
        group = lax.broadcasted_iota(jnp.int32, (8, LANES), 1) // fb
        for c in range(2):
            for ct in range(nsec // per_tile):
                for t in range(tiles):
                    out = [jnp.zeros((8, LANES), F32)] * per_tile
                    for j in range(per_tile):
                        at = t * per_tile + j
                        v = pa_all[c, at % 2, at // 2, :, ct * LANES:(ct + 1) * LANES].astype(F32)
                        for k in range(per_tile):
                            shift = (j - k) * fb % LANES
                            r = pltpu.roll(v, shift, 1) if shift else v
                            out[k] = jnp.where(group == j, r, out[k])
                    for k in range(per_tile):
                        to = ct * per_tile + k
                        pb[to // 2, c, to % 2, t] = out[k].astype(BF16)
        for d in x_order + [0]:
            send(pb.at[xat(d)], pc.at[ylo, pl.ds(2 * x, 2)], out_s.at[0], st_r.at[1], dev(x_=xat(d), core_=1))

    cut = tok // 2
    lo, hi = pl.ds(0, cut), pl.ds(cut, cut)
    ring = nx > 2

    def li_first():
        li_in.wait()
        src = li.at[core, x]
        send(src, src, out_s.at[1], li_r.at[0], dev(x_=xat(1)))
        if ring:
            send(src, src, out_s.at[1], li_r.at[1], dev(x_=xat(-1)))

    def li_second():
        await_bytes(li.at[0, 0], li_r.at[0])
        if ring:
            src = li.at[core, xat(-1), lo]
            send(src, src, out_s.at[1], li_r.at[2], dev(x_=xat(1)))
            await_bytes(li.at[0, 0], li_r.at[1])
            src = li.at[core, xat(1), hi]
            send(src, src, out_s.at[1], li_r.at[3], dev(x_=xat(-1)))

    def li_third():
        if ring:
            await_bytes(li.at[0, 0, lo], li_r.at[2])
            await_bytes(li.at[0, 0, hi], li_r.at[3])
        send(li.at[core], li.at[core], out_s.at[1], li_r.at[4], dev(core_=1 - core))

    def first_out_term():
        for s in range(nsec):
            v = pre_t[s].astype(F32)
            hall[s] = (v * gelu_parts(v)[0]).astype(BF16)
        go_out[...] = jnp.dot(hall[top], og[...].reshape(tok, width), preferred_element_type=F32)

    def first_in_term():
        await_bytes(li.at[0], li_r.at[4])
        gi_out[...] = jnp.dot(g_top[...], li[top % 2, top // 2], preferred_element_type=F32)

    block = 4 * nz

    def slot(t, x_, ylo_=0, z_=0):
        return ((((t * nx + x_) * 2 + ylo_) * nz) + z_) * 2

    def columns(t, x_, l):
        return up[pl.ds(slot(t, x_, l), 2 * nz)].reshape(nz, 2, 8, LANES)

    def out_term(t):
        rows = hall[t - 1]
        for l in range(2):
            parts = []
            for k in range(nx):
                v = columns(t, k, l)
                parts += [v[:, c].reshape(tok, LANES) for c in range(2)]
            go_out[:, l * fe:(l + 1) * fe] += jnp.dot(rows, jnp.concatenate(parts, axis=1), preferred_element_type=F32)

        @pl.when(sec == t)
        def _():
            for l in range(2):
                for k in range(nx):
                    v = columns(t, k, l)
                    for c in range(2):
                        at = l * fe + (2 * k + c) * LANES
                        ig_out[:, :, at:at + LANES] = v[:, c]

    def in_term(t):
        @pl.when(core == 1)
        def _():
            await_bytes(gz.at[pl.ds(0, nz - 1)], g_r.at[t])

        @pl.when(core == 0)
        def _():
            await_bytes(gz.at[pl.ds(0, nz)], g_r.at[t])

        gt[...] = jnp.swapaxes(gz[pl.ds(t * nz, nz)].astype(F32).reshape(tok, LANES), 0, 1)
        rows = gt[pl.ds(pl.multiple_of(lax.rem(z, per_tile) * fb, fb), fb), :].astype(BF16)
        gi_out[...] += jnp.dot(rows, li[lax.rem(t, 2), t // 2], preferred_element_type=F32)

    hu, hn, hj = 2 * nz * fb, fe // 2, nsec // 2
    def hop(m, k, which):
        l = ylo if which == 0 else other
        if k == 1:
            if which == 0:
                await_bytes(wbuf.at[m, 0, 0, 0], wd_r.at[m])
            else:
                for c in range(2):
                    await_bytes(wbuf.at[m, 0, 0, 0], wx_r.at[c * 2 + m])
        if k > 1:
            await_bytes(wbuf.at[m, 0, :, pl.ds(0, 2)], wz_r.at[((k - 2) * 2 + m) * 2 + l])
        for way, step in ((0, 1), (1, -1)):
            if k == 1 and which == 0:
                ring_send(wbuf.at[m, l, 0, z], m, l, 1, way)
            elif k == half:
                ring_send(wbuf.at[m, l, way, zat(-step * (k - 1))], m, l, k, way)
            else:
                ring_send(wbuf.at[m, l, :, zat(-step * (k - 1))], m, l, k, way)

    def await_last(m):
        for l in range(2):
            await_bytes(wbuf.at[m, 0, :, 0], wz_r.at[((half - 1) * 2 + m) * 2 + l])

    def all_met():
        pl.semaphore_wait(flag.at[half - 1], 1)

    def stage_c():
        await_bytes(pc.at[0], st_r.at[1])
        send(pc.at[ylo], pc.at[ylo], out_s.at[0], st_r.at[2], dev(y_=partner))

    def stage_d():
        await_bytes(pc.at[0], st_r.at[2])

        def one(s, carry):
            for l in range(2):
                v = pc[l, s].astype(F32)
                cdf, dens = gelu_parts(v)
                slope[s, l] = (cdf + v * dens).reshape(2 * tiles, 8, LANES)
            return carry

        lax.fori_loop(0, top, one, 0)

    def top_first():
        og_in.wait()
        rows = wbuf[1, :, :, z].reshape(4 * fb, fe)
        a_top[y] = lax.dot_general(
            rows, og[:, :, mine].reshape(tok, fe), (((1,), (1,)), ((), ())), preferred_element_type=F32
        ).astype(BF16)
        for d in y_order:
            send(a_top.at[y], a_top.at[y], out_s.at[0], top_r.at[0], dev(y_=yat(d)))
        spread_pre()

    def top_second():
        await_bytes(pre_t.at[pl.ds(0, 3)], pt_r.at[0])
        v = pre_top[...].astype(F32).reshape(4 * fb, tok)
        cdf, dens = gelu_parts(v)
        await_bytes(a_top.at[pl.ds(0, 3)], top_r.at[0])
        back = a_top[0].astype(F32)
        for k in range(1, 4):
            back = back + a_top[k].astype(F32)
        g = (back * (cdf + v * dens)).astype(BF16)
        g_pass[...] = jnp.where(ylo == 0, g[:fb], g[2 * fb:3 * fb])
        send(g_pass, g_top, out_s.at[0], top_r.at[4], dev(core_=0))
        g_top[...] = jnp.where(ylo == 0, g[fb:2 * fb], g[3 * fb:])
        rows = jnp.swapaxes(g.astype(F32), 0, 1).astype(BF16)
        part = jnp.dot(rows, wbuf[0, :, :, z].reshape(4 * fb, fe), preferred_element_type=F32).astype(BF16)
        for j in range(nsec):
            b_top[j // 2, :, j % 2] = part[:, j * LANES:(j + 1) * LANES].reshape(nz, 8, LANES)
        for d in x_order:
            send(b_top.at[xat(d)], r_top.at[x], out_s.at[0], top_r.at[1], dev(x_=xat(d)))
        r_top[x] = b_top[x]

    def top_third():
        await_bytes(r_top.at[pl.ds(0, nx - 1)], top_r.at[1])
        total = r_top[0].astype(F32)
        for k in range(1, nx):
            total = total + r_top[k].astype(F32)
        q_top[...] = total.astype(BF16)
        for d in z_order:
            send(q_top.at[zat(d)], z_top.at[z], out_s.at[0], top_r.at[2], dev(z_=zat(d)))
        z_top[z] = q_top[z]

    own = pl.ds(2 * x, 2)

    def top_fourth():
        await_bytes(z_top.at[pl.ds(0, nz - 1)], top_r.at[2])
        for c in range(2):
            at = pl.multiple_of(ylo * fe + (2 * x + c) * LANES, LANES)
            total = og[z, :, pl.ds(at, LANES)].astype(F32)
            for k in range(nz):
                total = total + z_top[k, c].astype(F32)
            xs[top - 1, 2 * x + c] = total.astype(BF16)
        src = xs.at[top - 1, own]
        for d in x_order:
            send(src, src, out_s.at[0], top_r.at[3], dev(x_=xat(d)))

    def spread_z(t):
        src = xs.at[t - 1, own]
        dst = up.at[pl.ds(slot(t, x, ylo, z), 2)]

        def both(d):
            for to in (partner, y):
                send(src, dst, out_s.at[0], wz_r.at[t], dev(core_=0, z_=zat(d), y_=to))

        both(half)

        def pair(i, c):
            both(half - i)
            both(half + i)
            return c

        lax.fori_loop(1, half, pair, 0)
        both(0)

    bounds = sorted({half // 2, 3 * half // 4, half})
    groups = [
        [r for r in range(nz) if (bounds[i - 1] if i else -1) < min(r, nz - r) <= b] for i, b in enumerate(bounds)
    ]
    group_of = {r: i for i, g in enumerate(groups) for r in g}

    def runs(g):
        out = []
        for r in g:
            if out and out[-1][1] == r:
                out[-1][1] = r + 1
            else:
                out.append([r, r + 1])
        return out

    owner = [p if min(p, nx - p) <= 1 else 0 for p in range(nx)]
    owned = {o: [p for p in range(nx) if owner[p] == o] for o in sorted(set(owner))}
    d_order = [half] + [d for i in range(1, half) for d in (half - i, half + i)] + [0]

    def last_z():
        for o, pairs in owned.items():
            @pl.when(x == o)
            def _():
                for d in d_order:
                    r = (nz - d) % nz
                    for p in pairs:
                        src = xs.at[nsec, pl.ds(2 * p, 2)]
                        dst = up.at[pl.ds(slot(0, p, ylo, r), 2)]
                        if o:
                            send(src, dst, out_s.at[0], wx_r.at[group_of[r]], dev(core_=1, z_=zat(d), y_=partner))
                        if d:
                            send(src, dst, out_s.at[0], wx_r.at[group_of[r]], dev(core_=1, z_=zat(d)))
                for p in pairs:
                    up[pl.ds(slot(0, p, ylo, 0), 2)] = xs[nsec, 2 * p:2 * p + 2]

    def last_x(i):
        for o, pairs in owned.items():
            @pl.when(x == o)
            def _():
                per_plane = 4 if o else 2 * len(pairs)
                here = (2 if o else 2 * len(pairs)) if i == 0 else 0
                await_bytes(up.at[pl.ds(0, per_plane * len(groups[i]) - here)], wx_r.at[i])
                for a, b in runs(groups[i]):
                    for p in pairs:
                        for l, to in ((0, y), (1, y)) if o else ((ylo, partner), (ylo, y)):
                            src = up.at[pl.ds(slot(0, p, l, a), 2 * (b - a))]
                            send(src, src, out_s.at[0], wz_r.at[2 * nsec + i], dev(x_=0, core_=0, y_=to))

    def last_out(i):
        await_bytes(up.at[pl.ds(0, nx * 4 * len(groups[i]))], wz_r.at[2 * nsec + i])
        for r in groups[i]:
            row = zat(r)
            for l in range(2):
                for k in range(nx):
                    for c in range(2):
                        at = l * fe + (2 * k + c) * LANES
                        ig_out[row, :, at:at + LANES] = up[slot(0, k, l, r) + c]

    def spread_g(t):
        def to(d, c):
            tile = zat(d) // per_tile
            for c_ in range(2):
                send(gbuf.at[t, ylo, c_ * tiles + tile], gz.at[t * nz + z], out_s.at[0], g_r.at[t], dev(core_=c_, z_=zat(d)))
            return c

        lax.fori_loop(1, nz, to, 0)
        tile = z // per_tile
        send(gbuf.at[t, ylo, tile], gz.at[t * nz + z], out_s.at[0], g_r.at[t], dev(core_=0))
        gz[t * nz + z] = gbuf[t, ylo, tiles + tile]

    def turn(away):
        t = lax.rem(z // per_tile + away + tiles, tiles)

        def one(i, c):
            l, c_ = i // 2, lax.rem(i, 2)
            v = wbuf[1, l, c_, pl.ds(t * per_tile, per_tile)].reshape(LANES, fe)
            w_t[l, c_ * tiles + t] = jnp.swapaxes(v, 0, 1)
            return c

        lax.fori_loop(0, 4, one, 0)

    def a_half(s, l, part=None):
        if part is not None:
            a_buf[s, l, y] = part.astype(BF16)
        for d in y_order:
            send(a_buf.at[s, l, y], a_buf.at[s, l, y], out_s.at[0], ph_r.at[0, l, s % 2 if isinstance(s, int) else lax.rem(s, 2)], dev(y_=yat(d)))

    def a_part(s, l, n):
        lhs = jnp.concatenate([xs[s, n * hj + j] for j in range(hj)], axis=1)
        w_out = jnp.concatenate([w_t[l, t, n * hn:(n + 1) * hn] for t in range(2 * tiles)], axis=1)
        return jnp.dot(lhs, w_out, preferred_element_type=F32)

    def a_tile(l, away, turned):
        lhs = jnp.concatenate([xs[top - 1, j] for j in range(nsec)], axis=1)
        t = lax.rem(z // per_tile + away + tiles, tiles)
        if turned:
            w_out = jnp.concatenate([w_t[l, c * tiles + t] for c in range(2)], axis=1)
            part = jnp.dot(lhs, w_out, preferred_element_type=F32)
        else:
            w_out = wbuf[1, l, :, pl.ds(t * per_tile, per_tile)].reshape(2 * LANES, fe)
            part = lax.dot_general(lhs, w_out, (((1,), (1,)), ((), ())), preferred_element_type=F32)
        for c in range(2):
            at = pl.multiple_of((c * tiles + t) * LANES, LANES)
            a_buf[top - 1, l, y, :, pl.ds(at, LANES)] = part[:, c * LANES:(c + 1) * LANES].astype(BF16)

    def release(t):
        pl.semaphore_signal(flag.at[t], inc=1, device_id=dev(core_=0), device_id_type=MESH_ID)

    def await_up(t):
        await_bytes(up.at[pl.ds(0, nx * block)], ud_r.at[t])

    def background_a(s):
        with scope("bg_a"):
            @pl.when(s <= top - 3)
            def _():
                release(s + 2)

            @pl.when(s <= top - 2)
            def _():
                spread_z(s + 1)

            @pl.when(s == top - 2)
            def _():
                first_in_term()

            @pl.when(s <= top - 3)
            def _():
                in_term(s + 2)

            @pl.when(s <= top - 4)
            def _():
                await_up(s + 4)
                out_term(s + 4)

    def g_half(s, l):
        with scope(f"wait_a{l}"):
            await_bytes(a_buf.at[s, l, pl.ds(0, 3)], ph_r.at[0, l, s % 2 if isinstance(s, int) else lax.rem(s, 2)])
        back = a_buf[s, l, 0].astype(F32)
        for k in range(1, 4):
            back = back + a_buf[s, l, k].astype(F32)
        g = []
        for t in range(2 * tiles):
            g_tile = (back[:, t * LANES:(t + 1) * LANES] * slope[s, l, t]).astype(BF16)
            gbuf[s, l, t] = g_tile
            g.append(g_tile)
        return jnp.concatenate(g, axis=1)

    def b_tile(n, away):
        t = lax.rem(z // per_tile + away + tiles, tiles)
        pairs = [(l, c) for l in range(2) for c in range(2)]
        lhs = jnp.concatenate([gbuf[top - 1, l, c * tiles + t] for l, c in pairs], axis=1)
        rows = pl.ds(t * per_tile, per_tile)
        w_in = jnp.concatenate([wbuf[0, l, c, rows, :, n * hn:(n + 1) * hn].reshape(LANES, hn) for l, c in pairs], axis=0)
        return jnp.dot(lhs, w_in, preferred_element_type=F32)

    def application(s, final=False, begin=False):
        if not begin:
            background_a(s)
            g_first = g_half(s, 0)
            for n in range(2):
                w_in = wbuf[0, 0, :, :, :, n * hn:(n + 1) * hn].reshape(hu, hn)
                b_acc[n] = jnp.dot(g_first, w_in, preferred_element_type=F32)
            g = g_half(s, 1)
        for n in range(2):
            if begin:
                part = b_tile(n, tiles // 2)
            else:
                w_in = wbuf[0, 1, :, :, :, n * hn:(n + 1) * hn].reshape(hu, hn)
                part = jnp.dot(g, w_in, preferred_element_type=F32)
            part = (b_acc[n] + part).astype(BF16)
            for j in range(hj):
                b_buf[s, n, x, j] = part[:, j * LANES:(j + 1) * LANES]
            if not final:
                src = b_buf.at[s, n, x]
                for d in x_order:
                    send(src, src, out_s.at[0], ph_r.at[1, n, s % 2 if isinstance(s, int) else lax.rem(s, 2)], dev(x_=xat(d)))
        hx = nx // 2
        if final:
            for p in range(nx):
                @pl.when(x != owner[p])
                def _():
                    src = b_buf.at[s, p // hx, x, pl.ds(2 * (p % hx), 2)]
                    send(src, src, out_s.at[0], ph_r.at[1, 0, s % 2], dev(x_=owner[p]))

        with scope("bg_b"):
            spread_g(s)
            if begin:
                spread_z(top)

        if final:
            for o, pairs in owned.items():
                @pl.when(x == o)
                def _():
                    with scope("wait_b"):
                        await_bytes(gz.at[pl.ds(0, 2 * (nx - 1) * len(pairs))], ph_r.at[1, 0, s % 2])
                    for p in pairs:
                        for c in range(2):
                            total = xs[s, 2 * p + c].astype(F32)
                            for k in range(nx):
                                total = total + b_buf[s, p // hx, k, 2 * (p % hx) + c].astype(F32)
                            xs[nsec, 2 * p + c] = total.astype(BF16)
            return
        for n in range(2):
            with scope(f"wait_b{n}"):
                await_bytes(b_buf.at[s, n, pl.ds(0, nx - 1)], ph_r.at[1, n, s % 2 if isinstance(s, int) else lax.rem(s, 2)])
            with scope(f"a_mm{n}"):
                for j in range(hj):
                    total = xs[s, n * hj + j].astype(F32)
                    for k in range(nx):
                        total = total + b_buf[s, n, k, j].astype(F32)
                    xs[s - 1, n * hj + j] = total.astype(BF16)
                if n == 0:
                    for l in range(2):
                        a_acc[l] = a_part(s - 1, l, 0)
        for l in range(2):
            with scope(f"a_last{l}"):
                a_half(s - 1, l, a_acc[l] + a_part(s - 1, l, 1))

    @pl.when(core == 1)
    def _():
        plan = [
            (1, top_first), (2, top_second), (2, li_first), (4, all_met), (4, top_third), (5, first_out_term), (6, li_second),
            (6, stage_c), (7, stage_d), (7, top_fourth),
        ]
        plan += [(half if d else 5, lambda d=d: turn(d)) for d in (0, -1, 1) if d % tiles != tiles // 2]
        for k in range(1, half + 1):
            with scope(f"hop{k}"):
                if k == 1:
                    blocks = ((1, 1, 0), (0, 1, 0), (1, 1, 1))
                elif k == 2:
                    blocks = ((1, 2, 0), (0, 1, 1), (1, 2, 1))
                else:
                    blocks = ((1, k, 0), (0, k - 1, 0), (1, k, 1), (0, k - 1, 1))
                for b in blocks:
                    hop(*b)
            with scope(f"stage{k}"):
                for at, f in plan:
                    if min(at, half) == k:
                        f()
        early = [d for d in (0, -1, 1) if d % tiles != tiles // 2]
        with scope("top_end"):
            await_bytes(xs.at[0, pl.ds(0, 2 * (nx - 1))], top_r.at[3])
            for l in range(2):
                for d in early:
                    a_tile(l, d, True)
        with scope("gather_out"):
            hop(0, half, 0)
            await_last(1)
        with scope("a_first"):
            for l in range(2):
                a_tile(l, tiles // 2, False)
                a_half(top - 1, l)
        with scope("hop_end"):
            hop(0, half, 1)
            turn(tiles // 2)
        with scope("b_early"):
            for l in range(2):
                g_half(top - 1, l)
            for n in range(2):
                b_acc[n] = sum((b_tile(n, d) for d in early), jnp.zeros((8, hn), F32))
        with scope("gather_in"):
            await_last(0)
        li_third()

        application(top - 1, begin=True)

        def step(i, carry):
            application(top - 2 - i)
            return carry

        lax.fori_loop(0, top - 2, step, 0)
        application(0, final=True)

        with scope("t_z0"):
            last_z()
            release(1)
        with scope("t_terms"):
            in_term(1)
            for t in range(min(top, 3), 2, -1):
                await_up(t)
                out_term(t)
        with scope("t_in0"):
            in_term(0)
        for i in range(len(groups)):
            with scope(f"t_last{i}"):
                last_x(i)
        with scope("t_up2"):
            await_up(2)
            out_term(2)
        with scope("t_up1"):
            await_up(1)
            out_term(1)

    def await_z(t):
        await_bytes(up.at[pl.ds(0, block)], wz_r.at[t])

    def spread_x(t):
        await_z(t)
        if not isinstance(t, int) or t < top:
            pl.semaphore_wait(flag.at[t], 1)
        src = up.at[pl.ds(slot(t, x), block)]
        for d in x_order:
            to_sem = wz_r.at[2 * nsec + 3 + d] if isinstance(t, int) and t == 1 else wz_r.at[nsec + t]
            send(src, src, out_s.at[0], to_sem, dev(x_=xat(d)))

    def to_core(t, x_, blocks):
        src = up.at[pl.ds(slot(t, x_), blocks * block)]
        send(src, src, out_s.at[2], ud_r.at[t], dev(core_=1))

    def spread_core(t):
        await_bytes(up.at[pl.ds(0, (nx - 1) * block)], wz_r.at[nsec + t])
        to_core(t, 0, nx)

    def spread_core_last():
        for d in reversed(x_order):
            await_bytes(up.at[pl.ds(0, block)], wz_r.at[2 * nsec + 3 + d])
            to_core(1, xat(-d), 1)

    @pl.when(core == 0)
    def _():
        spread_pre()
        for r in range(half - 1):
            meet(r)
        pl.semaphore_signal(flag.at[half - 1], inc=1, device_id=dev(core_=1), device_id_type=MESH_ID)
        pa_first()
        li_first()
        pa_second()
        stage_b()
        og_in.wait()
        first_out_term()
        li_second()
        li_third()
        await_bytes(g_top, top_r.at[4])
        first_in_term()

        def finish_one(t):
            with scope("s_core"):
                spread_core(t)
            with scope("s_out"):
                out_term(t)

        def move(i, carry):
            t = top - 1 - i
            with scope("s_x"):
                spread_x(t)
            with scope("s_in"):
                in_term(t)
            finish_one(t + 1)
            return carry

        with scope("s_x7"):
            spread_x(top)
        lax.fori_loop(0, top - 2, move, 0)
        with scope("s_x1"):
            spread_x(1)
            to_core(1, x, 1)
        finish_one(2)
        with scope("s_in"):
            for t in (1, 0):
                in_term(t)
        with scope("s_core1"):
            spread_core_last()
        with scope("s_out1"):
            out_term(1)

        @pl.when(x == 0)
        def _():
            for i in range(len(groups)):
                with scope(f"s_last{i}"):
                    last_out(i)

    def size(*shape):
        return math.prod(shape) // (8 * LANES)

    li_block, row = size(tok, width), size(fb, tok)
    both_cores = size(2, fb, fe) + nsec * row
    by_core = (
        size(2, fb, fe) + row + size(2, half, 8, nsec * fb) + nx * size(2, 2, tiles, 8, LANES) + top * (nx - 1) * block,
        size(nz, 8, nsec * fb)
        + size(nsec, 2, tiles, 8, LANES)
        + 3 * size(4 * fb, tok)
        + (nx - 1) * 2 * nz
        + (nz - 1) * 2
        + (nx - 1) * 2
        + row
        + top * 2 * 3 * size(8, hu)
        + (top - 1) * 2 * (nx - 1) * hj
        + top * (2 * nz - 1)
        + top * block,
    )
    with scope("drain"):
        await_bytes(spare.at[pl.ds(0, (nx + (3 if ring else 1)) * li_block)], out_s.at[1])

        @pl.when(core == 1)
        def _():
            for way in range(2):
                await_bytes(wbuf.at[0, :, :, pl.ds(0, nz - 1)], wz_s.at[way])

        for o in range(nx):
            pairs = owned.get(o, [])
            last_tiles = 2 * sum(owner[p] != o for p in range(nx))
            if pairs:
                last_tiles += (block - 2 if o else 2 * len(pairs) * (nz - 1)) + (block if o else block * len(pairs))

            @pl.when((core == 1) & (x == o))
            def _():
                await_bytes(spare.at[pl.ds(0, both_cores + by_core[1] + last_tiles)], out_s.at[0])

        @pl.when(core == 0)
        def _():
            await_bytes(spare.at[pl.ds(0, top * nx * block)], out_s.at[2])

        for h in range(2):
            @pl.when((core == 0) & (yhi == h))
            def _():
                pa_tiles = 2 * (half - 1 + h) * size(8, nsec * fb)
                await_bytes(spare.at[pl.ds(0, both_cores + by_core[0] + pa_tiles)], out_s.at[0])


def finish(ig, gi, go, ig_out, gi_out, go_out, sems):
    copies = [pltpu.make_async_copy(src, dst, sems.at[k]) for k, (src, dst) in enumerate(((ig, ig_out), (gi, gi_out), (go, go_out)))]
    for cp in copies:
        cp.start()
    for cp in copies:
        cp.wait()


def body(layer_inputs, pre_act, out_grad, w_in, w_out):
    nz, nx = lax.axis_size("z"), lax.axis_size("x")
    nsec = 2 * nx
    tok, width = out_grad.shape
    fb = w_in.shape[2]
    hid = pre_act.shape[2]
    fe = width // 2
    tiles = nz * fb // LANES
    half = nz // 2
    dma = pltpu.SemaphoreType.DMA
    vmem = pltpu.VMEM
    spare = 2048
    scratch = [
        vmem((2, fb, width), BF16),
        vmem((2, 2, 2, nz, fb, fe), BF16),
        vmem((2, nz, 8, hid), BF16),
        vmem((2, 2, half, 8, hid), BF16),
        vmem((nx, 2, 2, tiles, 8, LANES), BF16),
        vmem((2, nsec, 2, tiles, 8, LANES), BF16),
        vmem((nsec, 2, 2 * tiles, 8, LANES), F32),
        vmem((nsec, fb, tok), BF16),
        vmem((nsec, fb, tok), BF16),
        vmem((2, 2, fb, tok), BF16),
        vmem((nsec, fb, tok), BF16),
        vmem((2, nx, tok, width), BF16),
        vmem((nz, 8, width), BF16),
        vmem((4, 4 * fb, tok), BF16),
        vmem((nx, nz, 2, 8, LANES), BF16),
        vmem((nx, nz, 2, 8, LANES), BF16),
        vmem((nz, 2, 8, LANES), BF16),
        vmem((nz, 2, 8, LANES), BF16),
        vmem((fb, tok), BF16),
        vmem((fb, tok), BF16),
        vmem((2, 2 * tiles, fe, LANES), BF16),
        vmem((nsec + 1, nsec, 8, LANES), BF16),
        vmem((nsec, 2, 4, 8, 2 * nz * fb), BF16),
        vmem((nsec, 2, nx, nx, 8, LANES), BF16),
        vmem((2, 8, 2 * nz * fb), F32),
        vmem((2, 8, fe // 2), F32),
        vmem((nsec, 2, 2 * tiles, 8, LANES), BF16),
        vmem((nsec * nz, 8, LANES), BF16),
        vmem((LANES, tok), F32),
        vmem((nsec * nx * 4 * nz, 8, LANES), BF16),
        vmem((spare, 8, LANES), BF16),
        dma((7,)),
        dma((3,)), dma((2,)),
        dma((4,)),
        dma((2,)),
        dma((max(half * 4, 2 * nsec + 3 + nx),)),
        dma((6,)),
        dma((1,)),
        dma((5,)),
        dma((2, 2, 2)),
        dma((5,)),
        dma((nsec,)),
        dma((nsec,)),
        pltpu.SemaphoreType.REGULAR((max(nsec, half),)),
    ]
    hbm, on_chip = pl.BlockSpec(memory_space=pltpu.HBM), pl.BlockSpec(memory_space=pltpu.VMEM)
    shapes = (
        jax.ShapeDtypeStruct((nz, 8, width), BF16),
        jax.ShapeDtypeStruct((fb, width), F32),
        jax.ShapeDtypeStruct((fb, width), F32),
    )
    operands = (
        layer_inputs.reshape(tok, width),
        pre_act.reshape(nz, 8, hid),
        out_grad.reshape(nz, 8, width),
        w_in.reshape(fb, width),
        w_out.reshape(fb, width),
    )
    results = pl.pallas_call(
        kernel,
        out_shape=shapes,
        in_specs=[hbm] * 5,
        out_specs=(on_chip,) * 3,
        scratch_shapes=scratch,
        name="chain",
        compiler_params=pltpu.CompilerParams(
            collective_id=0, has_side_effects=True, vmem_limit_bytes=40 * 1024 * 1024
        ),
    )(*(pltpu.with_memory_space_constraint(v, pltpu.HBM) for v in operands))
    ig, gi, go = pl.pallas_call(
        finish,
        out_shape=shapes,
        in_specs=[on_chip] * 3,
        out_specs=(hbm,) * 3,
        scratch_shapes=[dma((3,))],
        name="finish",
    )(*(pltpu.with_memory_space_constraint(v, pltpu.VMEM) for v in results))
    return (
        ig.reshape(1, tok, width),
        gi.reshape(1, 1, fb, width),
        go.reshape(1, 1, fb, width),
    )


def solution(mesh):
    shape = mesh.shape
    split = Mesh(
        mesh.devices.reshape(shape["section"] // 2, 2, shape["dp"] // 2, 2, shape["mp"]), AXES
    )
    sec, dp = ("x", "core"), ("z", "ylo")
    placed = (
        P(sec, None, "yhi"),
        P(sec, None, dp),
        P(None, "yhi"),
        P(dp, sec, None, "yhi"),
        P(dp, sec, None, "yhi"),
    )
    return jax.shard_map(
        body,
        mesh=split,
        in_specs=placed,
        out_specs=(P(sec, None, "yhi"), P(dp, sec, None, "yhi"), P(dp, sec, None, "yhi")),
        check_vma=False,
    )
```

```python
import contextlib
import math

import jax
import jax.numpy as jnp
from jax import lax
from jax.experimental import pallas as pl
from jax.experimental.pallas import tpu as pltpu
from jax.sharding import Mesh
from jax.sharding import PartitionSpec as P

AXES = ("x", "core", "z", "ylo", "yhi")
MESH_ID = pl.DeviceIdType.MESH
BF16, F32 = jnp.bfloat16, jnp.float32
LANES = 128
PROFILE = False


def scope(name):
    return jax.named_scope(name) if PROFILE else contextlib.nullcontext()


def gelu_parts(v):
    cdf = 0.5 * (1.0 + lax.erf(v * 0.7071067811865476))
    dens = jnp.exp(-0.5 * v * v) * 0.3989422804014327
    return cdf, dens


def kernel(
    li_hbm, pa_hbm, og_hbm, wi_hbm, wo_hbm,
    ig_out, gi_out, go_out,
    w_own, wbuf, pa, pa_all, pb, pc, slope, pa_t, pre_t, pre_top, hall, li, og,
    a_top, b_top, r_top, q_top, z_top, g_top, g_pass,
    w_t, xs, a_buf, b_buf, a_acc, b_acc, gbuf, gz, gt, up,
    spare, lsem, out_s, wz_s, wx_r, wd_r, wz_r, st_r, pt_r, top_r, ph_r, li_r, g_r, ud_r, flag,
):
    nx, nz = lax.axis_size("x"), lax.axis_size("z")
    nsec = 2 * nx
    top = nsec - 1
    fb, width = wi_hbm.shape
    fe = width // 2
    tok = nz * 8
    tiles = nz * fb // LANES
    per_tile = LANES // fb
    x, core, z = lax.axis_index("x"), lax.axis_index("core"), lax.axis_index("z")
    ylo, yhi = lax.axis_index("ylo"), lax.axis_index("yhi")
    sec = x * 2 + core
    y = yhi * 2 + ylo
    other = 1 - ylo
    partner = yhi * 2 + other

    def dev(x_=None, core_=None, z_=None, y_=None):
        y_ = y if y_ is None else y_
        return (
            x if x_ is None else x_,
            core if core_ is None else core_,
            z if z_ is None else z_,
            lax.rem(y_, 2),
            y_ // 2,
        )

    def send(src, dst, ssem, rsem, to):
        cp = pltpu.make_async_remote_copy(
            src_ref=src, dst_ref=dst, send_sem=ssem, recv_sem=rsem, device_id=to, device_id_type=MESH_ID
        )
        cp.start()
        return cp

    def await_bytes(ref, sem):
        pltpu.make_async_copy(ref, ref, sem).wait()

    def zat(d):
        return lax.rem(z + d + nz, nz)

    def xat(d):
        return lax.rem(x + d + nx, nx)

    def yat(d):
        return lax.rem(y + d, 4)

    y_order = (2, 1, 3)
    x_order = sorted(range(1, nx), key=lambda d: -min(d, nx - d))
    z_order = sorted(range(1, nz), key=lambda d: -min(d, nz - d))
    sections = [(d, False) for d in x_order] + [(d, True) for d in x_order] + [(0, True)]

    def peer(d, cross):
        return xat(d), (1 - core if cross else core)

    mine = pl.ds(pl.multiple_of(ylo * fe, LANES), fe)
    theirs = pl.ds(pl.multiple_of(other * fe, LANES), fe)

    w_hbm = (wi_hbm, wo_hbm)
    pa_in = pltpu.make_async_copy(pa_hbm, pa.at[core], lsem.at[0])
    w_in_ = [pltpu.make_async_copy(w_hbm[m].at[:, mine], wbuf.at[m, ylo, 1, z], lsem.at[1 + m]) for m in range(2)]
    og_in = pltpu.make_async_copy(og_hbm, og, lsem.at[3])
    li_in = pltpu.make_async_copy(li_hbm, li.at[core, x], lsem.at[4])
    barrier = pltpu.get_barrier_semaphore()
    greeted = [dev(z_=zat(d)) for d in (1, -1)] + [dev(*peer(*p)) for p in sections]
    greeted += [dev(y_=yat(d)) for d in range(1, 4)] + [dev(core_=1 - core, y_=partner)]
    for to in greeted:
        pl.semaphore_signal(barrier, inc=1, device_id=to, device_id_type=MESH_ID)

    first = (1, 0)
    own_in = [pltpu.make_async_copy(w_hbm[m], w_own.at[m], lsem.at[5 + m]) for m in range(2)]
    for m in first:
        own_in[m].start()

        @pl.when(core == 1)
        def _():
            w_in_[m].start()

    pa_in.start()

    og_in.start()
    li_in.start()

    with scope("barrier"):
        pl.semaphore_wait(barrier, len(greeted))

    half = nz // 2

    def meet(r):
        for d in (1, -1):
            pl.semaphore_signal(flag.at[r], inc=1, device_id=dev(z_=zat(d)), device_id_type=MESH_ID)
        pl.semaphore_wait(flag.at[r], 2)

    def pa_first():
        await_bytes(pa.at[1], st_r.at[5])
        for h in range(2):
            @pl.when(yhi == h)
            def _():
                for d in z_order:
                    if d % 2 == h:
                        for c in range(2):
                            dst = pa_all.at[c, lax.rem(z, 2), z // 2]
                            send(pa.at[c, zat(d)], dst, out_s.at[0], st_r.at[0], dev(z_=zat(d)))
                if h == 0:
                    for c in range(2):
                        pa_all[c, lax.rem(z, 2), z // 2] = pa[c, z]

    def await_pa(sem):
        for h in range(2):
            @pl.when(yhi == h)
            def _():
                await_bytes(pa.at[0, pl.ds(0, 2 * (half - 1 + h))], sem)

    def pa_second():
        await_pa(st_r.at[0])
        mine_ = pa_all.at[:, lax.rem(z + yhi, 2)]
        send(mine_, mine_, out_s.at[0], st_r.at[4], dev(y_=yat(2)))

    def ring_send(src, m, l, k, way):
        send(src, src, wz_s.at[way], wz_r.at[((k - 1) % 2 * 2 + m) * 2 + l], dev(z_=zat(1 if way == 0 else -1)))

    swaps = []
    for m in first:
        own_in[m].wait()

        @pl.when(core == 0)
        def _():
            send(w_own.at[m, :, mine], wbuf.at[m, ylo, 0, z], out_s.at[0], wd_r.at[m], dev(core_=1))

        @pl.when(core == 1)
        def _():
            w_in_[m].wait()
            for way in range(2):
                ring_send(wbuf.at[m, ylo, 1, z], m, ylo, 1, way)

        dst = wbuf.at[m, ylo, core, z]
        swaps.append(send(w_own.at[m, :, theirs], dst, out_s.at[0], wx_r.at[core * 2 + m], dev(core_=1, y_=partner)))

    pa_in.wait()

    @pl.when(core == 1)
    def _():
        send(pa.at[1], pa.at[1], out_s.at[0], st_r.at[5], dev(core_=0))

    v = pa[core].astype(F32).reshape(tok, nsec * fb)
    pa_t[...] = jnp.swapaxes(v, 0, 1).astype(BF16).reshape(nsec, fb, tok)
    for p in sections:
        to = peer(*p)
        send(pa_t.at[to[0] * 2 + to[1]], pre_t.at[sec], out_s.at[0], st_r.at[3], dev(*to))
    pre_t[sec] = pa_t[sec]

    def spread_pre():
        await_bytes(pre_t.at[pl.ds(0, nsec - 1)], st_r.at[3])
        dst = pre_top.at[ylo, core]
        send(pre_t.at[top], dst, out_s.at[0], pt_r.at[0], dev(core_=1, y_=partner))

        @pl.when(core == 0)
        def _():
            send(pre_t.at[top], dst, out_s.at[0], pt_r.at[0], dev(core_=1))

        @pl.when(core == 1)
        def _():
            dst[...] = pre_t[top]

    def stage_b():
        await_bytes(pa_all.at[:, 0], st_r.at[4])
        group = lax.broadcasted_iota(jnp.int32, (8, LANES), 1) // fb
        for c in range(2):
            for ct in range(nsec // per_tile):
                for t in range(tiles):
                    out = [jnp.zeros((8, LANES), F32)] * per_tile
                    for j in range(per_tile):
                        at = t * per_tile + j
                        v = pa_all[c, at % 2, at // 2, :, ct * LANES:(ct + 1) * LANES].astype(F32)
                        for k in range(per_tile):
                            shift = (j - k) * fb % LANES
                            r = pltpu.roll(v, shift, 1) if shift else v
                            out[k] = jnp.where(group == j, r, out[k])
                    for k in range(per_tile):
                        to = ct * per_tile + k
                        pb[to // 2, c, to % 2, t] = out[k].astype(BF16)
        for d in x_order + [0]:
            send(pb.at[xat(d)], pc.at[ylo, pl.ds(2 * x, 2)], out_s.at[0], st_r.at[1], dev(x_=xat(d), core_=1))

    cut = tok // 2
    lo, hi = pl.ds(0, cut), pl.ds(cut, cut)
    ring = nx > 2

    def li_first():
        li_in.wait()
        src = li.at[core, x]
        send(src, src, out_s.at[1], li_r.at[0], dev(x_=xat(1)))
        if ring:
            send(src, src, out_s.at[1], li_r.at[1], dev(x_=xat(-1)))

    def li_second():
        await_bytes(li.at[0, 0], li_r.at[0])
        if ring:
            src = li.at[core, xat(-1), lo]
            send(src, src, out_s.at[1], li_r.at[2], dev(x_=xat(1)))
            await_bytes(li.at[0, 0], li_r.at[1])
            src = li.at[core, xat(1), hi]
            send(src, src, out_s.at[1], li_r.at[3], dev(x_=xat(-1)))

    def li_third():
        if ring:
            await_bytes(li.at[0, 0, lo], li_r.at[2])
            await_bytes(li.at[0, 0, hi], li_r.at[3])
        send(li.at[core], li.at[core], out_s.at[1], li_r.at[4], dev(core_=1 - core))

    def first_out_term():
        for s in range(nsec):
            v = pre_t[s].astype(F32)
            hall[s] = (v * gelu_parts(v)[0]).astype(BF16)
        go_out[...] = jnp.dot(hall[top], og[...].reshape(tok, width), preferred_element_type=F32)

    def first_in_term():
        await_bytes(li.at[0], li_r.at[4])
        gi_out[...] = jnp.dot(g_top[...], li[top % 2, top // 2], preferred_element_type=F32)

    block = 4 * nz

    def slot(t, x_, ylo_=0, z_=0):
        return ((((t * nx + x_) * 2 + ylo_) * nz) + z_) * 2

    def columns(t, x_, l):
        return up[pl.ds(slot(t, x_, l), 2 * nz)].reshape(nz, 2, 8, LANES)

    def out_term(t):
        rows = hall[t - 1]
        for l in range(2):
            parts = []
            for k in range(nx):
                v = columns(t, k, l)
                parts += [v[:, c].reshape(tok, LANES) for c in range(2)]
            go_out[:, l * fe:(l + 1) * fe] += jnp.dot(rows, jnp.concatenate(parts, axis=1), preferred_element_type=F32)

        @pl.when(sec == t)
        def _():
            for l in range(2):
                for k in range(nx):
                    v = columns(t, k, l)
                    for c in range(2):
                        at = l * fe + (2 * k + c) * LANES
                        ig_out[:, :, at:at + LANES] = v[:, c]

    def in_term(t):
        @pl.when(core == 1)
        def _():
            await_bytes(gz.at[pl.ds(0, nz - 1)], g_r.at[t])

        @pl.when(core == 0)
        def _():
            await_bytes(gz.at[pl.ds(0, nz)], g_r.at[t])

        gt[...] = jnp.swapaxes(gz[pl.ds(t * nz, nz)].astype(F32).reshape(tok, LANES), 0, 1)
        rows = gt[pl.ds(pl.multiple_of(lax.rem(z, per_tile) * fb, fb), fb), :].astype(BF16)
        gi_out[...] += jnp.dot(rows, li[lax.rem(t, 2), t // 2], preferred_element_type=F32)

    hu, hn, hj = 2 * nz * fb, fe // 2, nsec // 2
    def hop(m, k, which):
        l = ylo if which == 0 else other
        if k == 1:
            if which == 0:
                await_bytes(wbuf.at[m, 0, 0, 0], wd_r.at[m])
            else:
                for c in range(2):
                    await_bytes(wbuf.at[m, 0, 0, 0], wx_r.at[c * 2 + m])
        if k > 1:
            await_bytes(wbuf.at[m, 0, :, pl.ds(0, 2)], wz_r.at[(k % 2 * 2 + m) * 2 + l])
        for way, step in ((0, 1), (1, -1)):
            if k == 1 and which == 0:
                ring_send(wbuf.at[m, l, 0, z], m, l, 1, way)
            elif k == half:
                ring_send(wbuf.at[m, l, way, zat(-step * (k - 1))], m, l, k, way)
            else:
                ring_send(wbuf.at[m, l, :, zat(-step * (k - 1))], m, l, k, way)

    def await_last(m):
        for l in range(2):
            await_bytes(wbuf.at[m, 0, :, 0], wz_r.at[((half - 1) % 2 * 2 + m) * 2 + l])

    def all_met():
        pl.semaphore_wait(flag.at[half - 1], 1)

    def stage_c():
        await_bytes(pc.at[0], st_r.at[1])
        send(pc.at[ylo], pc.at[ylo], out_s.at[0], st_r.at[2], dev(y_=partner))

    def stage_d():
        await_bytes(pc.at[0], st_r.at[2])

        def one(s, carry):
            for l in range(2):
                v = pc[l, s].astype(F32)
                cdf, dens = gelu_parts(v)
                slope[s, l] = (cdf + v * dens).reshape(2 * tiles, 8, LANES)
            return carry

        lax.fori_loop(0, top, one, 0)

    def top_first():
        og_in.wait()
        rows = wbuf[1, :, :, z].reshape(4 * fb, fe)
        a_top[y] = lax.dot_general(
            rows, og[:, :, mine].reshape(tok, fe), (((1,), (1,)), ((), ())), preferred_element_type=F32
        ).astype(BF16)
        for d in y_order:
            send(a_top.at[y], a_top.at[y], out_s.at[0], top_r.at[0], dev(y_=yat(d)))
        spread_pre()

    def top_second():
        await_bytes(pre_t.at[pl.ds(0, 3)], pt_r.at[0])
        v = pre_top[...].astype(F32).reshape(4 * fb, tok)
        cdf, dens = gelu_parts(v)
        await_bytes(a_top.at[pl.ds(0, 3)], top_r.at[0])
        back = a_top[0].astype(F32)
        for k in range(1, 4):
            back = back + a_top[k].astype(F32)
        g = (back * (cdf + v * dens)).astype(BF16)
        g_pass[...] = jnp.where(ylo == 0, g[:fb], g[2 * fb:3 * fb])
        send(g_pass, g_top, out_s.at[0], top_r.at[4], dev(core_=0))
        g_top[...] = jnp.where(ylo == 0, g[fb:2 * fb], g[3 * fb:])
        rows = jnp.swapaxes(g.astype(F32), 0, 1).astype(BF16)
        part = jnp.dot(rows, wbuf[0, :, :, z].reshape(4 * fb, fe), preferred_element_type=F32).astype(BF16)
        for j in range(nsec):
            b_top[j // 2, :, j % 2] = part[:, j * LANES:(j + 1) * LANES].reshape(nz, 8, LANES)
        for d in x_order:
            send(b_top.at[xat(d)], r_top.at[x], out_s.at[0], top_r.at[1], dev(x_=xat(d)))
        r_top[x] = b_top[x]

    def top_third():
        await_bytes(r_top.at[pl.ds(0, nx - 1)], top_r.at[1])
        total = r_top[0].astype(F32)
        for k in range(1, nx):
            total = total + r_top[k].astype(F32)
        q_top[...] = total.astype(BF16)
        for d in z_order:
            send(q_top.at[zat(d)], z_top.at[z], out_s.at[0], top_r.at[2], dev(z_=zat(d)))
        z_top[z] = q_top[z]

    own = pl.ds(2 * x, 2)

    def top_fourth():
        await_bytes(z_top.at[pl.ds(0, nz - 1)], top_r.at[2])
        for c in range(2):
            at = pl.multiple_of(ylo * fe + (2 * x + c) * LANES, LANES)
            total = og[z, :, pl.ds(at, LANES)].astype(F32)
            for k in range(nz):
                total = total + z_top[k, c].astype(F32)
            xs[top - 1, 2 * x + c] = total.astype(BF16)
        src = xs.at[top - 1, own]
        for d in x_order:
            send(src, src, out_s.at[0], top_r.at[3], dev(x_=xat(d)))

    def spread_z(t):
        src = xs.at[t - 1, own]
        dst = up.at[pl.ds(slot(t, x, ylo, z), 2)]

        def both(d):
            for to in (partner, y):
                send(src, dst, out_s.at[0], ph_r.at[t], dev(core_=0, z_=zat(d), y_=to))

        both(half)

        def pair(i, c):
            both(half - i)
            both(half + i)
            return c

        lax.fori_loop(1, half, pair, 0)
        both(0)

    bounds = sorted({half // 2, 3 * half // 4, half})
    groups = [
        [r for r in range(nz) if (bounds[i - 1] if i else -1) < min(r, nz - r) <= b] for i, b in enumerate(bounds)
    ]
    group_of = {r: i for i, g in enumerate(groups) for r in g}

    def runs(g):
        out = []
        for r in g:
            if out and out[-1][1] == r:
                out[-1][1] = r + 1
            else:
                out.append([r, r + 1])
        return out

    owner = [p if min(p, nx - p) <= 1 else 0 for p in range(nx)]
    owned = {o: [p for p in range(nx) if owner[p] == o] for o in sorted(set(owner))}
    d_order = [half] + [d for i in range(1, half) for d in (half - i, half + i)] + [0]

    def last_z():
        for o, pairs in owned.items():
            @pl.when(x == o)
            def _():
                for d in d_order:
                    r = (nz - d) % nz
                    for p in pairs:
                        src = xs.at[nsec, pl.ds(2 * p, 2)]
                        dst = up.at[pl.ds(slot(0, p, ylo, r), 2)]
                        if o:
                            send(src, dst, out_s.at[0], wx_r.at[group_of[r]], dev(core_=1, z_=zat(d), y_=partner))
                        if d:
                            send(src, dst, out_s.at[0], wx_r.at[group_of[r]], dev(core_=1, z_=zat(d)))
                for p in pairs:
                    up[pl.ds(slot(0, p, ylo, 0), 2)] = xs[nsec, 2 * p:2 * p + 2]

    def last_x(i):
        for o, pairs in owned.items():
            @pl.when(x == o)
            def _():
                per_plane = 4 if o else 2 * len(pairs)
                here = (2 if o else 2 * len(pairs)) if i == 0 else 0
                await_bytes(up.at[pl.ds(0, per_plane * len(groups[i]) - here)], wx_r.at[i])
                for a, b in runs(groups[i]):
                    for p in pairs:
                        for l, to in ((0, y), (1, y)) if o else ((ylo, partner), (ylo, y)):
                            src = up.at[pl.ds(slot(0, p, l, a), 2 * (b - a))]
                            send(src, src, out_s.at[0], top_r.at[i], dev(x_=0, core_=0, y_=to))

    def last_out(i):
        await_bytes(up.at[pl.ds(0, nx * 4 * len(groups[i]))], top_r.at[i])
        for r in groups[i]:
            row = zat(r)
            for l in range(2):
                for k in range(nx):
                    for c in range(2):
                        at = l * fe + (2 * k + c) * LANES
                        ig_out[row, :, at:at + LANES] = up[slot(0, k, l, r) + c]

    def spread_g(t):
        def to(d, c):
            tile = zat(d) // per_tile
            for c_ in range(2):
                send(gbuf.at[t, ylo, c_ * tiles + tile], gz.at[t * nz + z], out_s.at[0], g_r.at[t], dev(core_=c_, z_=zat(d)))
            return c

        lax.fori_loop(1, nz, to, 0)
        tile = z // per_tile
        send(gbuf.at[t, ylo, tile], gz.at[t * nz + z], out_s.at[0], g_r.at[t], dev(core_=0))
        gz[t * nz + z] = gbuf[t, ylo, tiles + tile]

    def turn(away):
        t = lax.rem(z // per_tile + away + tiles, tiles)

        def one(i, c):
            l, c_ = i // 2, lax.rem(i, 2)
            v = wbuf[1, l, c_, pl.ds(t * per_tile, per_tile)].reshape(LANES, fe)
            w_t[l, c_ * tiles + t] = jnp.swapaxes(v, 0, 1)
            return c

        lax.fori_loop(0, 4, one, 0)

    def a_half(s, l, part=None):
        if part is not None:
            a_buf[s, l, y] = part.astype(BF16)
        for d in y_order:
            send(a_buf.at[s, l, y], a_buf.at[s, l, y], out_s.at[0], ph_r.at[l * 2 + (s % 2 if isinstance(s, int) else lax.rem(s, 2))], dev(y_=yat(d)))

    def a_part(s, l, n):
        lhs = jnp.concatenate([xs[s, n * hj + j] for j in range(hj)], axis=1)
        w_out = jnp.concatenate([w_t[l, t, n * hn:(n + 1) * hn] for t in range(2 * tiles)], axis=1)
        return jnp.dot(lhs, w_out, preferred_element_type=F32)

    def a_tiles(l, aways):
        lhs = jnp.concatenate([xs[top - 1, j] for j in range(nsec)], axis=1)
        at = [(c, lax.rem(z // per_tile + d + tiles, tiles)) for d in aways for c in range(2)]
        w_out = jnp.concatenate([wbuf[1, l, c, pl.ds(t * per_tile, per_tile)].reshape(LANES, fe) for c, t in at], axis=0)
        part = lax.dot_general(lhs, w_out, (((1,), (1,)), ((), ())), preferred_element_type=F32).astype(BF16)
        for i, (c, t) in enumerate(at):
            to = pl.ds(pl.multiple_of((c * tiles + t) * LANES, LANES), LANES)
            a_buf[top - 1, l, y, :, to] = part[:, i * LANES:(i + 1) * LANES]

    def release(t):
        pl.semaphore_signal(flag.at[t], inc=1, device_id=dev(core_=0), device_id_type=MESH_ID)

    def await_up(t):
        await_bytes(up.at[pl.ds(0, nx * block)], ud_r.at[t])

    def background_a(s):
        with scope("bg_a"):
            @pl.when(s <= top - 3)
            def _():
                release(s + 2)

            @pl.when(s <= top - 2)
            def _():
                spread_z(s + 1)

            @pl.when(s == top - 2)
            def _():
                first_in_term()

            @pl.when(s <= top - 3)
            def _():
                in_term(s + 2)

            @pl.when(s <= top - 5)
            def _():
                await_up(s + 5)
                out_term(s + 5)

    def g_half(s, l):
        with scope(f"wait_a{l}"):
            await_bytes(a_buf.at[s, l, pl.ds(0, 3)], ph_r.at[l * 2 + (s % 2 if isinstance(s, int) else lax.rem(s, 2))])
        back = a_buf[s, l, 0].astype(F32)
        for k in range(1, 4):
            back = back + a_buf[s, l, k].astype(F32)
        g = []
        for t in range(2 * tiles):
            g_tile = (back[:, t * LANES:(t + 1) * LANES] * slope[s, l, t]).astype(BF16)
            gbuf[s, l, t] = g_tile
            g.append(g_tile)
        return jnp.concatenate(g, axis=1)

    def b_tile(n, away):
        t = lax.rem(z // per_tile + away + tiles, tiles)
        pairs = [(l, c) for l in range(2) for c in range(2)]
        lhs = jnp.concatenate([gbuf[top - 1, l, c * tiles + t] for l, c in pairs], axis=1)
        rows = pl.ds(t * per_tile, per_tile)
        w_in = jnp.concatenate([wbuf[0, l, c, rows, :, n * hn:(n + 1) * hn].reshape(LANES, hn) for l, c in pairs], axis=0)
        return jnp.dot(lhs, w_in, preferred_element_type=F32)

    def application(s, final=False, begin=False):
        if not begin:
            background_a(s)
            g_first = g_half(s, 0)
            for n in range(2):
                w_in = wbuf[0, 0, :, :, :, n * hn:(n + 1) * hn].reshape(hu, hn)
                b_acc[n] = jnp.dot(g_first, w_in, preferred_element_type=F32)
            g = g_half(s, 1)
        for n in range(2):
            if begin:
                part = b_tile(n, tiles // 2)
            else:
                w_in = wbuf[0, 1, :, :, :, n * hn:(n + 1) * hn].reshape(hu, hn)
                part = jnp.dot(g, w_in, preferred_element_type=F32)
            part = (b_acc[n] + part).astype(BF16)
            for j in range(hj):
                b_buf[s, n, x, j] = part[:, j * LANES:(j + 1) * LANES]
            if not final:
                src = b_buf.at[s, n, x]
                for d in x_order:
                    send(src, src, out_s.at[0], ph_r.at[4 + n * 2 + (s % 2 if isinstance(s, int) else lax.rem(s, 2))], dev(x_=xat(d)))
        hx = nx // 2
        if final:
            for p in range(nx):
                @pl.when(x != owner[p])
                def _():
                    src = b_buf.at[s, p // hx, x, pl.ds(2 * (p % hx), 2)]
                    send(src, src, out_s.at[0], ph_r.at[4 + s % 2], dev(x_=owner[p]))

        with scope("bg_b"):
            spread_g(s)
            if begin:
                spread_z(top)

        if final:
            for o, pairs in owned.items():
                @pl.when(x == o)
                def _():
                    with scope("wait_b"):
                        await_bytes(gz.at[pl.ds(0, 2 * (nx - 1) * len(pairs))], ph_r.at[4 + s % 2])
                    for p in pairs:
                        for c in range(2):
                            total = xs[s, 2 * p + c].astype(F32)
                            for k in range(nx):
                                total = total + b_buf[s, p // hx, k, 2 * (p % hx) + c].astype(F32)
                            xs[nsec, 2 * p + c] = total.astype(BF16)
            return
        for n in range(2):
            with scope(f"wait_b{n}"):
                await_bytes(b_buf.at[s, n, pl.ds(0, nx - 1)], ph_r.at[4 + n * 2 + (s % 2 if isinstance(s, int) else lax.rem(s, 2))])
            with scope(f"a_mm{n}"):
                for j in range(hj):
                    total = xs[s, n * hj + j].astype(F32)
                    for k in range(nx):
                        total = total + b_buf[s, n, k, j].astype(F32)
                    xs[s - 1, n * hj + j] = total.astype(BF16)
                if n == 0:
                    for l in range(2):
                        a_acc[l] = a_part(s - 1, l, 0)
        for l in range(2):
            with scope(f"a_last{l}"):
                a_half(s - 1, l, a_acc[l] + a_part(s - 1, l, 1))

    @pl.when(core == 1)
    def _():
        plan = [
            (1, top_first), (2, top_second), (2, li_first), (4, all_met), (4, top_third), (5, first_out_term), (6, li_second),
            (6, stage_c), (7, stage_d), (7, top_fourth),
        ]
        plan += [(5, lambda: turn(0))] if tiles > 1 else []
        for k in range(1, half + 1):
            with scope(f"hop{k}"):
                if k == 1:
                    blocks = ((1, 1, 0), (0, 1, 0), (1, 1, 1))
                elif k == 2:
                    blocks = ((1, 2, 0), (0, 1, 1), (1, 2, 1))
                else:
                    blocks = ((1, k, 0), (0, k - 1, 0), (1, k, 1), (0, k - 1, 1))
                for b in blocks:
                    hop(*b)
            with scope(f"stage{k}"):
                for at, f in plan:
                    if min(at, half) == k:
                        f()
        early = [d for d in (0, -1, 1) if d % tiles != tiles // 2]
        with scope("top_end"):
            await_bytes(xs.at[0, pl.ds(0, 2 * (nx - 1))], top_r.at[3])
            for l in range(2):
                if early:
                    a_tiles(l, early)
        with scope("gather_out"):
            hop(0, half, 0)
            await_last(1)
        with scope("a_first"):
            for l in range(2):
                a_tiles(l, (tiles // 2,))
                a_half(top - 1, l)
        with scope("hop_end"):
            hop(0, half, 1)
        with scope("turn"):
            for d in sorted({1 % tiles, (tiles - 1) % tiles, tiles // 2} - ({0} if tiles > 1 else set())):
                turn(d)
        with scope("b_early"):
            for l in range(2):
                g_half(top - 1, l)
            for n in range(2):
                b_acc[n] = sum((b_tile(n, d) for d in early), jnp.zeros((8, hn), F32))
        with scope("gather_in"):
            await_last(0)
        li_third()

        application(top - 1, begin=True)

        def step(i, carry):
            application(top - 2 - i)
            return carry

        lax.fori_loop(0, top - 2, step, 0)
        application(0, final=True)

        with scope("t_z0"):
            last_z()
            release(1)
        with scope("t_terms"):
            in_term(1)
            for t in range(min(top, 4), 3, -1):
                await_up(t)
                out_term(t)
        with scope("t_in0"):
            in_term(0)
        for i in range(len(groups)):
            with scope(f"t_last{i}"):
                last_x(i)
        with scope("t_up2"):
            for t in (3, 2):
                await_up(t)
                out_term(t)
        with scope("t_up1"):
            await_up(1)
            out_term(1)

    def await_z(t):
        await_bytes(up.at[pl.ds(0, block)], ph_r.at[t])

    def spread_x(t):
        await_z(t)
        if not isinstance(t, int) or t < top:
            pl.semaphore_wait(flag.at[t], 1)
        src = up.at[pl.ds(slot(t, x), block)]
        if isinstance(t, int) and t == 1:
            for d in x_order:
                send(src, src, out_s.at[0], wx_r.at[d], dev(x_=xat(d)))
        else:
            for d in (1, nx - 1) if ring else x_order:
                send(src, src, out_s.at[0], ud_r.at[t], dev(x_=xat(d)))


    def pass_x(t):
        if ring:
            await_bytes(up.at[pl.ds(0, 2 * block)], ud_r.at[t])
            for l, d in ((0, 1), (1, -1)):
                src = up.at[pl.ds(slot(t, xat(-d), l), 2 * nz)]
                send(src, src, out_s.at[0], wz_r.at[t], dev(x_=xat(d)))

    def to_core(t, x_, blocks):
        src = up.at[pl.ds(slot(t, x_), blocks * block)]
        send(src, src, out_s.at[2], ud_r.at[t], dev(core_=1))

    def spread_core(t):
        if ring:
            await_bytes(up.at[pl.ds(0, block)], wz_r.at[t])
        else:
            await_bytes(up.at[pl.ds(0, (nx - 1) * block)], ud_r.at[t])
        to_core(t, 0, nx)

    def spread_core_last():
        for d in reversed(x_order):
            await_bytes(up.at[pl.ds(0, block)], wx_r.at[d])
            to_core(1, xat(-d), 1)

    @pl.when(core == 0)
    def _():
        spread_pre()
        for r in range(half - 1):
            meet(r)
        pl.semaphore_signal(flag.at[half - 1], inc=1, device_id=dev(core_=1), device_id_type=MESH_ID)
        pa_first()
        li_first()
        pa_second()
        stage_b()
        og_in.wait()
        first_out_term()
        li_second()
        li_third()
        await_bytes(g_top, top_r.at[4])
        first_in_term()

        def finish_one(t):
            with scope("s_core"):
                spread_core(t)
            with scope("s_out"):
                out_term(t)

        def move(i, carry):
            t = top - 1 - i
            with scope("s_x"):
                spread_x(t)
            with scope("s_in"):
                in_term(t)
            finish_one(t + 1)
            with scope("s_pass"):
                pass_x(t)
            return carry

        with scope("s_x7"):
            spread_x(top)
            pass_x(top)
        lax.fori_loop(0, top - 2, move, 0)
        with scope("s_x1"):
            spread_x(1)
            to_core(1, x, 1)
        finish_one(2)
        with scope("s_in"):
            for t in (1, 0):
                in_term(t)
        with scope("s_core1"):
            spread_core_last()
        with scope("s_out1"):
            out_term(1)

        @pl.when(x == 0)
        def _():
            for i in range(len(groups)):
                with scope(f"s_last{i}"):
                    last_out(i)

    def size(*shape):
        return math.prod(shape) // (8 * LANES)

    li_block, row = size(tok, width), size(fb, tok)
    both_cores = size(2, fb, fe) + nsec * row
    by_core = (
        size(2, fb, fe) + row + size(2, half, 8, nsec * fb) + nx * size(2, 2, tiles, 8, LANES) + top * (nx - 1) * block,
        size(nz, 8, nsec * fb)
        + size(nsec, 2, tiles, 8, LANES)
        + 3 * size(4 * fb, tok)
        + (nx - 1) * 2 * nz
        + (nz - 1) * 2
        + (nx - 1) * 2
        + row
        + top * 2 * 3 * size(8, hu)
        + (top - 1) * 2 * (nx - 1) * hj
        + top * (2 * nz - 1)
        + top * block,
    )
    with scope("drain"):
        await_bytes(spare.at[pl.ds(0, (nx + (3 if ring else 1)) * li_block)], out_s.at[1])

        @pl.when(core == 1)
        def _():
            for way in range(2):
                await_bytes(wbuf.at[0, :, :, pl.ds(0, nz - 1)], wz_s.at[way])

        for o in range(nx):
            pairs = owned.get(o, [])
            last_tiles = 2 * sum(owner[p] != o for p in range(nx))
            if pairs:
                last_tiles += (block - 2 if o else 2 * len(pairs) * (nz - 1)) + (block if o else block * len(pairs))

            @pl.when((core == 1) & (x == o))
            def _():
                await_bytes(spare.at[pl.ds(0, both_cores + by_core[1] + last_tiles)], out_s.at[0])

        @pl.when(core == 0)
        def _():
            await_bytes(spare.at[pl.ds(0, top * nx * block)], out_s.at[2])

        for h in range(2):
            @pl.when((core == 0) & (yhi == h))
            def _():
                pa_tiles = 2 * (half - 1 + h) * size(8, nsec * fb)
                await_bytes(spare.at[pl.ds(0, both_cores + by_core[0] + pa_tiles)], out_s.at[0])


def finish(ig, gi, go, ig_out, gi_out, go_out, sems):
    copies = [pltpu.make_async_copy(src, dst, sems.at[k]) for k, (src, dst) in enumerate(((ig, ig_out), (gi, gi_out), (go, go_out)))]
    for cp in copies:
        cp.start()
    for cp in copies:
        cp.wait()


def body(layer_inputs, pre_act, out_grad, w_in, w_out):
    nz, nx = lax.axis_size("z"), lax.axis_size("x")
    nsec = 2 * nx
    tok, width = out_grad.shape
    fb = w_in.shape[2]
    hid = pre_act.shape[2]
    fe = width // 2
    tiles = nz * fb // LANES
    half = nz // 2
    dma = pltpu.SemaphoreType.DMA
    vmem = pltpu.VMEM
    spare = 2048
    scratch = [
        vmem((2, fb, width), BF16),
        vmem((2, 2, 2, nz, fb, fe), BF16),
        vmem((2, nz, 8, hid), BF16),
        vmem((2, 2, half, 8, hid), BF16),
        vmem((nx, 2, 2, tiles, 8, LANES), BF16),
        vmem((2, nsec, 2, tiles, 8, LANES), BF16),
        vmem((nsec, 2, 2 * tiles, 8, LANES), F32),
        vmem((nsec, fb, tok), BF16),
        vmem((nsec, fb, tok), BF16),
        vmem((2, 2, fb, tok), BF16),
        vmem((nsec, fb, tok), BF16),
        vmem((2, nx, tok, width), BF16),
        vmem((nz, 8, width), BF16),
        vmem((4, 4 * fb, tok), BF16),
        vmem((nx, nz, 2, 8, LANES), BF16),
        vmem((nx, nz, 2, 8, LANES), BF16),
        vmem((nz, 2, 8, LANES), BF16),
        vmem((nz, 2, 8, LANES), BF16),
        vmem((fb, tok), BF16),
        vmem((fb, tok), BF16),
        vmem((2, 2 * tiles, fe, LANES), BF16),
        vmem((nsec + 1, nsec, 8, LANES), BF16),
        vmem((nsec, 2, 4, 8, 2 * nz * fb), BF16),
        vmem((nsec, 2, nx, nx, 8, LANES), BF16),
        vmem((2, 8, 2 * nz * fb), F32),
        vmem((2, 8, fe // 2), F32),
        vmem((nsec, 2, 2 * tiles, 8, LANES), BF16),
        vmem((nsec * nz, 8, LANES), BF16),
        vmem((LANES, tok), F32),
        vmem((nsec * nx * 4 * nz, 8, LANES), BF16),
        vmem((spare, 8, LANES), BF16),
        dma((7,)),
        dma((3,)), dma((2,)),
        dma((4,)),
        dma((2,)),
        dma((max(8, nsec),)),
        dma((6,)),
        dma((1,)),
        dma((5,)),
        dma((max(8, nsec),)),
        dma((5,)),
        dma((nsec,)),
        dma((nsec,)),
        pltpu.SemaphoreType.REGULAR((max(nsec, half),)),
    ]
    hbm, on_chip = pl.BlockSpec(memory_space=pltpu.HBM), pl.BlockSpec(memory_space=pltpu.VMEM)
    shapes = (
        jax.ShapeDtypeStruct((nz, 8, width), BF16),
        jax.ShapeDtypeStruct((fb, width), F32),
        jax.ShapeDtypeStruct((fb, width), F32),
    )
    operands = (
        layer_inputs.reshape(tok, width),
        pre_act.reshape(nz, 8, hid),
        out_grad.reshape(nz, 8, width),
        w_in.reshape(fb, width),
        w_out.reshape(fb, width),
    )
    results = pl.pallas_call(
        kernel,
        out_shape=shapes,
        in_specs=[hbm] * 5,
        out_specs=(on_chip,) * 3,
        scratch_shapes=scratch,
        name="chain",
        compiler_params=pltpu.CompilerParams(
            collective_id=0, has_side_effects=True, vmem_limit_bytes=40 * 1024 * 1024
        ),
    )(*(pltpu.with_memory_space_constraint(v, pltpu.HBM) for v in operands))
    ig, gi, go = pl.pallas_call(
        finish,
        out_shape=shapes,
        in_specs=[on_chip] * 3,
        out_specs=(hbm,) * 3,
        scratch_shapes=[dma((3,))],
        name="finish",
    )(*(pltpu.with_memory_space_constraint(v, pltpu.VMEM) for v in results))
    return (
        ig.reshape(1, tok, width),
        gi.reshape(1, 1, fb, width),
        go.reshape(1, 1, fb, width),
    )


def solution(mesh):
    shape = mesh.shape
    split = Mesh(
        mesh.devices.reshape(shape["section"] // 2, 2, shape["dp"] // 2, 2, shape["mp"]), AXES
    )
    sec, dp = ("x", "core"), ("z", "ylo")
    placed = (
        P(sec, None, "yhi"),
        P(sec, None, dp),
        P(None, "yhi"),
        P(dp, sec, None, "yhi"),
        P(dp, sec, None, "yhi"),
    )
    return jax.shard_map(
        body,
        mesh=split,
        in_specs=placed,
        out_specs=(P(sec, None, "yhi"), P(dp, sec, None, "yhi"), P(dp, sec, None, "yhi")),
        check_vma=False,
    )
```

```python
import contextlib
import math

import jax
import jax.numpy as jnp
from jax import lax
from jax.experimental import pallas as pl
from jax.experimental.pallas import tpu as pltpu
from jax.sharding import Mesh
from jax.sharding import PartitionSpec as P

AXES = ("x", "core", "z", "ylo", "yhi")
MESH_ID = pl.DeviceIdType.MESH
BF16, F32 = jnp.bfloat16, jnp.float32
LANES = 128
PROFILE = False


def scope(name):
    return jax.named_scope(name) if PROFILE else contextlib.nullcontext()


def gelu_parts(v):
    cdf = 0.5 * (1.0 + lax.erf(v * 0.7071067811865476))
    dens = jnp.exp(-0.5 * v * v) * 0.3989422804014327
    return cdf, dens


def kernel(
    li_hbm, pa_hbm, og_hbm, wi_hbm, wo_hbm,
    ig_out, gi_out, go_out,
    w_own, wbuf, pa, pa_all, pb, pc, slope, pa_t, pre_t, pre_top, hall, li, og,
    a_top, b_top, r_top, q_top, z_top, g_top, g_pass,
    w_t, xs, a_buf, b_buf, a_acc, b_acc, gbuf, gz, gt, up,
    spare, lsem, out_s, wz_s, wx_r, wd_r, wz_r, st_r, pt_r, top_r, ph_r, li_r, g_r, ud_r, flag,
):
    nx, nz = lax.axis_size("x"), lax.axis_size("z")
    nsec = 2 * nx
    top = nsec - 1
    fb, width = wi_hbm.shape
    fe = width // 2
    tok = nz * 8
    tiles = nz * fb // LANES
    per_tile = LANES // fb
    x, core, z = lax.axis_index("x"), lax.axis_index("core"), lax.axis_index("z")
    ylo, yhi = lax.axis_index("ylo"), lax.axis_index("yhi")
    sec = x * 2 + core
    y = yhi * 2 + ylo
    other = 1 - ylo
    partner = yhi * 2 + other

    def dev(x_=None, core_=None, z_=None, y_=None):
        y_ = y if y_ is None else y_
        return (
            x if x_ is None else x_,
            core if core_ is None else core_,
            z if z_ is None else z_,
            lax.rem(y_, 2),
            y_ // 2,
        )

    def send(src, dst, ssem, rsem, to):
        cp = pltpu.make_async_remote_copy(
            src_ref=src, dst_ref=dst, send_sem=ssem, recv_sem=rsem, device_id=to, device_id_type=MESH_ID
        )
        cp.start()
        return cp

    def await_bytes(ref, sem):
        pltpu.make_async_copy(ref, ref, sem).wait()

    def zat(d):
        return lax.rem(z + d + nz, nz)

    def xat(d):
        return lax.rem(x + d + nx, nx)

    def yat(d):
        return lax.rem(y + d, 4)

    y_order = (2, 1, 3)
    x_order = sorted(range(1, nx), key=lambda d: -min(d, nx - d))
    z_order = sorted(range(1, nz), key=lambda d: -min(d, nz - d))
    sections = [(d, False) for d in x_order] + [(d, True) for d in x_order] + [(0, True)]

    def peer(d, cross):
        return xat(d), (1 - core if cross else core)

    mine = pl.ds(pl.multiple_of(ylo * fe, LANES), fe)
    theirs = pl.ds(pl.multiple_of(other * fe, LANES), fe)

    w_hbm = (wi_hbm, wo_hbm)
    pa_in = pltpu.make_async_copy(pa_hbm, pa.at[core], lsem.at[0])
    w_in_ = [pltpu.make_async_copy(w_hbm[m].at[:, mine], wbuf.at[m, ylo, 1, z], lsem.at[1 + m]) for m in range(2)]
    og_in = pltpu.make_async_copy(og_hbm, og, lsem.at[3])
    li_in = pltpu.make_async_copy(li_hbm, li.at[core, x], lsem.at[4])
    barrier = pltpu.get_barrier_semaphore()
    greeted = [dev(z_=zat(d)) for d in (1, -1)] + [dev(*peer(*p)) for p in sections]
    greeted += [dev(y_=yat(d)) for d in range(1, 4)] + [dev(core_=1 - core, y_=partner)]
    for to in greeted:
        pl.semaphore_signal(barrier, inc=1, device_id=to, device_id_type=MESH_ID)

    first = (1, 0)
    own_in = [pltpu.make_async_copy(w_hbm[m], w_own.at[m], lsem.at[5 + m]) for m in range(2)]
    for m in first:
        own_in[m].start()

        @pl.when(core == 1)
        def _():
            w_in_[m].start()

    pa_in.start()

    og_in.start()
    li_in.start()

    with scope("barrier"):
        pl.semaphore_wait(barrier, len(greeted))

    half = nz // 2

    def meet(r):
        for d in (1, -1):
            pl.semaphore_signal(flag.at[r], inc=1, device_id=dev(z_=zat(d)), device_id_type=MESH_ID)
        pl.semaphore_wait(flag.at[r], 2)

    def pa_first():
        await_bytes(pa.at[1], st_r.at[5])
        for h in range(2):
            @pl.when(yhi == h)
            def _():
                for d in z_order:
                    if d % 2 == h:
                        for c in range(2):
                            dst = pa_all.at[c, lax.rem(z, 2), z // 2]
                            send(pa.at[c, zat(d)], dst, out_s.at[0], st_r.at[0], dev(z_=zat(d)))
                if h == 0:
                    for c in range(2):
                        pa_all[c, lax.rem(z, 2), z // 2] = pa[c, z]

    def await_pa(sem):
        for h in range(2):
            @pl.when(yhi == h)
            def _():
                await_bytes(pa.at[0, pl.ds(0, 2 * (half - 1 + h))], sem)

    def pa_second():
        await_pa(st_r.at[0])
        mine_ = pa_all.at[:, lax.rem(z + yhi, 2)]
        send(mine_, mine_, out_s.at[0], st_r.at[4], dev(y_=yat(2)))

    def ring_send(src, m, l, k, way):
        send(src, src, wz_s.at[way], wz_r.at[((k - 1) % 2 * 2 + m) * 2 + l], dev(z_=zat(1 if way == 0 else -1)))

    swaps = []
    for m in first:
        own_in[m].wait()

        @pl.when(core == 0)
        def _():
            send(w_own.at[m, :, mine], wbuf.at[m, ylo, 0, z], out_s.at[0], wd_r.at[m], dev(core_=1))

        @pl.when(core == 1)
        def _():
            w_in_[m].wait()
            for way in range(2):
                ring_send(wbuf.at[m, ylo, 1, z], m, ylo, 1, way)

        dst = wbuf.at[m, ylo, core, z]
        swaps.append(send(w_own.at[m, :, theirs], dst, out_s.at[0], wx_r.at[core * 2 + m], dev(core_=1, y_=partner)))

    pa_in.wait()

    @pl.when(core == 1)
    def _():
        send(pa.at[1], pa.at[1], out_s.at[0], st_r.at[5], dev(core_=0))

    v = pa[core].astype(F32).reshape(tok, nsec * fb)
    pa_t[...] = jnp.swapaxes(v, 0, 1).astype(BF16).reshape(nsec, fb, tok)
    for p in sections:
        to = peer(*p)
        send(pa_t.at[to[0] * 2 + to[1]], pre_t.at[sec], out_s.at[0], st_r.at[3], dev(*to))
    pre_t[sec] = pa_t[sec]

    def spread_pre():
        await_bytes(pre_t.at[pl.ds(0, nsec - 1)], st_r.at[3])
        dst = pre_top.at[ylo, core]
        send(pre_t.at[top], dst, out_s.at[0], pt_r.at[0], dev(core_=1, y_=partner))

        @pl.when(core == 0)
        def _():
            send(pre_t.at[top], dst, out_s.at[0], pt_r.at[0], dev(core_=1))

        @pl.when(core == 1)
        def _():
            dst[...] = pre_t[top]

    def stage_b():
        await_bytes(pa_all.at[:, 0], st_r.at[4])
        group = lax.broadcasted_iota(jnp.int32, (8, LANES), 1) // fb
        for c in range(2):
            for ct in range(nsec // per_tile):
                for t in range(tiles):
                    out = [jnp.zeros((8, LANES), F32)] * per_tile
                    for j in range(per_tile):
                        at = t * per_tile + j
                        v = pa_all[c, at % 2, at // 2, :, ct * LANES:(ct + 1) * LANES].astype(F32)
                        for k in range(per_tile):
                            shift = (j - k) * fb % LANES
                            r = pltpu.roll(v, shift, 1) if shift else v
                            out[k] = jnp.where(group == j, r, out[k])
                    for k in range(per_tile):
                        to = ct * per_tile + k
                        pb[to // 2, c, to % 2, t] = out[k].astype(BF16)
        for d in x_order + [0]:
            send(pb.at[xat(d)], pc.at[ylo, pl.ds(2 * x, 2)], out_s.at[0], st_r.at[1], dev(x_=xat(d), core_=1))

    cut = tok // 2
    lo, hi = pl.ds(0, cut), pl.ds(cut, cut)
    ring = nx > 2

    def li_first():
        li_in.wait()
        src = li.at[core, x]
        send(src, src, out_s.at[1], li_r.at[0], dev(x_=xat(1)))
        if ring:
            send(src, src, out_s.at[1], li_r.at[1], dev(x_=xat(-1)))

    def li_second():
        await_bytes(li.at[0, 0], li_r.at[0])
        if ring:
            src = li.at[core, xat(-1), lo]
            send(src, src, out_s.at[1], li_r.at[2], dev(x_=xat(1)))
            await_bytes(li.at[0, 0], li_r.at[1])
            src = li.at[core, xat(1), hi]
            send(src, src, out_s.at[1], li_r.at[3], dev(x_=xat(-1)))

    def li_third():
        if ring:
            await_bytes(li.at[0, 0, lo], li_r.at[2])
            await_bytes(li.at[0, 0, hi], li_r.at[3])
        send(li.at[core], li.at[core], out_s.at[1], li_r.at[4], dev(core_=1 - core))

    def first_out_term():
        for s in range(nsec):
            v = pre_t[s].astype(F32)
            hall[s] = (v * gelu_parts(v)[0]).astype(BF16)
        go_out[...] = jnp.dot(hall[top], og[...].reshape(tok, width), preferred_element_type=F32)

    def first_in_term():
        await_bytes(li.at[0], li_r.at[4])
        gi_out[...] = jnp.dot(g_top[...], li[top % 2, top // 2], preferred_element_type=F32)

    block = 4 * nz

    def slot(t, x_, ylo_=0, z_=0):
        return ((((t * nx + x_) * 2 + ylo_) * nz) + z_) * 2

    def columns(t, x_, l):
        return up[pl.ds(slot(t, x_, l), 2 * nz)].reshape(nz, 2, 8, LANES)

    def out_term(t):
        rows = hall[t - 1]
        for l in range(2):
            parts = []
            for k in range(nx):
                v = columns(t, k, l)
                parts += [v[:, c].reshape(tok, LANES) for c in range(2)]
            go_out[:, l * fe:(l + 1) * fe] += jnp.dot(rows, jnp.concatenate(parts, axis=1), preferred_element_type=F32)

        @pl.when(sec == t)
        def _():
            for l in range(2):
                for k in range(nx):
                    v = columns(t, k, l)
                    for c in range(2):
                        at = l * fe + (2 * k + c) * LANES
                        ig_out[:, :, at:at + LANES] = v[:, c]

    def in_term(t):
        @pl.when(core == 1)
        def _():
            await_bytes(gz.at[pl.ds(0, nz - 1)], g_r.at[t])

        @pl.when(core == 0)
        def _():
            await_bytes(gz.at[pl.ds(0, nz)], g_r.at[t])

        gt[...] = jnp.swapaxes(gz[pl.ds(t * nz, nz)].astype(F32).reshape(tok, LANES), 0, 1)
        rows = gt[pl.ds(pl.multiple_of(lax.rem(z, per_tile) * fb, fb), fb), :].astype(BF16)
        gi_out[...] += jnp.dot(rows, li[lax.rem(t, 2), t // 2], preferred_element_type=F32)

    hu, hn, hj = 2 * nz * fb, fe // 2, nsec // 2
    def hop(m, k, which):
        l = ylo if which == 0 else other
        if k == 1:
            if which == 0:
                await_bytes(wbuf.at[m, 0, 0, 0], wd_r.at[m])
            else:
                for c in range(2):
                    await_bytes(wbuf.at[m, 0, 0, 0], wx_r.at[c * 2 + m])
        if k > 1:
            await_bytes(wbuf.at[m, 0, :, pl.ds(0, 2)], wz_r.at[(k % 2 * 2 + m) * 2 + l])
        for way, step in ((0, 1), (1, -1)):
            if k == 1 and which == 0:
                ring_send(wbuf.at[m, l, 0, z], m, l, 1, way)
            elif k == half:
                ring_send(wbuf.at[m, l, way, zat(-step * (k - 1))], m, l, k, way)
            else:
                ring_send(wbuf.at[m, l, :, zat(-step * (k - 1))], m, l, k, way)

    def await_last(m):
        for l in range(2):
            await_bytes(wbuf.at[m, 0, :, 0], wz_r.at[((half - 1) % 2 * 2 + m) * 2 + l])

    def all_met():
        pl.semaphore_wait(flag.at[half - 1], 1)

    def stage_c():
        await_bytes(pc.at[0], st_r.at[1])
        send(pc.at[ylo], pc.at[ylo], out_s.at[0], st_r.at[2], dev(y_=partner))

    def stage_d():
        await_bytes(pc.at[0], st_r.at[2])

        def one(s, carry):
            for l in range(2):
                v = pc[l, s].astype(F32)
                cdf, dens = gelu_parts(v)
                slope[s, l] = (cdf + v * dens).reshape(2 * tiles, 8, LANES)
            return carry

        lax.fori_loop(0, top, one, 0)

    def top_first():
        og_in.wait()
        rows = wbuf[1, :, :, z].reshape(4 * fb, fe)
        a_top[y] = lax.dot_general(
            rows, og[:, :, mine].reshape(tok, fe), (((1,), (1,)), ((), ())), preferred_element_type=F32
        ).astype(BF16)
        for d in y_order:
            send(a_top.at[y], a_top.at[y], out_s.at[0], top_r.at[0], dev(y_=yat(d)))
        spread_pre()

    def top_second():
        await_bytes(pre_t.at[pl.ds(0, 3)], pt_r.at[0])
        v = pre_top[...].astype(F32).reshape(4 * fb, tok)
        cdf, dens = gelu_parts(v)
        await_bytes(a_top.at[pl.ds(0, 3)], top_r.at[0])
        back = a_top[0].astype(F32)
        for k in range(1, 4):
            back = back + a_top[k].astype(F32)
        g = (back * (cdf + v * dens)).astype(BF16)
        g_pass[...] = jnp.where(ylo == 0, g[:fb], g[2 * fb:3 * fb])
        send(g_pass, g_top, out_s.at[0], top_r.at[4], dev(core_=0))
        g_top[...] = jnp.where(ylo == 0, g[fb:2 * fb], g[3 * fb:])
        rows = jnp.swapaxes(g.astype(F32), 0, 1).astype(BF16)
        part = jnp.dot(rows, wbuf[0, :, :, z].reshape(4 * fb, fe), preferred_element_type=F32).astype(BF16)
        for j in range(nsec):
            b_top[j // 2, :, j % 2] = part[:, j * LANES:(j + 1) * LANES].reshape(nz, 8, LANES)
        for d in x_order:
            send(b_top.at[xat(d)], r_top.at[x], out_s.at[0], top_r.at[1], dev(x_=xat(d)))
        r_top[x] = b_top[x]

    def top_third():
        await_bytes(r_top.at[pl.ds(0, nx - 1)], top_r.at[1])
        total = r_top[0].astype(F32)
        for k in range(1, nx):
            total = total + r_top[k].astype(F32)
        q_top[...] = total.astype(BF16)
        for d in z_order:
            send(q_top.at[zat(d)], z_top.at[z], out_s.at[0], top_r.at[2], dev(z_=zat(d)))
        z_top[z] = q_top[z]

    own = pl.ds(2 * x, 2)

    def top_fourth():
        await_bytes(z_top.at[pl.ds(0, nz - 1)], top_r.at[2])
        for c in range(2):
            at = pl.multiple_of(ylo * fe + (2 * x + c) * LANES, LANES)
            total = og[z, :, pl.ds(at, LANES)].astype(F32)
            for k in range(nz):
                total = total + z_top[k, c].astype(F32)
            xs[top - 1, 2 * x + c] = total.astype(BF16)
        src = xs.at[top - 1, own]
        for d in x_order:
            send(src, src, out_s.at[0], top_r.at[3], dev(x_=xat(d)))

    def spread_z(t):
        src = xs.at[t - 1, own]
        dst = up.at[pl.ds(slot(t, x, ylo, z), 2)]

        def both(d):
            for to in (partner, y):
                send(src, dst, out_s.at[0], ph_r.at[t], dev(core_=0, z_=zat(d), y_=to))

        both(half)

        def pair(i, c):
            both(half - i)
            both(half + i)
            return c

        lax.fori_loop(1, half, pair, 0)
        both(0)

    bounds = sorted({half // 2, 3 * half // 4, half})
    groups = [
        [r for r in range(nz) if (bounds[i - 1] if i else -1) < min(r, nz - r) <= b] for i, b in enumerate(bounds)
    ]
    group_of = {r: i for i, g in enumerate(groups) for r in g}

    def runs(g):
        out = []
        for r in g:
            if out and out[-1][1] == r:
                out[-1][1] = r + 1
            else:
                out.append([r, r + 1])
        return out

    owner = [p if min(p, nx - p) <= 1 else 0 for p in range(nx)]
    owned = {o: [p for p in range(nx) if owner[p] == o] for o in sorted(set(owner))}
    d_order = [half] + [d for i in range(1, half) for d in (half - i, half + i)] + [0]

    def last_z():
        for o, pairs in owned.items():
            @pl.when(x == o)
            def _():
                for d in d_order:
                    r = (nz - d) % nz
                    for p in pairs:
                        src = xs.at[nsec, pl.ds(2 * p, 2)]
                        dst = up.at[pl.ds(slot(0, p, ylo, r), 2)]
                        if o:
                            send(src, dst, out_s.at[0], wx_r.at[group_of[r]], dev(core_=1, z_=zat(d), y_=partner))
                        if d:
                            send(src, dst, out_s.at[0], wx_r.at[group_of[r]], dev(core_=1, z_=zat(d)))
                for p in pairs:
                    up[pl.ds(slot(0, p, ylo, 0), 2)] = xs[nsec, 2 * p:2 * p + 2]

    def last_x(i):
        for o, pairs in owned.items():
            @pl.when(x == o)
            def _():
                per_plane = 4 if o else 2 * len(pairs)
                here = (2 if o else 2 * len(pairs)) if i == 0 else 0
                await_bytes(up.at[pl.ds(0, per_plane * len(groups[i]) - here)], wx_r.at[i])
                for a, b in runs(groups[i]):
                    for p in pairs:
                        for l, to in ((0, y), (1, y)) if o else ((ylo, partner), (ylo, y)):
                            src = up.at[pl.ds(slot(0, p, l, a), 2 * (b - a))]
                            send(src, src, out_s.at[0], top_r.at[i], dev(x_=0, core_=0, y_=to))

    def last_out(i):
        await_bytes(up.at[pl.ds(0, nx * 4 * len(groups[i]))], top_r.at[i])
        for r in groups[i]:
            row = zat(r)
            for l in range(2):
                for k in range(nx):
                    for c in range(2):
                        at = l * fe + (2 * k + c) * LANES
                        ig_out[row, :, at:at + LANES] = up[slot(0, k, l, r) + c]

    def spread_g(t):
        def to(d, c):
            tile = zat(d) // per_tile
            for c_ in range(2):
                send(gbuf.at[t, ylo, c_ * tiles + tile], gz.at[t * nz + z], out_s.at[0], g_r.at[t], dev(core_=c_, z_=zat(d)))
            return c

        lax.fori_loop(1, nz, to, 0)
        tile = z // per_tile
        send(gbuf.at[t, ylo, tile], gz.at[t * nz + z], out_s.at[0], g_r.at[t], dev(core_=0))
        gz[t * nz + z] = gbuf[t, ylo, tiles + tile]

    def turn(away):
        t = lax.rem(z // per_tile + away + tiles, tiles)

        def one(i, c):
            l, c_ = i // 2, lax.rem(i, 2)
            v = wbuf[1, l, c_, pl.ds(t * per_tile, per_tile)].reshape(LANES, fe)
            w_t[l, c_ * tiles + t] = jnp.swapaxes(v, 0, 1)
            return c

        lax.fori_loop(0, 4, one, 0)

    def a_half(s, l, part=None):
        if part is not None:
            a_buf[s, l, y] = part.astype(BF16)
        for d in y_order:
            send(a_buf.at[s, l, y], a_buf.at[s, l, y], out_s.at[0], ph_r.at[l * 2 + (s % 2 if isinstance(s, int) else lax.rem(s, 2))], dev(y_=yat(d)))

    def a_part(s, l, n):
        lhs = jnp.concatenate([xs[s, n * hj + j] for j in range(hj)], axis=1)
        w_out = jnp.concatenate([w_t[l, t, n * hn:(n + 1) * hn] for t in range(2 * tiles)], axis=1)
        return jnp.dot(lhs, w_out, preferred_element_type=F32)

    def a_tile(l, away, turned):
        lhs = jnp.concatenate([xs[top - 1, j] for j in range(nsec)], axis=1)
        t = lax.rem(z // per_tile + away + tiles, tiles)
        if turned:
            w_out = jnp.concatenate([w_t[l, c * tiles + t] for c in range(2)], axis=1)
            part = jnp.dot(lhs, w_out, preferred_element_type=F32)
        else:
            w_out = wbuf[1, l, :, pl.ds(t * per_tile, per_tile)].reshape(2 * LANES, fe)
            part = lax.dot_general(lhs, w_out, (((1,), (1,)), ((), ())), preferred_element_type=F32)
        for c in range(2):
            at = pl.multiple_of((c * tiles + t) * LANES, LANES)
            a_buf[top - 1, l, y, :, pl.ds(at, LANES)] = part[:, c * LANES:(c + 1) * LANES].astype(BF16)

    def release(t):
        pl.semaphore_signal(flag.at[t], inc=1, device_id=dev(core_=0), device_id_type=MESH_ID)

    def await_up(t):
        await_bytes(up.at[pl.ds(0, nx * block)], ud_r.at[t])

    def background_a(s):
        with scope("bg_a"):
            @pl.when(s <= top - 3)
            def _():
                release(s + 2)

            @pl.when(s <= top - 2)
            def _():
                spread_z(s + 1)

            @pl.when(s == top - 2)
            def _():
                first_in_term()

            @pl.when(s <= top - 3)
            def _():
                in_term(s + 2)

            @pl.when(s <= top - 4)
            def _():
                await_up(s + 4)
                out_term(s + 4)

    def g_half(s, l):
        with scope(f"wait_a{l}"):
            await_bytes(a_buf.at[s, l, pl.ds(0, 3)], ph_r.at[l * 2 + (s % 2 if isinstance(s, int) else lax.rem(s, 2))])
        back = a_buf[s, l, 0].astype(F32)
        for k in range(1, 4):
            back = back + a_buf[s, l, k].astype(F32)
        g = []
        for t in range(2 * tiles):
            g_tile = (back[:, t * LANES:(t + 1) * LANES] * slope[s, l, t]).astype(BF16)
            gbuf[s, l, t] = g_tile
            g.append(g_tile)
        return jnp.concatenate(g, axis=1)

    def b_tile(n, away):
        t = lax.rem(z // per_tile + away + tiles, tiles)
        pairs = [(l, c) for l in range(2) for c in range(2)]
        lhs = jnp.concatenate([gbuf[top - 1, l, c * tiles + t] for l, c in pairs], axis=1)
        rows = pl.ds(t * per_tile, per_tile)
        w_in = jnp.concatenate([wbuf[0, l, c, rows, :, n * hn:(n + 1) * hn].reshape(LANES, hn) for l, c in pairs], axis=0)
        return jnp.dot(lhs, w_in, preferred_element_type=F32)

    def application(s, final=False, begin=False):
        if not begin:
            background_a(s)
            g_first = g_half(s, 0)
            for n in range(2):
                w_in = wbuf[0, 0, :, :, :, n * hn:(n + 1) * hn].reshape(hu, hn)
                b_acc[n] = jnp.dot(g_first, w_in, preferred_element_type=F32)
            g = g_half(s, 1)
        for n in range(2):
            if begin:
                part = b_tile(n, tiles // 2)
            else:
                w_in = wbuf[0, 1, :, :, :, n * hn:(n + 1) * hn].reshape(hu, hn)
                part = jnp.dot(g, w_in, preferred_element_type=F32)
            part = (b_acc[n] + part).astype(BF16)
            for j in range(hj):
                b_buf[s, n, x, j] = part[:, j * LANES:(j + 1) * LANES]
            if not final:
                src = b_buf.at[s, n, x]
                for d in x_order:
                    send(src, src, out_s.at[0], ph_r.at[4 + n * 2 + (s % 2 if isinstance(s, int) else lax.rem(s, 2))], dev(x_=xat(d)))
        hx = nx // 2
        if final:
            for p in range(nx):
                @pl.when(x != owner[p])
                def _():
                    src = b_buf.at[s, p // hx, x, pl.ds(2 * (p % hx), 2)]
                    send(src, src, out_s.at[0], ph_r.at[4 + s % 2], dev(x_=owner[p]))

        with scope("bg_b"):
            spread_g(s)
            if begin:
                spread_z(top)

        if final:
            for o, pairs in owned.items():
                @pl.when(x == o)
                def _():
                    with scope("wait_b"):
                        await_bytes(gz.at[pl.ds(0, 2 * (nx - 1) * len(pairs))], ph_r.at[4 + s % 2])
                    for p in pairs:
                        for c in range(2):
                            total = xs[s, 2 * p + c].astype(F32)
                            for k in range(nx):
                                total = total + b_buf[s, p // hx, k, 2 * (p % hx) + c].astype(F32)
                            xs[nsec, 2 * p + c] = total.astype(BF16)
            return
        for n in range(2):
            with scope(f"wait_b{n}"):
                await_bytes(b_buf.at[s, n, pl.ds(0, nx - 1)], ph_r.at[4 + n * 2 + (s % 2 if isinstance(s, int) else lax.rem(s, 2))])
            with scope(f"a_mm{n}"):
                for j in range(hj):
                    total = xs[s, n * hj + j].astype(F32)
                    for k in range(nx):
                        total = total + b_buf[s, n, k, j].astype(F32)
                    xs[s - 1, n * hj + j] = total.astype(BF16)
                if n == 0:
                    for l in range(2):
                        a_acc[l] = a_part(s - 1, l, 0)
        for l in range(2):
            with scope(f"a_last{l}"):
                a_half(s - 1, l, a_acc[l] + a_part(s - 1, l, 1))

    @pl.when(core == 1)
    def _():
        plan = [
            (1, top_first), (2, top_second), (2, li_first), (4, all_met), (4, top_third), (5, first_out_term), (6, li_second),
            (6, stage_c), (7, stage_d), (7, top_fourth),
        ]
        plan += [(half if d else 5, lambda d=d: turn(d)) for d in (0, -1, 1) if d % tiles != tiles // 2]
        for k in range(1, half + 1):
            with scope(f"hop{k}"):
                if k == 1:
                    blocks = ((1, 1, 0), (0, 1, 0), (1, 1, 1))
                elif k == 2:
                    blocks = ((1, 2, 0), (0, 1, 1), (1, 2, 1))
                else:
                    blocks = ((1, k, 0), (0, k - 1, 0), (1, k, 1), (0, k - 1, 1))
                for b in blocks:
                    hop(*b)
            with scope(f"stage{k}"):
                for at, f in plan:
                    if min(at, half) == k:
                        f()
        early = [d for d in (0, -1, 1) if d % tiles != tiles // 2]
        with scope("top_end"):
            await_bytes(xs.at[0, pl.ds(0, 2 * (nx - 1))], top_r.at[3])
            for l in range(2):
                for d in early:
                    a_tile(l, d, True)
        with scope("gather_out"):
            hop(0, half, 0)
            await_last(1)
        with scope("a_first"):
            for l in range(2):
                a_tile(l, tiles // 2, False)
                a_half(top - 1, l)
        with scope("hop_end"):
            hop(0, half, 1)
            turn(tiles // 2)
        with scope("b_early"):
            for l in range(2):
                g_half(top - 1, l)
            for n in range(2):
                b_acc[n] = sum((b_tile(n, d) for d in early), jnp.zeros((8, hn), F32))
        with scope("gather_in"):
            await_last(0)
        li_third()

        application(top - 1, begin=True)

        def step(i, carry):
            application(top - 2 - i)
            return carry

        lax.fori_loop(0, top - 2, step, 0)
        application(0, final=True)

        with scope("t_z0"):
            last_z()
            release(1)
        with scope("t_terms"):
            in_term(1)
            for t in range(min(top, 3), 2, -1):
                await_up(t)
                out_term(t)
        with scope("t_in0"):
            in_term(0)
        for i in range(len(groups)):
            with scope(f"t_last{i}"):
                last_x(i)
        with scope("t_up2"):
            await_up(2)
            out_term(2)
        with scope("t_up1"):
            await_up(1)
            out_term(1)

    def await_z(t):
        await_bytes(up.at[pl.ds(0, block)], ph_r.at[t])

    def spread_x(t):
        await_z(t)
        if not isinstance(t, int) or t < top:
            pl.semaphore_wait(flag.at[t], 1)
        src = up.at[pl.ds(slot(t, x), block)]
        for d in x_order:
            to_sem = wx_r.at[d] if isinstance(t, int) and t == 1 else ud_r.at[t]
            send(src, src, out_s.at[0], to_sem, dev(x_=xat(d)))

    def to_core(t, x_, blocks):
        src = up.at[pl.ds(slot(t, x_), blocks * block)]
        send(src, src, out_s.at[2], ud_r.at[t], dev(core_=1))

    def spread_core(t):
        await_bytes(up.at[pl.ds(0, (nx - 1) * block)], ud_r.at[t])
        to_core(t, 0, nx)

    def spread_core_last():
        for d in reversed(x_order):
            await_bytes(up.at[pl.ds(0, block)], wx_r.at[d])
            to_core(1, xat(-d), 1)

    @pl.when(core == 0)
    def _():
        spread_pre()
        for r in range(half - 1):
            meet(r)
        pl.semaphore_signal(flag.at[half - 1], inc=1, device_id=dev(core_=1), device_id_type=MESH_ID)
        pa_first()
        li_first()
        pa_second()
        stage_b()
        og_in.wait()
        first_out_term()
        li_second()
        li_third()
        await_bytes(g_top, top_r.at[4])
        first_in_term()

        def finish_one(t):
            with scope("s_core"):
                spread_core(t)
            with scope("s_out"):
                out_term(t)

        def move(i, carry):
            t = top - 1 - i
            with scope("s_x"):
                spread_x(t)
            with scope("s_in"):
                in_term(t)
            finish_one(t + 1)
            return carry

        with scope("s_x7"):
            spread_x(top)
        lax.fori_loop(0, top - 2, move, 0)
        with scope("s_x1"):
            spread_x(1)
            to_core(1, x, 1)
        finish_one(2)
        with scope("s_in"):
            for t in (1, 0):
                in_term(t)
        with scope("s_core1"):
            spread_core_last()
        with scope("s_out1"):
            out_term(1)

        @pl.when(x == 0)
        def _():
            for i in range(len(groups)):
                with scope(f"s_last{i}"):
                    last_out(i)

    def size(*shape):
        return math.prod(shape) // (8 * LANES)

    li_block, row = size(tok, width), size(fb, tok)
    both_cores = size(2, fb, fe) + nsec * row
    by_core = (
        size(2, fb, fe) + row + size(2, half, 8, nsec * fb) + nx * size(2, 2, tiles, 8, LANES) + top * (nx - 1) * block,
        size(nz, 8, nsec * fb)
        + size(nsec, 2, tiles, 8, LANES)
        + 3 * size(4 * fb, tok)
        + (nx - 1) * 2 * nz
        + (nz - 1) * 2
        + (nx - 1) * 2
        + row
        + top * 2 * 3 * size(8, hu)
        + (top - 1) * 2 * (nx - 1) * hj
        + top * (2 * nz - 1)
        + top * block,
    )
    with scope("drain"):
        await_bytes(spare.at[pl.ds(0, (nx + (3 if ring else 1)) * li_block)], out_s.at[1])

        @pl.when(core == 1)
        def _():
            for way in range(2):
                await_bytes(wbuf.at[0, :, :, pl.ds(0, nz - 1)], wz_s.at[way])

        for o in range(nx):
            pairs = owned.get(o, [])
            last_tiles = 2 * sum(owner[p] != o for p in range(nx))
            if pairs:
                last_tiles += (block - 2 if o else 2 * len(pairs) * (nz - 1)) + (block if o else block * len(pairs))

            @pl.when((core == 1) & (x == o))
            def _():
                await_bytes(spare.at[pl.ds(0, both_cores + by_core[1] + last_tiles)], out_s.at[0])

        @pl.when(core == 0)
        def _():
            await_bytes(spare.at[pl.ds(0, top * nx * block)], out_s.at[2])

        for h in range(2):
            @pl.when((core == 0) & (yhi == h))
            def _():
                pa_tiles = 2 * (half - 1 + h) * size(8, nsec * fb)
                await_bytes(spare.at[pl.ds(0, both_cores + by_core[0] + pa_tiles)], out_s.at[0])


def finish(ig, gi, go, ig_out, gi_out, go_out, sems):
    copies = [pltpu.make_async_copy(src, dst, sems.at[k]) for k, (src, dst) in enumerate(((ig, ig_out), (gi, gi_out), (go, go_out)))]
    for cp in copies:
        cp.start()
    for cp in copies:
        cp.wait()


def body(layer_inputs, pre_act, out_grad, w_in, w_out):
    nz, nx = lax.axis_size("z"), lax.axis_size("x")
    nsec = 2 * nx
    tok, width = out_grad.shape
    fb = w_in.shape[2]
    hid = pre_act.shape[2]
    fe = width // 2
    tiles = nz * fb // LANES
    half = nz // 2
    dma = pltpu.SemaphoreType.DMA
    vmem = pltpu.VMEM
    spare = 2048
    scratch = [
        vmem((2, fb, width), BF16),
        vmem((2, 2, 2, nz, fb, fe), BF16),
        vmem((2, nz, 8, hid), BF16),
        vmem((2, 2, half, 8, hid), BF16),
        vmem((nx, 2, 2, tiles, 8, LANES), BF16),
        vmem((2, nsec, 2, tiles, 8, LANES), BF16),
        vmem((nsec, 2, 2 * tiles, 8, LANES), F32),
        vmem((nsec, fb, tok), BF16),
        vmem((nsec, fb, tok), BF16),
        vmem((2, 2, fb, tok), BF16),
        vmem((nsec, fb, tok), BF16),
        vmem((2, nx, tok, width), BF16),
        vmem((nz, 8, width), BF16),
        vmem((4, 4 * fb, tok), BF16),
        vmem((nx, nz, 2, 8, LANES), BF16),
        vmem((nx, nz, 2, 8, LANES), BF16),
        vmem((nz, 2, 8, LANES), BF16),
        vmem((nz, 2, 8, LANES), BF16),
        vmem((fb, tok), BF16),
        vmem((fb, tok), BF16),
        vmem((2, 2 * tiles, fe, LANES), BF16),
        vmem((nsec + 1, nsec, 8, LANES), BF16),
        vmem((nsec, 2, 4, 8, 2 * nz * fb), BF16),
        vmem((nsec, 2, nx, nx, 8, LANES), BF16),
        vmem((2, 8, 2 * nz * fb), F32),
        vmem((2, 8, fe // 2), F32),
        vmem((nsec, 2, 2 * tiles, 8, LANES), BF16),
        vmem((nsec * nz, 8, LANES), BF16),
        vmem((LANES, tok), F32),
        vmem((nsec * nx * 4 * nz, 8, LANES), BF16),
        vmem((spare, 8, LANES), BF16),
        dma((7,)),
        dma((3,)), dma((2,)),
        dma((4,)),
        dma((2,)),
        dma((8,)),
        dma((6,)),
        dma((1,)),
        dma((5,)),
        dma((max(8, nsec),)),
        dma((5,)),
        dma((nsec,)),
        dma((nsec,)),
        pltpu.SemaphoreType.REGULAR((max(nsec, half),)),
    ]
    hbm, on_chip = pl.BlockSpec(memory_space=pltpu.HBM), pl.BlockSpec(memory_space=pltpu.VMEM)
    shapes = (
        jax.ShapeDtypeStruct((nz, 8, width), BF16),
        jax.ShapeDtypeStruct((fb, width), F32),
        jax.ShapeDtypeStruct((fb, width), F32),
    )
    operands = (
        layer_inputs.reshape(tok, width),
        pre_act.reshape(nz, 8, hid),
        out_grad.reshape(nz, 8, width),
        w_in.reshape(fb, width),
        w_out.reshape(fb, width),
    )
    results = pl.pallas_call(
        kernel,
        out_shape=shapes,
        in_specs=[hbm] * 5,
        out_specs=(on_chip,) * 3,
        scratch_shapes=scratch,
        name="chain",
        compiler_params=pltpu.CompilerParams(
            collective_id=0, has_side_effects=True, vmem_limit_bytes=40 * 1024 * 1024
        ),
    )(*(pltpu.with_memory_space_constraint(v, pltpu.HBM) for v in operands))
    ig, gi, go = pl.pallas_call(
        finish,
        out_shape=shapes,
        in_specs=[on_chip] * 3,
        out_specs=(hbm,) * 3,
        scratch_shapes=[dma((3,))],
        name="finish",
    )(*(pltpu.with_memory_space_constraint(v, pltpu.VMEM) for v in results))
    return (
        ig.reshape(1, tok, width),
        gi.reshape(1, 1, fb, width),
        go.reshape(1, 1, fb, width),
    )


def solution(mesh):
    shape = mesh.shape
    split = Mesh(
        mesh.devices.reshape(shape["section"] // 2, 2, shape["dp"] // 2, 2, shape["mp"]), AXES
    )
    sec, dp = ("x", "core"), ("z", "ylo")
    placed = (
        P(sec, None, "yhi"),
        P(sec, None, dp),
        P(None, "yhi"),
        P(dp, sec, None, "yhi"),
        P(dp, sec, None, "yhi"),
    )
    return jax.shard_map(
        body,
        mesh=split,
        in_specs=placed,
        out_specs=(P(sec, None, "yhi"), P(dp, sec, None, "yhi"), P(dp, sec, None, "yhi")),
        check_vma=False,
    )
```

```python
import contextlib
import math

import jax
import jax.numpy as jnp
from jax import lax
from jax.experimental import pallas as pl
from jax.experimental.pallas import tpu as pltpu
from jax.sharding import Mesh
from jax.sharding import PartitionSpec as P

AXES = ("x", "core", "z", "ylo", "yhi")
MESH_ID = pl.DeviceIdType.MESH
BF16, F32 = jnp.bfloat16, jnp.float32
LANES = 128
PROFILE = False


def scope(name):
    return jax.named_scope(name) if PROFILE else contextlib.nullcontext()


def gelu_parts(v):
    cdf = 0.5 * (1.0 + lax.erf(v * 0.7071067811865476))
    dens = jnp.exp(-0.5 * v * v) * 0.3989422804014327
    return cdf, dens


def kernel(
    li_hbm, pa_hbm, og_hbm, wi_hbm, wo_hbm,
    ig_out, gi_out, go_out,
    w_own, wbuf, pa, pa_all, pb, pc, slope, pa_t, pre_t, pre_top, hall, li, og,
    a_top, b_top, r_top, q_top, z_top, g_top, g_pass,
    w_t, xs, a_buf, b_buf, a_acc, b_acc, gbuf, gz, gt, up,
    spare, lsem, out_s, wz_s, wx_r, wd_r, wz_r, st_r, pt_r, top_r, ph_r, li_r, g_r, ud_r, flag,
):
    nx, nz = lax.axis_size("x"), lax.axis_size("z")
    nsec = 2 * nx
    top = nsec - 1
    fb, width = wi_hbm.shape
    fe = width // 2
    tok = nz * 8
    tiles = nz * fb // LANES
    per_tile = LANES // fb
    x, core, z = lax.axis_index("x"), lax.axis_index("core"), lax.axis_index("z")
    ylo, yhi = lax.axis_index("ylo"), lax.axis_index("yhi")
    sec = x * 2 + core
    y = yhi * 2 + ylo
    other = 1 - ylo
    partner = yhi * 2 + other

    def dev(x_=None, core_=None, z_=None, y_=None):
        y_ = y if y_ is None else y_
        return (
            x if x_ is None else x_,
            core if core_ is None else core_,
            z if z_ is None else z_,
            lax.rem(y_, 2),
            y_ // 2,
        )

    def send(src, dst, ssem, rsem, to):
        cp = pltpu.make_async_remote_copy(
            src_ref=src, dst_ref=dst, send_sem=ssem, recv_sem=rsem, device_id=to, device_id_type=MESH_ID
        )
        cp.start()
        return cp

    def await_bytes(ref, sem):
        pltpu.make_async_copy(ref, ref, sem).wait()

    def zat(d):
        return lax.rem(z + d + nz, nz)

    def xat(d):
        return lax.rem(x + d + nx, nx)

    def yat(d):
        return lax.rem(y + d, 4)

    y_order = (2, 1, 3)
    x_order = sorted(range(1, nx), key=lambda d: -min(d, nx - d))
    z_order = sorted(range(1, nz), key=lambda d: -min(d, nz - d))
    sections = [(d, False) for d in x_order] + [(d, True) for d in x_order] + [(0, True)]

    def peer(d, cross):
        return xat(d), (1 - core if cross else core)

    mine = pl.ds(pl.multiple_of(ylo * fe, LANES), fe)
    theirs = pl.ds(pl.multiple_of(other * fe, LANES), fe)

    w_hbm = (wi_hbm, wo_hbm)
    pa_in = pltpu.make_async_copy(pa_hbm, pa.at[core], lsem.at[0])
    w_in_ = [pltpu.make_async_copy(w_hbm[m].at[:, mine], wbuf.at[m, ylo, 1, z], lsem.at[1 + m]) for m in range(2)]
    og_in = pltpu.make_async_copy(og_hbm, og, lsem.at[3])
    li_in = pltpu.make_async_copy(li_hbm, li.at[core, x], lsem.at[4])
    barrier = pltpu.get_barrier_semaphore()
    greeted = [dev(z_=zat(d)) for d in (1, -1)] + [dev(*peer(*p)) for p in sections]
    greeted += [dev(y_=yat(d)) for d in range(1, 4)] + [dev(core_=1 - core, y_=partner)]
    for to in greeted:
        pl.semaphore_signal(barrier, inc=1, device_id=to, device_id_type=MESH_ID)

    first = (1, 0)
    own_in = [pltpu.make_async_copy(w_hbm[m], w_own.at[m], lsem.at[5 + m]) for m in range(2)]
    for m in first:
        own_in[m].start()

        @pl.when(core == 1)
        def _():
            w_in_[m].start()

    pa_in.start()

    og_in.start()
    li_in.start()

    with scope("barrier"):
        pl.semaphore_wait(barrier, len(greeted))

    half = nz // 2

    def meet(r):
        for d in (1, -1):
            pl.semaphore_signal(flag.at[r], inc=1, device_id=dev(z_=zat(d)), device_id_type=MESH_ID)
        pl.semaphore_wait(flag.at[r], 2)

    def pa_first():
        await_bytes(pa.at[1], st_r.at[5])
        for h in range(2):
            @pl.when(yhi == h)
            def _():
                for d in z_order:
                    if d % 2 == h:
                        for c in range(2):
                            dst = pa_all.at[c, lax.rem(z, 2), z // 2]
                            send(pa.at[c, zat(d)], dst, out_s.at[0], st_r.at[0], dev(z_=zat(d)))
                if h == 0:
                    for c in range(2):
                        pa_all[c, lax.rem(z, 2), z // 2] = pa[c, z]

    def await_pa(sem):
        for h in range(2):
            @pl.when(yhi == h)
            def _():
                await_bytes(pa.at[0, pl.ds(0, 2 * (half - 1 + h))], sem)

    def pa_second():
        await_pa(st_r.at[0])
        mine_ = pa_all.at[:, lax.rem(z + yhi, 2)]
        send(mine_, mine_, out_s.at[0], st_r.at[4], dev(y_=yat(2)))

    def ring_send(src, m, l, k, way):
        send(src, src, wz_s.at[way], wz_r.at[((k - 1) % 2 * 2 + m) * 2 + l], dev(z_=zat(1 if way == 0 else -1)))

    swaps = []
    for m in first:
        own_in[m].wait()

        @pl.when(core == 0)
        def _():
            send(w_own.at[m, :, mine], wbuf.at[m, ylo, 0, z], out_s.at[0], wd_r.at[m], dev(core_=1))

        @pl.when(core == 1)
        def _():
            w_in_[m].wait()
            for way in range(2):
                ring_send(wbuf.at[m, ylo, 1, z], m, ylo, 1, way)

        dst = wbuf.at[m, ylo, core, z]
        swaps.append(send(w_own.at[m, :, theirs], dst, out_s.at[0], wx_r.at[core * 2 + m], dev(core_=1, y_=partner)))

    pa_in.wait()

    @pl.when(core == 1)
    def _():
        send(pa.at[1], pa.at[1], out_s.at[0], st_r.at[5], dev(core_=0))

    v = pa[core].astype(F32).reshape(tok, nsec * fb)
    pa_t[...] = jnp.swapaxes(v, 0, 1).astype(BF16).reshape(nsec, fb, tok)
    for p in sections:
        to = peer(*p)
        send(pa_t.at[to[0] * 2 + to[1]], pre_t.at[sec], out_s.at[0], st_r.at[3], dev(*to))
    pre_t[sec] = pa_t[sec]

    def spread_pre():
        await_bytes(pre_t.at[pl.ds(0, nsec - 1)], st_r.at[3])
        dst = pre_top.at[ylo, core]
        send(pre_t.at[top], dst, out_s.at[0], pt_r.at[0], dev(core_=1, y_=partner))

        @pl.when(core == 0)
        def _():
            send(pre_t.at[top], dst, out_s.at[0], pt_r.at[0], dev(core_=1))

        @pl.when(core == 1)
        def _():
            dst[...] = pre_t[top]

    def stage_b():
        await_bytes(pa_all.at[:, 0], st_r.at[4])
        group = lax.broadcasted_iota(jnp.int32, (8, LANES), 1) // fb
        for c in range(2):
            for ct in range(nsec // per_tile):
                for t in range(tiles):
                    out = [jnp.zeros((8, LANES), F32)] * per_tile
                    for j in range(per_tile):
                        at = t * per_tile + j
                        v = pa_all[c, at % 2, at // 2, :, ct * LANES:(ct + 1) * LANES].astype(F32)
                        for k in range(per_tile):
                            shift = (j - k) * fb % LANES
                            r = pltpu.roll(v, shift, 1) if shift else v
                            out[k] = jnp.where(group == j, r, out[k])
                    for k in range(per_tile):
                        to = ct * per_tile + k
                        pb[to // 2, c, to % 2, t] = out[k].astype(BF16)
        for d in x_order + [0]:
            send(pb.at[xat(d)], pc.at[ylo, pl.ds(2 * x, 2)], out_s.at[0], st_r.at[1], dev(x_=xat(d), core_=1))

    cut = tok // 2
    lo, hi = pl.ds(0, cut), pl.ds(cut, cut)
    ring = nx > 2

    def li_first():
        li_in.wait()
        src = li.at[core, x]
        send(src, src, out_s.at[1], li_r.at[0], dev(x_=xat(1)))
        if ring:
            send(src, src, out_s.at[1], li_r.at[1], dev(x_=xat(-1)))

    def li_second():
        await_bytes(li.at[0, 0], li_r.at[0])
        if ring:
            src = li.at[core, xat(-1), lo]
            send(src, src, out_s.at[1], li_r.at[2], dev(x_=xat(1)))
            await_bytes(li.at[0, 0], li_r.at[1])
            src = li.at[core, xat(1), hi]
            send(src, src, out_s.at[1], li_r.at[3], dev(x_=xat(-1)))

    def li_third():
        if ring:
            await_bytes(li.at[0, 0, lo], li_r.at[2])
            await_bytes(li.at[0, 0, hi], li_r.at[3])
        send(li.at[core], li.at[core], out_s.at[1], li_r.at[4], dev(core_=1 - core))

    def first_out_term():
        for s in range(nsec):
            v = pre_t[s].astype(F32)
            hall[s] = (v * gelu_parts(v)[0]).astype(BF16)
        go_out[...] = jnp.dot(hall[top], og[...].reshape(tok, width), preferred_element_type=F32)

    def first_in_term():
        await_bytes(li.at[0], li_r.at[4])
        gi_out[...] = jnp.dot(g_top[...], li[top % 2, top // 2], preferred_element_type=F32)

    block = 4 * nz

    def slot(t, x_, ylo_=0, z_=0):
        return ((((t * nx + x_) * 2 + ylo_) * nz) + z_) * 2

    def columns(t, x_, l):
        return up[pl.ds(slot(t, x_, l), 2 * nz)].reshape(nz, 2, 8, LANES)

    def out_term(t):
        rows = hall[t - 1]
        for l in range(2):
            parts = []
            for k in range(nx):
                v = columns(t, k, l)
                parts += [v[:, c].reshape(tok, LANES) for c in range(2)]
            go_out[:, l * fe:(l + 1) * fe] += jnp.dot(rows, jnp.concatenate(parts, axis=1), preferred_element_type=F32)

        @pl.when(sec == t)
        def _():
            for l in range(2):
                for k in range(nx):
                    v = columns(t, k, l)
                    for c in range(2):
                        at = l * fe + (2 * k + c) * LANES
                        ig_out[:, :, at:at + LANES] = v[:, c]

    def in_term(t):
        @pl.when(core == 1)
        def _():
            await_bytes(gz.at[pl.ds(0, nz - 1)], g_r.at[t])

        @pl.when(core == 0)
        def _():
            await_bytes(gz.at[pl.ds(0, nz)], g_r.at[t])

        gt[...] = jnp.swapaxes(gz[pl.ds(t * nz, nz)].astype(F32).reshape(tok, LANES), 0, 1)
        rows = gt[pl.ds(pl.multiple_of(lax.rem(z, per_tile) * fb, fb), fb), :].astype(BF16)
        gi_out[...] += jnp.dot(rows, li[lax.rem(t, 2), t // 2], preferred_element_type=F32)

    hu, hn, hj = 2 * nz * fb, fe // 2, nsec // 2
    def hop(m, k, which):
        l = ylo if which == 0 else other
        if k == 1:
            if which == 0:
                await_bytes(wbuf.at[m, 0, 0, 0], wd_r.at[m])
            else:
                for c in range(2):
                    await_bytes(wbuf.at[m, 0, 0, 0], wx_r.at[c * 2 + m])
        if k > 1:
            await_bytes(wbuf.at[m, 0, :, pl.ds(0, 2)], wz_r.at[(k % 2 * 2 + m) * 2 + l])
        for way, step in ((0, 1), (1, -1)):
            if k == 1 and which == 0:
                ring_send(wbuf.at[m, l, 0, z], m, l, 1, way)
            elif k == half:
                ring_send(wbuf.at[m, l, way, zat(-step * (k - 1))], m, l, k, way)
            else:
                ring_send(wbuf.at[m, l, :, zat(-step * (k - 1))], m, l, k, way)

    def await_last(m):
        for l in range(2):
            await_bytes(wbuf.at[m, 0, :, 0], wz_r.at[((half - 1) % 2 * 2 + m) * 2 + l])

    def all_met():
        pl.semaphore_wait(flag.at[half - 1], 1)

    def stage_c():
        await_bytes(pc.at[0], st_r.at[1])
        send(pc.at[ylo], pc.at[ylo], out_s.at[0], st_r.at[2], dev(y_=partner))

    def stage_d():
        await_bytes(pc.at[0], st_r.at[2])

        def one(s, carry):
            for l in range(2):
                v = pc[l, s].astype(F32)
                cdf, dens = gelu_parts(v)
                slope[s, l] = (cdf + v * dens).reshape(2 * tiles, 8, LANES)
            return carry

        lax.fori_loop(0, top, one, 0)

    def top_first():
        og_in.wait()
        rows = wbuf[1, :, :, z].reshape(4 * fb, fe)
        a_top[y] = lax.dot_general(
            rows, og[:, :, mine].reshape(tok, fe), (((1,), (1,)), ((), ())), preferred_element_type=F32
        ).astype(BF16)
        for d in y_order:
            send(a_top.at[y], a_top.at[y], out_s.at[0], top_r.at[0], dev(y_=yat(d)))
        spread_pre()

    def top_second():
        await_bytes(pre_t.at[pl.ds(0, 3)], pt_r.at[0])
        v = pre_top[...].astype(F32).reshape(4 * fb, tok)
        cdf, dens = gelu_parts(v)
        await_bytes(a_top.at[pl.ds(0, 3)], top_r.at[0])
        back = a_top[0].astype(F32)
        for k in range(1, 4):
            back = back + a_top[k].astype(F32)
        g = (back * (cdf + v * dens)).astype(BF16)
        g_pass[...] = jnp.where(ylo == 0, g[:fb], g[2 * fb:3 * fb])
        send(g_pass, g_top, out_s.at[0], top_r.at[4], dev(core_=0))
        g_top[...] = jnp.where(ylo == 0, g[fb:2 * fb], g[3 * fb:])
        rows = jnp.swapaxes(g.astype(F32), 0, 1).astype(BF16)
        part = jnp.dot(rows, wbuf[0, :, :, z].reshape(4 * fb, fe), preferred_element_type=F32).astype(BF16)
        for j in range(nsec):
            b_top[j // 2, :, j % 2] = part[:, j * LANES:(j + 1) * LANES].reshape(nz, 8, LANES)
        for d in x_order:
            send(b_top.at[xat(d)], r_top.at[x], out_s.at[0], top_r.at[1], dev(x_=xat(d)))
        r_top[x] = b_top[x]

    def top_third():
        await_bytes(r_top.at[pl.ds(0, nx - 1)], top_r.at[1])
        total = r_top[0].astype(F32)
        for k in range(1, nx):
            total = total + r_top[k].astype(F32)
        q_top[...] = total.astype(BF16)
        for d in z_order:
            send(q_top.at[zat(d)], z_top.at[z], out_s.at[0], top_r.at[2], dev(z_=zat(d)))
        z_top[z] = q_top[z]

    own = pl.ds(2 * x, 2)

    def top_fourth():
        await_bytes(z_top.at[pl.ds(0, nz - 1)], top_r.at[2])
        for c in range(2):
            at = pl.multiple_of(ylo * fe + (2 * x + c) * LANES, LANES)
            total = og[z, :, pl.ds(at, LANES)].astype(F32)
            for k in range(nz):
                total = total + z_top[k, c].astype(F32)
            xs[top - 1, 2 * x + c] = total.astype(BF16)
        src = xs.at[top - 1, own]
        for d in x_order:
            send(src, src, out_s.at[0], top_r.at[3], dev(x_=xat(d)))

    def spread_z(t):
        src = xs.at[t - 1, own]
        dst = up.at[pl.ds(slot(t, x, ylo, z), 2)]

        def both(d):
            for to in (partner, y):
                send(src, dst, out_s.at[0], ph_r.at[t], dev(core_=0, z_=zat(d), y_=to))

        both(half)

        def pair(i, c):
            both(half - i)
            both(half + i)
            return c

        lax.fori_loop(1, half, pair, 0)
        both(0)

    bounds = sorted({half // 2, 3 * half // 4, half})
    groups = [
        [r for r in range(nz) if (bounds[i - 1] if i else -1) < min(r, nz - r) <= b] for i, b in enumerate(bounds)
    ]
    group_of = {r: i for i, g in enumerate(groups) for r in g}

    def runs(g):
        out = []
        for r in g:
            if out and out[-1][1] == r:
                out[-1][1] = r + 1
            else:
                out.append([r, r + 1])
        return out

    owner = [p if min(p, nx - p) <= 1 else 0 for p in range(nx)]
    owned = {o: [p for p in range(nx) if owner[p] == o] for o in sorted(set(owner))}
    d_order = [half] + [d for i in range(1, half) for d in (half - i, half + i)] + [0]

    def last_z():
        for o, pairs in owned.items():
            @pl.when(x == o)
            def _():
                for d in d_order:
                    r = (nz - d) % nz
                    for p in pairs:
                        src = xs.at[nsec, pl.ds(2 * p, 2)]
                        dst = up.at[pl.ds(slot(0, p, ylo, r), 2)]
                        if o:
                            send(src, dst, out_s.at[0], wx_r.at[group_of[r]], dev(core_=1, z_=zat(d), y_=partner))
                        if d:
                            send(src, dst, out_s.at[0], wx_r.at[group_of[r]], dev(core_=1, z_=zat(d)))
                for p in pairs:
                    up[pl.ds(slot(0, p, ylo, 0), 2)] = xs[nsec, 2 * p:2 * p + 2]

    def last_x(i):
        for o, pairs in owned.items():
            @pl.when(x == o)
            def _():
                per_plane = 4 if o else 2 * len(pairs)
                here = (2 if o else 2 * len(pairs)) if i == 0 else 0
                await_bytes(up.at[pl.ds(0, per_plane * len(groups[i]) - here)], wx_r.at[i])
                for a, b in runs(groups[i]):
                    for p in pairs:
                        for l, to in ((0, y), (1, y)) if o else ((ylo, partner), (ylo, y)):
                            src = up.at[pl.ds(slot(0, p, l, a), 2 * (b - a))]
                            send(src, src, out_s.at[0], top_r.at[i], dev(x_=0, core_=0, y_=to))

    def last_out(i):
        await_bytes(up.at[pl.ds(0, nx * 4 * len(groups[i]))], top_r.at[i])
        for r in groups[i]:
            row = zat(r)
            for l in range(2):
                parts = [up[slot(0, k, l, r) + c] for k in range(nx) for c in range(2)]
                ig_out[row, :, l * fe:(l + 1) * fe] = jnp.concatenate(parts, axis=1)

    def spread_g(t):
        def to(d, c):
            tile = zat(d) // per_tile
            for c_ in range(2):
                send(gbuf.at[t, ylo, c_ * tiles + tile], gz.at[t * nz + z], out_s.at[0], g_r.at[t], dev(core_=c_, z_=zat(d)))
            return c

        lax.fori_loop(1, nz, to, 0)
        tile = z // per_tile
        send(gbuf.at[t, ylo, tile], gz.at[t * nz + z], out_s.at[0], g_r.at[t], dev(core_=0))
        gz[t * nz + z] = gbuf[t, ylo, tiles + tile]

    def turn(away):
        t = lax.rem(z // per_tile + away + tiles, tiles)

        def one(i, c):
            l, c_ = i // 2, lax.rem(i, 2)
            v = wbuf[1, l, c_, pl.ds(t * per_tile, per_tile)].reshape(LANES, fe)
            w_t[l, c_ * tiles + t] = jnp.swapaxes(v, 0, 1)
            return c

        lax.fori_loop(0, 4, one, 0)

    def a_half(s, l, part=None):
        if part is not None:
            a_buf[s, l, y] = part.astype(BF16)
        for d in y_order:
            send(a_buf.at[s, l, y], a_buf.at[s, l, y], out_s.at[0], ph_r.at[l * 2 + (s % 2 if isinstance(s, int) else lax.rem(s, 2))], dev(y_=yat(d)))

    def a_part(s, l, n):
        lhs = jnp.concatenate([xs[s, n * hj + j] for j in range(hj)], axis=1)
        w_out = jnp.concatenate([w_t[l, t, n * hn:(n + 1) * hn] for t in range(2 * tiles)], axis=1)
        return jnp.dot(lhs, w_out, preferred_element_type=F32)

    def a_tile(l, away, turned):
        lhs = jnp.concatenate([xs[top - 1, j] for j in range(nsec)], axis=1)
        t = lax.rem(z // per_tile + away + tiles, tiles)
        if turned:
            w_out = jnp.concatenate([w_t[l, c * tiles + t] for c in range(2)], axis=1)
            part = jnp.dot(lhs, w_out, preferred_element_type=F32)
        else:
            w_out = wbuf[1, l, :, pl.ds(t * per_tile, per_tile)].reshape(2 * LANES, fe)
            part = lax.dot_general(lhs, w_out, (((1,), (1,)), ((), ())), preferred_element_type=F32)
        for c in range(2):
            at = pl.multiple_of((c * tiles + t) * LANES, LANES)
            a_buf[top - 1, l, y, :, pl.ds(at, LANES)] = part[:, c * LANES:(c + 1) * LANES].astype(BF16)

    def release(t):
        pl.semaphore_signal(flag.at[t], inc=1, device_id=dev(core_=0), device_id_type=MESH_ID)

    def await_up(t):
        await_bytes(up.at[pl.ds(0, nx * block)], ud_r.at[t])

    def background_a(s):
        with scope("bg_a"):
            @pl.when(s <= top - 3)
            def _():
                release(s + 2)

            @pl.when(s <= top - 2)
            def _():
                spread_z(s + 1)

            @pl.when(s == top - 2)
            def _():
                first_in_term()

            @pl.when(s <= top - 3)
            def _():
                in_term(s + 2)

            @pl.when(s <= top - 4)
            def _():
                await_up(s + 4)
                out_term(s + 4)

    def g_half(s, l, keep=True):
        with scope(f"wait_a{l}"):
            await_bytes(a_buf.at[s, l, pl.ds(0, 3)], ph_r.at[l * 2 + (s % 2 if isinstance(s, int) else lax.rem(s, 2))])
        back = a_buf[s, l, 0].astype(F32)
        for k in range(1, 4):
            back = back + a_buf[s, l, k].astype(F32)
        g = []
        for t in range(2 * tiles):
            g_tile = (back[:, t * LANES:(t + 1) * LANES] * slope[s, l, t]).astype(BF16)
            if keep:
                gbuf[s, l, t] = g_tile
            g.append(g_tile)
        return jnp.concatenate(g, axis=1)

    def b_tile(n, away):
        t = lax.rem(z // per_tile + away + tiles, tiles)
        pairs = [(l, c) for l in range(2) for c in range(2)]
        lhs = jnp.concatenate([gbuf[top - 1, l, c * tiles + t] for l, c in pairs], axis=1)
        rows = pl.ds(t * per_tile, per_tile)
        w_in = jnp.concatenate([wbuf[0, l, c, rows, :, n * hn:(n + 1) * hn].reshape(LANES, hn) for l, c in pairs], axis=0)
        return jnp.dot(lhs, w_in, preferred_element_type=F32)

    def application(s, final=False, begin=False):
        if not begin:
            background_a(s)
            g_first = g_half(s, 0, False)
            for n in range(2):
                w_in = wbuf[0, 0, :, :, :, n * hn:(n + 1) * hn].reshape(hu, hn)
                b_acc[n] = jnp.dot(g_first, w_in, preferred_element_type=F32)
            g = g_half(s, 1, False)
        for n in range(2):
            if begin:
                part = b_tile(n, tiles // 2)
            else:
                w_in = wbuf[0, 1, :, :, :, n * hn:(n + 1) * hn].reshape(hu, hn)
                part = jnp.dot(g, w_in, preferred_element_type=F32)
            part = (b_acc[n] + part).astype(BF16)
            for j in range(hj):
                b_buf[s, n, x, j] = part[:, j * LANES:(j + 1) * LANES]
            if not final:
                src = b_buf.at[s, n, x]
                for d in x_order:
                    send(src, src, out_s.at[0], ph_r.at[4 + n * 2 + (s % 2 if isinstance(s, int) else lax.rem(s, 2))], dev(x_=xat(d)))
        hx = nx // 2
        if final:
            for p in range(nx):
                @pl.when(x != owner[p])
                def _():
                    src = b_buf.at[s, p // hx, x, pl.ds(2 * (p % hx), 2)]
                    send(src, src, out_s.at[0], ph_r.at[4 + s % 2], dev(x_=owner[p]))

        with scope("bg_b"):
            if not begin:
                for l, part in enumerate((g_first, g)):
                    for t in range(2 * tiles):
                        gbuf[s, l, t] = part[:, t * LANES:(t + 1) * LANES]
            spread_g(s)
            if begin:
                spread_z(top)

        if final:
            for o, pairs in owned.items():
                @pl.when(x == o)
                def _():
                    with scope("wait_b"):
                        await_bytes(gz.at[pl.ds(0, 2 * (nx - 1) * len(pairs))], ph_r.at[4 + s % 2])
                    for p in pairs:
                        for c in range(2):
                            total = xs[s, 2 * p + c].astype(F32)
                            for k in range(nx):
                                total = total + b_buf[s, p // hx, k, 2 * (p % hx) + c].astype(F32)
                            xs[nsec, 2 * p + c] = total.astype(BF16)
            return
        for n in range(2):
            with scope(f"wait_b{n}"):
                await_bytes(b_buf.at[s, n, pl.ds(0, nx - 1)], ph_r.at[4 + n * 2 + (s % 2 if isinstance(s, int) else lax.rem(s, 2))])
            with scope(f"a_mm{n}"):
                for j in range(hj):
                    total = xs[s, n * hj + j].astype(F32)
                    for k in range(nx):
                        total = total + b_buf[s, n, k, j].astype(F32)
                    xs[s - 1, n * hj + j] = total.astype(BF16)
                if n == 0:
                    for l in range(2):
                        a_acc[l] = a_part(s - 1, l, 0)
        for l in range(2):
            with scope(f"a_last{l}"):
                a_half(s - 1, l, a_acc[l] + a_part(s - 1, l, 1))

    @pl.when(core == 1)
    def _():
        plan = [
            (1, top_first), (2, top_second), (2, li_first), (4, all_met), (4, top_third), (5, first_out_term), (6, li_second),
            (6, stage_c), (7, stage_d), (7, top_fourth),
        ]
        plan += [(half if d else 5, lambda d=d: turn(d)) for d in (0, -1, 1) if d % tiles != tiles // 2]
        for k in range(1, half + 1):
            with scope(f"hop{k}"):
                if k == 1:
                    blocks = ((1, 1, 0), (0, 1, 0), (1, 1, 1))
                elif k == 2:
                    blocks = ((1, 2, 0), (0, 1, 1), (1, 2, 1))
                else:
                    blocks = ((1, k, 0), (0, k - 1, 0), (1, k, 1), (0, k - 1, 1))
                for b in blocks:
                    hop(*b)
            with scope(f"stage{k}"):
                for at, f in plan:
                    if min(at, half) == k:
                        f()
        early = [d for d in (0, -1, 1) if d % tiles != tiles // 2]
        with scope("top_end"):
            await_bytes(xs.at[0, pl.ds(0, 2 * (nx - 1))], top_r.at[3])
            for l in range(2):
                for d in early:
                    a_tile(l, d, True)
        with scope("gather_out"):
            hop(0, half, 0)
            await_last(1)
        with scope("a_first"):
            for l in range(2):
                a_tile(l, tiles // 2, False)
                a_half(top - 1, l)
        with scope("hop_end"):
            hop(0, half, 1)
            turn(tiles // 2)
        with scope("b_early"):
            for l in range(2):
                g_half(top - 1, l)
            for n in range(2):
                b_acc[n] = sum((b_tile(n, d) for d in early), jnp.zeros((8, hn), F32))
        with scope("gather_in"):
            await_last(0)
        li_third()

        application(top - 1, begin=True)

        def step(i, carry):
            application(top - 2 - i)
            return carry

        lax.fori_loop(0, top - 2, step, 0)
        application(0, final=True)

        with scope("t_z0"):
            last_z()
            release(1)
        with scope("t_terms"):
            in_term(1)
            for t in range(min(top, 3), 2, -1):
                await_up(t)
                out_term(t)
        with scope("t_in0"):
            in_term(0)
        for i in range(len(groups)):
            with scope(f"t_last{i}"):
                last_x(i)
        with scope("t_up2"):
            await_up(2)
            out_term(2)
        with scope("t_up1"):
            await_up(1)
            out_term(1)

    def await_z(t):
        await_bytes(up.at[pl.ds(0, block)], ph_r.at[t])

    def spread_x(t):
        await_z(t)
        if not isinstance(t, int) or t < top:
            pl.semaphore_wait(flag.at[t], 1)
        src = up.at[pl.ds(slot(t, x), block)]
        for d in x_order:
            to_sem = wx_r.at[d] if isinstance(t, int) and t == 1 else ud_r.at[t]
            send(src, src, out_s.at[0], to_sem, dev(x_=xat(d)))

    def to_core(t, x_, blocks):
        src = up.at[pl.ds(slot(t, x_), blocks * block)]
        send(src, src, out_s.at[2], ud_r.at[t], dev(core_=1))

    def spread_core(t):
        await_bytes(up.at[pl.ds(0, (nx - 1) * block)], ud_r.at[t])
        to_core(t, 0, nx)

    def spread_core_last():
        for d in reversed(x_order):
            await_bytes(up.at[pl.ds(0, block)], wx_r.at[d])
            to_core(1, xat(-d), 1)

    @pl.when(core == 0)
    def _():
        spread_pre()
        for r in range(half - 1):
            meet(r)
        pl.semaphore_signal(flag.at[half - 1], inc=1, device_id=dev(core_=1), device_id_type=MESH_ID)
        pa_first()
        li_first()
        pa_second()
        stage_b()
        og_in.wait()
        first_out_term()
        li_second()
        li_third()
        await_bytes(g_top, top_r.at[4])
        first_in_term()

        def finish_one(t):
            with scope("s_core"):
                spread_core(t)
            with scope("s_out"):
                out_term(t)

        def move(i, carry):
            t = top - 1 - i
            with scope("s_x"):
                spread_x(t)
            with scope("s_in"):
                in_term(t)
            finish_one(t + 1)
            return carry

        with scope("s_x7"):
            spread_x(top)
        lax.fori_loop(0, top - 2, move, 0)
        with scope("s_x1"):
            spread_x(1)
            to_core(1, x, 1)
        finish_one(2)
        with scope("s_in"):
            for t in (1, 0):
                in_term(t)
        with scope("s_core1"):
            spread_core_last()
        with scope("s_out1"):
            out_term(1)

        @pl.when(x == 0)
        def _():
            for i in range(len(groups)):
                with scope(f"s_last{i}"):
                    last_out(i)

    def size(*shape):
        return math.prod(shape) // (8 * LANES)

    li_block, row = size(tok, width), size(fb, tok)
    both_cores = size(2, fb, fe) + nsec * row
    by_core = (
        size(2, fb, fe) + row + size(2, half, 8, nsec * fb) + nx * size(2, 2, tiles, 8, LANES) + top * (nx - 1) * block,
        size(nz, 8, nsec * fb)
        + size(nsec, 2, tiles, 8, LANES)
        + 3 * size(4 * fb, tok)
        + (nx - 1) * 2 * nz
        + (nz - 1) * 2
        + (nx - 1) * 2
        + row
        + top * 2 * 3 * size(8, hu)
        + (top - 1) * 2 * (nx - 1) * hj
        + top * (2 * nz - 1)
        + top * block,
    )
    with scope("drain"):
        await_bytes(spare.at[pl.ds(0, (nx + (3 if ring else 1)) * li_block)], out_s.at[1])

        @pl.when(core == 1)
        def _():
            for way in range(2):
                await_bytes(wbuf.at[0, :, :, pl.ds(0, nz - 1)], wz_s.at[way])

        for o in range(nx):
            pairs = owned.get(o, [])
            last_tiles = 2 * sum(owner[p] != o for p in range(nx))
            if pairs:
                last_tiles += (block - 2 if o else 2 * len(pairs) * (nz - 1)) + (block if o else block * len(pairs))

            @pl.when((core == 1) & (x == o))
            def _():
                await_bytes(spare.at[pl.ds(0, both_cores + by_core[1] + last_tiles)], out_s.at[0])

        @pl.when(core == 0)
        def _():
            await_bytes(spare.at[pl.ds(0, top * nx * block)], out_s.at[2])

        for h in range(2):
            @pl.when((core == 0) & (yhi == h))
            def _():
                pa_tiles = 2 * (half - 1 + h) * size(8, nsec * fb)
                await_bytes(spare.at[pl.ds(0, both_cores + by_core[0] + pa_tiles)], out_s.at[0])


def finish(ig, gi, go, ig_out, gi_out, go_out, sems):
    copies = [pltpu.make_async_copy(src, dst, sems.at[k]) for k, (src, dst) in enumerate(((ig, ig_out), (gi, gi_out), (go, go_out)))]
    for cp in copies:
        cp.start()
    for cp in copies:
        cp.wait()


def body(layer_inputs, pre_act, out_grad, w_in, w_out):
    nz, nx = lax.axis_size("z"), lax.axis_size("x")
    nsec = 2 * nx
    tok, width = out_grad.shape
    fb = w_in.shape[2]
    hid = pre_act.shape[2]
    fe = width // 2
    tiles = nz * fb // LANES
    half = nz // 2
    dma = pltpu.SemaphoreType.DMA
    vmem = pltpu.VMEM
    spare = 2048
    scratch = [
        vmem((2, fb, width), BF16),
        vmem((2, 2, 2, nz, fb, fe), BF16),
        vmem((2, nz, 8, hid), BF16),
        vmem((2, 2, half, 8, hid), BF16),
        vmem((nx, 2, 2, tiles, 8, LANES), BF16),
        vmem((2, nsec, 2, tiles, 8, LANES), BF16),
        vmem((nsec, 2, 2 * tiles, 8, LANES), F32),
        vmem((nsec, fb, tok), BF16),
        vmem((nsec, fb, tok), BF16),
        vmem((2, 2, fb, tok), BF16),
        vmem((nsec, fb, tok), BF16),
        vmem((2, nx, tok, width), BF16),
        vmem((nz, 8, width), BF16),
        vmem((4, 4 * fb, tok), BF16),
        vmem((nx, nz, 2, 8, LANES), BF16),
        vmem((nx, nz, 2, 8, LANES), BF16),
        vmem((nz, 2, 8, LANES), BF16),
        vmem((nz, 2, 8, LANES), BF16),
        vmem((fb, tok), BF16),
        vmem((fb, tok), BF16),
        vmem((2, 2 * tiles, fe, LANES), BF16),
        vmem((nsec + 1, nsec, 8, LANES), BF16),
        vmem((nsec, 2, 4, 8, 2 * nz * fb), BF16),
        vmem((nsec, 2, nx, nx, 8, LANES), BF16),
        vmem((2, 8, 2 * nz * fb), F32),
        vmem((2, 8, fe // 2), F32),
        vmem((nsec, 2, 2 * tiles, 8, LANES), BF16),
        vmem((nsec * nz, 8, LANES), BF16),
        vmem((LANES, tok), F32),
        vmem((nsec * nx * 4 * nz, 8, LANES), BF16),
        vmem((spare, 8, LANES), BF16),
        dma((7,)),
        dma((3,)), dma((2,)),
        dma((4,)),
        dma((2,)),
        dma((8,)),
        dma((6,)),
        dma((1,)),
        dma((5,)),
        dma((max(8, nsec),)),
        dma((5,)),
        dma((nsec,)),
        dma((nsec,)),
        pltpu.SemaphoreType.REGULAR((max(nsec, half),)),
    ]
    hbm, on_chip = pl.BlockSpec(memory_space=pltpu.HBM), pl.BlockSpec(memory_space=pltpu.VMEM)
    shapes = (
        jax.ShapeDtypeStruct((nz, 8, width), BF16),
        jax.ShapeDtypeStruct((fb, width), F32),
        jax.ShapeDtypeStruct((fb, width), F32),
    )
    operands = (
        layer_inputs.reshape(tok, width),
        pre_act.reshape(nz, 8, hid),
        out_grad.reshape(nz, 8, width),
        w_in.reshape(fb, width),
        w_out.reshape(fb, width),
    )
    results = pl.pallas_call(
        kernel,
        out_shape=shapes,
        in_specs=[hbm] * 5,
        out_specs=(on_chip,) * 3,
        scratch_shapes=scratch,
        name="chain",
        compiler_params=pltpu.CompilerParams(
            collective_id=0, has_side_effects=True, vmem_limit_bytes=40 * 1024 * 1024
        ),
    )(*(pltpu.with_memory_space_constraint(v, pltpu.HBM) for v in operands))
    ig, gi, go = pl.pallas_call(
        finish,
        out_shape=shapes,
        in_specs=[on_chip] * 3,
        out_specs=(hbm,) * 3,
        scratch_shapes=[dma((3,))],
        name="finish",
    )(*(pltpu.with_memory_space_constraint(v, pltpu.VMEM) for v in results))
    return (
        ig.reshape(1, tok, width),
        gi.reshape(1, 1, fb, width),
        go.reshape(1, 1, fb, width),
    )


def solution(mesh):
    shape = mesh.shape
    split = Mesh(
        mesh.devices.reshape(shape["section"] // 2, 2, shape["dp"] // 2, 2, shape["mp"]), AXES
    )
    sec, dp = ("x", "core"), ("z", "ylo")
    placed = (
        P(sec, None, "yhi"),
        P(sec, None, dp),
        P(None, "yhi"),
        P(dp, sec, None, "yhi"),
        P(dp, sec, None, "yhi"),
    )
    return jax.shard_map(
        body,
        mesh=split,
        in_specs=placed,
        out_specs=(P(sec, None, "yhi"), P(dp, sec, None, "yhi"), P(dp, sec, None, "yhi")),
        check_vma=False,
    )
```

```python
import contextlib
import math

import jax
import jax.numpy as jnp
from jax import lax
from jax.experimental import pallas as pl
from jax.experimental.pallas import tpu as pltpu
from jax.sharding import Mesh
from jax.sharding import PartitionSpec as P

AXES = ("x", "core", "z", "ylo", "yhi")
MESH_ID = pl.DeviceIdType.MESH
BF16, F32 = jnp.bfloat16, jnp.float32
LANES = 128
PROFILE = False


def scope(name):
    return jax.named_scope(name) if PROFILE else contextlib.nullcontext()


def gelu_parts(v):
    cdf = 0.5 * (1.0 + lax.erf(v * 0.7071067811865476))
    dens = jnp.exp(-0.5 * v * v) * 0.3989422804014327
    return cdf, dens


def kernel(
    li_hbm, pa_hbm, og_hbm, wi_hbm, wo_hbm,
    ig_out, gi_out, go_out,
    w_own, wbuf, pa, pa_all, pb, pc, slope, pa_t, pre_t, pre_top, hall, li, og,
    a_top, b_top, r_top, q_top, z_top, g_top, g_pass,
    w_t, xs, a_buf, b_buf, a_acc, b_acc, gbuf, gz, gt, up,
    spare, lsem, out_s, wz_s, wx_r, wd_r, wz_r, st_r, pt_r, top_r, ph_r, li_r, g_r, ud_r, flag,
):
    nx, nz = lax.axis_size("x"), lax.axis_size("z")
    nsec = 2 * nx
    top = nsec - 1
    fb, width = wi_hbm.shape
    fe = width // 2
    tok = nz * 8
    tiles = nz * fb // LANES
    per_tile = LANES // fb
    x, core, z = lax.axis_index("x"), lax.axis_index("core"), lax.axis_index("z")
    ylo, yhi = lax.axis_index("ylo"), lax.axis_index("yhi")
    sec = x * 2 + core
    y = yhi * 2 + ylo
    other = 1 - ylo
    partner = yhi * 2 + other

    def dev(x_=None, core_=None, z_=None, y_=None):
        y_ = y if y_ is None else y_
        return (
            x if x_ is None else x_,
            core if core_ is None else core_,
            z if z_ is None else z_,
            lax.rem(y_, 2),
            y_ // 2,
        )

    def send(src, dst, ssem, rsem, to):
        cp = pltpu.make_async_remote_copy(
            src_ref=src, dst_ref=dst, send_sem=ssem, recv_sem=rsem, device_id=to, device_id_type=MESH_ID
        )
        cp.start()
        return cp

    def await_bytes(ref, sem):
        pltpu.make_async_copy(ref, ref, sem).wait()

    def zat(d):
        return lax.rem(z + d + nz, nz)

    def xat(d):
        return lax.rem(x + d + nx, nx)

    def yat(d):
        return lax.rem(y + d, 4)

    y_order = (2, 1, 3)
    x_order = sorted(range(1, nx), key=lambda d: -min(d, nx - d))
    z_order = sorted(range(1, nz), key=lambda d: -min(d, nz - d))
    sections = [(d, False) for d in x_order] + [(d, True) for d in x_order] + [(0, True)]

    def peer(d, cross):
        return xat(d), (1 - core if cross else core)

    mine = pl.ds(pl.multiple_of(ylo * fe, LANES), fe)
    theirs = pl.ds(pl.multiple_of(other * fe, LANES), fe)

    w_hbm = (wi_hbm, wo_hbm)
    pa_in = pltpu.make_async_copy(pa_hbm, pa.at[core], lsem.at[0])
    w_in_ = [pltpu.make_async_copy(w_hbm[m].at[:, mine], wbuf.at[m, ylo, 1, z], lsem.at[1 + m]) for m in range(2)]
    og_in = pltpu.make_async_copy(og_hbm, og, lsem.at[3])
    li_in = pltpu.make_async_copy(li_hbm, li.at[core, x], lsem.at[4])
    barrier = pltpu.get_barrier_semaphore()
    greeted = [dev(z_=zat(d)) for d in (1, -1)] + [dev(*peer(*p)) for p in sections]
    greeted += [dev(y_=yat(d)) for d in range(1, 4)] + [dev(core_=1 - core, y_=partner)]
    for to in greeted:
        pl.semaphore_signal(barrier, inc=1, device_id=to, device_id_type=MESH_ID)

    first = (1, 0)
    own_in = [pltpu.make_async_copy(w_hbm[m], w_own.at[m], lsem.at[5 + m]) for m in range(2)]
    for m in first:
        own_in[m].start()

        @pl.when(core == 1)
        def _():
            w_in_[m].start()

    pa_in.start()

    og_in.start()
    li_in.start()

    with scope("barrier"):
        pl.semaphore_wait(barrier, len(greeted))

    half = nz // 2

    def meet(r):
        for d in (1, -1):
            pl.semaphore_signal(flag.at[r], inc=1, device_id=dev(z_=zat(d)), device_id_type=MESH_ID)
        pl.semaphore_wait(flag.at[r], 2)

    def pa_first():
        await_bytes(pa.at[1], st_r.at[5])
        for h in range(2):
            @pl.when(yhi == h)
            def _():
                for d in z_order:
                    if d % 2 == h:
                        for c in range(2):
                            dst = pa_all.at[c, lax.rem(z, 2), z // 2]
                            send(pa.at[c, zat(d)], dst, out_s.at[0], st_r.at[0], dev(z_=zat(d)))
                if h == 0:
                    for c in range(2):
                        pa_all[c, lax.rem(z, 2), z // 2] = pa[c, z]

    def await_pa(sem):
        for h in range(2):
            @pl.when(yhi == h)
            def _():
                await_bytes(pa.at[0, pl.ds(0, 2 * (half - 1 + h))], sem)

    def pa_second():
        await_pa(st_r.at[0])
        mine_ = pa_all.at[:, lax.rem(z + yhi, 2)]
        send(mine_, mine_, out_s.at[0], st_r.at[4], dev(y_=yat(2)))

    def ring_send(src, m, l, k, way):
        send(src, src, wz_s.at[way], wz_r.at[((k - 1) * 2 + m) * 2 + l], dev(z_=zat(1 if way == 0 else -1)))

    swaps = []
    for m in first:
        own_in[m].wait()

        @pl.when(core == 0)
        def _():
            send(w_own.at[m, :, mine], wbuf.at[m, ylo, 0, z], out_s.at[0], wd_r.at[m], dev(core_=1))

        @pl.when(core == 1)
        def _():
            w_in_[m].wait()
            for way in range(2):
                ring_send(wbuf.at[m, ylo, 1, z], m, ylo, 1, way)

        dst = wbuf.at[m, ylo, core, z]
        swaps.append(send(w_own.at[m, :, theirs], dst, out_s.at[0], wx_r.at[core * 2 + m], dev(core_=1, y_=partner)))

    pa_in.wait()

    @pl.when(core == 1)
    def _():
        send(pa.at[1], pa.at[1], out_s.at[0], st_r.at[5], dev(core_=0))

    v = pa[core].astype(F32).reshape(tok, nsec * fb)
    pa_t[...] = jnp.swapaxes(v, 0, 1).astype(BF16).reshape(nsec, fb, tok)
    for p in sections:
        to = peer(*p)
        send(pa_t.at[to[0] * 2 + to[1]], pre_t.at[sec], out_s.at[0], st_r.at[3], dev(*to))
    pre_t[sec] = pa_t[sec]

    def spread_pre():
        await_bytes(pre_t.at[pl.ds(0, nsec - 1)], st_r.at[3])
        dst = pre_top.at[ylo, core]
        send(pre_t.at[top], dst, out_s.at[0], pt_r.at[0], dev(core_=1, y_=partner))

        @pl.when(core == 0)
        def _():
            send(pre_t.at[top], dst, out_s.at[0], pt_r.at[0], dev(core_=1))

        @pl.when(core == 1)
        def _():
            dst[...] = pre_t[top]

    def stage_b():
        await_bytes(pa_all.at[:, 0], st_r.at[4])
        group = lax.broadcasted_iota(jnp.int32, (8, LANES), 1) // fb
        for c in range(2):
            for ct in range(nsec // per_tile):
                for t in range(tiles):
                    out = [jnp.zeros((8, LANES), F32)] * per_tile
                    for j in range(per_tile):
                        at = t * per_tile + j
                        v = pa_all[c, at % 2, at // 2, :, ct * LANES:(ct + 1) * LANES].astype(F32)
                        for k in range(per_tile):
                            shift = (j - k) * fb % LANES
                            r = pltpu.roll(v, shift, 1) if shift else v
                            out[k] = jnp.where(group == j, r, out[k])
                    for k in range(per_tile):
                        to = ct * per_tile + k
                        pb[to // 2, c, to % 2, t] = out[k].astype(BF16)
        for d in x_order + [0]:
            send(pb.at[xat(d)], pc.at[ylo, pl.ds(2 * x, 2)], out_s.at[0], st_r.at[1], dev(x_=xat(d), core_=1))

    cut = tok // 2
    lo, hi = pl.ds(0, cut), pl.ds(cut, cut)
    ring = nx > 2

    def li_first():
        li_in.wait()
        src = li.at[core, x]
        send(src, src, out_s.at[1], li_r.at[0], dev(x_=xat(1)))
        if ring:
            send(src, src, out_s.at[1], li_r.at[1], dev(x_=xat(-1)))

    def li_second():
        await_bytes(li.at[0, 0], li_r.at[0])
        if ring:
            src = li.at[core, xat(-1), lo]
            send(src, src, out_s.at[1], li_r.at[2], dev(x_=xat(1)))
            await_bytes(li.at[0, 0], li_r.at[1])
            src = li.at[core, xat(1), hi]
            send(src, src, out_s.at[1], li_r.at[3], dev(x_=xat(-1)))

    def li_third():
        if ring:
            await_bytes(li.at[0, 0, lo], li_r.at[2])
            await_bytes(li.at[0, 0, hi], li_r.at[3])
        send(li.at[core], li.at[core], out_s.at[1], li_r.at[4], dev(core_=1 - core))

    def first_out_term():
        for s in range(nsec):
            v = pre_t[s].astype(F32)
            hall[s] = (v * gelu_parts(v)[0]).astype(BF16)
        go_out[...] = jnp.dot(hall[top], og[...].reshape(tok, width), preferred_element_type=F32)

    def first_in_term():
        await_bytes(li.at[0], li_r.at[4])
        gi_out[...] = jnp.dot(g_top[...], li[top % 2, top // 2], preferred_element_type=F32)

    block = 4 * nz

    def slot(t, x_, ylo_=0, z_=0):
        return ((((t * nx + x_) * 2 + ylo_) * nz) + z_) * 2

    def columns(t, x_, l):
        return up[pl.ds(slot(t, x_, l), 2 * nz)].reshape(nz, 2, 8, LANES)

    def out_term(t):
        rows = hall[t - 1]
        for l in range(2):
            parts = []
            for k in range(nx):
                v = columns(t, k, l)
                parts += [v[:, c].reshape(tok, LANES) for c in range(2)]
            go_out[:, l * fe:(l + 1) * fe] += jnp.dot(rows, jnp.concatenate(parts, axis=1), preferred_element_type=F32)

        @pl.when(sec == t)
        def _():
            for l in range(2):
                for k in range(nx):
                    v = columns(t, k, l)
                    for c in range(2):
                        at = l * fe + (2 * k + c) * LANES
                        ig_out[:, :, at:at + LANES] = v[:, c]

    def in_term(t):
        @pl.when(core == 1)
        def _():
            await_bytes(gz.at[pl.ds(0, nz - 1)], g_r.at[t])

        @pl.when(core == 0)
        def _():
            await_bytes(gz.at[pl.ds(0, nz)], g_r.at[t])

        gt[...] = jnp.swapaxes(gz[pl.ds(t * nz, nz)].astype(F32).reshape(tok, LANES), 0, 1)
        rows = gt[pl.ds(pl.multiple_of(lax.rem(z, per_tile) * fb, fb), fb), :].astype(BF16)
        gi_out[...] += jnp.dot(rows, li[lax.rem(t, 2), t // 2], preferred_element_type=F32)

    nb = 4 if nx % 4 == 0 else 2
    hu, hn, hj = 2 * nz * fb, fe // nb, nsec // nb
    def hop(m, k, which):
        l = ylo if which == 0 else other
        if k == 1:
            if which == 0:
                await_bytes(wbuf.at[m, 0, 0, 0], wd_r.at[m])
            else:
                for c in range(2):
                    await_bytes(wbuf.at[m, 0, 0, 0], wx_r.at[c * 2 + m])
        if k > 1:
            await_bytes(wbuf.at[m, 0, :, pl.ds(0, 2)], wz_r.at[((k - 2) * 2 + m) * 2 + l])
        for way, step in ((0, 1), (1, -1)):
            if k == 1 and which == 0:
                ring_send(wbuf.at[m, l, 0, z], m, l, 1, way)
            elif k == half:
                ring_send(wbuf.at[m, l, way, zat(-step * (k - 1))], m, l, k, way)
            else:
                ring_send(wbuf.at[m, l, :, zat(-step * (k - 1))], m, l, k, way)

    def await_last(m):
        for l in range(2):
            await_bytes(wbuf.at[m, 0, :, 0], wz_r.at[((half - 1) * 2 + m) * 2 + l])

    def all_met():
        pl.semaphore_wait(flag.at[half - 1], 1)

    def stage_c():
        await_bytes(pc.at[0], st_r.at[1])
        send(pc.at[ylo], pc.at[ylo], out_s.at[0], st_r.at[2], dev(y_=partner))

    def stage_d():
        await_bytes(pc.at[0], st_r.at[2])

        def one(s, carry):
            for l in range(2):
                v = pc[l, s].astype(F32)
                cdf, dens = gelu_parts(v)
                slope[s, l] = (cdf + v * dens).reshape(2 * tiles, 8, LANES)
            return carry

        lax.fori_loop(0, top, one, 0)

    def top_first():
        og_in.wait()
        rows = wbuf[1, :, :, z].reshape(4 * fb, fe)
        a_top[y] = lax.dot_general(
            rows, og[:, :, mine].reshape(tok, fe), (((1,), (1,)), ((), ())), preferred_element_type=F32
        ).astype(BF16)
        for d in y_order:
            send(a_top.at[y], a_top.at[y], out_s.at[0], top_r.at[0], dev(y_=yat(d)))
        spread_pre()

    def top_second():
        await_bytes(pre_t.at[pl.ds(0, 3)], pt_r.at[0])
        v = pre_top[...].astype(F32).reshape(4 * fb, tok)
        cdf, dens = gelu_parts(v)
        await_bytes(a_top.at[pl.ds(0, 3)], top_r.at[0])
        back = a_top[0].astype(F32)
        for k in range(1, 4):
            back = back + a_top[k].astype(F32)
        g = (back * (cdf + v * dens)).astype(BF16)
        g_pass[...] = jnp.where(ylo == 0, g[:fb], g[2 * fb:3 * fb])
        send(g_pass, g_top, out_s.at[0], top_r.at[4], dev(core_=0))
        g_top[...] = jnp.where(ylo == 0, g[fb:2 * fb], g[3 * fb:])
        rows = jnp.swapaxes(g.astype(F32), 0, 1).astype(BF16)
        part = jnp.dot(rows, wbuf[0, :, :, z].reshape(4 * fb, fe), preferred_element_type=F32).astype(BF16)
        for j in range(nsec):
            b_top[j // 2, :, j % 2] = part[:, j * LANES:(j + 1) * LANES].reshape(nz, 8, LANES)
        for d in x_order:
            send(b_top.at[xat(d)], r_top.at[x], out_s.at[0], top_r.at[1], dev(x_=xat(d)))
        r_top[x] = b_top[x]

    def top_third():
        await_bytes(r_top.at[pl.ds(0, nx - 1)], top_r.at[1])
        total = r_top[0].astype(F32)
        for k in range(1, nx):
            total = total + r_top[k].astype(F32)
        q_top[...] = total.astype(BF16)
        for d in z_order:
            send(q_top.at[zat(d)], z_top.at[z], out_s.at[0], top_r.at[2], dev(z_=zat(d)))
        z_top[z] = q_top[z]

    own = pl.ds(2 * x, 2)

    def top_fourth():
        await_bytes(z_top.at[pl.ds(0, nz - 1)], top_r.at[2])
        for c in range(2):
            at = pl.multiple_of(ylo * fe + (2 * x + c) * LANES, LANES)
            total = og[z, :, pl.ds(at, LANES)].astype(F32)
            for k in range(nz):
                total = total + z_top[k, c].astype(F32)
            xs[top - 1, 2 * x + c] = total.astype(BF16)
        src = xs.at[top - 1, own]
        for d in x_order:
            send(src, src, out_s.at[0], top_r.at[3], dev(x_=xat(d)))

    def spread_z(t):
        src = xs.at[t - 1, own]
        dst = up.at[pl.ds(slot(t, x, ylo, z), 2)]

        def both(d):
            for to in (partner, y):
                send(src, dst, out_s.at[0], wz_r.at[t], dev(core_=0, z_=zat(d), y_=to))

        both(half)

        def pair(i, c):
            both(half - i)
            both(half + i)
            return c

        lax.fori_loop(1, half, pair, 0)
        both(0)

    bounds = sorted({half // 2, 3 * half // 4, half})
    groups = [
        [r for r in range(nz) if (bounds[i - 1] if i else -1) < min(r, nz - r) <= b] for i, b in enumerate(bounds)
    ]
    group_of = {r: i for i, g in enumerate(groups) for r in g}

    def runs(g):
        out = []
        for r in g:
            if out and out[-1][1] == r:
                out[-1][1] = r + 1
            else:
                out.append([r, r + 1])
        return out

    owner = [p if min(p, nx - p) <= 1 else 0 for p in range(nx)]
    owned = {o: [p for p in range(nx) if owner[p] == o] for o in sorted(set(owner))}
    d_order = [half] + [d for i in range(1, half) for d in (half - i, half + i)] + [0]

    def last_z():
        for o, pairs in owned.items():
            @pl.when(x == o)
            def _():
                for d in d_order:
                    r = (nz - d) % nz
                    for p in pairs:
                        src = xs.at[nsec, pl.ds(2 * p, 2)]
                        dst = up.at[pl.ds(slot(0, p, ylo, r), 2)]
                        if o:
                            send(src, dst, out_s.at[0], wx_r.at[group_of[r]], dev(core_=1, z_=zat(d), y_=partner))
                        if d:
                            send(src, dst, out_s.at[0], wx_r.at[group_of[r]], dev(core_=1, z_=zat(d)))
                for p in pairs:
                    up[pl.ds(slot(0, p, ylo, 0), 2)] = xs[nsec, 2 * p:2 * p + 2]

    def last_x(i):
        for o, pairs in owned.items():
            @pl.when(x == o)
            def _():
                per_plane = 4 if o else 2 * len(pairs)
                here = (2 if o else 2 * len(pairs)) if i == 0 else 0
                await_bytes(up.at[pl.ds(0, per_plane * len(groups[i]) - here)], wx_r.at[i])
                for a, b in runs(groups[i]):
                    for p in pairs:
                        for l, to in ((0, y), (1, y)) if o else ((ylo, partner), (ylo, y)):
                            src = up.at[pl.ds(slot(0, p, l, a), 2 * (b - a))]
                            send(src, src, out_s.at[0], wz_r.at[2 * nsec + i], dev(x_=0, core_=0, y_=to))

    def last_out(i):
        await_bytes(up.at[pl.ds(0, nx * 4 * len(groups[i]))], wz_r.at[2 * nsec + i])
        for r in groups[i]:
            row = zat(r)
            for l in range(2):
                for k in range(nx):
                    for c in range(2):
                        at = l * fe + (2 * k + c) * LANES
                        ig_out[row, :, at:at + LANES] = up[slot(0, k, l, r) + c]

    def spread_g(t):
        def to(d, c):
            tile = zat(d) // per_tile
            for c_ in range(2):
                send(gbuf.at[t, ylo, c_ * tiles + tile], gz.at[t * nz + z], out_s.at[0], g_r.at[t], dev(core_=c_, z_=zat(d)))
            return c

        lax.fori_loop(1, nz, to, 0)
        tile = z // per_tile
        send(gbuf.at[t, ylo, tile], gz.at[t * nz + z], out_s.at[0], g_r.at[t], dev(core_=0))
        gz[t * nz + z] = gbuf[t, ylo, tiles + tile]

    def turn(away):
        t = lax.rem(z // per_tile + away + tiles, tiles)

        def one(i, c):
            l, c_ = i // 2, lax.rem(i, 2)
            v = wbuf[1, l, c_, pl.ds(t * per_tile, per_tile)].reshape(LANES, fe)
            w_t[l, c_ * tiles + t] = jnp.swapaxes(v, 0, 1)
            return c

        lax.fori_loop(0, 4, one, 0)

    def a_half(s, l, part=None):
        if part is not None:
            a_buf[s, l, y] = part.astype(BF16)
        for d in y_order:
            send(a_buf.at[s, l, y], a_buf.at[s, l, y], out_s.at[0], ph_r.at[0, l, s % 2 if isinstance(s, int) else lax.rem(s, 2)], dev(y_=yat(d)))

    def a_part(s, l, n):
        lhs = jnp.concatenate([xs[s, n * hj + j] for j in range(hj)], axis=1)
        w_out = jnp.concatenate([w_t[l, t, n * hn:(n + 1) * hn] for t in range(2 * tiles)], axis=1)
        return jnp.dot(lhs, w_out, preferred_element_type=F32)

    def a_tile(l, away, turned):
        lhs = jnp.concatenate([xs[top - 1, j] for j in range(nsec)], axis=1)
        t = lax.rem(z // per_tile + away + tiles, tiles)
        if turned:
            w_out = jnp.concatenate([w_t[l, c * tiles + t] for c in range(2)], axis=1)
            part = jnp.dot(lhs, w_out, preferred_element_type=F32)
        else:
            w_out = wbuf[1, l, :, pl.ds(t * per_tile, per_tile)].reshape(2 * LANES, fe)
            part = lax.dot_general(lhs, w_out, (((1,), (1,)), ((), ())), preferred_element_type=F32)
        for c in range(2):
            at = pl.multiple_of((c * tiles + t) * LANES, LANES)
            a_buf[top - 1, l, y, :, pl.ds(at, LANES)] = part[:, c * LANES:(c + 1) * LANES].astype(BF16)

    def release(t):
        pl.semaphore_signal(flag.at[t], inc=1, device_id=dev(core_=0), device_id_type=MESH_ID)

    def await_up(t):
        await_bytes(up.at[pl.ds(0, nx * block)], ud_r.at[t])

    def background_a(s):
        with scope("bg_a"):
            @pl.when(s <= top - 3)
            def _():
                release(s + 2)

            @pl.when(s <= top - 2)
            def _():
                spread_z(s + 1)

            @pl.when(s == top - 2)
            def _():
                first_in_term()

            @pl.when(s <= top - 3)
            def _():
                in_term(s + 2)

            @pl.when(s <= top - 4)
            def _():
                await_up(s + 4)
                out_term(s + 4)

    def g_half(s, l):
        with scope(f"wait_a{l}"):
            await_bytes(a_buf.at[s, l, pl.ds(0, 3)], ph_r.at[0, l, s % 2 if isinstance(s, int) else lax.rem(s, 2)])
        back = a_buf[s, l, 0].astype(F32)
        for k in range(1, 4):
            back = back + a_buf[s, l, k].astype(F32)
        g = []
        for t in range(2 * tiles):
            g_tile = (back[:, t * LANES:(t + 1) * LANES] * slope[s, l, t]).astype(BF16)
            gbuf[s, l, t] = g_tile
            g.append(g_tile)
        return jnp.concatenate(g, axis=1)

    def b_tile(n, away):
        t = lax.rem(z // per_tile + away + tiles, tiles)
        pairs = [(l, c) for l in range(2) for c in range(2)]
        lhs = jnp.concatenate([gbuf[top - 1, l, c * tiles + t] for l, c in pairs], axis=1)
        rows = pl.ds(t * per_tile, per_tile)
        w_in = jnp.concatenate([wbuf[0, l, c, rows, :, n * hn:(n + 1) * hn].reshape(LANES, hn) for l, c in pairs], axis=0)
        return jnp.dot(lhs, w_in, preferred_element_type=F32)

    def application(s, final=False, begin=False):
        if not begin:
            background_a(s)
            g_first = g_half(s, 0)
            for n in range(nb):
                w_in = wbuf[0, 0, :, :, :, n * hn:(n + 1) * hn].reshape(hu, hn)
                b_acc[n] = jnp.dot(g_first, w_in, preferred_element_type=F32)
            g = g_half(s, 1)
        for n in range(nb):
            if begin:
                part = b_tile(n, tiles // 2)
            else:
                w_in = wbuf[0, 1, :, :, :, n * hn:(n + 1) * hn].reshape(hu, hn)
                part = jnp.dot(g, w_in, preferred_element_type=F32)
            part = (b_acc[n] + part).astype(BF16)
            for j in range(hj):
                b_buf[s, n, x, j] = part[:, j * LANES:(j + 1) * LANES]
            if not final:
                src = b_buf.at[s, n, x]
                for d in x_order:
                    send(src, src, out_s.at[0], ph_r.at[1, n, s % 2 if isinstance(s, int) else lax.rem(s, 2)], dev(x_=xat(d)))
        hx = nx // nb
        if final:
            for p in range(nx):
                @pl.when(x != owner[p])
                def _():
                    src = b_buf.at[s, p // hx, x, pl.ds(2 * (p % hx), 2)]
                    send(src, src, out_s.at[0], ph_r.at[1, 0, s % 2], dev(x_=owner[p]))

        with scope("bg_b"):
            spread_g(s)
            if begin:
                spread_z(top)

        if final:
            for o, pairs in owned.items():
                @pl.when(x == o)
                def _():
                    with scope("wait_b"):
                        await_bytes(gz.at[pl.ds(0, 2 * (nx - 1) * len(pairs))], ph_r.at[1, 0, s % 2])
                    for p in pairs:
                        for c in range(2):
                            total = xs[s, 2 * p + c].astype(F32)
                            for k in range(nx):
                                total = total + b_buf[s, p // hx, k, 2 * (p % hx) + c].astype(F32)
                            xs[nsec, 2 * p + c] = total.astype(BF16)
            return
        for n in range(nb):
            with scope(f"wait_b{n}"):
                await_bytes(b_buf.at[s, n, pl.ds(0, nx - 1)], ph_r.at[1, n, s % 2 if isinstance(s, int) else lax.rem(s, 2)])
            with scope(f"a_mm{n}"):
                for j in range(hj):
                    total = xs[s, n * hj + j].astype(F32)
                    for k in range(nx):
                        total = total + b_buf[s, n, k, j].astype(F32)
                    xs[s - 1, n * hj + j] = total.astype(BF16)
                if n < nb - 1:
                    for l in range(2):
                        part = a_part(s - 1, l, n)
                        a_acc[l] = a_acc[l] + part if n else part
        for l in range(2):
            with scope(f"a_last{l}"):
                a_half(s - 1, l, a_acc[l] + a_part(s - 1, l, nb - 1))

    @pl.when(core == 1)
    def _():
        plan = [
            (1, top_first), (2, top_second), (2, li_first), (4, all_met), (4, top_third), (5, first_out_term), (6, li_second),
            (6, stage_c), (7, stage_d), (7, top_fourth),
        ]
        plan += [(half if d else 5, lambda d=d: turn(d)) for d in (0, -1, 1) if d % tiles != tiles // 2]
        for k in range(1, half + 1):
            with scope(f"hop{k}"):
                if k == 1:
                    blocks = ((1, 1, 0), (0, 1, 0), (1, 1, 1))
                elif k == 2:
                    blocks = ((1, 2, 0), (0, 1, 1), (1, 2, 1))
                else:
                    blocks = ((1, k, 0), (0, k - 1, 0), (1, k, 1), (0, k - 1, 1))
                for b in blocks:
                    hop(*b)
            with scope(f"stage{k}"):
                for at, f in plan:
                    if min(at, half) == k:
                        f()
        early = [d for d in (0, -1, 1) if d % tiles != tiles // 2]
        with scope("top_end"):
            await_bytes(xs.at[0, pl.ds(0, 2 * (nx - 1))], top_r.at[3])
            for l in range(2):
                for d in early:
                    a_tile(l, d, True)
        with scope("gather_out"):
            hop(0, half, 0)
            await_last(1)
        with scope("a_first"):
            for l in range(2):
                a_tile(l, tiles // 2, False)
                a_half(top - 1, l)
        with scope("hop_end"):
            hop(0, half, 1)
            turn(tiles // 2)
        with scope("b_early"):
            for l in range(2):
                g_half(top - 1, l)
            for n in range(nb):
                b_acc[n] = sum((b_tile(n, d) for d in early), jnp.zeros((8, hn), F32))
        with scope("gather_in"):
            await_last(0)
        li_third()

        application(top - 1, begin=True)

        def step(i, carry):
            application(top - 2 - i)
            return carry

        lax.fori_loop(0, top - 2, step, 0)
        application(0, final=True)

        with scope("t_z0"):
            last_z()
            release(1)
        with scope("t_terms"):
            in_term(1)
            for t in range(min(top, 3), 2, -1):
                await_up(t)
                out_term(t)
        with scope("t_in0"):
            in_term(0)
        for i in range(len(groups)):
            with scope(f"t_last{i}"):
                last_x(i)
        with scope("t_up2"):
            await_up(2)
            out_term(2)
        with scope("t_up1"):
            await_up(1)
            out_term(1)

    def await_z(t):
        await_bytes(up.at[pl.ds(0, block)], wz_r.at[t])

    def spread_x(t):
        await_z(t)
        if not isinstance(t, int) or t < top:
            pl.semaphore_wait(flag.at[t], 1)
        src = up.at[pl.ds(slot(t, x), block)]
        for d in x_order:
            to_sem = wz_r.at[2 * nsec + 3 + d] if isinstance(t, int) and t == 1 else wz_r.at[nsec + t]
            send(src, src, out_s.at[0], to_sem, dev(x_=xat(d)))

    def to_core(t, x_, blocks):
        src = up.at[pl.ds(slot(t, x_), blocks * block)]
        send(src, src, out_s.at[2], ud_r.at[t], dev(core_=1))

    def spread_core(t):
        await_bytes(up.at[pl.ds(0, (nx - 1) * block)], wz_r.at[nsec + t])
        to_core(t, 0, nx)

    def spread_core_last():
        for d in reversed(x_order):
            await_bytes(up.at[pl.ds(0, block)], wz_r.at[2 * nsec + 3 + d])
            to_core(1, xat(-d), 1)

    @pl.when(core == 0)
    def _():
        spread_pre()
        for r in range(half - 1):
            meet(r)
        pl.semaphore_signal(flag.at[half - 1], inc=1, device_id=dev(core_=1), device_id_type=MESH_ID)
        pa_first()
        li_first()
        pa_second()
        stage_b()
        og_in.wait()
        first_out_term()
        li_second()
        li_third()
        await_bytes(g_top, top_r.at[4])
        first_in_term()

        def finish_one(t):
            with scope("s_core"):
                spread_core(t)
            with scope("s_out"):
                out_term(t)

        def move(i, carry):
            t = top - 1 - i
            with scope("s_x"):
                spread_x(t)
            with scope("s_in"):
                in_term(t)
            finish_one(t + 1)
            return carry

        with scope("s_x7"):
            spread_x(top)
        lax.fori_loop(0, top - 2, move, 0)
        with scope("s_x1"):
            spread_x(1)
            to_core(1, x, 1)
        finish_one(2)
        with scope("s_in"):
            for t in (1, 0):
                in_term(t)
        with scope("s_core1"):
            spread_core_last()
        with scope("s_out1"):
            out_term(1)

        @pl.when(x == 0)
        def _():
            for i in range(len(groups)):
                with scope(f"s_last{i}"):
                    last_out(i)

    def size(*shape):
        return math.prod(shape) // (8 * LANES)

    li_block, row = size(tok, width), size(fb, tok)
    both_cores = size(2, fb, fe) + nsec * row
    by_core = (
        size(2, fb, fe) + row + size(2, half, 8, nsec * fb) + nx * size(2, 2, tiles, 8, LANES) + top * (nx - 1) * block,
        size(nz, 8, nsec * fb)
        + size(nsec, 2, tiles, 8, LANES)
        + 3 * size(4 * fb, tok)
        + (nx - 1) * 2 * nz
        + (nz - 1) * 2
        + (nx - 1) * 2
        + row
        + top * 2 * 3 * size(8, hu)
        + (top - 1) * nb * (nx - 1) * hj
        + top * (2 * nz - 1)
        + top * block,
    )
    with scope("drain"):
        await_bytes(spare.at[pl.ds(0, (nx + (3 if ring else 1)) * li_block)], out_s.at[1])

        @pl.when(core == 1)
        def _():
            for way in range(2):
                await_bytes(wbuf.at[0, :, :, pl.ds(0, nz - 1)], wz_s.at[way])

        for o in range(nx):
            pairs = owned.get(o, [])
            last_tiles = 2 * sum(owner[p] != o for p in range(nx))
            if pairs:
                last_tiles += (block - 2 if o else 2 * len(pairs) * (nz - 1)) + (block if o else block * len(pairs))

            @pl.when((core == 1) & (x == o))
            def _():
                await_bytes(spare.at[pl.ds(0, both_cores + by_core[1] + last_tiles)], out_s.at[0])

        @pl.when(core == 0)
        def _():
            await_bytes(spare.at[pl.ds(0, top * nx * block)], out_s.at[2])

        for h in range(2):
            @pl.when((core == 0) & (yhi == h))
            def _():
                pa_tiles = 2 * (half - 1 + h) * size(8, nsec * fb)
                await_bytes(spare.at[pl.ds(0, both_cores + by_core[0] + pa_tiles)], out_s.at[0])


def finish(ig, gi, go, ig_out, gi_out, go_out, sems):
    copies = [pltpu.make_async_copy(src, dst, sems.at[k]) for k, (src, dst) in enumerate(((ig, ig_out), (gi, gi_out), (go, go_out)))]
    for cp in copies:
        cp.start()
    for cp in copies:
        cp.wait()


def body(layer_inputs, pre_act, out_grad, w_in, w_out):
    nz, nx = lax.axis_size("z"), lax.axis_size("x")
    nsec = 2 * nx
    tok, width = out_grad.shape
    fb = w_in.shape[2]
    hid = pre_act.shape[2]
    fe = width // 2
    tiles = nz * fb // LANES
    half = nz // 2
    dma = pltpu.SemaphoreType.DMA
    vmem = pltpu.VMEM
    nb = 4 if nx % 4 == 0 else 2
    spare = 2048
    scratch = [
        vmem((2, fb, width), BF16),
        vmem((2, 2, 2, nz, fb, fe), BF16),
        vmem((2, nz, 8, hid), BF16),
        vmem((2, 2, half, 8, hid), BF16),
        vmem((nx, 2, 2, tiles, 8, LANES), BF16),
        vmem((2, nsec, 2, tiles, 8, LANES), BF16),
        vmem((nsec, 2, 2 * tiles, 8, LANES), F32),
        vmem((nsec, fb, tok), BF16),
        vmem((nsec, fb, tok), BF16),
        vmem((2, 2, fb, tok), BF16),
        vmem((nsec, fb, tok), BF16),
        vmem((2, nx, tok, width), BF16),
        vmem((nz, 8, width), BF16),
        vmem((4, 4 * fb, tok), BF16),
        vmem((nx, nz, 2, 8, LANES), BF16),
        vmem((nx, nz, 2, 8, LANES), BF16),
        vmem((nz, 2, 8, LANES), BF16),
        vmem((nz, 2, 8, LANES), BF16),
        vmem((fb, tok), BF16),
        vmem((fb, tok), BF16),
        vmem((2, 2 * tiles, fe, LANES), BF16),
        vmem((nsec + 1, nsec, 8, LANES), BF16),
        vmem((nsec, 2, 4, 8, 2 * nz * fb), BF16),
        vmem((nsec, nb, nx, nsec // nb, 8, LANES), BF16),
        vmem((2, 8, 2 * nz * fb), F32),
        vmem((nb, 8, fe // nb), F32),
        vmem((nsec, 2, 2 * tiles, 8, LANES), BF16),
        vmem((nsec * nz, 8, LANES), BF16),
        vmem((LANES, tok), F32),
        vmem((nsec * nx * 4 * nz, 8, LANES), BF16),
        vmem((spare, 8, LANES), BF16),
        dma((7,)),
        dma((3,)), dma((2,)),
        dma((4,)),
        dma((2,)),
        dma((max(half * 4, 2 * nsec + 3 + nx),)),
        dma((6,)),
        dma((1,)),
        dma((5,)),
        dma((2, 4, 2)),
        dma((5,)),
        dma((nsec,)),
        dma((nsec,)),
        pltpu.SemaphoreType.REGULAR((max(nsec, half),)),
    ]
    hbm, on_chip = pl.BlockSpec(memory_space=pltpu.HBM), pl.BlockSpec(memory_space=pltpu.VMEM)
    shapes = (
        jax.ShapeDtypeStruct((nz, 8, width), BF16),
        jax.ShapeDtypeStruct((fb, width), F32),
        jax.ShapeDtypeStruct((fb, width), F32),
    )
    operands = (
        layer_inputs.reshape(tok, width),
        pre_act.reshape(nz, 8, hid),
        out_grad.reshape(nz, 8, width),
        w_in.reshape(fb, width),
        w_out.reshape(fb, width),
    )
    results = pl.pallas_call(
        kernel,
        out_shape=shapes,
        in_specs=[hbm] * 5,
        out_specs=(on_chip,) * 3,
        scratch_shapes=scratch,
        name="chain",
        compiler_params=pltpu.CompilerParams(
            collective_id=0, has_side_effects=True, vmem_limit_bytes=40 * 1024 * 1024
        ),
    )(*(pltpu.with_memory_space_constraint(v, pltpu.HBM) for v in operands))
    ig, gi, go = pl.pallas_call(
        finish,
        out_shape=shapes,
        in_specs=[on_chip] * 3,
        out_specs=(hbm,) * 3,
        scratch_shapes=[dma((3,))],
        name="finish",
    )(*(pltpu.with_memory_space_constraint(v, pltpu.VMEM) for v in results))
    return (
        ig.reshape(1, tok, width),
        gi.reshape(1, 1, fb, width),
        go.reshape(1, 1, fb, width),
    )


def solution(mesh):
    shape = mesh.shape
    split = Mesh(
        mesh.devices.reshape(shape["section"] // 2, 2, shape["dp"] // 2, 2, shape["mp"]), AXES
    )
    sec, dp = ("x", "core"), ("z", "ylo")
    placed = (
        P(sec, None, "yhi"),
        P(sec, None, dp),
        P(None, "yhi"),
        P(dp, sec, None, "yhi"),
        P(dp, sec, None, "yhi"),
    )
    return jax.shard_map(
        body,
        mesh=split,
        in_specs=placed,
        out_specs=(P(sec, None, "yhi"), P(dp, sec, None, "yhi"), P(dp, sec, None, "yhi")),
        check_vma=False,
    )
```

```python
import contextlib
import math

import jax
import jax.numpy as jnp
from jax import lax
from jax.experimental import pallas as pl
from jax.experimental.pallas import tpu as pltpu
from jax.sharding import Mesh
from jax.sharding import PartitionSpec as P

AXES = ("x", "core", "z", "ylo", "yhi")
MESH_ID = pl.DeviceIdType.MESH
BF16, F32 = jnp.bfloat16, jnp.float32
LANES = 128
PROFILE = False


def scope(name):
    return jax.named_scope(name) if PROFILE else contextlib.nullcontext()


def gelu_parts(v):
    cdf = 0.5 * (1.0 + lax.erf(v * 0.7071067811865476))
    dens = jnp.exp(-0.5 * v * v) * 0.3989422804014327
    return cdf, dens


def kernel(
    li_hbm, pa_hbm, og_hbm, wi_hbm, wo_hbm,
    ig_out, gi_out, go_out,
    w_own, wbuf, pa, pa_all, pb, pc, slope, pa_t, pre_t, pre_top, hall, li, og,
    a_top, b_top, r_top, q_top, z_top, g_top, g_pass,
    w_t, xs, a_buf, b_buf, a_acc, b_acc, gbuf, gz, gt, up,
    spare, lsem, out_s, wz_s, wx_r, wd_r, wz_r, st_r, pt_r, top_r, ph_r, li_r, g_r, ud_r, flag,
):
    nx, nz = lax.axis_size("x"), lax.axis_size("z")
    nsec = 2 * nx
    top = nsec - 1
    fb, width = wi_hbm.shape
    fe = width // 2
    tok = nz * 8
    tiles = nz * fb // LANES
    per_tile = LANES // fb
    x, core, z = lax.axis_index("x"), lax.axis_index("core"), lax.axis_index("z")
    ylo, yhi = lax.axis_index("ylo"), lax.axis_index("yhi")
    sec = x * 2 + core
    y = yhi * 2 + ylo
    other = 1 - ylo
    partner = yhi * 2 + other

    def dev(x_=None, core_=None, z_=None, y_=None):
        y_ = y if y_ is None else y_
        return (
            x if x_ is None else x_,
            core if core_ is None else core_,
            z if z_ is None else z_,
            lax.rem(y_, 2),
            y_ // 2,
        )

    def send(src, dst, ssem, rsem, to):
        cp = pltpu.make_async_remote_copy(
            src_ref=src, dst_ref=dst, send_sem=ssem, recv_sem=rsem, device_id=to, device_id_type=MESH_ID
        )
        cp.start()
        return cp

    def await_bytes(ref, sem):
        pltpu.make_async_copy(ref, ref, sem).wait()

    def zat(d):
        return lax.rem(z + d + nz, nz)

    def xat(d):
        return lax.rem(x + d + nx, nx)

    def yat(d):
        return lax.rem(y + d, 4)

    y_order = (2, 3, 1)
    x_order = sorted(range(1, nx), key=lambda d: (-min(d, nx - d), -d))
    z_order = sorted(range(1, nz), key=lambda d: -min(d, nz - d))
    sections = [(d, False) for d in x_order] + [(d, True) for d in x_order] + [(0, True)]

    def peer(d, cross):
        return xat(d), (1 - core if cross else core)

    mine = pl.ds(pl.multiple_of(ylo * fe, LANES), fe)
    theirs = pl.ds(pl.multiple_of(other * fe, LANES), fe)

    w_hbm = (wi_hbm, wo_hbm)
    pa_in = pltpu.make_async_copy(pa_hbm, pa.at[core], lsem.at[0])
    w_in_ = [pltpu.make_async_copy(w_hbm[m].at[:, mine], wbuf.at[m, ylo, 1, z], lsem.at[1 + m]) for m in range(2)]
    og_in = pltpu.make_async_copy(og_hbm, og, lsem.at[3])
    li_in = pltpu.make_async_copy(li_hbm, li.at[core, x], lsem.at[4])
    barrier = pltpu.get_barrier_semaphore()
    greeted = [dev(z_=zat(d)) for d in (1, -1)] + [dev(*peer(*p)) for p in sections]
    greeted += [dev(y_=yat(d)) for d in range(1, 4)] + [dev(core_=1 - core, y_=partner)]
    for to in greeted:
        pl.semaphore_signal(barrier, inc=1, device_id=to, device_id_type=MESH_ID)

    first = (1, 0)
    own_in = [pltpu.make_async_copy(w_hbm[m], w_own.at[m], lsem.at[5 + m]) for m in range(2)]
    for m in first:
        own_in[m].start()

        @pl.when(core == 1)
        def _():
            w_in_[m].start()

    pa_in.start()

    og_in.start()
    li_in.start()

    with scope("barrier"):
        pl.semaphore_wait(barrier, len(greeted))

    half = nz // 2

    def meet(r):
        for d in (1, -1):
            pl.semaphore_signal(flag.at[r], inc=1, device_id=dev(z_=zat(d)), device_id_type=MESH_ID)
        pl.semaphore_wait(flag.at[r], 2)

    def pa_first():
        await_bytes(pa.at[1], st_r.at[5])
        for h in range(2):
            @pl.when(yhi == h)
            def _():
                for d in z_order:
                    if d % 2 == h:
                        for c in range(2):
                            dst = pa_all.at[c, lax.rem(z, 2), z // 2]
                            send(pa.at[c, zat(d)], dst, out_s.at[0], st_r.at[0], dev(z_=zat(d)))
                if h == 0:
                    for c in range(2):
                        pa_all[c, lax.rem(z, 2), z // 2] = pa[c, z]

    def await_pa(sem):
        for h in range(2):
            @pl.when(yhi == h)
            def _():
                await_bytes(pa.at[0, pl.ds(0, 2 * (half - 1 + h))], sem)

    def pa_second():
        await_pa(st_r.at[0])
        mine_ = pa_all.at[:, lax.rem(z + yhi, 2)]
        send(mine_, mine_, out_s.at[0], st_r.at[4], dev(y_=yat(2)))

    def ring_send(src, m, l, k, way):
        send(src, src, wz_s.at[way], wz_r.at[((k - 1) * 2 + m) * 2 + l], dev(z_=zat(1 if way == 0 else -1)))

    swaps = []
    for m in first:
        own_in[m].wait()

        @pl.when(core == 0)
        def _():
            send(w_own.at[m, :, mine], wbuf.at[m, ylo, 0, z], out_s.at[0], wd_r.at[m], dev(core_=1))

        @pl.when(core == 1)
        def _():
            w_in_[m].wait()
            for way in range(2):
                ring_send(wbuf.at[m, ylo, 1, z], m, ylo, 1, way)

        dst = wbuf.at[m, ylo, core, z]
        swaps.append(send(w_own.at[m, :, theirs], dst, out_s.at[0], wx_r.at[core * 2 + m], dev(core_=1, y_=partner)))

    pa_in.wait()

    @pl.when(core == 1)
    def _():
        send(pa.at[1], pa.at[1], out_s.at[0], st_r.at[5], dev(core_=0))

    v = pa[core].astype(F32).reshape(tok, nsec * fb)
    pa_t[...] = jnp.swapaxes(v, 0, 1).astype(BF16).reshape(nsec, fb, tok)
    for p in sections:
        to = peer(*p)
        send(pa_t.at[to[0] * 2 + to[1]], pre_t.at[sec], out_s.at[0], st_r.at[3], dev(*to))
    pre_t[sec] = pa_t[sec]

    def spread_pre():
        await_bytes(pre_t.at[pl.ds(0, nsec - 1)], st_r.at[3])
        dst = pre_top.at[ylo, core]
        send(pre_t.at[top], dst, out_s.at[0], pt_r.at[0], dev(core_=1, y_=partner))

        @pl.when(core == 0)
        def _():
            send(pre_t.at[top], dst, out_s.at[0], pt_r.at[0], dev(core_=1))

        @pl.when(core == 1)
        def _():
            dst[...] = pre_t[top]

    def stage_b():
        await_bytes(pa_all.at[:, 0], st_r.at[4])
        group = lax.broadcasted_iota(jnp.int32, (8, LANES), 1) // fb
        for c in range(2):
            for ct in range(nsec // per_tile):
                for t in range(tiles):
                    out = [jnp.zeros((8, LANES), F32)] * per_tile
                    for j in range(per_tile):
                        at = t * per_tile + j
                        v = pa_all[c, at % 2, at // 2, :, ct * LANES:(ct + 1) * LANES].astype(F32)
                        for k in range(per_tile):
                            shift = (j - k) * fb % LANES
                            r = pltpu.roll(v, shift, 1) if shift else v
                            out[k] = jnp.where(group == j, r, out[k])
                    for k in range(per_tile):
                        to = ct * per_tile + k
                        pb[to // 2, c, to % 2, t] = out[k].astype(BF16)
        for d in x_order + [0]:
            send(pb.at[xat(d)], pc.at[ylo, pl.ds(2 * x, 2)], out_s.at[0], st_r.at[1], dev(x_=xat(d), core_=1))

    cut = tok // 2
    lo, hi = pl.ds(0, cut), pl.ds(cut, cut)
    ring = nx > 2

    def li_first():
        li_in.wait()
        src = li.at[core, x]
        send(src, src, out_s.at[1], li_r.at[0], dev(x_=xat(1)))
        if ring:
            send(src, src, out_s.at[1], li_r.at[1], dev(x_=xat(-1)))

    def li_second():
        await_bytes(li.at[0, 0], li_r.at[0])
        if ring:
            src = li.at[core, xat(-1), lo]
            send(src, src, out_s.at[1], li_r.at[2], dev(x_=xat(1)))
            await_bytes(li.at[0, 0], li_r.at[1])
            src = li.at[core, xat(1), hi]
            send(src, src, out_s.at[1], li_r.at[3], dev(x_=xat(-1)))

    def li_third():
        if ring:
            await_bytes(li.at[0, 0, lo], li_r.at[2])
            await_bytes(li.at[0, 0, hi], li_r.at[3])
        send(li.at[core], li.at[core], out_s.at[1], li_r.at[4], dev(core_=1 - core))

    def first_out_term():
        for s in range(nsec):
            v = pre_t[s].astype(F32)
            hall[s] = (v * gelu_parts(v)[0]).astype(BF16)
        go_out[...] = jnp.dot(hall[top], og[...].reshape(tok, width), preferred_element_type=F32)

    def first_in_term():
        await_bytes(li.at[0], li_r.at[4])
        gi_out[...] = jnp.dot(g_top[...], li[top % 2, top // 2], preferred_element_type=F32)

    block = 4 * nz

    def slot(t, x_, ylo_=0, z_=0):
        return ((((t * nx + x_) * 2 + ylo_) * nz) + z_) * 2

    def columns(t, x_, l):
        return up[pl.ds(slot(t, x_, l), 2 * nz)].reshape(nz, 2, 8, LANES)

    def out_term(t):
        rows = hall[t - 1]
        for l in range(2):
            parts = []
            for k in range(nx):
                v = columns(t, k, l)
                parts += [v[:, c].reshape(tok, LANES) for c in range(2)]
            go_out[:, l * fe:(l + 1) * fe] += jnp.dot(rows, jnp.concatenate(parts, axis=1), preferred_element_type=F32)

        @pl.when(sec == t)
        def _():
            for l in range(2):
                for k in range(nx):
                    v = columns(t, k, l)
                    for c in range(2):
                        at = l * fe + (2 * k + c) * LANES
                        ig_out[:, :, at:at + LANES] = v[:, c]

    def in_term(t):
        @pl.when(core == 1)
        def _():
            await_bytes(gz.at[pl.ds(0, nz - 1)], g_r.at[t])

        @pl.when(core == 0)
        def _():
            await_bytes(gz.at[pl.ds(0, nz)], g_r.at[t])

        gt[...] = jnp.swapaxes(gz[pl.ds(t * nz, nz)].astype(F32).reshape(tok, LANES), 0, 1)
        rows = gt[pl.ds(pl.multiple_of(lax.rem(z, per_tile) * fb, fb), fb), :].astype(BF16)
        gi_out[...] += jnp.dot(rows, li[lax.rem(t, 2), t // 2], preferred_element_type=F32)

    hu, hn, hj = 2 * nz * fb, fe // 2, nsec // 2
    def hop(m, k, which):
        l = ylo if which == 0 else other
        if k == 1:
            if which == 0:
                await_bytes(wbuf.at[m, 0, 0, 0], wd_r.at[m])
            else:
                for c in range(2):
                    await_bytes(wbuf.at[m, 0, 0, 0], wx_r.at[c * 2 + m])
        if k > 1:
            await_bytes(wbuf.at[m, 0, :, pl.ds(0, 2)], wz_r.at[((k - 2) * 2 + m) * 2 + l])
        for way, step in ((0, 1), (1, -1)):
            if k == 1 and which == 0:
                ring_send(wbuf.at[m, l, 0, z], m, l, 1, way)
            elif k == half:
                ring_send(wbuf.at[m, l, way, zat(-step * (k - 1))], m, l, k, way)
            else:
                ring_send(wbuf.at[m, l, :, zat(-step * (k - 1))], m, l, k, way)

    def await_last(m):
        for l in range(2):
            await_bytes(wbuf.at[m, 0, :, 0], wz_r.at[((half - 1) * 2 + m) * 2 + l])

    def all_met():
        pl.semaphore_wait(flag.at[half - 1], 1)

    def stage_c():
        await_bytes(pc.at[0], st_r.at[1])
        send(pc.at[ylo], pc.at[ylo], out_s.at[0], st_r.at[2], dev(y_=partner))

    def stage_d():
        await_bytes(pc.at[0], st_r.at[2])

        def one(s, carry):
            for l in range(2):
                v = pc[l, s].astype(F32)
                cdf, dens = gelu_parts(v)
                slope[s, l] = (cdf + v * dens).reshape(2 * tiles, 8, LANES)
            return carry

        lax.fori_loop(0, top, one, 0)

    def top_first():
        og_in.wait()
        rows = wbuf[1, :, :, z].reshape(4 * fb, fe)
        a_top[y] = lax.dot_general(
            rows, og[:, :, mine].reshape(tok, fe), (((1,), (1,)), ((), ())), preferred_element_type=F32
        ).astype(BF16)
        for d in y_order:
            send(a_top.at[y], a_top.at[y], out_s.at[0], top_r.at[0], dev(y_=yat(d)))
        spread_pre()

    def top_second():
        await_bytes(pre_t.at[pl.ds(0, 3)], pt_r.at[0])
        v = pre_top[...].astype(F32).reshape(4 * fb, tok)
        cdf, dens = gelu_parts(v)
        await_bytes(a_top.at[pl.ds(0, 3)], top_r.at[0])
        back = a_top[0].astype(F32)
        for k in range(1, 4):
            back = back + a_top[k].astype(F32)
        g = (back * (cdf + v * dens)).astype(BF16)
        g_pass[...] = jnp.where(ylo == 0, g[:fb], g[2 * fb:3 * fb])
        send(g_pass, g_top, out_s.at[0], top_r.at[4], dev(core_=0))
        g_top[...] = jnp.where(ylo == 0, g[fb:2 * fb], g[3 * fb:])
        rows = jnp.swapaxes(g.astype(F32), 0, 1).astype(BF16)
        part = jnp.dot(rows, wbuf[0, :, :, z].reshape(4 * fb, fe), preferred_element_type=F32).astype(BF16)
        for j in range(nsec):
            b_top[j // 2, :, j % 2] = part[:, j * LANES:(j + 1) * LANES].reshape(nz, 8, LANES)
        for d in x_order:
            send(b_top.at[xat(d)], r_top.at[x], out_s.at[0], top_r.at[1], dev(x_=xat(d)))
        r_top[x] = b_top[x]

    def top_third():
        await_bytes(r_top.at[pl.ds(0, nx - 1)], top_r.at[1])
        total = r_top[0].astype(F32)
        for k in range(1, nx):
            total = total + r_top[k].astype(F32)
        q_top[...] = total.astype(BF16)
        for d in z_order:
            send(q_top.at[zat(d)], z_top.at[z], out_s.at[0], top_r.at[2], dev(z_=zat(d)))
        z_top[z] = q_top[z]

    own = pl.ds(2 * x, 2)

    def top_fourth():
        await_bytes(z_top.at[pl.ds(0, nz - 1)], top_r.at[2])
        for c in range(2):
            at = pl.multiple_of(ylo * fe + (2 * x + c) * LANES, LANES)
            total = og[z, :, pl.ds(at, LANES)].astype(F32)
            for k in range(nz):
                total = total + z_top[k, c].astype(F32)
            xs[top - 1, 2 * x + c] = total.astype(BF16)
        src = xs.at[top - 1, own]
        for d in x_order:
            send(src, src, out_s.at[0], top_r.at[3], dev(x_=xat(d)))

    def spread_z(t):
        src = xs.at[t - 1, own]
        dst = up.at[pl.ds(slot(t, x, ylo, z), 2)]

        def both(d):
            for to in (partner, y):
                send(src, dst, out_s.at[0], wz_r.at[t], dev(core_=0, z_=zat(d), y_=to))

        both(half)

        def pair(i, c):
            both(half - i)
            both(half + i)
            return c

        lax.fori_loop(1, half, pair, 0)
        both(0)

    bounds = sorted({half // 2, 3 * half // 4, half})
    groups = [
        [r for r in range(nz) if (bounds[i - 1] if i else -1) < min(r, nz - r) <= b] for i, b in enumerate(bounds)
    ]
    group_of = {r: i for i, g in enumerate(groups) for r in g}

    def runs(g):
        out = []
        for r in g:
            if out and out[-1][1] == r:
                out[-1][1] = r + 1
            else:
                out.append([r, r + 1])
        return out

    owner = [p if min(p, nx - p) <= 1 else 0 for p in range(nx)]
    owned = {o: [p for p in range(nx) if owner[p] == o] for o in sorted(set(owner))}
    d_order = [half] + [d for i in range(1, half) for d in (half - i, half + i)] + [0]

    def last_z():
        for o, pairs in owned.items():
            @pl.when(x == o)
            def _():
                for d in d_order:
                    r = (nz - d) % nz
                    for p in pairs:
                        src = xs.at[nsec, pl.ds(2 * p, 2)]
                        dst = up.at[pl.ds(slot(0, p, ylo, r), 2)]
                        if o:
                            send(src, dst, out_s.at[0], wx_r.at[group_of[r]], dev(core_=1, z_=zat(d), y_=partner))
                        if d:
                            send(src, dst, out_s.at[0], wx_r.at[group_of[r]], dev(core_=1, z_=zat(d)))
                for p in pairs:
                    up[pl.ds(slot(0, p, ylo, 0), 2)] = xs[nsec, 2 * p:2 * p + 2]

    def last_x(i):
        for o, pairs in owned.items():
            @pl.when(x == o)
            def _():
                per_plane = 4 if o else 2 * len(pairs)
                here = (2 if o else 2 * len(pairs)) if i == 0 else 0
                await_bytes(up.at[pl.ds(0, per_plane * len(groups[i]) - here)], wx_r.at[i])
                for a, b in runs(groups[i]):
                    for p in pairs:
                        for l, to in ((0, y), (1, y)) if o else ((ylo, partner), (ylo, y)):
                            src = up.at[pl.ds(slot(0, p, l, a), 2 * (b - a))]
                            send(src, src, out_s.at[0], wz_r.at[2 * nsec + i], dev(x_=0, core_=0, y_=to))

    def last_out(i):
        await_bytes(up.at[pl.ds(0, nx * 4 * len(groups[i]))], wz_r.at[2 * nsec + i])
        for r in groups[i]:
            row = zat(r)
            for l in range(2):
                for k in range(nx):
                    for c in range(2):
                        at = l * fe + (2 * k + c) * LANES
                        ig_out[row, :, at:at + LANES] = up[slot(0, k, l, r) + c]

    def spread_g(t):
        def to(d, c):
            tile = zat(d) // per_tile
            for c_ in range(2):
                send(gbuf.at[t, ylo, c_ * tiles + tile], gz.at[t * nz + z], out_s.at[0], g_r.at[t], dev(core_=c_, z_=zat(d)))
            return c

        lax.fori_loop(1, nz, to, 0)
        tile = z // per_tile
        send(gbuf.at[t, ylo, tile], gz.at[t * nz + z], out_s.at[0], g_r.at[t], dev(core_=0))
        gz[t * nz + z] = gbuf[t, ylo, tiles + tile]

    def turn(away):
        t = lax.rem(z // per_tile + away + tiles, tiles)

        def one(i, c):
            l, c_ = i // 2, lax.rem(i, 2)
            v = wbuf[1, l, c_, pl.ds(t * per_tile, per_tile)].reshape(LANES, fe)
            w_t[l, c_ * tiles + t] = jnp.swapaxes(v, 0, 1)
            return c

        lax.fori_loop(0, 4, one, 0)

    def a_half(s, l, part=None):
        if part is not None:
            a_buf[s, l, y] = part.astype(BF16)
        for d in y_order:
            send(a_buf.at[s, l, y], a_buf.at[s, l, y], out_s.at[0], ph_r.at[0, l, s % 2 if isinstance(s, int) else lax.rem(s, 2)], dev(y_=yat(d)))

    def a_part(s, l, n):
        lhs = jnp.concatenate([xs[s, n * hj + j] for j in range(hj)], axis=1)
        w_out = jnp.concatenate([w_t[l, t, n * hn:(n + 1) * hn] for t in range(2 * tiles)], axis=1)
        return jnp.dot(lhs, w_out, preferred_element_type=F32)

    def a_tile(l, away, turned):
        lhs = jnp.concatenate([xs[top - 1, j] for j in range(nsec)], axis=1)
        t = lax.rem(z // per_tile + away + tiles, tiles)
        if turned:
            w_out = jnp.concatenate([w_t[l, c * tiles + t] for c in range(2)], axis=1)
            part = jnp.dot(lhs, w_out, preferred_element_type=F32)
        else:
            w_out = wbuf[1, l, :, pl.ds(t * per_tile, per_tile)].reshape(2 * LANES, fe)
            part = lax.dot_general(lhs, w_out, (((1,), (1,)), ((), ())), preferred_element_type=F32)
        for c in range(2):
            at = pl.multiple_of((c * tiles + t) * LANES, LANES)
            a_buf[top - 1, l, y, :, pl.ds(at, LANES)] = part[:, c * LANES:(c + 1) * LANES].astype(BF16)

    def release(t):
        pl.semaphore_signal(flag.at[t], inc=1, device_id=dev(core_=0), device_id_type=MESH_ID)

    def await_up(t):
        await_bytes(up.at[pl.ds(0, nx * block)], ud_r.at[t])

    def background_a(s):
        with scope("bg_a"):
            @pl.when(s <= top - 3)
            def _():
                release(s + 2)

            @pl.when(s <= top - 2)
            def _():
                spread_z(s + 1)

            @pl.when(s == top - 2)
            def _():
                first_in_term()

            @pl.when(s <= top - 3)
            def _():
                in_term(s + 2)

            @pl.when(s <= top - 4)
            def _():
                await_up(s + 4)
                out_term(s + 4)

    def g_half(s, l):
        with scope(f"wait_a{l}"):
            await_bytes(a_buf.at[s, l, pl.ds(0, 3)], ph_r.at[0, l, s % 2 if isinstance(s, int) else lax.rem(s, 2)])
        back = a_buf[s, l, 0].astype(F32)
        for k in range(1, 4):
            back = back + a_buf[s, l, k].astype(F32)
        g = []
        for t in range(2 * tiles):
            g_tile = (back[:, t * LANES:(t + 1) * LANES] * slope[s, l, t]).astype(BF16)
            gbuf[s, l, t] = g_tile
            g.append(g_tile)
        return jnp.concatenate(g, axis=1)

    def b_tile(n, away):
        t = lax.rem(z // per_tile + away + tiles, tiles)
        pairs = [(l, c) for l in range(2) for c in range(2)]
        lhs = jnp.concatenate([gbuf[top - 1, l, c * tiles + t] for l, c in pairs], axis=1)
        rows = pl.ds(t * per_tile, per_tile)
        w_in = jnp.concatenate([wbuf[0, l, c, rows, :, n * hn:(n + 1) * hn].reshape(LANES, hn) for l, c in pairs], axis=0)
        return jnp.dot(lhs, w_in, preferred_element_type=F32)

    def application(s, final=False, begin=False):
        if not begin:
            background_a(s)
            g_first = g_half(s, 0)
            for n in range(2):
                w_in = wbuf[0, 0, :, :, :, n * hn:(n + 1) * hn].reshape(hu, hn)
                b_acc[n] = jnp.dot(g_first, w_in, preferred_element_type=F32)
            g = g_half(s, 1)
        for n in range(2):
            if begin:
                part = b_tile(n, tiles // 2)
            else:
                w_in = wbuf[0, 1, :, :, :, n * hn:(n + 1) * hn].reshape(hu, hn)
                part = jnp.dot(g, w_in, preferred_element_type=F32)
            part = (b_acc[n] + part).astype(BF16)
            for j in range(hj):
                b_buf[s, n, x, j] = part[:, j * LANES:(j + 1) * LANES]
            if not final:
                src = b_buf.at[s, n, x]
                for d in x_order:
                    send(src, src, out_s.at[0], ph_r.at[1, n, s % 2 if isinstance(s, int) else lax.rem(s, 2)], dev(x_=xat(d)))
        hx = nx // 2
        if final:
            for p in range(nx):
                @pl.when(x != owner[p])
                def _():
                    src = b_buf.at[s, p // hx, x, pl.ds(2 * (p % hx), 2)]
                    send(src, src, out_s.at[0], ph_r.at[1, 0, s % 2], dev(x_=owner[p]))

        with scope("bg_b"):
            spread_g(s)
            if begin:
                spread_z(top)

        if final:
            for o, pairs in owned.items():
                @pl.when(x == o)
                def _():
                    with scope("wait_b"):
                        await_bytes(gz.at[pl.ds(0, 2 * (nx - 1) * len(pairs))], ph_r.at[1, 0, s % 2])
                    for p in pairs:
                        for c in range(2):
                            total = xs[s, 2 * p + c].astype(F32)
                            for k in range(nx):
                                total = total + b_buf[s, p // hx, k, 2 * (p % hx) + c].astype(F32)
                            xs[nsec, 2 * p + c] = total.astype(BF16)
            return
        for n in range(2):
            with scope(f"wait_b{n}"):
                await_bytes(b_buf.at[s, n, pl.ds(0, nx - 1)], ph_r.at[1, n, s % 2 if isinstance(s, int) else lax.rem(s, 2)])
            with scope(f"a_mm{n}"):
                for j in range(hj):
                    total = xs[s, n * hj + j].astype(F32)
                    for k in range(nx):
                        total = total + b_buf[s, n, k, j].astype(F32)
                    xs[s - 1, n * hj + j] = total.astype(BF16)
                if n == 0:
                    for l in range(2):
                        a_acc[l] = a_part(s - 1, l, 0)
        for l in range(2):
            with scope(f"a_last{l}"):
                a_half(s - 1, l, a_acc[l] + a_part(s - 1, l, 1))

    @pl.when(core == 1)
    def _():
        plan = [
            (1, top_first), (2, top_second), (2, li_first), (4, all_met), (4, top_third), (5, first_out_term), (6, li_second),
            (6, stage_c), (7, stage_d), (7, top_fourth),
        ]
        plan += [(half if d else 5, lambda d=d: turn(d)) for d in (0, -1, 1) if d % tiles != tiles // 2]
        for k in range(1, half + 1):
            with scope(f"hop{k}"):
                if k == 1:
                    blocks = ((1, 1, 0), (0, 1, 0), (1, 1, 1))
                elif k == 2:
                    blocks = ((1, 2, 0), (0, 1, 1), (1, 2, 1))
                else:
                    blocks = ((1, k, 0), (0, k - 1, 0), (1, k, 1), (0, k - 1, 1))
                for b in blocks:
                    hop(*b)
            with scope(f"stage{k}"):
                for at, f in plan:
                    if min(at, half) == k:
                        f()
        early = [d for d in (0, -1, 1) if d % tiles != tiles // 2]
        with scope("top_end"):
            await_bytes(xs.at[0, pl.ds(0, 2 * (nx - 1))], top_r.at[3])
            for l in range(2):
                for d in early:
                    a_tile(l, d, True)
        with scope("gather_out"):
            hop(0, half, 0)
            await_last(1)
        with scope("a_first"):
            for l in range(2):
                a_tile(l, tiles // 2, False)
                a_half(top - 1, l)
        with scope("hop_end"):
            hop(0, half, 1)
            turn(tiles // 2)
        with scope("b_early"):
            for l in range(2):
                g_half(top - 1, l)
            for n in range(2):
                b_acc[n] = sum((b_tile(n, d) for d in early), jnp.zeros((8, hn), F32))
        with scope("gather_in"):
            await_last(0)
        li_third()

        application(top - 1, begin=True)

        def step(i, carry):
            application(top - 2 - i)
            return carry

        lax.fori_loop(0, top - 2, step, 0)
        application(0, final=True)

        with scope("t_z0"):
            last_z()
            release(1)
        with scope("t_terms"):
            in_term(1)
            for t in range(min(top, 3), 2, -1):
                await_up(t)
                out_term(t)
        with scope("t_in0"):
            in_term(0)
        for i in range(len(groups)):
            with scope(f"t_last{i}"):
                last_x(i)
        with scope("t_up2"):
            await_up(2)
            out_term(2)
        with scope("t_up1"):
            await_up(1)
            out_term(1)

    def await_z(t):
        await_bytes(up.at[pl.ds(0, block)], wz_r.at[t])

    def spread_x(t):
        await_z(t)
        if not isinstance(t, int) or t < top:
            pl.semaphore_wait(flag.at[t], 1)
        src = up.at[pl.ds(slot(t, x), block)]
        for d in x_order:
            to_sem = wz_r.at[2 * nsec + 3 + d] if isinstance(t, int) and t == 1 else wz_r.at[nsec + t]
            send(src, src, out_s.at[0], to_sem, dev(x_=xat(d)))

    def to_core(t, x_, blocks):
        src = up.at[pl.ds(slot(t, x_), blocks * block)]
        send(src, src, out_s.at[2], ud_r.at[t], dev(core_=1))

    def spread_core(t):
        await_bytes(up.at[pl.ds(0, (nx - 1) * block)], wz_r.at[nsec + t])
        to_core(t, 0, nx)

    def spread_core_last():
        for d in reversed(x_order):
            await_bytes(up.at[pl.ds(0, block)], wz_r.at[2 * nsec + 3 + d])
            to_core(1, xat(-d), 1)

    @pl.when(core == 0)
    def _():
        spread_pre()
        for r in range(half - 1):
            meet(r)
        pl.semaphore_signal(flag.at[half - 1], inc=1, device_id=dev(core_=1), device_id_type=MESH_ID)
        pa_first()
        li_first()
        pa_second()
        stage_b()
        og_in.wait()
        first_out_term()
        li_second()
        li_third()
        await_bytes(g_top, top_r.at[4])
        first_in_term()

        def finish_one(t):
            with scope("s_core"):
                spread_core(t)
            with scope("s_out"):
                out_term(t)

        def move(i, carry):
            t = top - 1 - i
            with scope("s_x"):
                spread_x(t)
            with scope("s_in"):
                in_term(t)
            finish_one(t + 1)
            return carry

        with scope("s_x7"):
            spread_x(top)
        lax.fori_loop(0, top - 2, move, 0)
        with scope("s_x1"):
            spread_x(1)
            to_core(1, x, 1)
        finish_one(2)
        with scope("s_in"):
            for t in (1, 0):
                in_term(t)
        with scope("s_core1"):
            spread_core_last()
        with scope("s_out1"):
            out_term(1)

        @pl.when(x == 0)
        def _():
            for i in range(len(groups)):
                with scope(f"s_last{i}"):
                    last_out(i)

    def size(*shape):
        return math.prod(shape) // (8 * LANES)

    li_block, row = size(tok, width), size(fb, tok)
    both_cores = size(2, fb, fe) + nsec * row
    by_core = (
        size(2, fb, fe) + row + size(2, half, 8, nsec * fb) + nx * size(2, 2, tiles, 8, LANES) + top * (nx - 1) * block,
        size(nz, 8, nsec * fb)
        + size(nsec, 2, tiles, 8, LANES)
        + 3 * size(4 * fb, tok)
        + (nx - 1) * 2 * nz
        + (nz - 1) * 2
        + (nx - 1) * 2
        + row
        + top * 2 * 3 * size(8, hu)
        + (top - 1) * 2 * (nx - 1) * hj
        + top * (2 * nz - 1)
        + top * block,
    )
    with scope("drain"):
        await_bytes(spare.at[pl.ds(0, (nx + (3 if ring else 1)) * li_block)], out_s.at[1])

        @pl.when(core == 1)
        def _():
            for way in range(2):
                await_bytes(wbuf.at[0, :, :, pl.ds(0, nz - 1)], wz_s.at[way])

        for o in range(nx):
            pairs = owned.get(o, [])
            last_tiles = 2 * sum(owner[p] != o for p in range(nx))
            if pairs:
                last_tiles += (block - 2 if o else 2 * len(pairs) * (nz - 1)) + (block if o else block * len(pairs))

            @pl.when((core == 1) & (x == o))
            def _():
                await_bytes(spare.at[pl.ds(0, both_cores + by_core[1] + last_tiles)], out_s.at[0])

        @pl.when(core == 0)
        def _():
            await_bytes(spare.at[pl.ds(0, top * nx * block)], out_s.at[2])

        for h in range(2):
            @pl.when((core == 0) & (yhi == h))
            def _():
                pa_tiles = 2 * (half - 1 + h) * size(8, nsec * fb)
                await_bytes(spare.at[pl.ds(0, both_cores + by_core[0] + pa_tiles)], out_s.at[0])


def finish(ig, gi, go, ig_out, gi_out, go_out, sems):
    copies = [pltpu.make_async_copy(src, dst, sems.at[k]) for k, (src, dst) in enumerate(((ig, ig_out), (gi, gi_out), (go, go_out)))]
    for cp in copies:
        cp.start()
    for cp in copies:
        cp.wait()


def body(layer_inputs, pre_act, out_grad, w_in, w_out):
    nz, nx = lax.axis_size("z"), lax.axis_size("x")
    nsec = 2 * nx
    tok, width = out_grad.shape
    fb = w_in.shape[2]
    hid = pre_act.shape[2]
    fe = width // 2
    tiles = nz * fb // LANES
    half = nz // 2
    dma = pltpu.SemaphoreType.DMA
    vmem = pltpu.VMEM
    spare = 2048
    scratch = [
        vmem((2, fb, width), BF16),
        vmem((2, 2, 2, nz, fb, fe), BF16),
        vmem((2, nz, 8, hid), BF16),
        vmem((2, 2, half, 8, hid), BF16),
        vmem((nx, 2, 2, tiles, 8, LANES), BF16),
        vmem((2, nsec, 2, tiles, 8, LANES), BF16),
        vmem((nsec, 2, 2 * tiles, 8, LANES), F32),
        vmem((nsec, fb, tok), BF16),
        vmem((nsec, fb, tok), BF16),
        vmem((2, 2, fb, tok), BF16),
        vmem((nsec, fb, tok), BF16),
        vmem((2, nx, tok, width), BF16),
        vmem((nz, 8, width), BF16),
        vmem((4, 4 * fb, tok), BF16),
        vmem((nx, nz, 2, 8, LANES), BF16),
        vmem((nx, nz, 2, 8, LANES), BF16),
        vmem((nz, 2, 8, LANES), BF16),
        vmem((nz, 2, 8, LANES), BF16),
        vmem((fb, tok), BF16),
        vmem((fb, tok), BF16),
        vmem((2, 2 * tiles, fe, LANES), BF16),
        vmem((nsec + 1, nsec, 8, LANES), BF16),
        vmem((nsec, 2, 4, 8, 2 * nz * fb), BF16),
        vmem((nsec, 2, nx, nx, 8, LANES), BF16),
        vmem((2, 8, 2 * nz * fb), F32),
        vmem((2, 8, fe // 2), F32),
        vmem((nsec, 2, 2 * tiles, 8, LANES), BF16),
        vmem((nsec * nz, 8, LANES), BF16),
        vmem((LANES, tok), F32),
        vmem((nsec * nx * 4 * nz, 8, LANES), BF16),
        vmem((spare, 8, LANES), BF16),
        dma((7,)),
        dma((3,)), dma((2,)),
        dma((4,)),
        dma((2,)),
        dma((max(half * 4, 2 * nsec + 3 + nx),)),
        dma((6,)),
        dma((1,)),
        dma((5,)),
        dma((2, 2, 2)),
        dma((5,)),
        dma((nsec,)),
        dma((nsec,)),
        pltpu.SemaphoreType.REGULAR((max(nsec, half),)),
    ]
    hbm, on_chip = pl.BlockSpec(memory_space=pltpu.HBM), pl.BlockSpec(memory_space=pltpu.VMEM)
    shapes = (
        jax.ShapeDtypeStruct((nz, 8, width), BF16),
        jax.ShapeDtypeStruct((fb, width), F32),
        jax.ShapeDtypeStruct((fb, width), F32),
    )
    operands = (
        layer_inputs.reshape(tok, width),
        pre_act.reshape(nz, 8, hid),
        out_grad.reshape(nz, 8, width),
        w_in.reshape(fb, width),
        w_out.reshape(fb, width),
    )
    results = pl.pallas_call(
        kernel,
        out_shape=shapes,
        in_specs=[hbm] * 5,
        out_specs=(on_chip,) * 3,
        scratch_shapes=scratch,
        name="chain",
        compiler_params=pltpu.CompilerParams(
            collective_id=0, has_side_effects=True, vmem_limit_bytes=40 * 1024 * 1024
        ),
    )(*(pltpu.with_memory_space_constraint(v, pltpu.HBM) for v in operands))
    ig, gi, go = pl.pallas_call(
        finish,
        out_shape=shapes,
        in_specs=[on_chip] * 3,
        out_specs=(hbm,) * 3,
        scratch_shapes=[dma((3,))],
        name="finish",
    )(*(pltpu.with_memory_space_constraint(v, pltpu.VMEM) for v in results))
    return (
        ig.reshape(1, tok, width),
        gi.reshape(1, 1, fb, width),
        go.reshape(1, 1, fb, width),
    )


def solution(mesh):
    shape = mesh.shape
    split = Mesh(
        mesh.devices.reshape(shape["section"] // 2, 2, shape["dp"] // 2, 2, shape["mp"]), AXES
    )
    sec, dp = ("x", "core"), ("z", "ylo")
    placed = (
        P(sec, None, "yhi"),
        P(sec, None, dp),
        P(None, "yhi"),
        P(dp, sec, None, "yhi"),
        P(dp, sec, None, "yhi"),
    )
    return jax.shard_map(
        body,
        mesh=split,
        in_specs=placed,
        out_specs=(P(sec, None, "yhi"), P(dp, sec, None, "yhi"), P(dp, sec, None, "yhi")),
        check_vma=False,
    )
```
